32 devices in a mesh: dp: 4 (over y, x), ctx: 4 (over z), tp: 2 (over core).
Axes of the slice: x: 2, y: 2, z: 4, core: 2. Of those that a mesh axis runs over, the one named last changes fastest.
Arguments:
- tokens: bfloat16 [8, 512, 1536], P('dp', 'ctx'), may hold values from -6 to 6
- cotangent: bfloat16 [8, 512, 1536], P('dp', 'ctx'), may hold values from -6 to 6
- segments: int32 [8, 512], P('dp'), may hold values from 0 to 2, as said below
- positions: int32 [8, 512], P('dp', 'ctx'), may hold values from 0 to 511, as said below
- counts: int32 [4], P('dp'), may hold values from 1 to 2, as said below
- attn_gain: bfloat16 [1, 1536], P(None, ('dp', 'ctx')), may hold values from 0.099609375 to 1.8984375
- q_weight: bfloat16 [1, 1536, 1536], P(None, ('dp', 'ctx'), 'tp'), may hold values from -0.15625 to 0.15625
- q_bias: bfloat16 [1, 768, 2], P(None, ('dp', 'ctx'), 'tp'), may hold values from -5 to 5
- k_weight: bfloat16 [1, 1536, 256], P(None, ('dp', 'ctx'), 'tp'), may hold values from -0.15625 to 0.15625
- v_weight: bfloat16 [1, 1536, 256], P(None, ('dp', 'ctx'), 'tp'), may hold values from -0.15625 to 0.15625
- kv_bias: bfloat16 [1, 256, 2], P(None, ('dp', 'ctx'), 'tp'), may hold values from -5 to 5
- o_weight: bfloat16 [1, 1536, 1536], P(None, ('dp', 'ctx'), 'tp'), may hold values from -0.3125 to 0.3125
- mlp_gain: bfloat16 [1, 1536], P(None, ('dp', 'ctx')), may hold values from 0.099609375 to 1.8984375
- gate_weight: bfloat16 [1, 1536, 8960], P(None, ('dp', 'ctx'), 'tp'), may hold values from -0.15625 to 0.15625
- up_weight: bfloat16 [1, 1536, 8960], P(None, ('dp', 'ctx'), 'tp'), may hold values from -0.15625 to 0.15625
- down_weight: bfloat16 [1, 1536, 8960], P(None, ('dp', 'ctx'), 'tp'), may hold values from -0.0625 to 0.0625
Outputs:
- activations: float32 [8, 512, 1536], P('dp', 'ctx')
- input_grad: float32 [8, 512, 1536], P('dp', 'ctx')
- attn_gain_grad: float32 [1, 1536], P(None, ('dp', 'ctx'))
- q_weight_grad: float32 [1, 1536, 1536], P(None, ('dp', 'ctx'), 'tp')
- q_bias_grad: float32 [1, 768, 2], P(None, ('dp', 'ctx'), 'tp')
- k_weight_grad: float32 [1, 1536, 256], P(None, ('dp', 'ctx'), 'tp')
- v_weight_grad: float32 [1, 1536, 256], P(None, ('dp', 'ctx'), 'tp')
- kv_bias_grad: float32 [1, 256, 2], P(None, ('dp', 'ctx'), 'tp')
- o_weight_grad: float32 [1, 1536, 1536], P(None, ('dp', 'ctx'), 'tp')
- mlp_gain_grad: float32 [1, 1536], P(None, ('dp', 'ctx'))
- gate_weight_grad: float32 [1, 1536, 8960], P(None, ('dp', 'ctx'), 'tp')
- up_weight_grad: float32 [1, 1536, 8960], P(None, ('dp', 'ctx'), 'tp')
- down_weight_grad: float32 [1, 1536, 8960], P(None, ('dp', 'ctx'), 'tp')
The draws below stay inside these ranges and needn't reach their ends.
Inputs may be any that keep to these rules, and one draw needn't show every extreme that they name: `segments`: in each sequence the segment numbers never fall and the first token has segment 0. Within a document positions rise by one a token; every document but the first of its sequence starts at 0, and the first one ends at position 511. `counts`: some data group has 2 live slots and some group one.
All inputs are finite; a program needn't handle non-finite values.
Results may differ from the reference program's by a relative error of at most 0.03.
The reference program's roundings to bfloat16 on the way count: a program that leaves them out, or rounds other values in their place, can miss the bound.
Values may be sent and summed in bfloat16 or wider, within the bound.
A program may use at most 256 MiB of HBM per device.

```python
import jax
import jax.numpy as jnp
from jax import lax

D = 1536
HEADS = 12
KV_HEADS = 2
HEAD_DIM = 128
FF = 8960
LAYERS = 1
SEQ_LEN = 512
MB = 2
GROUPS = 4
SEQS = 8


def doc_layout(base_key):
    cut_draw = jax.random.randint(jax.random.fold_in(base_key, 31), (SEQS, 2), 1, SEQ_LEN)
    first_cut = jnp.min(cut_draw, axis=1, keepdims=True)
    second_cut = jnp.max(cut_draw, axis=1, keepdims=True)
    token_idx = jnp.arange(SEQ_LEN, dtype=jnp.int32)[None, :]
    segment = (token_idx >= first_cut).astype(jnp.int32) + (token_idx >= second_cut).astype(jnp.int32)
    doc_start = jnp.where(segment == 0, first_cut - SEQ_LEN, jnp.where(segment == 1, first_cut, second_cut))
    return (segment, token_idx - doc_start)


def draw_segments(key, part):
    return doc_layout(key)[0]


def draw_positions(key, part):
    return doc_layout(key)[1]


def draw_counts(key, part):
    count_draw = jax.random.randint(jax.random.fold_in(key, 41), (GROUPS,), 1, MB + 1)
    fullest = jax.random.randint(jax.random.fold_in(key, 42), (), 0, GROUPS)
    emptiest = (fullest + jax.random.randint(jax.random.fold_in(key, 43), (), 1, GROUPS)) % GROUPS
    return count_draw.at[fullest].set(MB).at[emptiest].set(1)


def draw_q_bias(key, part):
    group_size = HEADS // KV_HEADS
    noise_draw = jax.random.normal(jax.random.fold_in(key, 52), (LAYERS, group_size * HEAD_DIM, KV_HEADS), jnp.float32)
    values = 0.5 * noise_draw
    return jnp.clip(values, -5.0, 5.0).astype(jnp.bfloat16)


def draw_kv_bias(key, part):
    noise_draw = jax.random.normal(jax.random.fold_in(key, 53), (LAYERS, 2 * HEAD_DIM, KV_HEADS), jnp.float32)
    values = 0.5 * noise_draw
    return jnp.clip(values, -5.0, 5.0).astype(jnp.bfloat16)


def steps_of(own_key, dims, split, least, largest):
    def one(position, parts):
        heights = jax.random.uniform(jax.random.fold_in(jax.random.fold_in(own_key, 6), position), (parts,), jnp.float32, least / len(split), largest / len(split))
        return jnp.repeat(jnp.exp(heights), dims[position] // parts).reshape((-1,) + (1,) * (len(dims) - position - 1))

    factor_of = one(*split[0])
    for cut in split[1:]:
        factor_of = factor_of * one(*cut)
    return factor_of


def noise(stream_key, dims, scale, reach, cuts=(), held_as=jnp.bfloat16):
    result = scale * jax.random.normal(stream_key, dims, jnp.float32)
    if cuts:
        result = result * steps_of(stream_key, dims, cuts, -0.22, 0.18)
    return jnp.clip(result, -reach, reach).astype(held_as)


def setup_inputs(seed: int = 0) -> dict:
    splits = jax.random.split(jax.random.key(seed), 17)
    return {
        "tokens": noise(splits[0], (SEQS, SEQ_LEN, D), 1.0, 6.0, ((0, 4), (1, 4))),
        "cotangent": noise(splits[1], (SEQS, SEQ_LEN, D), 1.0, 6.0, ((0, 4), (1, 4))),
        "segments": draw_segments(jax.random.fold_in(splits[16], 71), 0),
        "positions": draw_positions(jax.random.fold_in(splits[16], 71), 0),
        "counts": draw_counts(jax.random.fold_in(splits[16], 71), 0),
        "attn_gain": jnp.clip(1.0 + 0.18 * jax.random.normal(splits[5], (LAYERS, D), jnp.float32), 0.099609375, 1.8984375).astype(jnp.bfloat16),
        "q_weight": noise(splits[6], (LAYERS, D, HEADS * HEAD_DIM), D ** -0.5, 0.15625, ((1, 16), (2, 2))),
        "q_bias": draw_q_bias(jax.random.fold_in(splits[16], 71), 0),
        "k_weight": noise(splits[8], (LAYERS, D, KV_HEADS * HEAD_DIM), D ** -0.5, 0.15625, ((1, 16), (2, 2))),
        "v_weight": noise(splits[9], (LAYERS, D, KV_HEADS * HEAD_DIM), D ** -0.5, 0.15625, ((1, 16), (2, 2))),
        "kv_bias": draw_kv_bias(jax.random.fold_in(splits[16], 71), 0),
        "o_weight": noise(splits[11], (LAYERS, D, HEADS * HEAD_DIM), (HEADS * HEAD_DIM // 4) ** -0.5, 0.3125, ((1, 16), (2, 2))),
        "mlp_gain": jnp.clip(1.0 + 0.18 * jax.random.normal(splits[12], (LAYERS, D), jnp.float32), 0.099609375, 1.8984375).astype(jnp.bfloat16),
        "gate_weight": noise(splits[13], (LAYERS, D, FF), D ** -0.5, 0.15625, ((1, 16), (2, 2))),
        "up_weight": noise(splits[14], (LAYERS, D, FF), D ** -0.5, 0.15625, ((1, 16), (2, 2))),
        "down_weight": noise(splits[15], (LAYERS, D, FF), FF ** -0.5, 0.0625, ((1, 16), (2, 2))),
    }


theta_base = 1000000.0
norm_eps = 1e-06
masked_score = -1e+30

def mat_mul(left, right):
    return jnp.dot(left, right, preferred_element_type=jnp.float32)

def rope_tables(pos_vals):
    half_dim = HEAD_DIM // 2
    frequency = theta_base ** (-(jnp.arange(half_dim, dtype=jnp.float32) * (2.0 / HEAD_DIM)))
    angles = pos_vals.astype(jnp.float32)[..., None] * frequency
    cos_half = jnp.cos(angles)
    sin_half = jnp.sin(angles)
    return (jnp.concatenate([cos_half, cos_half], -1), jnp.concatenate([sin_half, sin_half], -1))

def rotate(values, cos_tab, sin_tab):
    half_dim = values.shape[-1] // 2
    turned = jnp.concatenate([-values[..., half_dim:], values[..., :half_dim]], -1)
    return values * cos_tab + turned * sin_tab

def unrotate(grad_vals, cos_tab, sin_tab):
    half_dim = grad_vals.shape[-1] // 2
    scaled = grad_vals * sin_tab
    turned = jnp.concatenate([scaled[..., half_dim:], -scaled[..., :half_dim]], -1)
    return grad_vals * cos_tab + turned

def norm_forward(residual, gain_vec):
    inv_rms = lax.rsqrt(lax.optimization_barrier(jnp.mean(residual * residual, axis=-1, keepdims=True)) + norm_eps)
    normed = (residual * inv_rms * gain_vec.astype(jnp.float32)).astype(jnp.bfloat16)
    return (inv_rms, normed)

def norm_backward(residual, inv_rms, gain_vec, grad_normed):
    weighted = grad_normed * gain_vec.astype(jnp.float32)
    inner_mean = lax.optimization_barrier(jnp.mean(weighted * residual, axis=-1, keepdims=True))
    grad_resid = inv_rms * weighted - residual * (inv_rms * inv_rms * inv_rms) * inner_mean
    grad_gain = lax.optimization_barrier(jnp.sum(grad_normed * residual * inv_rms, axis=0))
    return (grad_resid, grad_gain)

def attend_forward(query_bf, keys_bf, values_bf, allowed):
    scores = jnp.einsum('qkgd,skd->kgqs', query_bf.astype(jnp.float32), keys_bf.astype(jnp.float32)) * HEAD_DIM ** (-0.5)
    scores = jnp.where(allowed, scores, masked_score)
    top_score = lax.optimization_barrier(jnp.max(scores, axis=-1, keepdims=True))
    shifted_exp = jnp.exp(scores - top_score)
    totals = lax.optimization_barrier(jnp.sum(shifted_exp, axis=-1, keepdims=True))
    prob_bf = (shifted_exp / totals).astype(jnp.bfloat16)
    output = jnp.einsum('kgqs,skd->qkgd', prob_bf.astype(jnp.float32), values_bf.astype(jnp.float32))
    return (output.astype(jnp.bfloat16), top_score + jnp.log(totals))

def attend_backward(query_bf, keys_bf, values_bf, attn_bf, log_total, grad_attn, allowed):
    scores = jnp.einsum('qkgd,skd->kgqs', query_bf.astype(jnp.float32), keys_bf.astype(jnp.float32)) * HEAD_DIM ** (-0.5)
    prob_full = jnp.exp(jnp.where(allowed, scores, masked_score) - log_total)
    prob_bf = prob_full.astype(jnp.bfloat16)
    grad_attn_f = grad_attn.astype(jnp.float32)
    grad_value = jnp.einsum('kgqs,qkgd->skd', prob_bf.astype(jnp.float32), grad_attn_f)
    grad_prob = jnp.einsum('qkgd,skd->kgqs', grad_attn_f, values_bf.astype(jnp.float32))
    row_dot = lax.optimization_barrier(jnp.sum(grad_attn_f * attn_bf.astype(jnp.float32), axis=-1))
    row_dot = jnp.transpose(row_dot, (1, 2, 0))[..., None]
    grad_score = (prob_full * (grad_prob - row_dot) * HEAD_DIM ** (-0.5)).astype(jnp.bfloat16)
    grad_query = jnp.einsum('kgqs,skd->qkgd', grad_score.astype(jnp.float32), keys_bf.astype(jnp.float32))
    grad_key = jnp.einsum('kgqs,qkgd->skd', grad_score.astype(jnp.float32), query_bf.astype(jnp.float32))
    return (grad_query, grad_key, grad_value)

def layer_forward(residual, weights, allowed, cos_tab, sin_tab):
    gain_in, w_query, b_query, w_key, w_value, b_keyval, w_out, gain_mid, w_gate, w_up, w_down = weights
    row_count = residual.shape[0]
    group_size = HEADS // KV_HEADS
    inv_in, normed_in = norm_forward(residual, gain_in)
    query_val = mat_mul(normed_in, w_query) + b_query.astype(jnp.float32).T.reshape(-1)
    key_val = mat_mul(normed_in, w_key) + b_keyval[:HEAD_DIM].astype(jnp.float32).T.reshape(-1)
    value_val = mat_mul(normed_in, w_value) + b_keyval[HEAD_DIM:].astype(jnp.float32).T.reshape(-1)
    query_rot = rotate(query_val.reshape(row_count, HEADS, HEAD_DIM), cos_tab[:, None, :], sin_tab[:, None, :])
    query_bf = query_rot.astype(jnp.bfloat16).reshape(row_count, KV_HEADS, group_size, HEAD_DIM)
    keys_bf = rotate(key_val.reshape(row_count, KV_HEADS, HEAD_DIM), cos_tab[:, None, :], sin_tab[:, None, :]).astype(jnp.bfloat16)
    values_bf = value_val.astype(jnp.bfloat16).reshape(row_count, KV_HEADS, HEAD_DIM)
    attn_bf, log_total = attend_forward(query_bf, keys_bf, values_bf, allowed)
    resid_mid = residual + mat_mul(attn_bf.reshape(row_count, -1), w_out.T)
    inv_mid, normed_mid = norm_forward(resid_mid, gain_mid)
    gate_pre = mat_mul(normed_mid, w_gate)
    up_pre = mat_mul(normed_mid, w_up)
    hidden_bf = (jax.nn.silu(gate_pre) * up_pre).astype(jnp.bfloat16)
    layer_out = resid_mid + mat_mul(hidden_bf, w_down.T)
    stored = (residual, inv_in, normed_in, query_bf, keys_bf, values_bf, attn_bf, log_total, resid_mid, inv_mid, normed_mid, gate_pre, up_pre, hidden_bf)
    return (layer_out, stored)

def layer_backward(grad_out, stored, weights, allowed, cos_tab, sin_tab):
    gain_in, w_query, b_query, w_key, w_value, b_keyval, w_out, gain_mid, w_gate, w_up, w_down = weights
    residual, inv_in, normed_in, query_bf, keys_bf, values_bf, attn_bf, log_total, resid_mid, inv_mid, normed_mid, gate_pre, up_pre, hidden_bf = stored
    row_count = residual.shape[0]
    grad_out_bf = grad_out.astype(jnp.bfloat16)
    grad_hidden = mat_mul(grad_out_bf, w_down)
    grad_w_down = mat_mul(grad_out_bf.T, hidden_bf)
    sigmoid_gate = jax.nn.sigmoid(gate_pre)
    grad_gate = (grad_hidden * up_pre * sigmoid_gate * (1.0 + gate_pre * (1.0 - sigmoid_gate))).astype(jnp.bfloat16)
    grad_up = (grad_hidden * gate_pre * sigmoid_gate).astype(jnp.bfloat16)
    grad_normed_mid = mat_mul(grad_gate, w_gate.T) + mat_mul(grad_up, w_up.T)
    grad_w_gate = mat_mul(normed_mid.T, grad_gate)
    grad_w_up = mat_mul(normed_mid.T, grad_up)
    grad_mid_norm, grad_gain_mid = norm_backward(resid_mid, inv_mid, gain_mid, grad_normed_mid)
    grad_mid = grad_out + grad_mid_norm
    grad_mid_bf = grad_mid.astype(jnp.bfloat16)
    grad_attn = mat_mul(grad_mid_bf, w_out).astype(jnp.bfloat16)
    grad_w_out = mat_mul(grad_mid_bf.T, attn_bf.reshape(row_count, -1))
    grad_query, grad_key, grad_value = attend_backward(query_bf, keys_bf, values_bf, attn_bf, log_total, grad_attn.reshape(attn_bf.shape), allowed)
    grad_query = unrotate(grad_query.reshape(row_count, HEADS, HEAD_DIM), cos_tab[:, None, :], sin_tab[:, None, :]).reshape(row_count, -1)
    grad_key = unrotate(grad_key, cos_tab[:, None, :], sin_tab[:, None, :]).reshape(row_count, -1)
    grad_value = grad_value.reshape(row_count, -1)
    grad_b_query = lax.optimization_barrier(jnp.sum(grad_query, axis=0)).reshape(KV_HEADS, -1).T
    grad_b_keyval = jnp.concatenate([lax.optimization_barrier(jnp.sum(grad_key, axis=0)).reshape(KV_HEADS, HEAD_DIM).T, lax.optimization_barrier(jnp.sum(grad_value, axis=0)).reshape(KV_HEADS, HEAD_DIM).T], 0)
    grad_query_bf = grad_query.astype(jnp.bfloat16)
    grad_key_bf = grad_key.astype(jnp.bfloat16)
    grad_value_bf = grad_value.astype(jnp.bfloat16)
    grad_normed_in = mat_mul(grad_query_bf, w_query.T) + mat_mul(grad_key_bf, w_key.T) + mat_mul(grad_value_bf, w_value.T)
    grad_w_query = mat_mul(normed_in.T, grad_query_bf)
    grad_w_key = mat_mul(normed_in.T, grad_key_bf)
    grad_w_value = mat_mul(normed_in.T, grad_value_bf)
    grad_in_norm, grad_gain_in = norm_backward(residual, inv_in, gain_in, grad_normed_in)
    grad_in = grad_mid + grad_in_norm
    grad_terms = (grad_gain_in, grad_w_query, grad_b_query, grad_w_key, grad_w_value, grad_b_keyval, grad_w_out, grad_gain_mid, grad_w_gate, grad_w_up, grad_w_down)
    return (grad_in, grad_terms)

def reference(tokens, cotangent, segments, positions, counts, attn_gain, q_weight, q_bias, k_weight, v_weight, kv_bias, o_weight, mlp_gain, gate_weight, up_weight, down_weight):
    params = (attn_gain, q_weight, q_bias, k_weight, v_weight, kv_bias, o_weight, mlp_gain, gate_weight, up_weight, down_weight)
    token_idx = jnp.arange(SEQ_LEN, dtype=jnp.int32)
    causal = token_idx[None, :] <= token_idx[:, None]

    def one_sequence(running, inputs):
        tok_seq, grad_seq, seg_seq, pos_seq, seq_no = inputs
        live_val = (seq_no % MB < counts[seq_no // MB]).astype(jnp.float32)
        allowed = causal & (seg_seq[:, None] == seg_seq[None, :])
        cos_tab, sin_tab = rope_tables(pos_seq)
        residual = tok_seq.astype(jnp.float32)
        stored_all = []
        for layer_no in range(LAYERS):
            weights = tuple((param_arr[layer_no] for param_arr in params))
            residual, stored = layer_forward(residual, weights, allowed, cos_tab, sin_tab)
            stored_all.append(stored)
        grad_rows = grad_seq.astype(jnp.float32) * live_val
        layer_terms = [None] * LAYERS
        for layer_no in reversed(range(LAYERS)):
            weights = tuple((param_arr[layer_no] for param_arr in params))
            grad_rows, grad_terms = layer_backward(grad_rows, stored_all[layer_no], weights, allowed, cos_tab, sin_tab)
            layer_terms[layer_no] = grad_terms
        stacked = tuple((jnp.stack([layer_terms[layer_no][member] for layer_no in range(LAYERS)]) for member in range(11)))
        running = tuple((total_a + total_b for total_a, total_b in zip(running, stacked)))
        return (running, (residual * live_val, grad_rows))
    zero_grads = tuple((jnp.zeros(param_arr.shape, jnp.float32) for param_arr in params))
    seq_ids = jnp.arange(SEQS, dtype=jnp.int32)
    totals, (acts_all, grads_all) = lax.scan(one_sequence, zero_grads, (tokens, cotangent, segments, positions, seq_ids))
    return (acts_all, grads_all, totals[0], totals[1], totals[2], totals[3], totals[4], totals[5], totals[6], totals[7], totals[8], totals[9], totals[10])
```

```python
import jax
import jax.numpy as jnp
from jax import lax
from jax.sharding import PartitionSpec as P

HEADS = 12
KV_HEADS = 2
HEAD_DIM = 128
LAYERS = 1


theta_base = 1000000.0
norm_eps = 1e-06
masked_score = -1e30


def mat_mul(left, right):
    return jnp.dot(left, right, preferred_element_type=jnp.float32)


def mat_mul_t(left, right):
    return lax.dot_general(
        left, right, (((1,), (1,)), ((), ())), preferred_element_type=jnp.float32
    )


def rows_mul(left, right):
    return lax.dot_general(
        left, right, (((0,), (0,)), ((), ())), preferred_element_type=jnp.float32
    )


def rope_tables(pos_vals):
    half_dim = HEAD_DIM // 2
    frequency = theta_base ** (-(jnp.arange(half_dim, dtype=jnp.float32) * (2.0 / HEAD_DIM)))
    angles = pos_vals.astype(jnp.float32)[..., None] * frequency
    cos_half = jnp.cos(angles)
    sin_half = jnp.sin(angles)
    return (jnp.concatenate([cos_half, cos_half], -1), jnp.concatenate([sin_half, sin_half], -1))


def rotate(values, cos_tab, sin_tab):
    half_dim = values.shape[-1] // 2
    turned = jnp.concatenate([-values[..., half_dim:], values[..., :half_dim]], -1)
    return values * cos_tab + turned * sin_tab


def unrotate(grad_vals, cos_tab, sin_tab):
    half_dim = grad_vals.shape[-1] // 2
    scaled = grad_vals * sin_tab
    turned = jnp.concatenate([scaled[..., half_dim:], -scaled[..., :half_dim]], -1)
    return grad_vals * cos_tab + turned


def norm_forward(residual, gain_vec):
    inv_rms = lax.rsqrt(jnp.mean(residual * residual, axis=-1, keepdims=True) + norm_eps)
    normed = (residual * inv_rms * gain_vec.astype(jnp.float32)).astype(jnp.bfloat16)
    return (inv_rms, normed)


def norm_backward(residual, inv_rms, gain_vec, grad_normed):
    weighted = grad_normed * gain_vec.astype(jnp.float32)
    inner_mean = jnp.mean(weighted * residual, axis=-1, keepdims=True)
    grad_resid = inv_rms * weighted - residual * (inv_rms * inv_rms * inv_rms) * inner_mean
    grad_gain = jnp.sum(grad_normed * residual * inv_rms, axis=0)
    return (grad_resid, grad_gain)


def split_heads(keys_all, values_all):
    seq_count, full_len, kv_width = keys_all.shape
    kv_local = kv_width // HEAD_DIM
    return (
        keys_all.reshape(seq_count, full_len, kv_local, HEAD_DIM),
        values_all.reshape(seq_count, full_len, kv_local, HEAD_DIM),
    )


def attend_forward(query_bf, keys_all, values_all, allowed):
    key_heads, value_heads = split_heads(keys_all, values_all)
    scores = jnp.einsum(
        "bqkgd,bskd->bkgqs", query_bf, key_heads, preferred_element_type=jnp.float32
    ) * HEAD_DIM ** (-0.5)
    scores = jnp.where(allowed[:, None, None], scores, masked_score)
    top_score = jnp.max(scores, axis=-1, keepdims=True)
    shifted_exp = jnp.exp(scores - top_score)
    totals = jnp.sum(shifted_exp, axis=-1, keepdims=True)
    prob_bf = (shifted_exp / totals).astype(jnp.bfloat16)
    output = jnp.einsum(
        "bkgqs,bskd->bqkgd", prob_bf, value_heads, preferred_element_type=jnp.float32
    )
    return (output.astype(jnp.bfloat16), top_score + jnp.log(totals))


def attend_backward(query_bf, keys_all, values_all, attn_bf, log_total, grad_attn, allowed):
    key_heads, value_heads = split_heads(keys_all, values_all)
    scores = jnp.einsum(
        "bqkgd,bskd->bkgqs", query_bf, key_heads, preferred_element_type=jnp.float32
    ) * HEAD_DIM ** (-0.5)
    prob_full = jnp.exp(jnp.where(allowed[:, None, None], scores, masked_score) - log_total)
    prob_bf = prob_full.astype(jnp.bfloat16)
    grad_value = jnp.einsum(
        "bkgqs,bqkgd->bskd", prob_bf, grad_attn, preferred_element_type=jnp.float32
    )
    grad_prob = jnp.einsum(
        "bqkgd,bskd->bkgqs", grad_attn, value_heads, preferred_element_type=jnp.float32
    )
    row_dot = jnp.sum(grad_attn.astype(jnp.float32) * attn_bf.astype(jnp.float32), axis=-1)
    row_dot = jnp.transpose(row_dot, (0, 2, 3, 1))[..., None]
    grad_score = (prob_full * (grad_prob - row_dot) * HEAD_DIM ** (-0.5)).astype(jnp.bfloat16)
    grad_query = jnp.einsum(
        "bkgqs,bskd->bqkgd", grad_score, key_heads, preferred_element_type=jnp.float32
    )
    grad_key = jnp.einsum(
        "bkgqs,bqkgd->bskd", grad_score, query_bf, preferred_element_type=jnp.float32
    )
    return (grad_query, grad_key.reshape(keys_all.shape), grad_value.reshape(values_all.shape))


def xor_permute(value, axis_name, step):
    count = lax.axis_size(axis_name)
    return lax.ppermute(value, axis_name, [(rank, rank ^ step) for rank in range(count)])


def axis_bits(axis_name):
    return [1 << shift for shift in range(lax.axis_size(axis_name).bit_length() - 1)]


def partner(value):
    return xor_permute(value, "tp", 1)


def place(pieces, rank, dim):
    width = pieces[0].shape[dim]
    whole_shape = list(pieces[0].shape)
    whole_shape[dim] = width * len(pieces)
    whole = jnp.zeros(whole_shape, pieces[0].dtype)
    for offset, piece in enumerate(pieces):
        whole = lax.dynamic_update_slice_in_dim(whole, piece, (rank ^ offset) * width, dim)
    return whole


def join_halves(mine, other, core, dim):
    return jnp.where(
        core == 0, jnp.concatenate([mine, other], dim), jnp.concatenate([other, mine], dim)
    )


def gather_direct(value, axis_name):
    count = lax.axis_size(axis_name)
    return [value] + [xor_permute(value, axis_name, step) for step in range(1, count)]


def gather_halves(value, axis_name):
    rows = value.shape[0]
    half = rows // 2
    bits = axis_bits(axis_name)
    parts = []
    for piece, order in ((value[:half], bits), (value[half:], bits[::-1])):
        held = {0: piece}
        for bit in order:
            for key in list(held):
                held[key | bit] = xor_permute(held[key], axis_name, bit)
        parts.append(held)
    return [(parts[0][key], parts[1][key]) for key in range(len(parts[0]))]


def scatter_halves(blocks, axis_name):
    half = blocks[0].shape[0] // 2
    bits = axis_bits(axis_name)
    done = []
    for low, high, order in ((0, half, bits[::-1]), (half, 2 * half, bits)):
        held = {key: block[low:high] for key, block in enumerate(blocks)}
        for bit in order:
            for key in [key for key in held if key & bit]:
                sent = held.pop(key).astype(jnp.bfloat16)
                held[key ^ bit] = held[key ^ bit] + xor_permute(sent, axis_name, bit).astype(jnp.float32)
        done.append(held[0])
    return jnp.concatenate(done, 0)


def scatter_small(blocks, axis_name):
    held = dict(enumerate(blocks))
    for bit in axis_bits(axis_name)[::-1]:
        for key in [key for key in held if key & bit]:
            held[key ^ bit] = held[key ^ bit] + xor_permute(held.pop(key), axis_name, bit)
    return held[0]


def scatter_direct(block_of, axis_name):
    total = block_of(0)
    for step in range(1, lax.axis_size(axis_name)):
        got = xor_permute(block_of(step).astype(jnp.bfloat16), axis_name, step)
        total = total + got.astype(jnp.float32)
    return total


def rows_at(value, index, size):
    return lax.dynamic_slice_in_dim(value, index * size, size, 0)


def columns_at(value, index, size):
    return lax.dynamic_slice_in_dim(value, index * size, size, 1)


def on_device(
    tokens,
    cotangent,
    segments,
    positions,
    counts,
    attn_gain,
    q_weight,
    q_bias,
    k_weight,
    v_weight,
    kv_bias,
    o_weight,
    mlp_gain,
    gate_weight,
    up_weight,
    down_weight,
):
    dp_count, ctx_count = lax.axis_size("dp"), lax.axis_size("ctx")
    dp_rank, ctx_rank, core = lax.axis_index("dp"), lax.axis_index("ctx"), lax.axis_index("tp")
    seq_count, local_len, width = tokens.shape
    full_len = segments.shape[1]
    row_count = seq_count * local_len
    half_width = width // 2
    own_rows = q_weight.shape[1]
    group_rows = own_rows * ctx_count
    q_cols, k_cols, ff_cols = q_weight.shape[2], k_weight.shape[2], gate_weight.shape[2]
    kv_local = k_cols // HEAD_DIM
    group_size = q_cols // k_cols
    qkv_cols = q_cols + 2 * k_cols
    lane = 128
    ff_block = -(-ff_cols // (lane * ctx_count)) * lane
    ff_pad = ff_block * ctx_count - ff_cols
    f32, bf16 = jnp.float32, jnp.bfloat16

    small = jnp.concatenate(
        [attn_gain[0], mlp_gain[0], q_bias[0].reshape(-1), kv_bias[0].reshape(-1)]
    )[None]
    sizes = (attn_gain.shape[1], mlp_gain.shape[1], q_bias.shape[1] * q_bias.shape[2], kv_bias.shape[1] * kv_bias.shape[2])
    small_ctx = place(gather_direct(small, "ctx"), ctx_rank, 0)[None]
    held = {0: small_ctx}
    for bit in axis_bits("dp"):
        for key in list(held):
            held[key | bit] = xor_permute(held[key], "dp", bit)
    small_all = place([held[key] for key in range(dp_count)], dp_rank, 0)
    small_all = small_all.reshape(dp_count * ctx_count, -1)
    cuts = [0]
    for size in sizes:
        cuts.append(cuts[-1] + size)
    gain_in, gain_mid, b_query, b_keyval = (
        small_all[:, low:high].reshape(-1) for low, high in zip(cuts[:-1], cuts[1:])
    )
    b_query = b_query.reshape(-1, kv_local).T.reshape(-1).astype(f32)
    b_keyval = b_keyval.reshape(-1, kv_local).astype(f32)
    b_qkv = jnp.concatenate(
        [b_query, b_keyval[:HEAD_DIM].T.reshape(-1), b_keyval[HEAD_DIM:].T.reshape(-1)]
    )

    attn_own = jnp.concatenate([q_weight[0], k_weight[0], v_weight[0], o_weight[0]], 1)
    attn_group = place(gather_direct(attn_own, "ctx"), ctx_rank, 0)
    attn_pairs = gather_halves(attn_group, "dp")
    w_attn = place([jnp.concatenate(pair, 0) for pair in attn_pairs], dp_rank, 0)
    w_qkv, w_out = w_attn[:, :qkv_cols], w_attn[:, qkv_cols:]

    live_seq = (jnp.arange(seq_count, dtype=jnp.int32) < counts[0]).astype(f32)
    live_rows = jnp.repeat(live_seq, local_len)[:, None]
    grad_out = cotangent.astype(f32).reshape(-1, width) * live_rows

    def spread(rows_bf):
        mine = jnp.concatenate(gather_direct(columns_at(rows_bf, core, half_width), "ctx"), 0)
        return join_halves(mine, partner(mine), core, 1)

    grad_all = spread(grad_out.astype(bf16))

    def spread_weight(weight):
        padded = jnp.pad(weight[0], ((0, 0), (0, ff_pad)))
        pieces = [columns_at(padded, ctx_rank, ff_block)]
        for step in range(1, ctx_count):
            pieces.append(xor_permute(columns_at(padded, ctx_rank ^ step, ff_block), "ctx", step))
        pairs = gather_halves(place(pieces, ctx_rank, 0), "dp")
        return place([jnp.concatenate(pair, 0) for pair in pairs], dp_rank, 0)

    w_gate = spread_weight(gate_weight)
    w_up = spread_weight(up_weight)
    w_down = spread_weight(down_weight)

    query_pos = ctx_rank * local_len + jnp.arange(local_len, dtype=jnp.int32)
    key_pos = jnp.arange(full_len, dtype=jnp.int32)
    query_seg = lax.dynamic_slice_in_dim(segments, ctx_rank * local_len, local_len, 1)
    allowed = (query_seg[:, :, None] == segments[:, None, :]) & (
        key_pos[None, None, :] <= query_pos[None, :, None]
    )
    cos_tab, sin_tab = rope_tables(positions.reshape(-1))
    cos_tab, sin_tab = cos_tab[:, None, :], sin_tab[:, None, :]
    residual = tokens.astype(f32).reshape(-1, width)
    inv_in, normed_in = norm_forward(residual, gain_in)
    qkv_val = mat_mul(normed_in, w_qkv) + b_qkv
    query_bf = rotate(
        qkv_val[:, :q_cols].reshape(row_count, -1, HEAD_DIM), cos_tab, sin_tab
    ).astype(bf16).reshape(seq_count, -1, kv_local, group_size, HEAD_DIM)
    key_bf = rotate(
        qkv_val[:, q_cols : q_cols + k_cols].reshape(row_count, -1, HEAD_DIM), cos_tab, sin_tab
    ).astype(bf16).reshape(row_count, -1)
    value_bf = qkv_val[:, q_cols + k_cols :].astype(bf16)
    keyval = jnp.concatenate([key_bf, value_bf], 1).reshape(seq_count, local_len, -1)
    keyval_all = place(gather_direct(keyval, "ctx"), ctx_rank, 1)
    keys_all, values_all = keyval_all[..., :k_cols], keyval_all[..., k_cols:]
    attn_bf, log_total = attend_forward(query_bf, keys_all, values_all, allowed)
    attn_flat = attn_bf.reshape(row_count, -1)
    out_part = mat_mul_t(attn_flat, w_out)
    resid_mid = residual + (out_part + partner(out_part))
    inv_mid, normed_mid = norm_forward(resid_mid, gain_mid)

    mid_all = spread(normed_mid)
    gate_pre = mat_mul(mid_all, w_gate)
    up_pre = mat_mul(mid_all, w_up)
    hidden_bf = (jax.nn.silu(gate_pre) * up_pre).astype(bf16)
    grad_hidden = mat_mul(grad_all, w_down)
    sigmoid_gate = jax.nn.sigmoid(gate_pre)
    grad_gate = (
        grad_hidden * up_pre * sigmoid_gate * (1.0 + gate_pre * (1.0 - sigmoid_gate))
    ).astype(bf16)
    grad_up = (grad_hidden * gate_pre * sigmoid_gate).astype(bf16)

    def collect(part):
        part_bf = columns_at(part, 1 - core, half_width).astype(bf16)
        mine = columns_at(part, core, half_width) + partner(part_bf).astype(f32)
        total = scatter_direct(lambda step: mine[step * row_count : (step + 1) * row_count], "ctx")
        return join_halves(total, partner(total), core, 1)

    grad_normed_mid = collect(mat_mul_t(grad_gate, w_gate) + mat_mul_t(grad_up, w_up))

    def owner_weight(left, right):
        blocks = [
            rows_mul(columns_at(left, dp_rank ^ step, group_rows), right)
            for step in range(dp_count)
        ]
        group = scatter_halves(blocks, "dp").astype(bf16)
        pieces = [rows_at(group, ctx_rank, own_rows)]
        for step in range(1, ctx_count):
            pieces.append(xor_permute(rows_at(group, ctx_rank ^ step, own_rows), "ctx", step))
        return place(pieces, ctx_rank, 1)[:, :ff_cols].astype(f32)

    grad_w_down = owner_weight(grad_all, hidden_bf)
    grad_w_gate = owner_weight(mid_all, grad_gate)
    grad_w_up = owner_weight(mid_all, grad_up)

    layer_out = resid_mid + collect(mat_mul_t(hidden_bf, w_down))
    activations = (layer_out * live_rows).reshape(tokens.shape)

    grad_mid_norm, grad_gain_mid = norm_backward(resid_mid, inv_mid, gain_mid, grad_normed_mid)
    grad_mid = grad_out + grad_mid_norm
    grad_mid_bf = grad_mid.astype(bf16)
    grad_attn = mat_mul(grad_mid_bf, w_out).astype(bf16)

    def owner_attn(left, right):
        blocks = [
            rows_mul(columns_at(left, dp_rank ^ step, group_rows), right)
            for step in range(dp_count)
        ]
        group = scatter_halves(blocks, "dp")
        return scatter_direct(lambda step: rows_at(group, ctx_rank ^ step, own_rows), "ctx")

    grad_w_out = owner_attn(grad_mid_bf, attn_flat)
    grad_query, grad_key_all, grad_value_all = attend_backward(
        query_bf, keys_all, values_all, attn_bf, log_total, grad_attn.reshape(attn_bf.shape), allowed
    )
    grad_keyval_all = jnp.concatenate([grad_key_all, grad_value_all], 2)
    grad_keyval = scatter_direct(
        lambda step: lax.dynamic_slice_in_dim(
            grad_keyval_all, (ctx_rank ^ step) * local_len, local_len, 1
        ),
        "ctx",
    ).reshape(row_count, -1)
    grad_query = unrotate(
        grad_query.reshape(row_count, -1, HEAD_DIM), cos_tab, sin_tab
    ).reshape(row_count, -1)
    grad_key = unrotate(
        grad_keyval[:, :k_cols].reshape(row_count, -1, HEAD_DIM), cos_tab, sin_tab
    ).reshape(row_count, -1)
    grad_qkv = jnp.concatenate([grad_query, grad_key, grad_keyval[:, k_cols:]], 1)
    grad_qkv_bf = grad_qkv.astype(bf16)
    grad_w_qkv = owner_attn(normed_in, grad_qkv_bf)
    dot_part = mat_mul_t(grad_qkv_bf, w_qkv)
    grad_normed_in = dot_part + partner(dot_part)
    grad_in_norm, grad_gain_in = norm_backward(residual, inv_in, gain_in, grad_normed_in)
    input_grad = (grad_mid + grad_in_norm).reshape(tokens.shape)

    bias_sum = jnp.sum(grad_qkv, axis=0)
    device_count = dp_count * ctx_count
    grad_small = jnp.concatenate(
        [
            grad_gain_in.reshape(device_count, -1),
            grad_gain_mid.reshape(device_count, -1),
            bias_sum[:q_cols].reshape(kv_local, -1).T.reshape(device_count, -1),
            jnp.concatenate(
                [
                    bias_sum[q_cols : q_cols + k_cols].reshape(kv_local, -1).T,
                    bias_sum[q_cols + k_cols :].reshape(kv_local, -1).T,
                ],
                0,
            ).reshape(device_count, -1),
        ],
        1,
    )
    small_group = scatter_small(
        [rows_at(grad_small, dp_rank ^ step, ctx_count) for step in range(dp_count)], "dp"
    )
    small_own = scatter_small(
        [rows_at(small_group, ctx_rank ^ step, 1) for step in range(ctx_count)], "ctx"
    )
    own = [small_own[:, low:high] for low, high in zip(cuts[:-1], cuts[1:])]
    return (
        activations,
        input_grad,
        own[0],
        grad_w_qkv[None, :, :q_cols],
        own[2].reshape(q_bias.shape),
        grad_w_qkv[None, :, q_cols : q_cols + k_cols],
        grad_w_qkv[None, :, q_cols + k_cols :],
        own[3].reshape(kv_bias.shape),
        grad_w_out[None],
        own[1],
        grad_w_gate[None],
        grad_w_up[None],
        grad_w_down[None],
    )


def solution(mesh):
    in_specs = (
        P("dp", "ctx", None),
        P("dp", "ctx", None),
        P("dp", None),
        P("dp", "ctx"),
        P("dp"),
        P(None, ("dp", "ctx")),
        P(None, ("dp", "ctx"), "tp"),
        P(None, ("dp", "ctx"), "tp"),
        P(None, ("dp", "ctx"), "tp"),
        P(None, ("dp", "ctx"), "tp"),
        P(None, ("dp", "ctx"), "tp"),
        P(None, ("dp", "ctx"), "tp"),
        P(None, ("dp", "ctx")),
        P(None, ("dp", "ctx"), "tp"),
        P(None, ("dp", "ctx"), "tp"),
        P(None, ("dp", "ctx"), "tp"),
    )
    out_specs = (
        P("dp", "ctx", None),
        P("dp", "ctx", None),
        P(None, ("dp", "ctx")),
        P(None, ("dp", "ctx"), "tp"),
        P(None, ("dp", "ctx"), "tp"),
        P(None, ("dp", "ctx"), "tp"),
        P(None, ("dp", "ctx"), "tp"),
        P(None, ("dp", "ctx"), "tp"),
        P(None, ("dp", "ctx"), "tp"),
        P(None, ("dp", "ctx")),
        P(None, ("dp", "ctx"), "tp"),
        P(None, ("dp", "ctx"), "tp"),
        P(None, ("dp", "ctx"), "tp"),
    )
    return jax.shard_map(
        on_device, mesh=mesh, in_specs=in_specs, out_specs=out_specs, check_vma=False
    )
```

```python
import functools

import jax
import jax.numpy as jnp
from jax import lax
from jax.experimental import pallas as pl
from jax.experimental.pallas import tpu as pltpu
from jax.sharding import PartitionSpec as P

HEADS = 12
KV_HEADS = 2
HEAD_DIM = 128
LAYERS = 1


theta_base = 1000000.0
norm_eps = 1e-06
masked_score = -1e30


def mat_mul(left, right):
    return jnp.dot(left, right, preferred_element_type=jnp.float32)


def mat_mul_t(left, right):
    return lax.dot_general(
        left, right, (((1,), (1,)), ((), ())), preferred_element_type=jnp.float32
    )


def rows_mul(left, right):
    return lax.dot_general(
        left, right, (((0,), (0,)), ((), ())), preferred_element_type=jnp.float32
    )


def rope_tables(pos_vals):
    half_dim = HEAD_DIM // 2
    frequency = theta_base ** (-(jnp.arange(half_dim, dtype=jnp.float32) * (2.0 / HEAD_DIM)))
    angles = pos_vals.astype(jnp.float32)[..., None] * frequency
    cos_half = jnp.cos(angles)
    sin_half = jnp.sin(angles)
    return (jnp.concatenate([cos_half, cos_half], -1), jnp.concatenate([sin_half, sin_half], -1))


def rotate(values, cos_tab, sin_tab):
    half_dim = values.shape[-1] // 2
    turned = jnp.concatenate([-values[..., half_dim:], values[..., :half_dim]], -1)
    return values * cos_tab + turned * sin_tab


def unrotate(grad_vals, cos_tab, sin_tab):
    half_dim = grad_vals.shape[-1] // 2
    scaled = grad_vals * sin_tab
    turned = jnp.concatenate([scaled[..., half_dim:], -scaled[..., :half_dim]], -1)
    return grad_vals * cos_tab + turned


def norm_forward(residual, gain_vec):
    inv_rms = lax.rsqrt(jnp.mean(residual * residual, axis=-1, keepdims=True) + norm_eps)
    normed = (residual * inv_rms * gain_vec.astype(jnp.float32)).astype(jnp.bfloat16)
    return (inv_rms, normed)


def norm_backward(residual, inv_rms, gain_vec, grad_normed):
    weighted = grad_normed * gain_vec.astype(jnp.float32)
    inner_mean = jnp.mean(weighted * residual, axis=-1, keepdims=True)
    grad_resid = inv_rms * weighted - residual * (inv_rms * inv_rms * inv_rms) * inner_mean
    grad_gain = jnp.sum(grad_normed * residual * inv_rms, axis=0)
    return (grad_resid, grad_gain)


def split_heads(keys_all, values_all):
    seq_count, full_len, kv_width = keys_all.shape
    kv_local = kv_width // HEAD_DIM
    return (
        keys_all.reshape(seq_count, full_len, kv_local, HEAD_DIM),
        values_all.reshape(seq_count, full_len, kv_local, HEAD_DIM),
    )


def attend_forward(query_bf, keys_all, values_all, allowed):
    key_heads, value_heads = split_heads(keys_all, values_all)
    scores = jnp.einsum(
        "bqkgd,bskd->bkgqs", query_bf, key_heads, preferred_element_type=jnp.float32
    ) * HEAD_DIM ** (-0.5)
    scores = jnp.where(allowed[:, None, None], scores, masked_score)
    top_score = jnp.max(scores, axis=-1, keepdims=True)
    shifted_exp = jnp.exp(scores - top_score)
    totals = jnp.sum(shifted_exp, axis=-1, keepdims=True)
    prob_bf = (shifted_exp / totals).astype(jnp.bfloat16)
    output = jnp.einsum(
        "bkgqs,bskd->bqkgd", prob_bf, value_heads, preferred_element_type=jnp.float32
    )
    return (output.astype(jnp.bfloat16), top_score + jnp.log(totals))


def attend_backward(query_bf, keys_all, values_all, attn_bf, log_total, grad_attn, allowed):
    key_heads, value_heads = split_heads(keys_all, values_all)
    scores = jnp.einsum(
        "bqkgd,bskd->bkgqs", query_bf, key_heads, preferred_element_type=jnp.float32
    ) * HEAD_DIM ** (-0.5)
    prob_full = jnp.exp(jnp.where(allowed[:, None, None], scores, masked_score) - log_total)
    prob_bf = prob_full.astype(jnp.bfloat16)
    grad_value = jnp.einsum(
        "bkgqs,bqkgd->bskd", prob_bf, grad_attn, preferred_element_type=jnp.float32
    )
    grad_prob = jnp.einsum(
        "bqkgd,bskd->bkgqs", grad_attn, value_heads, preferred_element_type=jnp.float32
    )
    row_dot = jnp.sum(grad_attn.astype(jnp.float32) * attn_bf.astype(jnp.float32), axis=-1)
    row_dot = jnp.transpose(row_dot, (0, 2, 3, 1))[..., None]
    grad_score = (prob_full * (grad_prob - row_dot) * HEAD_DIM ** (-0.5)).astype(jnp.bfloat16)
    grad_query = jnp.einsum(
        "bkgqs,bskd->bqkgd", grad_score, key_heads, preferred_element_type=jnp.float32
    )
    grad_key = jnp.einsum(
        "bkgqs,bqkgd->bskd", grad_score, query_bf, preferred_element_type=jnp.float32
    )
    return (grad_query, grad_key.reshape(keys_all.shape), grad_value.reshape(values_all.shape))


def xor_permute(value, axis_name, step):
    count = lax.axis_size(axis_name)
    return lax.ppermute(value, axis_name, [(rank, rank ^ step) for rank in range(count)])


def axis_bits(axis_name):
    return [1 << shift for shift in range(lax.axis_size(axis_name).bit_length() - 1)]


def partner(value):
    return xor_permute(value, "tp", 1)


def place(pieces, rank, dim):
    width = pieces[0].shape[dim]
    whole_shape = list(pieces[0].shape)
    whole_shape[dim] = width * len(pieces)
    whole = jnp.zeros(whole_shape, pieces[0].dtype)
    for offset, piece in enumerate(pieces):
        whole = lax.dynamic_update_slice_in_dim(whole, piece, (rank ^ offset) * width, dim)
    return whole


def join_halves(mine, other, core, dim):
    return jnp.where(
        core == 0, jnp.concatenate([mine, other], dim), jnp.concatenate([other, mine], dim)
    )


def gather_direct(value, axis_name):
    count = lax.axis_size(axis_name)
    return [value] + [xor_permute(value, axis_name, step) for step in range(1, count)]


def gather_halves(value, axis_name):
    rows = value.shape[0]
    half = rows // 2
    bits = axis_bits(axis_name)
    parts = []
    for piece, order in ((value[:half], bits), (value[half:], bits[::-1])):
        held = {0: piece}
        for bit in order:
            for key in list(held):
                held[key | bit] = xor_permute(held[key], axis_name, bit)
        parts.append(held)
    return [(parts[0][key], parts[1][key]) for key in range(len(parts[0]))]


def scatter_halves(blocks, axis_name):
    half = blocks[0].shape[0] // 2
    bits = axis_bits(axis_name)
    done = []
    for low, high, order in ((0, half, bits[::-1]), (half, 2 * half, bits)):
        held = {key: block[low:high] for key, block in enumerate(blocks)}
        for bit in order:
            for key in [key for key in held if key & bit]:
                sent = held.pop(key).astype(jnp.bfloat16)
                held[key ^ bit] = held[key ^ bit] + xor_permute(sent, axis_name, bit).astype(jnp.float32)
        done.append(held[0])
    return jnp.concatenate(done, 0)


def scatter_small(blocks, axis_name):
    held = dict(enumerate(blocks))
    for bit in axis_bits(axis_name)[::-1]:
        for key in [key for key in held if key & bit]:
            held[key ^ bit] = held[key ^ bit] + xor_permute(held.pop(key), axis_name, bit)
    return held[0]


def scatter_direct(block_of, axis_name):
    total = block_of(0)
    for step in range(1, lax.axis_size(axis_name)):
        got = xor_permute(block_of(step).astype(jnp.bfloat16), axis_name, step)
        total = total + got.astype(jnp.float32)
    return total


def rows_at(value, index, size):
    return lax.dynamic_slice_in_dim(value, index * size, size, 0)


def columns_at(value, index, size):
    return lax.dynamic_slice_in_dim(value, index * size, size, 1)


def on_device(
    tokens,
    cotangent,
    segments,
    positions,
    counts,
    attn_gain,
    q_weight,
    q_bias,
    k_weight,
    v_weight,
    kv_bias,
    o_weight,
    mlp_gain,
    gate_weight,
    up_weight,
    down_weight,
):
    dp_count, ctx_count = lax.axis_size("dp"), lax.axis_size("ctx")
    dp_rank, ctx_rank, core = lax.axis_index("dp"), lax.axis_index("ctx"), lax.axis_index("tp")
    seq_count, local_len, width = tokens.shape
    full_len = segments.shape[1]
    row_count = seq_count * local_len
    half_width = width // 2
    own_rows = q_weight.shape[1]
    group_rows = own_rows * ctx_count
    q_cols, k_cols, ff_cols = q_weight.shape[2], k_weight.shape[2], gate_weight.shape[2]
    kv_local = k_cols // HEAD_DIM
    group_size = q_cols // k_cols
    qkv_cols = q_cols + 2 * k_cols
    lane = 128
    ff_block = -(-ff_cols // (lane * ctx_count)) * lane
    ff_pad = ff_block * ctx_count - ff_cols
    f32, bf16 = jnp.float32, jnp.bfloat16

    small = jnp.concatenate(
        [attn_gain[0], mlp_gain[0], q_bias[0].reshape(-1), kv_bias[0].reshape(-1)]
    )[None]
    sizes = (attn_gain.shape[1], mlp_gain.shape[1], q_bias.shape[1] * q_bias.shape[2], kv_bias.shape[1] * kv_bias.shape[2])
    small_ctx = place(gather_direct(small, "ctx"), ctx_rank, 0)[None]
    held = {0: small_ctx}
    for bit in axis_bits("dp"):
        for key in list(held):
            held[key | bit] = xor_permute(held[key], "dp", bit)
    small_all = place([held[key] for key in range(dp_count)], dp_rank, 0)
    small_all = small_all.reshape(dp_count * ctx_count, -1)
    cuts = [0]
    for size in sizes:
        cuts.append(cuts[-1] + size)
    gain_in, gain_mid, b_query, b_keyval = (
        small_all[:, low:high].reshape(-1) for low, high in zip(cuts[:-1], cuts[1:])
    )
    b_query = b_query.reshape(-1, kv_local).T.reshape(-1).astype(f32)
    b_keyval = b_keyval.reshape(-1, kv_local).astype(f32)
    b_qkv = jnp.concatenate(
        [b_query, b_keyval[:HEAD_DIM].T.reshape(-1), b_keyval[HEAD_DIM:].T.reshape(-1)]
    )

    attn_own = jnp.concatenate([q_weight[0], k_weight[0], v_weight[0], o_weight[0]], 1)
    attn_group = place(gather_direct(attn_own, "ctx"), ctx_rank, 0)
    attn_pairs = gather_halves(attn_group, "dp")
    w_attn = place([jnp.concatenate(pair, 0) for pair in attn_pairs], dp_rank, 0)
    w_qkv, w_out = w_attn[:, :qkv_cols], w_attn[:, qkv_cols:]

    live_seq = (jnp.arange(seq_count, dtype=jnp.int32) < counts[0]).astype(f32)
    live_rows = jnp.repeat(live_seq, local_len)[:, None]
    grad_out = cotangent.astype(f32).reshape(-1, width) * live_rows

    def spread(rows_bf):
        mine = jnp.concatenate(gather_direct(columns_at(rows_bf, core, half_width), "ctx"), 0)
        return join_halves(mine, partner(mine), core, 1)

    grad_all = spread(grad_out.astype(bf16))

    def spread_weight(weight):
        padded = jnp.pad(weight[0], ((0, 0), (0, ff_pad)))
        pieces = [columns_at(padded, ctx_rank, ff_block)]
        for step in range(1, ctx_count):
            pieces.append(xor_permute(columns_at(padded, ctx_rank ^ step, ff_block), "ctx", step))
        pairs = gather_halves(place(pieces, ctx_rank, 0), "dp")
        return place([jnp.concatenate(pair, 0) for pair in pairs], dp_rank, 0)

    w_gate = spread_weight(gate_weight)
    w_up = spread_weight(up_weight)
    w_down = spread_weight(down_weight)

    query_pos = ctx_rank * local_len + jnp.arange(local_len, dtype=jnp.int32)
    key_pos = jnp.arange(full_len, dtype=jnp.int32)
    query_seg = lax.dynamic_slice_in_dim(segments, ctx_rank * local_len, local_len, 1)
    allowed = (query_seg[:, :, None] == segments[:, None, :]) & (
        key_pos[None, None, :] <= query_pos[None, :, None]
    )
    cos_tab, sin_tab = rope_tables(positions.reshape(-1))
    cos_tab, sin_tab = cos_tab[:, None, :], sin_tab[:, None, :]
    residual = tokens.astype(f32).reshape(-1, width)
    inv_in, normed_in = norm_forward(residual, gain_in)
    qkv_val = mat_mul(normed_in, w_qkv) + b_qkv
    query_bf = rotate(
        qkv_val[:, :q_cols].reshape(row_count, -1, HEAD_DIM), cos_tab, sin_tab
    ).astype(bf16).reshape(seq_count, -1, kv_local, group_size, HEAD_DIM)
    key_bf = rotate(
        qkv_val[:, q_cols : q_cols + k_cols].reshape(row_count, -1, HEAD_DIM), cos_tab, sin_tab
    ).astype(bf16).reshape(row_count, -1)
    value_bf = qkv_val[:, q_cols + k_cols :].astype(bf16)
    keyval = jnp.concatenate([key_bf, value_bf], 1).reshape(seq_count, local_len, -1)
    keyval_all = place(gather_direct(keyval, "ctx"), ctx_rank, 1)
    keys_all, values_all = keyval_all[..., :k_cols], keyval_all[..., k_cols:]
    attn_bf, log_total = attend_forward(query_bf, keys_all, values_all, allowed)
    attn_flat = attn_bf.reshape(row_count, -1)
    out_part = mat_mul_t(attn_flat, w_out)
    resid_mid = residual + (out_part + partner(out_part))
    inv_mid, normed_mid = norm_forward(resid_mid, gain_mid)

    mid_all = spread(normed_mid)
    gate_pre = mat_mul(mid_all, w_gate)
    up_pre = mat_mul(mid_all, w_up)
    hidden_bf = (jax.nn.silu(gate_pre) * up_pre).astype(bf16)
    grad_hidden = mat_mul(grad_all, w_down)
    sigmoid_gate = jax.nn.sigmoid(gate_pre)
    grad_gate = (
        grad_hidden * up_pre * sigmoid_gate * (1.0 + gate_pre * (1.0 - sigmoid_gate))
    ).astype(bf16)
    grad_up = (grad_hidden * gate_pre * sigmoid_gate).astype(bf16)

    def collect(part):
        part_bf = columns_at(part, 1 - core, half_width).astype(bf16)
        mine = columns_at(part, core, half_width) + partner(part_bf).astype(f32)
        total = scatter_direct(lambda step: mine[step * row_count : (step + 1) * row_count], "ctx")
        return join_halves(total, partner(total), core, 1)

    grad_normed_mid = collect(mat_mul_t(grad_gate, w_gate) + mat_mul_t(grad_up, w_up))

    def owner_weight(left, right):
        blocks = [
            rows_mul(columns_at(left, dp_rank ^ step, group_rows), right)
            for step in range(dp_count)
        ]
        group = scatter_halves(blocks, "dp").astype(bf16)
        pieces = [rows_at(group, ctx_rank, own_rows)]
        for step in range(1, ctx_count):
            pieces.append(xor_permute(rows_at(group, ctx_rank ^ step, own_rows), "ctx", step))
        return place(pieces, ctx_rank, 1)[:, :ff_cols].astype(f32)

    grad_w_down = owner_weight(grad_all, hidden_bf)
    grad_w_gate = owner_weight(mid_all, grad_gate)
    grad_w_up = owner_weight(mid_all, grad_up)

    layer_out = resid_mid + collect(mat_mul_t(hidden_bf, w_down))
    activations = (layer_out * live_rows).reshape(tokens.shape)

    grad_mid_norm, grad_gain_mid = norm_backward(resid_mid, inv_mid, gain_mid, grad_normed_mid)
    grad_mid = grad_out + grad_mid_norm
    grad_mid_bf = grad_mid.astype(bf16)
    grad_attn = mat_mul(grad_mid_bf, w_out).astype(bf16)

    def owner_attn(left, right):
        blocks = [
            rows_mul(columns_at(left, dp_rank ^ step, group_rows), right)
            for step in range(dp_count)
        ]
        group = scatter_halves(blocks, "dp")
        return scatter_direct(lambda step: rows_at(group, ctx_rank ^ step, own_rows), "ctx")

    grad_w_out = owner_attn(grad_mid_bf, attn_flat)
    grad_query, grad_key_all, grad_value_all = attend_backward(
        query_bf, keys_all, values_all, attn_bf, log_total, grad_attn.reshape(attn_bf.shape), allowed
    )
    grad_keyval_all = jnp.concatenate([grad_key_all, grad_value_all], 2)
    grad_keyval = scatter_direct(
        lambda step: lax.dynamic_slice_in_dim(
            grad_keyval_all, (ctx_rank ^ step) * local_len, local_len, 1
        ),
        "ctx",
    ).reshape(row_count, -1)
    grad_query = unrotate(
        grad_query.reshape(row_count, -1, HEAD_DIM), cos_tab, sin_tab
    ).reshape(row_count, -1)
    grad_key = unrotate(
        grad_keyval[:, :k_cols].reshape(row_count, -1, HEAD_DIM), cos_tab, sin_tab
    ).reshape(row_count, -1)
    grad_qkv = jnp.concatenate([grad_query, grad_key, grad_keyval[:, k_cols:]], 1)
    grad_qkv_bf = grad_qkv.astype(bf16)
    grad_w_qkv = owner_attn(normed_in, grad_qkv_bf)
    dot_part = mat_mul_t(grad_qkv_bf, w_qkv)
    grad_normed_in = dot_part + partner(dot_part)
    grad_in_norm, grad_gain_in = norm_backward(residual, inv_in, gain_in, grad_normed_in)
    input_grad = (grad_mid + grad_in_norm).reshape(tokens.shape)

    bias_sum = jnp.sum(grad_qkv, axis=0)
    device_count = dp_count * ctx_count
    grad_small = jnp.concatenate(
        [
            grad_gain_in.reshape(device_count, -1),
            grad_gain_mid.reshape(device_count, -1),
            bias_sum[:q_cols].reshape(kv_local, -1).T.reshape(device_count, -1),
            jnp.concatenate(
                [
                    bias_sum[q_cols : q_cols + k_cols].reshape(kv_local, -1).T,
                    bias_sum[q_cols + k_cols :].reshape(kv_local, -1).T,
                ],
                0,
            ).reshape(device_count, -1),
        ],
        1,
    )
    small_group = scatter_small(
        [rows_at(grad_small, dp_rank ^ step, ctx_count) for step in range(dp_count)], "dp"
    )
    small_own = scatter_small(
        [rows_at(small_group, ctx_rank ^ step, 1) for step in range(ctx_count)], "ctx"
    )
    own = [small_own[:, low:high] for low, high in zip(cuts[:-1], cuts[1:])]
    return (
        activations,
        input_grad,
        own[0],
        grad_w_qkv[None, :, :q_cols],
        own[2].reshape(q_bias.shape),
        grad_w_qkv[None, :, q_cols : q_cols + k_cols],
        grad_w_qkv[None, :, q_cols + k_cols :],
        own[3].reshape(kv_bias.shape),
        grad_w_out[None],
        own[1],
        grad_w_gate[None],
        grad_w_up[None],
        grad_w_down[None],
    )


MESH = pl.DeviceIdType.MESH


def remote(src, dst, send_sem, recv_sem, target):
    return pltpu.make_async_remote_copy(
        src_ref=src, dst_ref=dst, send_sem=send_sem, recv_sem=recv_sem, device_id=target, device_id_type=MESH
    )


def greet(partners):
    barrier = pltpu.get_barrier_semaphore()
    for partner_id in partners:
        pl.semaphore_signal(barrier, inc=1, device_id=partner_id, device_id_type=MESH)
    pl.semaphore_wait(barrier, len(partners))


def spread_row(values, row_cols, period, total):
    left = lax.broadcasted_iota(jnp.int32, (period, total), 0)
    right = lax.broadcasted_iota(jnp.int32, (period, total), 1)
    pick = (lax.rem(right, period) == left).astype(jnp.float32).astype(jnp.bfloat16)
    spread = jnp.dot(values.astype(jnp.bfloat16), pick, preferred_element_type=jnp.float32)
    block = lax.broadcasted_iota(jnp.int32, spread.shape, 0) // 8
    owner = lax.broadcasted_iota(jnp.int32, spread.shape, 1) // period
    return jnp.sum(jnp.where(block == owner, spread, 0.0), axis=0, keepdims=True)


def forward_kernel(
    sizes,
    tok_ref,
    cot_ref,
    attn_own,
    mlp_own,
    small_own,
    cos_ref,
    sin_ref,
    qseg_ref,
    kseg_ref,
    wattn,
    wmlp,
    e_all,
    b_all,
    h_ref,
    a_ref,
    q_ref,
    kv_ref,
    o_ref,
    lse_ref,
    row_ref,
    small,
    part,
    part_in,
    b_buf,
    zs,
    zr,
    xs,
    xr,
    ys,
    yr,
    fs,
    fr,
    ks,
    kr,
    ps,
    pr,
    bs,
    br,
    loc,
):
    dp_count, ctx_count, own, qkv_cols, q_cols, gain_cut = sizes
    dp, ctx, core = lax.axis_index("dp"), lax.axis_index("ctx"), lax.axis_index("tp")
    bf16, f32 = jnp.bfloat16, jnp.float32
    width = tok_ref.shape[1]
    rows = tok_ref.shape[0]
    seqs = cot_ref.shape[0]
    local = cot_ref.shape[1]
    tiles = range(ctx_count)

    def at_x(d):
        return d + 1 - 2 * lax.rem(d, 2)

    def at_y(d):
        return lax.rem(d + 2, 4)

    dpx, dpy = at_x(dp), at_y(dp)
    dpd = at_x(dpy)
    peers = [ctx]
    for step in range(1, ctx_count):
        value = jnp.int32(0)
        for bit in (1, 2, 4, 8):
            if bit < ctx_count:
                digit = lax.rem(ctx // bit, 2)
                value = value + bit * (digit + (1 - 2 * digit) * ((step // bit) % 2))
        peers.append(value)
    other = 1 - core

    greet(
        [{"dp": dpx}, {"dp": dpy}, {"tp": other}] + [{"ctx": peers[step]} for step in range(1, ctx_count)]
    )
    sent = []

    def start(copy):
        copy.start()
        sent.append(copy)
        return copy

    def block_rows(d, c):
        return pl.ds(pl.multiple_of((d * ctx_count + c) * own, own), own)

    def slot(item, d, c):
        if item == 0:
            return small.at[d * ctx_count + c]
        if item == 1:
            return wattn.at[block_rows(d, c), :]
        return wmlp.at[item - 2, block_rows(d, c), :]

    def source(item, tile):
        if item == 0:
            return small_own
        if item == 1:
            return attn_own
        return mlp_own.at[item - 2, peers[tile]]

    items = range(5)
    local_copies = []
    for item in items:
        copy = pltpu.make_async_copy(source(item, 0), slot(item, dp, ctx), loc.at[item])
        copy.start()
        local_copies.append(copy)
    z_copy = {}

    def z_send(item):
        for tile in range(1, ctx_count):
            z_copy[item, tile] = start(
                remote(source(item, tile), slot(item, dp, ctx), zs.at[item, tile], zr.at[item, tile], {"ctx": peers[tile]})
            )

    x_copy, y_copy, f_copy = {}, {}, {}

    def xy_send(item, tile):
        src = source(item, 0) if tile == 0 else slot(item, dp, peers[tile])
        if tile:
            z_copy[item, tile].wait_recv()
        dst = slot(item, dp, peers[tile])
        x_copy[item, tile] = start(remote(src, dst, xs.at[item, tile], xr.at[item, tile], {"dp": dpx}))
        y_copy[item, tile] = start(remote(src, dst, ys.at[item, tile], yr.at[item, tile], {"dp": dpy}))

    def forward(item, tile):
        if (item + tile) % 2 == 0:
            x_copy[item, tile].wait_recv()
            place_at = slot(item, dpx, peers[tile])
            target = {"dp": dpy}
        else:
            y_copy[item, tile].wait_recv()
            place_at = slot(item, dpy, peers[tile])
            target = {"dp": dpx}
        f_copy[item, tile] = start(remote(place_at, place_at, fs.at[item, tile], fr.at[item, tile], target))

    def settle(item, tile):
        if (item + tile) % 2 == 0:
            y_copy[item, tile].wait_recv()
        else:
            x_copy[item, tile].wait_recv()
        f_copy[item, tile].wait_recv()

    def group_send(index, src, dst):
        return [
            start(
                remote(
                    src.at[core],
                    dst.at[ctx, core],
                    bs.at[index, 0, tile],
                    br.at[index, 0, tile],
                    {"ctx": peers[tile]},
                )
            )
            for tile in range(1, ctx_count)
        ]

    def group_relay(index, copies, dst, tile):
        copies[tile - 1].wait_recv()
        piece = dst.at[peers[tile], core]
        return start(remote(piece, piece, bs.at[index, 1, tile], br.at[index, 1, tile], {"tp": other}))

    z_send(0)
    z_send(1)
    xy_send(0, 0)
    xy_send(1, 0)
    for item in (2, 3, 4):
        z_send(item)
    e_local = pltpu.make_async_copy(cot_ref, e_all.at[ctx], loc.at[5])
    e_local.start()
    e_copies = group_send(0, cot_ref, e_all)
    for tile in range(1, ctx_count):
        xy_send(0, tile)
        xy_send(1, tile)
    for tile in tiles:
        forward(0, tile)
        forward(1, tile)
    for item in (2, 3, 4):
        xy_send(item, 0)
    for tile in tiles:
        settle(0, tile)
    local_copies[0].wait()

    flat = small[...].reshape(dp_count * ctx_count * 8, small.shape[2])
    row_ref[0:1, :] = spread_row(flat[:, gain_cut[0] : gain_cut[1]], None, gain_cut[1] - gain_cut[0], width)
    row_ref[1:2, :] = spread_row(flat[:, gain_cut[1] : gain_cut[2]], None, gain_cut[2] - gain_cut[1], width)
    row_ref[2:3, :q_cols] = spread_row(flat[:, gain_cut[2] : gain_cut[3]], None, gain_cut[3] - gain_cut[2], q_cols)
    row_ref[2:3, q_cols:qkv_cols] = spread_row(
        flat[:, gain_cut[3] : gain_cut[4]], None, gain_cut[4] - gain_cut[3], qkv_cols - q_cols
    )

    step_rows = 32

    def norm_in(index, _):
        piece = pl.ds(index * step_rows, step_rows)
        val = tok_ref[piece, :].astype(f32)
        inv = lax.rsqrt(jnp.mean(val * val, axis=-1, keepdims=True) + norm_eps)
        a_ref[piece, :] = (val * inv * row_ref[0:1, :]).astype(bf16)
        return 0

    lax.fori_loop(0, rows // step_rows, norm_in, 0)
    xy_send(2, 1)
    for tile in tiles:
        settle(1, tile)
    local_copies[1].wait()

    pending = []
    for item in (2, 3, 4):
        pending.append((forward, item, 0))
    pending.append((xy_send, 3, 1))
    pending.append((xy_send, 4, 1))
    for item in (2, 3, 4):
        pending.append((xy_send, item, 2))
        pending.append((forward, item, 1))
    for item in (2, 3, 4):
        pending.append((xy_send, item, 3))
        pending.append((forward, item, 2))
    for item in (2, 3, 4):
        pending.append((forward, item, 3))

    def pump(count):
        for _ in range(min(count, len(pending))):
            action, item, tile = pending.pop(0)
            action(item, tile)

    own_keys = pl.ds(pl.multiple_of(ctx * local, local), local)
    order = [qkv_cols - 256] + list(range(0, q_cols, 256))
    kv_copies = []
    for low in order:
        val = jnp.dot(a_ref[...], wattn[:, low : low + 256], preferred_element_type=f32) + row_ref[2:3, low : low + 256]
        for head_low in (0, 128):
            head = val[:, head_low : head_low + 128]
            if low + head_low < qkv_cols - 128:
                head = head * cos_ref[...] + pltpu.roll(head, 64, 1) * sin_ref[...]
            head = head.astype(bf16)
            for seq in range(seqs):
                piece = head[seq * local : (seq + 1) * local]
                if low == qkv_cols - 256:
                    kv_ref[seq, head_low // 128, own_keys, :] = piece
                else:
                    q_ref[seq, (low + head_low) // 128] = piece
        if low == qkv_cols - 256:
            for tile in range(1, ctx_count):
                piece = kv_ref.at[:, :, own_keys, :]
                kv_copies.append(start(remote(piece, piece, ks.at[tile], kr.at[tile], {"ctx": peers[tile]})))
        pump(1)
    pump(1)
    for copy in kv_copies:
        copy.wait_recv()

    keys = kv_ref.shape[2]
    key_no = lax.broadcasted_iota(jnp.int32, (local, keys), 1)
    query_no = lax.broadcasted_iota(jnp.int32, (local, keys), 0) + ctx * local
    for seq in range(seqs):
        seen = (qseg_ref[seq] == kseg_ref[seq]) & (key_no <= query_no)
        hide = jnp.where(seen, 0.0, masked_score)

        def one_head(head, _):
            score = lax.dot_general(
                q_ref[seq, head], kv_ref[seq, 0], (((1,), (1,)), ((), ())), preferred_element_type=f32
            )
            score = jnp.where(hide < 0.0, masked_score, score * HEAD_DIM ** (-0.5))
            top = jnp.max(score, axis=-1, keepdims=True)
            weight = jnp.exp(score - top)
            total = jnp.sum(weight, axis=-1, keepdims=True)
            prob = (weight / total).astype(bf16)
            lse_ref[seq, head] = top + jnp.log(total)
            out = jnp.dot(prob, kv_ref[seq, 1], preferred_element_type=f32)
            o_ref[seq, head] = out.astype(bf16)
            return 0

        lax.fori_loop(0, q_cols // 128, one_head, 0)
        pump(3)

    o_rows = jnp.concatenate(
        [jnp.concatenate([o_ref[seq, head] for head in range(q_cols // 128)], 1) for seq in range(seqs)], 0
    )
    part_copies = []
    for index in range(width // 256):
        part[index] = lax.dot_general(
            o_rows,
            wattn[index * 256 : (index + 1) * 256, qkv_cols:],
            (((1,), (1,)), ((), ())),
            preferred_element_type=f32,
        )
        part_copies.append(
            start(remote(part.at[index], part_in.at[index], ps.at[index], pr.at[index], {"tp": other}))
        )
    pump(2)
    for index, copy in enumerate(part_copies):
        copy.wait_recv()
        span = slice(index * 256, (index + 1) * 256)
        h_ref[:, span] = tok_ref[:, span].astype(f32) + (part[index] + part_in[index])

    def norm_mid(index, _):
        piece = pl.ds(index * step_rows, step_rows)
        val = h_ref[piece, :]
        inv = lax.rsqrt(jnp.mean(val * val, axis=-1, keepdims=True) + norm_eps)
        per_seq = local // step_rows
        b_buf[index // per_seq, pl.ds(lax.rem(index, per_seq) * step_rows, step_rows), :] = (
            val * inv * row_ref[1:2, :]
        ).astype(bf16)
        return 0

    lax.fori_loop(0, rows // step_rows, norm_mid, 0)
    b_copies = group_send(1, b_buf, b_all)
    b_local = pltpu.make_async_copy(b_buf, b_all.at[ctx], loc.at[6])
    b_local.start()
    relays = []
    for tile in range(1, ctx_count):
        relays.append(group_relay(0, e_copies, e_all, tile))
    pump(2)
    while pending:
        pump(1)
    for tile in range(1, ctx_count):
        relays.append(group_relay(1, b_copies, b_all, tile))
    for item in (2, 3, 4):
        for tile in tiles:
            settle(item, tile)
    for copy in relays:
        copy.wait_recv()
    for copy in local_copies[2:] + [e_local, b_local]:
        copy.wait()
    for copy in sent:
        copy.wait_send()


def forward_call(tok, cot, attn_own, mlp_own, small_own, cos, sin, qseg, kseg, qkv_cols, q_cols, gain_cut):
    dp_count, ctx_count = lax.axis_size("dp"), lax.axis_size("ctx")
    own = attn_own.shape[0]
    rows, width = tok.shape
    seqs, local = cot.shape[:2]
    full_rows = own * dp_count * ctx_count
    heads = q_cols // 128
    bf16, f32 = jnp.bfloat16, jnp.float32
    vmem, hbm = pl.BlockSpec(memory_space=pltpu.VMEM), pl.BlockSpec(memory_space=pl.ANY)
    shapes = [
        ((full_rows, attn_own.shape[1]), bf16, vmem),
        ((mlp_own.shape[0], full_rows, mlp_own.shape[3]), bf16, hbm),
        ((ctx_count, seqs, local, width), bf16, hbm),
        ((ctx_count, seqs, local, width), bf16, hbm),
        ((rows, width), f32, vmem),
        ((rows, width), bf16, vmem),
        ((seqs, heads, local, 128), bf16, vmem),
        ((seqs, 2, local * ctx_count, 128), bf16, vmem),
        ((seqs, heads, local, 128), bf16, vmem),
        ((seqs, heads, local, 1), f32, vmem),
        ((8, width), f32, vmem),
    ]
    dma = pltpu.SemaphoreType.DMA
    chunks = width // 256
    return pl.pallas_call(
        functools.partial(forward_kernel, (dp_count, ctx_count, own, qkv_cols, q_cols, gain_cut)),
        out_shape=[jax.ShapeDtypeStruct(shape, kind) for shape, kind, _ in shapes],
        in_specs=[vmem, hbm, hbm, hbm, vmem, vmem, vmem, vmem, vmem],
        out_specs=[spec for _, _, spec in shapes],
        scratch_shapes=[
            pltpu.VMEM((dp_count * ctx_count, 8, small_own.shape[1]), f32),
            pltpu.VMEM((chunks, rows, 256), f32),
            pltpu.VMEM((chunks, rows, 256), f32),
            pltpu.VMEM((seqs, local, width), bf16),
        ]
        + [dma((5, ctx_count)) for _ in range(8)]
        + [dma((ctx_count,)), dma((ctx_count,)), dma((chunks,)), dma((chunks,))]
        + [dma((2, 2, ctx_count)), dma((2, 2, ctx_count)), dma((8,))],
        compiler_params=pltpu.CompilerParams(
            collective_id=0, has_side_effects=True, vmem_limit_bytes=60 * 1024 * 1024
        ),
        name="forward_kernel",
    )(tok, cot, attn_own, mlp_own, small_own, cos, sin, qseg, kseg)


def on_device_kernels(
    tokens,
    cotangent,
    segments,
    positions,
    counts,
    attn_gain,
    q_weight,
    q_bias,
    k_weight,
    v_weight,
    kv_bias,
    o_weight,
    mlp_gain,
    gate_weight,
    up_weight,
    down_weight,
):
    dp_count, ctx_count = lax.axis_size("dp"), lax.axis_size("ctx")
    dp_rank, ctx_rank, core = lax.axis_index("dp"), lax.axis_index("ctx"), lax.axis_index("tp")
    seq_count, local_len, width = tokens.shape
    full_len = segments.shape[1]
    row_count = seq_count * local_len
    half_width = width // 2
    own_rows = q_weight.shape[1]
    group_rows = own_rows * ctx_count
    q_cols, k_cols, ff_cols = q_weight.shape[2], k_weight.shape[2], gate_weight.shape[2]
    kv_local = k_cols // HEAD_DIM
    group_size = q_cols // k_cols
    qkv_cols = q_cols + 2 * k_cols
    lane = 128
    ff_block = -(-ff_cols // (lane * ctx_count)) * lane
    ff_pad = ff_block * ctx_count - ff_cols
    f32, bf16 = jnp.float32, jnp.bfloat16

    parts = (attn_gain[0], mlp_gain[0], q_bias[0].reshape(-1), kv_bias[0].reshape(-1))
    cuts = [0]
    for part_vec in parts:
        cuts.append(cuts[-1] + part_vec.shape[0])
    small_own = jnp.pad(jnp.concatenate(parts).astype(f32)[None], ((0, 7), (0, 0)))
    attn_own = jnp.concatenate([q_weight[0], k_weight[0], v_weight[0], o_weight[0]], 1)
    mlp_own = jnp.stack(
        [
            jnp.pad(weight[0], ((0, 0), (0, ff_pad))).reshape(own_rows, ctx_count, ff_block).transpose(1, 0, 2)
            for weight in (gate_weight, up_weight, down_weight)
        ]
    )
    live_seq = (jnp.arange(seq_count, dtype=jnp.int32) < counts[0]).astype(f32)
    live_rows = jnp.repeat(live_seq, local_len)[:, None]
    grad_out = cotangent.astype(f32).reshape(-1, width) * live_rows
    query_pos = ctx_rank * local_len + jnp.arange(local_len, dtype=jnp.int32)
    key_pos = jnp.arange(full_len, dtype=jnp.int32)
    query_seg = lax.dynamic_slice_in_dim(segments, ctx_rank * local_len, local_len, 1)
    allowed = (query_seg[:, :, None] == segments[:, None, :]) & (
        key_pos[None, None, :] <= query_pos[None, :, None]
    )
    cos_tab, sin_tab = rope_tables(positions.reshape(-1))
    sign = jnp.where(jnp.arange(HEAD_DIM) < HEAD_DIM // 2, -1.0, 1.0)
    (
        w_attn,
        w_mlp,
        grad_all,
        mid_all,
        resid_mid,
        normed_in,
        query_hm,
        keyval_hm,
        attn_hm,
        log_total,
        small_rows,
    ) = forward_call(
        tokens.reshape(-1, width),
        grad_out.astype(bf16).reshape(seq_count, local_len, width),
        attn_own,
        mlp_own,
        small_own,
        cos_tab,
        sin_tab * sign,
        query_seg[:, :, None],
        segments[:, None, :],
        qkv_cols,
        q_cols,
        cuts,
    )
    cos_tab, sin_tab = cos_tab[:, None, :], sin_tab[:, None, :]
    gain_in, gain_mid = small_rows[0], small_rows[1]
    w_qkv, w_out = w_attn[:, :qkv_cols], w_attn[:, qkv_cols:]
    w_gate, w_up, w_down = w_mlp[0], w_mlp[1], w_mlp[2]
    grad_all, mid_all = grad_all.reshape(-1, width), mid_all.reshape(-1, width)
    residual = tokens.astype(f32).reshape(-1, width)
    inv_in = lax.rsqrt(jnp.mean(residual * residual, axis=-1, keepdims=True) + norm_eps)
    inv_mid = lax.rsqrt(jnp.mean(resid_mid * resid_mid, axis=-1, keepdims=True) + norm_eps)
    query_bf = query_hm.transpose(0, 2, 1, 3)[:, :, None]
    keys_all, values_all = keyval_hm[:, 0], keyval_hm[:, 1]
    attn_bf = attn_hm.transpose(0, 2, 1, 3)[:, :, None]
    attn_flat = attn_bf.reshape(row_count, -1)
    log_total = log_total[:, None]
    gate_pre = mat_mul(mid_all, w_gate)
    up_pre = mat_mul(mid_all, w_up)
    hidden_bf = (jax.nn.silu(gate_pre) * up_pre).astype(bf16)
    grad_hidden = mat_mul(grad_all, w_down)
    sigmoid_gate = jax.nn.sigmoid(gate_pre)
    grad_gate = (
        grad_hidden * up_pre * sigmoid_gate * (1.0 + gate_pre * (1.0 - sigmoid_gate))
    ).astype(bf16)
    grad_up = (grad_hidden * gate_pre * sigmoid_gate).astype(bf16)

    def collect(part):
        part_bf = columns_at(part, 1 - core, half_width).astype(bf16)
        mine = columns_at(part, core, half_width) + partner(part_bf).astype(f32)
        total = scatter_direct(lambda step: rows_at(mine, ctx_rank ^ step, row_count), "ctx")
        return join_halves(total, partner(total), core, 1)

    grad_normed_mid = collect(mat_mul_t(grad_gate, w_gate) + mat_mul_t(grad_up, w_up))

    def owner_weight(left, right):
        blocks = [
            rows_mul(columns_at(left, dp_rank ^ step, group_rows), right)
            for step in range(dp_count)
        ]
        group = scatter_halves(blocks, "dp").astype(bf16)
        pieces = [rows_at(group, ctx_rank, own_rows)]
        for step in range(1, ctx_count):
            pieces.append(xor_permute(rows_at(group, ctx_rank ^ step, own_rows), "ctx", step))
        return place(pieces, ctx_rank, 1)[:, :ff_cols].astype(f32)

    grad_w_down = owner_weight(grad_all, hidden_bf)
    grad_w_gate = owner_weight(mid_all, grad_gate)
    grad_w_up = owner_weight(mid_all, grad_up)

    layer_out = resid_mid + collect(mat_mul_t(hidden_bf, w_down))
    activations = (layer_out * live_rows).reshape(tokens.shape)

    grad_mid_norm, grad_gain_mid = norm_backward(resid_mid, inv_mid, gain_mid, grad_normed_mid)
    grad_mid = grad_out + grad_mid_norm
    grad_mid_bf = grad_mid.astype(bf16)
    grad_attn = mat_mul(grad_mid_bf, w_out).astype(bf16)

    def owner_attn(left, right):
        blocks = [
            rows_mul(columns_at(left, dp_rank ^ step, group_rows), right)
            for step in range(dp_count)
        ]
        group = scatter_halves(blocks, "dp")
        return scatter_direct(lambda step: rows_at(group, ctx_rank ^ step, own_rows), "ctx")

    grad_w_out = owner_attn(grad_mid_bf, attn_flat)
    grad_query, grad_key_all, grad_value_all = attend_backward(
        query_bf, keys_all, values_all, attn_bf, log_total, grad_attn.reshape(attn_bf.shape), allowed
    )
    grad_keyval_all = jnp.concatenate([grad_key_all, grad_value_all], 2)
    grad_keyval = scatter_direct(
        lambda step: lax.dynamic_slice_in_dim(
            grad_keyval_all, (ctx_rank ^ step) * local_len, local_len, 1
        ),
        "ctx",
    ).reshape(row_count, -1)
    grad_query = unrotate(
        grad_query.reshape(row_count, -1, HEAD_DIM), cos_tab, sin_tab
    ).reshape(row_count, -1)
    grad_key = unrotate(
        grad_keyval[:, :k_cols].reshape(row_count, -1, HEAD_DIM), cos_tab, sin_tab
    ).reshape(row_count, -1)
    grad_qkv = jnp.concatenate([grad_query, grad_key, grad_keyval[:, k_cols:]], 1)
    grad_qkv_bf = grad_qkv.astype(bf16)
    grad_w_qkv = owner_attn(normed_in, grad_qkv_bf)
    dot_part = mat_mul_t(grad_qkv_bf, w_qkv)
    grad_normed_in = dot_part + partner(dot_part)
    grad_in_norm, grad_gain_in = norm_backward(residual, inv_in, gain_in, grad_normed_in)
    input_grad = (grad_mid + grad_in_norm).reshape(tokens.shape)

    bias_sum = jnp.sum(grad_qkv, axis=0)
    device_count = dp_count * ctx_count
    grad_small = jnp.concatenate(
        [
            grad_gain_in.reshape(device_count, -1),
            grad_gain_mid.reshape(device_count, -1),
            bias_sum[:q_cols].reshape(kv_local, -1).T.reshape(device_count, -1),
            jnp.concatenate(
                [
                    bias_sum[q_cols : q_cols + k_cols].reshape(kv_local, -1).T,
                    bias_sum[q_cols + k_cols :].reshape(kv_local, -1).T,
                ],
                0,
            ).reshape(device_count, -1),
        ],
        1,
    )
    small_group = scatter_small(
        [rows_at(grad_small, dp_rank ^ step, ctx_count) for step in range(dp_count)], "dp"
    )
    small_own = scatter_small(
        [rows_at(small_group, ctx_rank ^ step, 1) for step in range(ctx_count)], "ctx"
    )
    own = [small_own[:, low:high] for low, high in zip(cuts[:-1], cuts[1:])]
    return (
        activations,
        input_grad,
        own[0],
        grad_w_qkv[None, :, :q_cols],
        own[2].reshape(q_bias.shape),
        grad_w_qkv[None, :, q_cols : q_cols + k_cols],
        grad_w_qkv[None, :, q_cols + k_cols :],
        own[3].reshape(kv_bias.shape),
        grad_w_out[None],
        own[1],
        grad_w_gate[None],
        grad_w_up[None],
        grad_w_down[None],
    )


def solution(mesh):
    in_specs = (
        P("dp", "ctx", None),
        P("dp", "ctx", None),
        P("dp", None),
        P("dp", "ctx"),
        P("dp"),
        P(None, ("dp", "ctx")),
        P(None, ("dp", "ctx"), "tp"),
        P(None, ("dp", "ctx"), "tp"),
        P(None, ("dp", "ctx"), "tp"),
        P(None, ("dp", "ctx"), "tp"),
        P(None, ("dp", "ctx"), "tp"),
        P(None, ("dp", "ctx"), "tp"),
        P(None, ("dp", "ctx")),
        P(None, ("dp", "ctx"), "tp"),
        P(None, ("dp", "ctx"), "tp"),
        P(None, ("dp", "ctx"), "tp"),
    )
    out_specs = (
        P("dp", "ctx", None),
        P("dp", "ctx", None),
        P(None, ("dp", "ctx")),
        P(None, ("dp", "ctx"), "tp"),
        P(None, ("dp", "ctx"), "tp"),
        P(None, ("dp", "ctx"), "tp"),
        P(None, ("dp", "ctx"), "tp"),
        P(None, ("dp", "ctx"), "tp"),
        P(None, ("dp", "ctx"), "tp"),
        P(None, ("dp", "ctx")),
        P(None, ("dp", "ctx"), "tp"),
        P(None, ("dp", "ctx"), "tp"),
        P(None, ("dp", "ctx"), "tp"),
    )
    kernels_fit = mesh.shape["dp"] == 4 and mesh.shape["ctx"] == 4 and mesh.shape["tp"] == KV_HEADS
    return jax.shard_map(
        on_device_kernels if kernels_fit else on_device, mesh=mesh, in_specs=in_specs, out_specs=out_specs, check_vma=False
    )
```

```python
import functools

import jax
import jax.numpy as jnp
from jax import lax
from jax.experimental import pallas as pl
from jax.experimental.pallas import tpu as pltpu
from jax.sharding import PartitionSpec as P

HEADS = 12
KV_HEADS = 2
HEAD_DIM = 128
LAYERS = 1


theta_base = 1000000.0
norm_eps = 1e-06
masked_score = -1e30


def mat_mul(left, right):
    return jnp.dot(left, right, preferred_element_type=jnp.float32)


def mat_mul_t(left, right):
    return lax.dot_general(
        left, right, (((1,), (1,)), ((), ())), preferred_element_type=jnp.float32
    )


def rows_mul(left, right):
    return lax.dot_general(
        left, right, (((0,), (0,)), ((), ())), preferred_element_type=jnp.float32
    )


def rope_tables(pos_vals):
    half_dim = HEAD_DIM // 2
    frequency = theta_base ** (-(jnp.arange(half_dim, dtype=jnp.float32) * (2.0 / HEAD_DIM)))
    angles = pos_vals.astype(jnp.float32)[..., None] * frequency
    cos_half = jnp.cos(angles)
    sin_half = jnp.sin(angles)
    return (jnp.concatenate([cos_half, cos_half], -1), jnp.concatenate([sin_half, sin_half], -1))


def rotate(values, cos_tab, sin_tab):
    half_dim = values.shape[-1] // 2
    turned = jnp.concatenate([-values[..., half_dim:], values[..., :half_dim]], -1)
    return values * cos_tab + turned * sin_tab


def unrotate(grad_vals, cos_tab, sin_tab):
    half_dim = grad_vals.shape[-1] // 2
    scaled = grad_vals * sin_tab
    turned = jnp.concatenate([scaled[..., half_dim:], -scaled[..., :half_dim]], -1)
    return grad_vals * cos_tab + turned


def norm_forward(residual, gain_vec):
    inv_rms = lax.rsqrt(jnp.mean(residual * residual, axis=-1, keepdims=True) + norm_eps)
    normed = (residual * inv_rms * gain_vec.astype(jnp.float32)).astype(jnp.bfloat16)
    return (inv_rms, normed)


def norm_backward(residual, inv_rms, gain_vec, grad_normed):
    weighted = grad_normed * gain_vec.astype(jnp.float32)
    inner_mean = jnp.mean(weighted * residual, axis=-1, keepdims=True)
    grad_resid = inv_rms * weighted - residual * (inv_rms * inv_rms * inv_rms) * inner_mean
    grad_gain = jnp.sum(grad_normed * residual * inv_rms, axis=0)
    return (grad_resid, grad_gain)


def split_heads(keys_all, values_all):
    seq_count, full_len, kv_width = keys_all.shape
    kv_local = kv_width // HEAD_DIM
    return (
        keys_all.reshape(seq_count, full_len, kv_local, HEAD_DIM),
        values_all.reshape(seq_count, full_len, kv_local, HEAD_DIM),
    )


def attend_forward(query_bf, keys_all, values_all, allowed):
    key_heads, value_heads = split_heads(keys_all, values_all)
    scores = jnp.einsum(
        "bqkgd,bskd->bkgqs", query_bf, key_heads, preferred_element_type=jnp.float32
    ) * HEAD_DIM ** (-0.5)
    scores = jnp.where(allowed[:, None, None], scores, masked_score)
    top_score = jnp.max(scores, axis=-1, keepdims=True)
    shifted_exp = jnp.exp(scores - top_score)
    totals = jnp.sum(shifted_exp, axis=-1, keepdims=True)
    prob_bf = (shifted_exp / totals).astype(jnp.bfloat16)
    output = jnp.einsum(
        "bkgqs,bskd->bqkgd", prob_bf, value_heads, preferred_element_type=jnp.float32
    )
    return (output.astype(jnp.bfloat16), top_score + jnp.log(totals))


def attend_backward(query_bf, keys_all, values_all, attn_bf, log_total, grad_attn, allowed):
    key_heads, value_heads = split_heads(keys_all, values_all)
    scores = jnp.einsum(
        "bqkgd,bskd->bkgqs", query_bf, key_heads, preferred_element_type=jnp.float32
    ) * HEAD_DIM ** (-0.5)
    prob_full = jnp.exp(jnp.where(allowed[:, None, None], scores, masked_score) - log_total)
    prob_bf = prob_full.astype(jnp.bfloat16)
    grad_value = jnp.einsum(
        "bkgqs,bqkgd->bskd", prob_bf, grad_attn, preferred_element_type=jnp.float32
    )
    grad_prob = jnp.einsum(
        "bqkgd,bskd->bkgqs", grad_attn, value_heads, preferred_element_type=jnp.float32
    )
    row_dot = jnp.sum(grad_attn.astype(jnp.float32) * attn_bf.astype(jnp.float32), axis=-1)
    row_dot = jnp.transpose(row_dot, (0, 2, 3, 1))[..., None]
    grad_score = (prob_full * (grad_prob - row_dot) * HEAD_DIM ** (-0.5)).astype(jnp.bfloat16)
    grad_query = jnp.einsum(
        "bkgqs,bskd->bqkgd", grad_score, key_heads, preferred_element_type=jnp.float32
    )
    grad_key = jnp.einsum(
        "bkgqs,bqkgd->bskd", grad_score, query_bf, preferred_element_type=jnp.float32
    )
    return (grad_query, grad_key.reshape(keys_all.shape), grad_value.reshape(values_all.shape))


def xor_permute(value, axis_name, step):
    count = lax.axis_size(axis_name)
    return lax.ppermute(value, axis_name, [(rank, rank ^ step) for rank in range(count)])


def axis_bits(axis_name):
    return [1 << shift for shift in range(lax.axis_size(axis_name).bit_length() - 1)]


def partner(value):
    return xor_permute(value, "tp", 1)


def place(pieces, rank, dim):
    width = pieces[0].shape[dim]
    whole_shape = list(pieces[0].shape)
    whole_shape[dim] = width * len(pieces)
    whole = jnp.zeros(whole_shape, pieces[0].dtype)
    for offset, piece in enumerate(pieces):
        whole = lax.dynamic_update_slice_in_dim(whole, piece, (rank ^ offset) * width, dim)
    return whole


def join_halves(mine, other, core, dim):
    return jnp.where(
        core == 0, jnp.concatenate([mine, other], dim), jnp.concatenate([other, mine], dim)
    )


def gather_direct(value, axis_name):
    count = lax.axis_size(axis_name)
    return [value] + [xor_permute(value, axis_name, step) for step in range(1, count)]


def gather_halves(value, axis_name):
    rows = value.shape[0]
    half = rows // 2
    bits = axis_bits(axis_name)
    parts = []
    for piece, order in ((value[:half], bits), (value[half:], bits[::-1])):
        held = {0: piece}
        for bit in order:
            for key in list(held):
                held[key | bit] = xor_permute(held[key], axis_name, bit)
        parts.append(held)
    return [(parts[0][key], parts[1][key]) for key in range(len(parts[0]))]


def scatter_halves(blocks, axis_name):
    half = blocks[0].shape[0] // 2
    bits = axis_bits(axis_name)
    done = []
    for low, high, order in ((0, half, bits[::-1]), (half, 2 * half, bits)):
        held = {key: block[low:high] for key, block in enumerate(blocks)}
        for bit in order:
            for key in [key for key in held if key & bit]:
                sent = held.pop(key).astype(jnp.bfloat16)
                held[key ^ bit] = held[key ^ bit] + xor_permute(sent, axis_name, bit).astype(jnp.float32)
        done.append(held[0])
    return jnp.concatenate(done, 0)


def scatter_small(blocks, axis_name):
    held = dict(enumerate(blocks))
    for bit in axis_bits(axis_name)[::-1]:
        for key in [key for key in held if key & bit]:
            held[key ^ bit] = held[key ^ bit] + xor_permute(held.pop(key), axis_name, bit)
    return held[0]


def scatter_direct(block_of, axis_name):
    total = block_of(0)
    for step in range(1, lax.axis_size(axis_name)):
        got = xor_permute(block_of(step).astype(jnp.bfloat16), axis_name, step)
        total = total + got.astype(jnp.float32)
    return total


def rows_at(value, index, size):
    return lax.dynamic_slice_in_dim(value, index * size, size, 0)


def columns_at(value, index, size):
    return lax.dynamic_slice_in_dim(value, index * size, size, 1)


def on_device(
    tokens,
    cotangent,
    segments,
    positions,
    counts,
    attn_gain,
    q_weight,
    q_bias,
    k_weight,
    v_weight,
    kv_bias,
    o_weight,
    mlp_gain,
    gate_weight,
    up_weight,
    down_weight,
):
    dp_count, ctx_count = lax.axis_size("dp"), lax.axis_size("ctx")
    dp_rank, ctx_rank, core = lax.axis_index("dp"), lax.axis_index("ctx"), lax.axis_index("tp")
    seq_count, local_len, width = tokens.shape
    full_len = segments.shape[1]
    row_count = seq_count * local_len
    half_width = width // 2
    own_rows = q_weight.shape[1]
    group_rows = own_rows * ctx_count
    q_cols, k_cols, ff_cols = q_weight.shape[2], k_weight.shape[2], gate_weight.shape[2]
    kv_local = k_cols // HEAD_DIM
    group_size = q_cols // k_cols
    qkv_cols = q_cols + 2 * k_cols
    lane = 128
    ff_block = -(-ff_cols // (lane * ctx_count)) * lane
    ff_pad = ff_block * ctx_count - ff_cols
    f32, bf16 = jnp.float32, jnp.bfloat16

    small = jnp.concatenate(
        [attn_gain[0], mlp_gain[0], q_bias[0].reshape(-1), kv_bias[0].reshape(-1)]
    )[None]
    sizes = (attn_gain.shape[1], mlp_gain.shape[1], q_bias.shape[1] * q_bias.shape[2], kv_bias.shape[1] * kv_bias.shape[2])
    small_ctx = place(gather_direct(small, "ctx"), ctx_rank, 0)[None]
    held = {0: small_ctx}
    for bit in axis_bits("dp"):
        for key in list(held):
            held[key | bit] = xor_permute(held[key], "dp", bit)
    small_all = place([held[key] for key in range(dp_count)], dp_rank, 0)
    small_all = small_all.reshape(dp_count * ctx_count, -1)
    cuts = [0]
    for size in sizes:
        cuts.append(cuts[-1] + size)
    gain_in, gain_mid, b_query, b_keyval = (
        small_all[:, low:high].reshape(-1) for low, high in zip(cuts[:-1], cuts[1:])
    )
    b_query = b_query.reshape(-1, kv_local).T.reshape(-1).astype(f32)
    b_keyval = b_keyval.reshape(-1, kv_local).astype(f32)
    b_qkv = jnp.concatenate(
        [b_query, b_keyval[:HEAD_DIM].T.reshape(-1), b_keyval[HEAD_DIM:].T.reshape(-1)]
    )

    attn_own = jnp.concatenate([q_weight[0], k_weight[0], v_weight[0], o_weight[0]], 1)
    attn_group = place(gather_direct(attn_own, "ctx"), ctx_rank, 0)
    attn_pairs = gather_halves(attn_group, "dp")
    w_attn = place([jnp.concatenate(pair, 0) for pair in attn_pairs], dp_rank, 0)
    w_qkv, w_out = w_attn[:, :qkv_cols], w_attn[:, qkv_cols:]

    live_seq = (jnp.arange(seq_count, dtype=jnp.int32) < counts[0]).astype(f32)
    live_rows = jnp.repeat(live_seq, local_len)[:, None]
    grad_out = cotangent.astype(f32).reshape(-1, width) * live_rows

    def spread(rows_bf):
        mine = jnp.concatenate(gather_direct(columns_at(rows_bf, core, half_width), "ctx"), 0)
        return join_halves(mine, partner(mine), core, 1)

    grad_all = spread(grad_out.astype(bf16))

    def spread_weight(weight):
        padded = jnp.pad(weight[0], ((0, 0), (0, ff_pad)))
        pieces = [columns_at(padded, ctx_rank, ff_block)]
        for step in range(1, ctx_count):
            pieces.append(xor_permute(columns_at(padded, ctx_rank ^ step, ff_block), "ctx", step))
        pairs = gather_halves(place(pieces, ctx_rank, 0), "dp")
        return place([jnp.concatenate(pair, 0) for pair in pairs], dp_rank, 0)

    w_gate = spread_weight(gate_weight)
    w_up = spread_weight(up_weight)
    w_down = spread_weight(down_weight)

    query_pos = ctx_rank * local_len + jnp.arange(local_len, dtype=jnp.int32)
    key_pos = jnp.arange(full_len, dtype=jnp.int32)
    query_seg = lax.dynamic_slice_in_dim(segments, ctx_rank * local_len, local_len, 1)
    allowed = (query_seg[:, :, None] == segments[:, None, :]) & (
        key_pos[None, None, :] <= query_pos[None, :, None]
    )
    cos_tab, sin_tab = rope_tables(positions.reshape(-1))
    cos_tab, sin_tab = cos_tab[:, None, :], sin_tab[:, None, :]
    residual = tokens.astype(f32).reshape(-1, width)
    inv_in, normed_in = norm_forward(residual, gain_in)
    qkv_val = mat_mul(normed_in, w_qkv) + b_qkv
    query_bf = rotate(
        qkv_val[:, :q_cols].reshape(row_count, -1, HEAD_DIM), cos_tab, sin_tab
    ).astype(bf16).reshape(seq_count, -1, kv_local, group_size, HEAD_DIM)
    key_bf = rotate(
        qkv_val[:, q_cols : q_cols + k_cols].reshape(row_count, -1, HEAD_DIM), cos_tab, sin_tab
    ).astype(bf16).reshape(row_count, -1)
    value_bf = qkv_val[:, q_cols + k_cols :].astype(bf16)
    keyval = jnp.concatenate([key_bf, value_bf], 1).reshape(seq_count, local_len, -1)
    keyval_all = place(gather_direct(keyval, "ctx"), ctx_rank, 1)
    keys_all, values_all = keyval_all[..., :k_cols], keyval_all[..., k_cols:]
    attn_bf, log_total = attend_forward(query_bf, keys_all, values_all, allowed)
    attn_flat = attn_bf.reshape(row_count, -1)
    out_part = mat_mul_t(attn_flat, w_out)
    resid_mid = residual + (out_part + partner(out_part))
    inv_mid, normed_mid = norm_forward(resid_mid, gain_mid)

    mid_all = spread(normed_mid)
    gate_pre = mat_mul(mid_all, w_gate)
    up_pre = mat_mul(mid_all, w_up)
    hidden_bf = (jax.nn.silu(gate_pre) * up_pre).astype(bf16)
    grad_hidden = mat_mul(grad_all, w_down)
    sigmoid_gate = jax.nn.sigmoid(gate_pre)
    grad_gate = (
        grad_hidden * up_pre * sigmoid_gate * (1.0 + gate_pre * (1.0 - sigmoid_gate))
    ).astype(bf16)
    grad_up = (grad_hidden * gate_pre * sigmoid_gate).astype(bf16)

    def collect(part):
        part_bf = columns_at(part, 1 - core, half_width).astype(bf16)
        mine = columns_at(part, core, half_width) + partner(part_bf).astype(f32)
        total = scatter_direct(lambda step: mine[step * row_count : (step + 1) * row_count], "ctx")
        return join_halves(total, partner(total), core, 1)

    grad_normed_mid = collect(mat_mul_t(grad_gate, w_gate) + mat_mul_t(grad_up, w_up))

    def owner_weight(left, right):
        blocks = [
            rows_mul(columns_at(left, dp_rank ^ step, group_rows), right)
            for step in range(dp_count)
        ]
        group = scatter_halves(blocks, "dp").astype(bf16)
        pieces = [rows_at(group, ctx_rank, own_rows)]
        for step in range(1, ctx_count):
            pieces.append(xor_permute(rows_at(group, ctx_rank ^ step, own_rows), "ctx", step))
        return place(pieces, ctx_rank, 1)[:, :ff_cols].astype(f32)

    grad_w_down = owner_weight(grad_all, hidden_bf)
    grad_w_gate = owner_weight(mid_all, grad_gate)
    grad_w_up = owner_weight(mid_all, grad_up)

    layer_out = resid_mid + collect(mat_mul_t(hidden_bf, w_down))
    activations = (layer_out * live_rows).reshape(tokens.shape)

    grad_mid_norm, grad_gain_mid = norm_backward(resid_mid, inv_mid, gain_mid, grad_normed_mid)
    grad_mid = grad_out + grad_mid_norm
    grad_mid_bf = grad_mid.astype(bf16)
    grad_attn = mat_mul(grad_mid_bf, w_out).astype(bf16)

    def owner_attn(left, right):
        blocks = [
            rows_mul(columns_at(left, dp_rank ^ step, group_rows), right)
            for step in range(dp_count)
        ]
        group = scatter_halves(blocks, "dp")
        return scatter_direct(lambda step: rows_at(group, ctx_rank ^ step, own_rows), "ctx")

    grad_w_out = owner_attn(grad_mid_bf, attn_flat)
    grad_query, grad_key_all, grad_value_all = attend_backward(
        query_bf, keys_all, values_all, attn_bf, log_total, grad_attn.reshape(attn_bf.shape), allowed
    )
    grad_keyval_all = jnp.concatenate([grad_key_all, grad_value_all], 2)
    grad_keyval = scatter_direct(
        lambda step: lax.dynamic_slice_in_dim(
            grad_keyval_all, (ctx_rank ^ step) * local_len, local_len, 1
        ),
        "ctx",
    ).reshape(row_count, -1)
    grad_query = unrotate(
        grad_query.reshape(row_count, -1, HEAD_DIM), cos_tab, sin_tab
    ).reshape(row_count, -1)
    grad_key = unrotate(
        grad_keyval[:, :k_cols].reshape(row_count, -1, HEAD_DIM), cos_tab, sin_tab
    ).reshape(row_count, -1)
    grad_qkv = jnp.concatenate([grad_query, grad_key, grad_keyval[:, k_cols:]], 1)
    grad_qkv_bf = grad_qkv.astype(bf16)
    grad_w_qkv = owner_attn(normed_in, grad_qkv_bf)
    dot_part = mat_mul_t(grad_qkv_bf, w_qkv)
    grad_normed_in = dot_part + partner(dot_part)
    grad_in_norm, grad_gain_in = norm_backward(residual, inv_in, gain_in, grad_normed_in)
    input_grad = (grad_mid + grad_in_norm).reshape(tokens.shape)

    bias_sum = jnp.sum(grad_qkv, axis=0)
    device_count = dp_count * ctx_count
    grad_small = jnp.concatenate(
        [
            grad_gain_in.reshape(device_count, -1),
            grad_gain_mid.reshape(device_count, -1),
            bias_sum[:q_cols].reshape(kv_local, -1).T.reshape(device_count, -1),
            jnp.concatenate(
                [
                    bias_sum[q_cols : q_cols + k_cols].reshape(kv_local, -1).T,
                    bias_sum[q_cols + k_cols :].reshape(kv_local, -1).T,
                ],
                0,
            ).reshape(device_count, -1),
        ],
        1,
    )
    small_group = scatter_small(
        [rows_at(grad_small, dp_rank ^ step, ctx_count) for step in range(dp_count)], "dp"
    )
    small_own = scatter_small(
        [rows_at(small_group, ctx_rank ^ step, 1) for step in range(ctx_count)], "ctx"
    )
    own = [small_own[:, low:high] for low, high in zip(cuts[:-1], cuts[1:])]
    return (
        activations,
        input_grad,
        own[0],
        grad_w_qkv[None, :, :q_cols],
        own[2].reshape(q_bias.shape),
        grad_w_qkv[None, :, q_cols : q_cols + k_cols],
        grad_w_qkv[None, :, q_cols + k_cols :],
        own[3].reshape(kv_bias.shape),
        grad_w_out[None],
        own[1],
        grad_w_gate[None],
        grad_w_up[None],
        grad_w_down[None],
    )


MESH = pl.DeviceIdType.MESH


def remote(src, dst, send_sem, recv_sem, target):
    return pltpu.make_async_remote_copy(
        src_ref=src, dst_ref=dst, send_sem=send_sem, recv_sem=recv_sem, device_id=target, device_id_type=MESH
    )


def greet(partners):
    barrier = pltpu.get_barrier_semaphore()
    for partner_id in partners:
        pl.semaphore_signal(barrier, inc=1, device_id=partner_id, device_id_type=MESH)
    pl.semaphore_wait(barrier, len(partners))


def spread_row(values, row_cols, period, total):
    left = lax.broadcasted_iota(jnp.int32, (period, total), 0)
    right = lax.broadcasted_iota(jnp.int32, (period, total), 1)
    pick = (lax.rem(right, period) == left).astype(jnp.float32).astype(jnp.bfloat16)
    spread = jnp.dot(values.astype(jnp.bfloat16), pick, preferred_element_type=jnp.float32)
    block = lax.broadcasted_iota(jnp.int32, spread.shape, 0) // 8
    owner = lax.broadcasted_iota(jnp.int32, spread.shape, 1) // period
    return jnp.sum(jnp.where(block == owner, spread, 0.0), axis=0, keepdims=True)


def forward_kernel(
    sizes,
    tok_ref,
    cot_ref,
    attn_own,
    mlp_own,
    small_own,
    cos_ref,
    sin_ref,
    qseg_ref,
    kseg_ref,
    wattn,
    wmlp,
    e_all,
    b_all,
    h_ref,
    a_ref,
    q_ref,
    kv_ref,
    o_ref,
    lse_ref,
    row_ref,
    small,
    part,
    part_in,
    b_buf,
    zs,
    zr,
    xs,
    xr,
    ys,
    yr,
    fs,
    fr,
    ks,
    kr,
    ps,
    pr,
    bs,
    br,
    loc,
):
    dp_count, ctx_count, own, qkv_cols, q_cols, gain_cut = sizes
    dp, ctx, core = lax.axis_index("dp"), lax.axis_index("ctx"), lax.axis_index("tp")
    bf16, f32 = jnp.bfloat16, jnp.float32
    width = tok_ref.shape[1]
    rows = tok_ref.shape[0]
    seqs = cot_ref.shape[0]
    local = cot_ref.shape[1]
    tiles = range(ctx_count)

    def at_x(d):
        return d + 1 - 2 * lax.rem(d, 2)

    def at_y(d):
        return lax.rem(d + 2, 4)

    dpx, dpy = at_x(dp), at_y(dp)
    dpd = at_x(dpy)
    peers = [ctx]
    for step in range(1, ctx_count):
        value = jnp.int32(0)
        for bit in (1, 2, 4, 8):
            if bit < ctx_count:
                digit = lax.rem(ctx // bit, 2)
                value = value + bit * (digit + (1 - 2 * digit) * ((step // bit) % 2))
        peers.append(value)
    other = 1 - core

    greet(
        [{"dp": dpx}, {"dp": dpy}, {"tp": other}] + [{"ctx": peers[step]} for step in range(1, ctx_count)]
    )
    sent = []

    def start(copy):
        copy.start()
        sent.append(copy)
        return copy

    def block_rows(d, c):
        return pl.ds(pl.multiple_of((d * ctx_count + c) * own, own), own)

    def slot(item, d, c):
        if item == 0:
            return small.at[d * ctx_count + c]
        if item == 1:
            return wattn.at[block_rows(d, c), :]
        return wmlp.at[item - 2, block_rows(d, c), :]

    def source(item, tile):
        if item == 0:
            return small_own
        if item == 1:
            return attn_own
        return mlp_own.at[item - 2, peers[tile]]

    items = range(5)
    local_copies = []
    for item in items:
        copy = pltpu.make_async_copy(source(item, 0), slot(item, dp, ctx), loc.at[item])
        copy.start()
        local_copies.append(copy)
    z_copy = {}

    def z_send(item):
        for tile in range(1, ctx_count):
            z_copy[item, tile] = start(
                remote(source(item, tile), slot(item, dp, ctx), zs.at[item, tile], zr.at[item, tile], {"ctx": peers[tile]})
            )

    x_copy, y_copy, f_copy = {}, {}, {}

    def xy_send(item, tile):
        src = source(item, 0) if tile == 0 else slot(item, dp, peers[tile])
        if tile:
            z_copy[item, tile].wait_recv()
        dst = slot(item, dp, peers[tile])
        x_copy[item, tile] = start(remote(src, dst, xs.at[item, tile], xr.at[item, tile], {"dp": dpx}))
        y_copy[item, tile] = start(remote(src, dst, ys.at[item, tile], yr.at[item, tile], {"dp": dpy}))

    def forward(item, tile):
        if (item + tile) % 2 == 0:
            x_copy[item, tile].wait_recv()
            place_at = slot(item, dpx, peers[tile])
            target = {"dp": dpy}
        else:
            y_copy[item, tile].wait_recv()
            place_at = slot(item, dpy, peers[tile])
            target = {"dp": dpx}
        f_copy[item, tile] = start(remote(place_at, place_at, fs.at[item, tile], fr.at[item, tile], target))

    def settle(item, tile):
        if (item + tile) % 2 == 0:
            y_copy[item, tile].wait_recv()
        else:
            x_copy[item, tile].wait_recv()
        f_copy[item, tile].wait_recv()

    def group_send(index, src, dst):
        return [
            start(
                remote(
                    src.at[core],
                    dst.at[ctx, core],
                    bs.at[index, 0, tile],
                    br.at[index, 0, tile],
                    {"ctx": peers[tile]},
                )
            )
            for tile in range(1, ctx_count)
        ]

    def group_relay(index, copies, dst, tile):
        copies[tile - 1].wait_recv()
        piece = dst.at[peers[tile], core]
        return start(remote(piece, piece, bs.at[index, 1, tile], br.at[index, 1, tile], {"tp": other}))

    z_send(0)
    z_send(1)
    xy_send(0, 0)
    xy_send(1, 0)
    for item in (2, 3, 4):
        z_send(item)
    e_local = pltpu.make_async_copy(cot_ref, e_all.at[ctx], loc.at[5])
    e_local.start()
    e_copies = group_send(0, cot_ref, e_all)
    for tile in range(1, ctx_count):
        xy_send(0, tile)
        xy_send(1, tile)
    for tile in tiles:
        forward(0, tile)
        forward(1, tile)
    for item in (2, 3, 4):
        xy_send(item, 0)
    for tile in tiles:
        settle(0, tile)
    local_copies[0].wait()

    flat = small[...].reshape(dp_count * ctx_count * 8, small.shape[2])
    row_ref[0:1, :] = spread_row(flat[:, gain_cut[0] : gain_cut[1]], None, gain_cut[1] - gain_cut[0], width)
    row_ref[1:2, :] = spread_row(flat[:, gain_cut[1] : gain_cut[2]], None, gain_cut[2] - gain_cut[1], width)
    row_ref[2:3, :q_cols] = spread_row(flat[:, gain_cut[2] : gain_cut[3]], None, gain_cut[3] - gain_cut[2], q_cols)
    row_ref[2:3, q_cols:qkv_cols] = spread_row(
        flat[:, gain_cut[3] : gain_cut[4]], None, gain_cut[4] - gain_cut[3], qkv_cols - q_cols
    )

    step_rows = 32

    def norm_in(index, _):
        piece = pl.ds(index * step_rows, step_rows)
        val = tok_ref[piece, :].astype(f32)
        inv = lax.rsqrt(jnp.mean(val * val, axis=-1, keepdims=True) + norm_eps)
        a_ref[piece, :] = (val * inv * row_ref[0:1, :]).astype(bf16)
        return 0

    lax.fori_loop(0, rows // step_rows, norm_in, 0)
    xy_send(2, 1)
    for tile in tiles:
        settle(1, tile)
    local_copies[1].wait()

    pending = []
    for item in (2, 3, 4):
        pending.append((forward, item, 0))
    pending.append((xy_send, 3, 1))
    pending.append((xy_send, 4, 1))
    for item in (2, 3, 4):
        pending.append((xy_send, item, 2))
        pending.append((forward, item, 1))
    for item in (2, 3, 4):
        pending.append((xy_send, item, 3))
        pending.append((forward, item, 2))
    for item in (2, 3, 4):
        pending.append((forward, item, 3))

    def pump(count):
        for _ in range(min(count, len(pending))):
            action, item, tile = pending.pop(0)
            action(item, tile)

    own_keys = pl.ds(pl.multiple_of(ctx * local, local), local)
    order = [qkv_cols - 256] + list(range(0, q_cols, 256))
    kv_copies = []
    for low in order:
        val = jnp.dot(a_ref[...], wattn[:, low : low + 256], preferred_element_type=f32) + row_ref[2:3, low : low + 256]
        for head_low in (0, 128):
            head = val[:, head_low : head_low + 128]
            if low + head_low < qkv_cols - 128:
                head = head * cos_ref[...] + pltpu.roll(head, 64, 1) * sin_ref[...]
            head = head.astype(bf16)
            for seq in range(seqs):
                piece = head[seq * local : (seq + 1) * local]
                if low == qkv_cols - 256:
                    kv_ref[seq, head_low // 128, own_keys, :] = piece
                else:
                    q_ref[seq, (low + head_low) // 128] = piece
        if low == qkv_cols - 256:
            for tile in range(1, ctx_count):
                piece = kv_ref.at[:, :, own_keys, :]
                kv_copies.append(start(remote(piece, piece, ks.at[tile], kr.at[tile], {"ctx": peers[tile]})))
        pump(1)
    pump(1)
    for copy in kv_copies:
        copy.wait_recv()

    keys = kv_ref.shape[2]
    key_no = lax.broadcasted_iota(jnp.int32, (local, keys), 1)
    query_no = lax.broadcasted_iota(jnp.int32, (local, keys), 0) + ctx * local
    for seq in range(seqs):
        seen = (qseg_ref[seq] == kseg_ref[seq]) & (key_no <= query_no)
        hide = jnp.where(seen, 0.0, masked_score)

        def one_head(head, _):
            score = lax.dot_general(
                q_ref[seq, head], kv_ref[seq, 0], (((1,), (1,)), ((), ())), preferred_element_type=f32
            )
            score = jnp.where(hide < 0.0, masked_score, score * HEAD_DIM ** (-0.5))
            top = jnp.max(score, axis=-1, keepdims=True)
            weight = jnp.exp(score - top)
            total = jnp.sum(weight, axis=-1, keepdims=True)
            prob = (weight / total).astype(bf16)
            lse_ref[seq, head] = top + jnp.log(total)
            out = jnp.dot(prob, kv_ref[seq, 1], preferred_element_type=f32)
            o_ref[seq, head] = out.astype(bf16)
            return 0

        lax.fori_loop(0, q_cols // 128, one_head, 0)
        pump(3)

    o_rows = jnp.concatenate(
        [jnp.concatenate([o_ref[seq, head] for head in range(q_cols // 128)], 1) for seq in range(seqs)], 0
    )
    part_copies = []
    for index in range(width // 256):
        part[index] = lax.dot_general(
            o_rows,
            wattn[index * 256 : (index + 1) * 256, qkv_cols:],
            (((1,), (1,)), ((), ())),
            preferred_element_type=f32,
        )
        part_copies.append(
            start(remote(part.at[index], part_in.at[index], ps.at[index], pr.at[index], {"tp": other}))
        )
    pump(2)
    for index, copy in enumerate(part_copies):
        copy.wait_recv()
        span = slice(index * 256, (index + 1) * 256)
        h_ref[:, span] = tok_ref[:, span].astype(f32) + (part[index] + part_in[index])

    def norm_mid(index, _):
        piece = pl.ds(index * step_rows, step_rows)
        val = h_ref[piece, :]
        inv = lax.rsqrt(jnp.mean(val * val, axis=-1, keepdims=True) + norm_eps)
        per_seq = local // step_rows
        b_buf[index // per_seq, pl.ds(lax.rem(index, per_seq) * step_rows, step_rows), :] = (
            val * inv * row_ref[1:2, :]
        ).astype(bf16)
        return 0

    lax.fori_loop(0, rows // step_rows, norm_mid, 0)
    b_copies = group_send(1, b_buf, b_all)
    b_local = pltpu.make_async_copy(b_buf, b_all.at[ctx], loc.at[6])
    b_local.start()
    relays = []
    for tile in range(1, ctx_count):
        relays.append(group_relay(0, e_copies, e_all, tile))
    pump(2)
    while pending:
        pump(1)
    for tile in range(1, ctx_count):
        relays.append(group_relay(1, b_copies, b_all, tile))
    for item in (2, 3, 4):
        for tile in tiles:
            settle(item, tile)
    for copy in relays:
        copy.wait_recv()
    for copy in local_copies[2:] + [e_local, b_local]:
        copy.wait()
    for copy in sent:
        copy.wait_send()


def forward_call(tok, cot, attn_own, mlp_own, small_own, cos, sin, qseg, kseg, qkv_cols, q_cols, gain_cut):
    dp_count, ctx_count = lax.axis_size("dp"), lax.axis_size("ctx")
    own = attn_own.shape[0]
    rows, width = tok.shape
    seqs, local = cot.shape[:2]
    full_rows = own * dp_count * ctx_count
    heads = q_cols // 128
    bf16, f32 = jnp.bfloat16, jnp.float32
    vmem, hbm = pl.BlockSpec(memory_space=pltpu.VMEM), pl.BlockSpec(memory_space=pl.ANY)
    shapes = [
        ((full_rows, attn_own.shape[1]), bf16, vmem),
        ((mlp_own.shape[0], full_rows, mlp_own.shape[3]), bf16, hbm),
        ((ctx_count, seqs, local, width), bf16, hbm),
        ((ctx_count, seqs, local, width), bf16, hbm),
        ((rows, width), f32, vmem),
        ((rows, width), bf16, vmem),
        ((seqs, heads, local, 128), bf16, vmem),
        ((seqs, 2, local * ctx_count, 128), bf16, vmem),
        ((seqs, heads, local, 128), bf16, vmem),
        ((seqs, heads, local, 1), f32, vmem),
        ((8, width), f32, vmem),
    ]
    dma = pltpu.SemaphoreType.DMA
    chunks = width // 256
    return pl.pallas_call(
        functools.partial(forward_kernel, (dp_count, ctx_count, own, qkv_cols, q_cols, gain_cut)),
        out_shape=[jax.ShapeDtypeStruct(shape, kind) for shape, kind, _ in shapes],
        in_specs=[vmem, hbm, hbm, hbm, vmem, vmem, vmem, vmem, vmem],
        out_specs=[spec for _, _, spec in shapes],
        scratch_shapes=[
            pltpu.VMEM((dp_count * ctx_count, 8, small_own.shape[1]), f32),
            pltpu.VMEM((chunks, rows, 256), f32),
            pltpu.VMEM((chunks, rows, 256), f32),
            pltpu.VMEM((seqs, local, width), bf16),
        ]
        + [dma((5, ctx_count)) for _ in range(8)]
        + [dma((ctx_count,)), dma((ctx_count,)), dma((chunks,)), dma((chunks,))]
        + [dma((2, 2, ctx_count)), dma((2, 2, ctx_count)), dma((8,))],
        compiler_params=pltpu.CompilerParams(
            collective_id=0, has_side_effects=True, vmem_limit_bytes=60 * 1024 * 1024
        ),
        name="forward_kernel",
    )(tok, cot, attn_own, mlp_own, small_own, cos, sin, qseg, kseg)


def xor_rank(rank, step, count):
    value = jnp.int32(0)
    bit = 1
    while bit < count:
        digit = lax.rem(rank // bit, 2)
        value = value + bit * (digit + (1 - 2 * digit) * ((step // bit) % 2))
        bit *= 2
    return value


def backward_kernel(
    sizes,
    db_mine,
    db_send,
    out_mine,
    out_send,
    grad_down,
    grad_gate,
    grad_up,
    cot_ref,
    live_ref,
    tok_ref,
    h_ref,
    a_ref,
    q_ref,
    kv_ref,
    o_ref,
    lse_ref,
    row_ref,
    cos_ref,
    sin_ref,
    qseg_ref,
    kseg_ref,
    wattn,
    act_ref,
    dx_ref,
    zin,
    gat_ref,
    rows_ref,
    tpr,
    zrc,
    fin,
    stage,
    keep,
    r1,
    r2,
    keep_at,
    send_at,
    r1_at,
    r2_at,
    zin_at,
    hb_ref,
    do_ref,
    prob_ref,
    ds_ref,
    dq_ref,
    dkv_ref,
    dkv_bf,
    dkv_in,
    dqkv_ref,
    part,
    part_in,
    da_ref,
    tps,
    tpz,
    zss,
    zrs,
    fs,
    fr,
    ld,
    kd,
    s1,
    v1,
    s2,
    v2,
    s3,
    v3,
    ks,
    kr,
    ps,
    pr,
    gs,
    gr,
    acc_ref,
    sm_in,
    sm_sum,
):
    dp_count, ctx_count, own, qkv_cols, q_cols = sizes
    dp, ctx, core = lax.axis_index("dp"), lax.axis_index("ctx"), lax.axis_index("tp")
    bf16, f32 = jnp.bfloat16, jnp.float32
    seqs, local, width = cot_ref.shape
    group = own * ctx_count
    grads = (grad_down, grad_gate, grad_up)
    ff = grad_down.shape[2]
    heads = q_cols // 128
    other = 1 - core
    peers = [xor_rank(ctx, step, ctx_count) for step in range(ctx_count)]
    nodes = [xor_rank(dp, step, dp_count) for step in range(dp_count)]
    to_x, to_y, to_core = {"dp": nodes[1]}, {"dp": nodes[2]}, {"tp": other}
    greet([to_x, to_y, to_core] + [{"ctx": peers[step]} for step in range(1, ctx_count)])
    sent = []

    def start(copy):
        copy.start()
        sent.append(copy)
        return copy

    def rows_of(count, size, body):
        def one(index, _):
            body(pl.ds(pl.multiple_of(index * size, size), size))
            return 0

        lax.fori_loop(0, count // size, one, 0)

    tp_copy, z_copy, load_copy, fin_copy = {}, {}, {}, {}
    order = list(range(1, ctx_count)) + [0]

    def collect_start(index, send):
        for tile in order:
            tp_copy[index, tile] = start(
                remote(send.at[peers[tile]], tpr.at[index, peers[tile]], tps.at[index, tile], tpz.at[index, tile], to_core)
            )

    def collect_load(index, mine):
        for tile in order:
            load_copy[index, tile] = pltpu.make_async_copy(mine.at[peers[tile]], stage.at[tile], ld.at[index, tile])
            load_copy[index, tile].start()

    def collect_sum(index):
        for tile in order[:-1]:
            load_copy[index, tile].wait()
            tp_copy[index, tile].wait_recv()
            peer = peers[tile]

            def add(piece):
                tpr[index, peer, piece, :] = (stage[tile, piece, :] + tpr[index, peer, piece, :].astype(f32)).astype(bf16)

            rows_of(local, 32, add)
            z_copy[index, tile] = start(
                remote(tpr.at[index, peer], zrc.at[index, ctx], zss.at[index, tile], zrs.at[index, tile], {"ctx": peer})
            )

    def collect_fin(index):
        load_copy[index, 0].wait()
        tp_copy[index, 0].wait_recv()
        for tile in order[:-1]:
            z_copy[index, tile].wait_recv()

        def add(piece):
            total = stage[0, piece, :] + tpr[index, ctx, piece, :].astype(f32)
            for tile in order[:-1]:
                total = total + zrc[index, peers[tile], piece, :].astype(f32)
            fin[index, core, piece, :] = total

        rows_of(local, 32, add)
        fin_copy[index] = start(
            remote(fin.at[index, core], fin.at[index, core], fs.at[index], fr.at[index], to_core)
        )

    halves = {}
    for item in range(3):
        cut = (ff // 256 + 1) * 128
        halves[item] = ((0, cut), (cut, ff)) if item != 1 else ((cut, ff), (0, cut))
    middle = qkv_cols + (wattn.shape[1] - qkv_cols) // 2
    halves[3] = ((qkv_cols, middle), (middle, wattn.shape[1]))
    halves[4] = ((0, qkv_cols // 2), (qkv_cols // 2, qkv_cols))
    first_to, second_to = (to_y, to_x), (to_x, to_y)
    first_keys = ((2, 3), (1, 3))
    one_copy, two_copy, three_copy, keep_copy = {}, {}, {}, {}

    def cols(item, half):
        low, high = halves[item][half]
        return slice(low, high)

    def refs(item):
        if item < 3:
            return keep.at[item], r1.at[item], r2.at[item]
        return keep_at, r1_at, r2_at

    def stage_one(item, half):
        span = cols(item, half)
        for slot, key in enumerate(first_keys[half]):
            src = grads[item].at[nodes[key], :, span] if item < 3 else send_at.at[slot, :, span]
            one_copy[item, half, slot] = start(
                remote(
                    src,
                    refs(item)[1].at[slot, :, span],
                    s1.at[item, half, slot],
                    v1.at[item, half, slot],
                    first_to[half],
                )
            )

    def stage_two(item, half):
        span = cols(item, half)
        mine, first, second = refs(item)
        if item < 3:
            keep_copy[item, half].wait()
        one_copy[item, half, 1].wait_recv()

        def add(piece):
            mine[1, piece, span] = (mine[1, piece, span].astype(f32) + first[1, piece, span].astype(f32)).astype(bf16)

        rows_of(group, 96, add)
        two_copy[item, half] = start(
            remote(mine.at[1, :, span], second.at[:, span], s2.at[item, half], v2.at[item, half], second_to[half])
        )

    def stage_three(item, half):
        span = cols(item, half)
        mine, first, second = refs(item)
        if item < 3:
            keep_copy[item, 2].wait() if half == 0 else None
        one_copy[item, half, 0].wait_recv()
        two_copy[item, half].wait_recv()

        def total(piece):
            return mine[0, piece, span].astype(f32) + first[0, piece, span].astype(f32) + second[piece, span].astype(f32)

        if item >= 3:
            gat_ref[:, span] = total(pl.ds(pl.multiple_of(ctx * own, own), own))

        def add(piece):
            mine[0, piece, span] = total(piece).astype(bf16)

        rows_of(group, 96, add)
        target = zin.at[item] if item < 3 else zin_at
        for tile in range(1, ctx_count):
            piece = pl.ds(pl.multiple_of(peers[tile] * own, own), own)
            three_copy[item, half, tile] = start(
                remote(
                    mine.at[0, piece, span],
                    target.at[ctx, :, span],
                    s3.at[item, half, tile],
                    v3.at[item, half, tile],
                    {"ctx": peers[tile]},
                )
            )
        if item < 3:
            piece = pl.ds(pl.multiple_of(ctx * own, own), own)
            copy = pltpu.make_async_copy(mine.at[0, piece, span], target.at[ctx, :, span], kd.at[item, 3 + half])
            copy.start()
            three_copy[item, half, 0] = copy

    def stage_four(item, half):
        span = cols(item, half)
        for tile in range(1, ctx_count):
            three_copy[item, half, tile].wait_recv()
        if item < 3:
            three_copy[item, half, 0].wait()
        else:
            total = gat_ref[:, span]
            for tile in range(1, ctx_count):
                total = total + zin_at[peers[tile], :, span].astype(f32)
            gat_ref[:, span] = total

    collect_start(0, db_send)
    collect_load(0, db_mine)
    for item in range(3):
        stage_one(item, 0)
        stage_one(item, 1)
        for half in range(2):
            span = cols(item, half)
            copy = pltpu.make_async_copy(
                grads[item].at[nodes[1 + half], :, span], keep.at[item, 1, :, span], kd.at[item, half]
            )
            copy.start()
            keep_copy[item, half] = copy
        copy = pltpu.make_async_copy(grads[item].at[dp], keep.at[item, 0], kd.at[item, 2])
        copy.start()
        keep_copy[item, 2] = copy
    collect_start(1, out_send)
    collect_sum(0)

    pending = []
    for item in range(3):
        pending += [(stage_two, item, 0), (stage_two, item, 1)]
    for item in range(3):
        pending += [(stage_three, item, 0), (stage_three, item, 1)]

    def pump(count):
        for _ in range(min(count, len(pending))):
            action, item, half = pending.pop(0)
            action(item, half)

    collect_fin(0)
    collect_load(1, out_mine)
    collect_sum(1)
    pump(1)
    fin_copy[0].wait_recv()

    size = 32
    per_seq = local // size

    def split(index):
        return index // per_seq, pl.ds(pl.multiple_of(lax.rem(index, per_seq) * size, size), size)

    acc_ref[...] = jnp.zeros_like(acc_ref)

    def norm_mid(index, total):
        seq, piece = split(index)
        whole = pl.ds(pl.multiple_of(index * size, size), size)
        grad, val = fin[0, seq, piece, :], h_ref[whole, :]
        inv = lax.rsqrt(jnp.mean(val * val, axis=-1, keepdims=True) + norm_eps)
        weighted = grad * row_ref[1:2, :]
        inner = jnp.mean(weighted * val, axis=-1, keepdims=True)
        out = cot_ref[seq, piece, :].astype(f32) + (inv * weighted - val * (inv * inv * inv) * inner)
        dx_ref[seq, piece, :] = out
        hb_ref[whole, :] = out.astype(bf16)
        return total + jnp.sum(grad * val * inv, axis=0, keepdims=True)

    acc_ref[1:2, :] = lax.fori_loop(0, seqs * per_seq, norm_mid, jnp.zeros((1, width), f32))
    pump(1)

    for low in range(0, q_cols, 256):
        val = jnp.dot(hb_ref[...], wattn[:, qkv_cols + low : qkv_cols + low + 256], preferred_element_type=f32).astype(bf16)
        for head_low in (0, 128):
            for seq in range(seqs):
                do_ref[seq, (low + head_low) // 128] = val[seq * local : (seq + 1) * local, head_low : head_low + 128]
    pump(1)

    keys = kv_ref.shape[2]
    key_no = lax.broadcasted_iota(jnp.int32, (local, keys), 1)
    query_no = lax.broadcasted_iota(jnp.int32, (local, keys), 0) + ctx * local
    scale = HEAD_DIM ** (-0.5)
    kv_copies = []
    for seq in range(seqs):
        seen = (qseg_ref[seq] == kseg_ref[seq]) & (key_no <= query_no)
        hide = jnp.where(seen, 0.0, masked_score)

        def one_head(head, _):
            query, grad_out, keys_bf, values_bf = q_ref[seq, head], do_ref[seq, head], kv_ref[seq, 0], kv_ref[seq, 1]
            score = lax.dot_general(query, keys_bf, (((1,), (1,)), ((), ())), preferred_element_type=f32) * scale
            prob = jnp.exp(jnp.where(hide < 0.0, masked_score, score) - lse_ref[seq, head])
            grad_prob = lax.dot_general(grad_out, values_bf, (((1,), (1,)), ((), ())), preferred_element_type=f32)
            row_dot = jnp.sum(grad_out.astype(f32) * o_ref[seq, head].astype(f32), axis=-1, keepdims=True)
            grad_score = (prob * (grad_prob - row_dot) * scale).astype(bf16)
            prob_ref[head] = prob.astype(bf16)
            ds_ref[head] = grad_score
            grad_query = jnp.dot(grad_score, keys_bf, preferred_element_type=f32)
            turned = grad_query * cos_ref[seq * local : (seq + 1) * local, :] + pltpu.roll(
                grad_query * sin_ref[seq * local : (seq + 1) * local, :], 64, 1
            )
            dq_ref[seq, head] = turned
            return 0

        lax.fori_loop(0, heads, one_head, 0)
        stacked = (heads * local, 128)
        dkv_ref[seq, 0] = lax.dot_general(
            ds_ref[...].reshape(heads * local, keys),
            q_ref[seq].reshape(stacked),
            (((0,), (0,)), ((), ())),
            preferred_element_type=f32,
        )
        dkv_ref[seq, 1] = lax.dot_general(
            prob_ref[...].reshape(heads * local, keys),
            do_ref[seq].reshape(stacked),
            (((0,), (0,)), ((), ())),
            preferred_element_type=f32,
        )
        dkv_bf[seq] = dkv_ref[seq].astype(bf16)
        pump(2)
    for tile in range(1, ctx_count):
        piece = pl.ds(pl.multiple_of(peers[tile] * local, local), local)
        kv_copies.append(
            start(remote(dkv_bf.at[:, :, piece, :], dkv_in.at[ctx], ks.at[tile], kr.at[tile], {"ctx": peers[tile]}))
        )

    def weight_blocks(item, left_ref, right, low, high):
        for key in (3, 2, 1, 0):
            left = left_ref[:, pl.ds(pl.multiple_of(nodes[key] * group, group), group)]
            val = lax.dot_general(left, right, (((0,), (0,)), ((), ())), preferred_element_type=f32).astype(bf16)
            for half in range(2):
                span = cols(item, half)
                piece = val[:, span.start - low : span.stop - low]
                if key in first_keys[half]:
                    send_at[first_keys[half].index(key), :, span] = piece
                else:
                    keep_at[0 if key == 0 else 1, :, span] = piece
            if key == 2:
                stage_one(item, 0)
            if key == 1:
                stage_one(item, 1)

    o_rows = jnp.concatenate(
        [jnp.concatenate([o_ref[seq, head] for head in range(heads)], 1) for seq in range(seqs)], 0
    )
    weight_blocks(3, hb_ref, o_rows, qkv_cols, wattn.shape[1])

    for seq in range(seqs):
        for head in range(heads):
            val = dq_ref[seq, head]
            span = slice(head * 128, (head + 1) * 128)
            dqkv_ref[seq * local : (seq + 1) * local, span] = val.astype(bf16)
            acc_ref[2:3, span] = acc_ref[2:3, span] + jnp.sum(val, axis=0, keepdims=True)
    for copy in kv_copies:
        copy.wait_recv()
    own_keys = pl.ds(pl.multiple_of(ctx * local, local), local)
    for seq in range(seqs):
        for part_no in range(2):
            val = dkv_ref[seq, part_no, own_keys, :]
            for tile in range(1, ctx_count):
                val = val + dkv_in[peers[tile], seq, part_no].astype(f32)
            here = slice(seq * local, (seq + 1) * local)
            if part_no == 0:
                val = val * cos_ref[here, :] + pltpu.roll(val * sin_ref[here, :], 64, 1)
            span = slice(q_cols + part_no * 128, q_cols + (part_no + 1) * 128)
            dqkv_ref[here, span] = val.astype(bf16)
            acc_ref[2:3, span] = acc_ref[2:3, span] + jnp.sum(val, axis=0, keepdims=True)
    weight_blocks(4, a_ref, dqkv_ref[...], 0, qkv_cols)

    part_copies = []
    for index in range(width // 256):
        part[index] = lax.dot_general(
            dqkv_ref[...],
            wattn[index * 256 : (index + 1) * 256, :qkv_cols],
            (((1,), (1,)), ((), ())),
            preferred_element_type=f32,
        )
        part_copies.append(
            start(remote(part.at[index], part_in.at[index], ps.at[index], pr.at[index], to_core))
        )
    pump(4)
    for index, copy in enumerate(part_copies):
        copy.wait_recv()
        da_ref[:, index * 256 : (index + 1) * 256] = part[index] + part_in[index]

    def norm_in(index, total):
        seq, piece = split(index)
        whole = pl.ds(pl.multiple_of(index * size, size), size)
        grad, val = da_ref[whole, :], tok_ref[whole, :].astype(f32)
        inv = lax.rsqrt(jnp.mean(val * val, axis=-1, keepdims=True) + norm_eps)
        weighted = grad * row_ref[0:1, :]
        inner = jnp.mean(weighted * val, axis=-1, keepdims=True)
        dx_ref[seq, piece, :] = dx_ref[seq, piece, :] + (inv * weighted - val * (inv * inv * inv) * inner)
        return total + jnp.sum(grad * val * inv, axis=0, keepdims=True)

    acc_ref[0:1, :] = lax.fori_loop(0, seqs * per_seq, norm_in, jnp.zeros((1, width), f32))

    small_copies = [
        start(remote(acc_ref, sm_in.at[tile], gs.at[tile], gr.at[tile], {"ctx": peers[tile]}))
        for tile in range(1, ctx_count)
    ]
    collect_fin(1)
    while pending:
        pump(1)
    for item in (3, 4):
        for half in range(2):
            stage_two(item, half)
    total = acc_ref[...]
    for tile, copy in enumerate(small_copies):
        copy.wait_recv()
        total = total + sm_in[tile + 1]
    sm_sum[0] = total
    for turn, target in ((0, to_x), (1, to_y)):
        slot = ctx_count + turn
        copy = start(remote(sm_sum.at[turn], sm_in.at[slot], gs.at[slot], gr.at[slot], target))
        if turn == 0:
            fin_copy[1].wait_recv()
        copy.wait_recv()
        total = sm_sum[turn] + sm_in[slot]
        if turn == 0:
            sm_sum[1] = total
        else:
            rows_ref[...] = total

    def act_rows(index, _):
        seq, piece = split(index)
        whole = pl.ds(pl.multiple_of(index * size, size), size)
        act_ref[seq, piece, :] = (h_ref[whole, :] + fin[1, seq, piece, :]) * live_ref[seq, piece, :]
        return 0

    lax.fori_loop(0, seqs * per_seq, act_rows, 0)
    for item in (3, 4):
        for half in range(2):
            stage_three(item, half)
    for item in (0, 1, 2, 3, 4):
        for half in range(2):
            stage_four(item, half)
    for copy in sent:
        copy.wait_send()


def backward_call(inputs, sizes):
    dp_count, ctx_count, own, qkv_cols, q_cols = sizes
    bf16, f32 = jnp.bfloat16, jnp.float32
    vmem, hbm = pl.BlockSpec(memory_space=pltpu.VMEM), pl.BlockSpec(memory_space=pl.ANY)
    seqs, local, width = inputs[7].shape
    group, ff = inputs[4].shape[1:]
    rows, keys = seqs * local, local * ctx_count
    heads = q_cols // 128
    attn_cols = inputs[-1].shape[1]
    chunks = width // 256
    outs = [
        ((seqs, local, width), f32, vmem),
        ((seqs, local, width), f32, vmem),
        ((3, ctx_count, own, ff), bf16, hbm),
        ((own, attn_cols), f32, vmem),
        ((8, width), f32, vmem),
    ]
    scratch = [
        ((2, ctx_count, local, width), bf16),
        ((2, ctx_count, local, width), bf16),
        ((2, seqs, local, width), f32),
        ((ctx_count, local, width), f32),
        ((3, 2, group, ff), bf16),
        ((3, 2, group, ff), bf16),
        ((3, group, ff), bf16),
        ((2, group, attn_cols), bf16),
        ((2, group, attn_cols), bf16),
        ((2, group, attn_cols), bf16),
        ((group, attn_cols), bf16),
        ((ctx_count, own, attn_cols), bf16),
        ((rows, width), bf16),
        ((seqs, heads, local, 128), bf16),
        ((heads, local, keys), bf16),
        ((heads, local, keys), bf16),
        ((seqs, heads, local, 128), f32),
        ((seqs, 2, keys, 128), f32),
        ((seqs, 2, keys, 128), bf16),
        ((ctx_count, seqs, 2, local, 128), bf16),
        ((rows, qkv_cols), bf16),
        ((chunks, rows, 256), f32),
        ((chunks, rows, 256), f32),
        ((rows, width), f32),
    ]
    dma = pltpu.SemaphoreType.DMA
    pairs = [(2, ctx_count), (2, ctx_count), (2,)]
    sems = [dma(shape) for shape in pairs for _ in range(2)]
    sems += [dma((2, ctx_count)), dma((3, 5))]
    sems += [dma(shape) for shape in ((5, 2, 2), (5, 2), (5, 2, ctx_count), (ctx_count,), (chunks,), (ctx_count + 2,)) for _ in range(2)]
    last = [((8, width), f32), ((ctx_count + 2, 8, width), f32), ((2, 8, width), f32)]
    return pl.pallas_call(
        functools.partial(backward_kernel, sizes),
        out_shape=[jax.ShapeDtypeStruct(shape, kind) for shape, kind, _ in outs],
        in_specs=[hbm] * 7 + [vmem] * (len(inputs) - 7),
        out_specs=[spec for _, _, spec in outs],
        scratch_shapes=[pltpu.VMEM(*entry) for entry in scratch] + sems + [pltpu.VMEM(*entry) for entry in last],
        compiler_params=pltpu.CompilerParams(
            collective_id=1, has_side_effects=True, vmem_limit_bytes=65 * 1024 * 1024 - 65536
        ),
        name="backward_kernel",
    )(*inputs)


def on_device_kernels(
    tokens,
    cotangent,
    segments,
    positions,
    counts,
    attn_gain,
    q_weight,
    q_bias,
    k_weight,
    v_weight,
    kv_bias,
    o_weight,
    mlp_gain,
    gate_weight,
    up_weight,
    down_weight,
):
    dp_count, ctx_count = lax.axis_size("dp"), lax.axis_size("ctx")
    dp_rank, ctx_rank, core = lax.axis_index("dp"), lax.axis_index("ctx"), lax.axis_index("tp")
    seq_count, local_len, width = tokens.shape
    full_len = segments.shape[1]
    row_count = seq_count * local_len
    half_width = width // 2
    own_rows = q_weight.shape[1]
    group_rows = own_rows * ctx_count
    q_cols, k_cols, ff_cols = q_weight.shape[2], k_weight.shape[2], gate_weight.shape[2]
    kv_local = k_cols // HEAD_DIM
    group_size = q_cols // k_cols
    qkv_cols = q_cols + 2 * k_cols
    lane = 128
    ff_block = -(-ff_cols // (lane * ctx_count)) * lane
    ff_pad = ff_block * ctx_count - ff_cols
    f32, bf16 = jnp.float32, jnp.bfloat16

    parts = (attn_gain[0], mlp_gain[0], q_bias[0].reshape(-1), kv_bias[0].reshape(-1))
    cuts = [0]
    for part_vec in parts:
        cuts.append(cuts[-1] + part_vec.shape[0])
    small_own = jnp.pad(jnp.concatenate(parts).astype(f32)[None], ((0, 7), (0, 0)))
    attn_own = jnp.concatenate([q_weight[0], k_weight[0], v_weight[0], o_weight[0]], 1)
    mlp_own = jnp.stack(
        [
            jnp.pad(weight[0], ((0, 0), (0, ff_pad))).reshape(own_rows, ctx_count, ff_block).transpose(1, 0, 2)
            for weight in (gate_weight, up_weight, down_weight)
        ]
    )
    live_seq = (jnp.arange(seq_count, dtype=jnp.int32) < counts[0]).astype(f32)
    cot_live = (cotangent.astype(f32) * live_seq[:, None, None]).astype(bf16)
    query_seg = lax.dynamic_slice_in_dim(segments, ctx_rank * local_len, local_len, 1)
    cos_tab, sin_tab = rope_tables(positions.reshape(-1))
    sign = jnp.where(jnp.arange(HEAD_DIM) < HEAD_DIM // 2, -1.0, 1.0)
    (
        w_attn,
        w_mlp,
        grad_all,
        mid_all,
        resid_mid,
        normed_in,
        query_hm,
        keyval_hm,
        attn_hm,
        log_total,
        small_rows,
    ) = forward_call(
        tokens.reshape(-1, width),
        cot_live,
        attn_own,
        mlp_own,
        small_own,
        cos_tab,
        sin_tab * sign,
        query_seg[:, :, None],
        segments[:, None, :],
        qkv_cols,
        q_cols,
        cuts,
    )
    w_gate, w_up, w_down = w_mlp[0], w_mlp[1], w_mlp[2]
    grad_all, mid_all = grad_all.reshape(-1, width), mid_all.reshape(-1, width)
    gate_pre = mat_mul(mid_all, w_gate)
    up_pre = mat_mul(mid_all, w_up)
    hidden_bf = (jax.nn.silu(gate_pre) * up_pre).astype(bf16)
    grad_hidden = mat_mul(grad_all, w_down)
    sigmoid_gate = jax.nn.sigmoid(gate_pre)
    grad_gate = (
        grad_hidden * up_pre * sigmoid_gate * (1.0 + gate_pre * (1.0 - sigmoid_gate))
    ).astype(bf16)
    grad_up = (grad_hidden * gate_pre * sigmoid_gate).astype(bf16)

    def by_sequence(part):
        part = part.reshape(ctx_count, seq_count, local_len, width)
        mine = lax.dynamic_index_in_dim(part, core, 1, keepdims=False)
        return mine, lax.dynamic_index_in_dim(part, 1 - core, 1, keepdims=False).astype(bf16)

    def by_rank(left, right):
        return rows_mul(left, right).astype(bf16).reshape(dp_count, group_rows, ff_block)

    db_mine, db_send = by_sequence(mat_mul_t(grad_gate, w_gate) + mat_mul_t(grad_up, w_up))
    out_mine, out_send = by_sequence(mat_mul_t(hidden_bf, w_down))
    activations, input_grad, grad_ff, grad_w_attn, rows_sum = backward_call(
        (
            db_mine,
            db_send,
            out_mine,
            out_send,
            by_rank(grad_all, hidden_bf),
            by_rank(mid_all, grad_gate),
            by_rank(mid_all, grad_up),
            cot_live,
            jnp.broadcast_to(live_seq[:, None, None], (seq_count, local_len, 1)),
            tokens.reshape(-1, width),
            resid_mid,
            normed_in,
            query_hm,
            keyval_hm,
            attn_hm,
            log_total,
            small_rows,
            cos_tab,
            sin_tab * sign,
            query_seg[:, :, None],
            segments[:, None, :],
            w_attn,
        ),
        (dp_count, ctx_count, own_rows, qkv_cols, q_cols),
    )
    grad_w_down, grad_w_gate, grad_w_up = (
        jnp.concatenate([grad_ff[item, block] for block in range(ctx_count)], 1)[:, :ff_cols].astype(f32)
        for item in range(3)
    )
    rank = dp_rank * ctx_count + ctx_rank

    def own_part(vector, size):
        return lax.dynamic_slice_in_dim(vector, rank * size, size, 0)

    bias_kv = jnp.concatenate(
        [
            rows_sum[2, q_cols : q_cols + k_cols].reshape(kv_local, -1).T,
            rows_sum[2, q_cols + k_cols : qkv_cols].reshape(kv_local, -1).T,
        ],
        0,
    ).reshape(-1)
    own = [
        own_part(rows_sum[0], own_rows)[None],
        own_part(rows_sum[1], own_rows)[None],
        own_part(rows_sum[2, :q_cols].reshape(kv_local, -1).T.reshape(-1), cuts[3] - cuts[2]),
        own_part(bias_kv, cuts[4] - cuts[3]),
    ]
    grad_w_qkv, grad_w_out = grad_w_attn[:, :qkv_cols], grad_w_attn[:, qkv_cols:]
    return (
        activations.reshape(tokens.shape),
        input_grad.reshape(tokens.shape),
        own[0],
        grad_w_qkv[None, :, :q_cols],
        own[2].reshape(q_bias.shape),
        grad_w_qkv[None, :, q_cols : q_cols + k_cols],
        grad_w_qkv[None, :, q_cols + k_cols :],
        own[3].reshape(kv_bias.shape),
        grad_w_out[None],
        own[1],
        grad_w_gate[None],
        grad_w_up[None],
        grad_w_down[None],
    )


def solution(mesh):
    in_specs = (
        P("dp", "ctx", None),
        P("dp", "ctx", None),
        P("dp", None),
        P("dp", "ctx"),
        P("dp"),
        P(None, ("dp", "ctx")),
        P(None, ("dp", "ctx"), "tp"),
        P(None, ("dp", "ctx"), "tp"),
        P(None, ("dp", "ctx"), "tp"),
        P(None, ("dp", "ctx"), "tp"),
        P(None, ("dp", "ctx"), "tp"),
        P(None, ("dp", "ctx"), "tp"),
        P(None, ("dp", "ctx")),
        P(None, ("dp", "ctx"), "tp"),
        P(None, ("dp", "ctx"), "tp"),
        P(None, ("dp", "ctx"), "tp"),
    )
    out_specs = (
        P("dp", "ctx", None),
        P("dp", "ctx", None),
        P(None, ("dp", "ctx")),
        P(None, ("dp", "ctx"), "tp"),
        P(None, ("dp", "ctx"), "tp"),
        P(None, ("dp", "ctx"), "tp"),
        P(None, ("dp", "ctx"), "tp"),
        P(None, ("dp", "ctx"), "tp"),
        P(None, ("dp", "ctx"), "tp"),
        P(None, ("dp", "ctx")),
        P(None, ("dp", "ctx"), "tp"),
        P(None, ("dp", "ctx"), "tp"),
        P(None, ("dp", "ctx"), "tp"),
    )
    kernels_fit = mesh.shape["dp"] == 4 and mesh.shape["ctx"] == 4 and mesh.shape["tp"] == KV_HEADS
    return jax.shard_map(
        on_device_kernels if kernels_fit else on_device, mesh=mesh, in_specs=in_specs, out_specs=out_specs, check_vma=False
    )
```

```python
import functools

import jax
import jax.numpy as jnp
from jax import lax
from jax.experimental import pallas as pl
from jax.experimental.pallas import tpu as pltpu
from jax.sharding import PartitionSpec as P

HEADS = 12
KV_HEADS = 2
HEAD_DIM = 128
LAYERS = 1


theta_base = 1000000.0
norm_eps = 1e-06
masked_score = -1e30


def mat_mul(left, right):
    return jnp.dot(left, right, preferred_element_type=jnp.float32)


def mat_mul_t(left, right):
    return lax.dot_general(
        left, right, (((1,), (1,)), ((), ())), preferred_element_type=jnp.float32
    )


def rows_mul(left, right):
    return lax.dot_general(
        left, right, (((0,), (0,)), ((), ())), preferred_element_type=jnp.float32
    )


def rope_tables(pos_vals):
    half_dim = HEAD_DIM // 2
    frequency = theta_base ** (-(jnp.arange(half_dim, dtype=jnp.float32) * (2.0 / HEAD_DIM)))
    angles = pos_vals.astype(jnp.float32)[..., None] * frequency
    cos_half = jnp.cos(angles)
    sin_half = jnp.sin(angles)
    return (jnp.concatenate([cos_half, cos_half], -1), jnp.concatenate([sin_half, sin_half], -1))


def rotate(values, cos_tab, sin_tab):
    half_dim = values.shape[-1] // 2
    turned = jnp.concatenate([-values[..., half_dim:], values[..., :half_dim]], -1)
    return values * cos_tab + turned * sin_tab


def unrotate(grad_vals, cos_tab, sin_tab):
    half_dim = grad_vals.shape[-1] // 2
    scaled = grad_vals * sin_tab
    turned = jnp.concatenate([scaled[..., half_dim:], -scaled[..., :half_dim]], -1)
    return grad_vals * cos_tab + turned


def norm_forward(residual, gain_vec):
    inv_rms = lax.rsqrt(jnp.mean(residual * residual, axis=-1, keepdims=True) + norm_eps)
    normed = (residual * inv_rms * gain_vec.astype(jnp.float32)).astype(jnp.bfloat16)
    return (inv_rms, normed)


def norm_backward(residual, inv_rms, gain_vec, grad_normed):
    weighted = grad_normed * gain_vec.astype(jnp.float32)
    inner_mean = jnp.mean(weighted * residual, axis=-1, keepdims=True)
    grad_resid = inv_rms * weighted - residual * (inv_rms * inv_rms * inv_rms) * inner_mean
    grad_gain = jnp.sum(grad_normed * residual * inv_rms, axis=0)
    return (grad_resid, grad_gain)


def split_heads(keys_all, values_all):
    seq_count, full_len, kv_width = keys_all.shape
    kv_local = kv_width // HEAD_DIM
    return (
        keys_all.reshape(seq_count, full_len, kv_local, HEAD_DIM),
        values_all.reshape(seq_count, full_len, kv_local, HEAD_DIM),
    )


def attend_forward(query_bf, keys_all, values_all, allowed):
    key_heads, value_heads = split_heads(keys_all, values_all)
    scores = jnp.einsum(
        "bqkgd,bskd->bkgqs", query_bf, key_heads, preferred_element_type=jnp.float32
    ) * HEAD_DIM ** (-0.5)
    scores = jnp.where(allowed[:, None, None], scores, masked_score)
    top_score = jnp.max(scores, axis=-1, keepdims=True)
    shifted_exp = jnp.exp(scores - top_score)
    totals = jnp.sum(shifted_exp, axis=-1, keepdims=True)
    prob_bf = (shifted_exp / totals).astype(jnp.bfloat16)
    output = jnp.einsum(
        "bkgqs,bskd->bqkgd", prob_bf, value_heads, preferred_element_type=jnp.float32
    )
    return (output.astype(jnp.bfloat16), top_score + jnp.log(totals))


def attend_backward(query_bf, keys_all, values_all, attn_bf, log_total, grad_attn, allowed):
    key_heads, value_heads = split_heads(keys_all, values_all)
    scores = jnp.einsum(
        "bqkgd,bskd->bkgqs", query_bf, key_heads, preferred_element_type=jnp.float32
    ) * HEAD_DIM ** (-0.5)
    prob_full = jnp.exp(jnp.where(allowed[:, None, None], scores, masked_score) - log_total)
    prob_bf = prob_full.astype(jnp.bfloat16)
    grad_value = jnp.einsum(
        "bkgqs,bqkgd->bskd", prob_bf, grad_attn, preferred_element_type=jnp.float32
    )
    grad_prob = jnp.einsum(
        "bqkgd,bskd->bkgqs", grad_attn, value_heads, preferred_element_type=jnp.float32
    )
    row_dot = jnp.sum(grad_attn.astype(jnp.float32) * attn_bf.astype(jnp.float32), axis=-1)
    row_dot = jnp.transpose(row_dot, (0, 2, 3, 1))[..., None]
    grad_score = (prob_full * (grad_prob - row_dot) * HEAD_DIM ** (-0.5)).astype(jnp.bfloat16)
    grad_query = jnp.einsum(
        "bkgqs,bskd->bqkgd", grad_score, key_heads, preferred_element_type=jnp.float32
    )
    grad_key = jnp.einsum(
        "bkgqs,bqkgd->bskd", grad_score, query_bf, preferred_element_type=jnp.float32
    )
    return (grad_query, grad_key.reshape(keys_all.shape), grad_value.reshape(values_all.shape))


def xor_permute(value, axis_name, step):
    count = lax.axis_size(axis_name)
    return lax.ppermute(value, axis_name, [(rank, rank ^ step) for rank in range(count)])


def axis_bits(axis_name):
    return [1 << shift for shift in range(lax.axis_size(axis_name).bit_length() - 1)]


def partner(value):
    return xor_permute(value, "tp", 1)


def place(pieces, rank, dim):
    width = pieces[0].shape[dim]
    whole_shape = list(pieces[0].shape)
    whole_shape[dim] = width * len(pieces)
    whole = jnp.zeros(whole_shape, pieces[0].dtype)
    for offset, piece in enumerate(pieces):
        whole = lax.dynamic_update_slice_in_dim(whole, piece, (rank ^ offset) * width, dim)
    return whole


def join_halves(mine, other, core, dim):
    return jnp.where(
        core == 0, jnp.concatenate([mine, other], dim), jnp.concatenate([other, mine], dim)
    )


def gather_direct(value, axis_name):
    count = lax.axis_size(axis_name)
    return [value] + [xor_permute(value, axis_name, step) for step in range(1, count)]


def gather_halves(value, axis_name):
    rows = value.shape[0]
    half = rows // 2
    bits = axis_bits(axis_name)
    parts = []
    for piece, order in ((value[:half], bits), (value[half:], bits[::-1])):
        held = {0: piece}
        for bit in order:
            for key in list(held):
                held[key | bit] = xor_permute(held[key], axis_name, bit)
        parts.append(held)
    return [(parts[0][key], parts[1][key]) for key in range(len(parts[0]))]


def scatter_halves(blocks, axis_name):
    half = blocks[0].shape[0] // 2
    bits = axis_bits(axis_name)
    done = []
    for low, high, order in ((0, half, bits[::-1]), (half, 2 * half, bits)):
        held = {key: block[low:high] for key, block in enumerate(blocks)}
        for bit in order:
            for key in [key for key in held if key & bit]:
                sent = held.pop(key).astype(jnp.bfloat16)
                held[key ^ bit] = held[key ^ bit] + xor_permute(sent, axis_name, bit).astype(jnp.float32)
        done.append(held[0])
    return jnp.concatenate(done, 0)


def scatter_small(blocks, axis_name):
    held = dict(enumerate(blocks))
    for bit in axis_bits(axis_name)[::-1]:
        for key in [key for key in held if key & bit]:
            held[key ^ bit] = held[key ^ bit] + xor_permute(held.pop(key), axis_name, bit)
    return held[0]


def scatter_direct(block_of, axis_name):
    total = block_of(0)
    for step in range(1, lax.axis_size(axis_name)):
        got = xor_permute(block_of(step).astype(jnp.bfloat16), axis_name, step)
        total = total + got.astype(jnp.float32)
    return total


def rows_at(value, index, size):
    return lax.dynamic_slice_in_dim(value, index * size, size, 0)


def columns_at(value, index, size):
    return lax.dynamic_slice_in_dim(value, index * size, size, 1)


def on_device(
    tokens,
    cotangent,
    segments,
    positions,
    counts,
    attn_gain,
    q_weight,
    q_bias,
    k_weight,
    v_weight,
    kv_bias,
    o_weight,
    mlp_gain,
    gate_weight,
    up_weight,
    down_weight,
):
    dp_count, ctx_count = lax.axis_size("dp"), lax.axis_size("ctx")
    dp_rank, ctx_rank, core = lax.axis_index("dp"), lax.axis_index("ctx"), lax.axis_index("tp")
    seq_count, local_len, width = tokens.shape
    full_len = segments.shape[1]
    row_count = seq_count * local_len
    half_width = width // 2
    own_rows = q_weight.shape[1]
    group_rows = own_rows * ctx_count
    q_cols, k_cols, ff_cols = q_weight.shape[2], k_weight.shape[2], gate_weight.shape[2]
    kv_local = k_cols // HEAD_DIM
    group_size = q_cols // k_cols
    qkv_cols = q_cols + 2 * k_cols
    lane = 128
    ff_block = -(-ff_cols // (lane * ctx_count)) * lane
    ff_pad = ff_block * ctx_count - ff_cols
    f32, bf16 = jnp.float32, jnp.bfloat16

    small = jnp.concatenate(
        [attn_gain[0], mlp_gain[0], q_bias[0].reshape(-1), kv_bias[0].reshape(-1)]
    )[None]
    sizes = (attn_gain.shape[1], mlp_gain.shape[1], q_bias.shape[1] * q_bias.shape[2], kv_bias.shape[1] * kv_bias.shape[2])
    small_ctx = place(gather_direct(small, "ctx"), ctx_rank, 0)[None]
    held = {0: small_ctx}
    for bit in axis_bits("dp"):
        for key in list(held):
            held[key | bit] = xor_permute(held[key], "dp", bit)
    small_all = place([held[key] for key in range(dp_count)], dp_rank, 0)
    small_all = small_all.reshape(dp_count * ctx_count, -1)
    cuts = [0]
    for size in sizes:
        cuts.append(cuts[-1] + size)
    gain_in, gain_mid, b_query, b_keyval = (
        small_all[:, low:high].reshape(-1) for low, high in zip(cuts[:-1], cuts[1:])
    )
    b_query = b_query.reshape(-1, kv_local).T.reshape(-1).astype(f32)
    b_keyval = b_keyval.reshape(-1, kv_local).astype(f32)
    b_qkv = jnp.concatenate(
        [b_query, b_keyval[:HEAD_DIM].T.reshape(-1), b_keyval[HEAD_DIM:].T.reshape(-1)]
    )

    attn_own = jnp.concatenate([q_weight[0], k_weight[0], v_weight[0], o_weight[0]], 1)
    attn_group = place(gather_direct(attn_own, "ctx"), ctx_rank, 0)
    attn_pairs = gather_halves(attn_group, "dp")
    w_attn = place([jnp.concatenate(pair, 0) for pair in attn_pairs], dp_rank, 0)
    w_qkv, w_out = w_attn[:, :qkv_cols], w_attn[:, qkv_cols:]

    live_seq = (jnp.arange(seq_count, dtype=jnp.int32) < counts[0]).astype(f32)
    live_rows = jnp.repeat(live_seq, local_len)[:, None]
    grad_out = cotangent.astype(f32).reshape(-1, width) * live_rows

    def spread(rows_bf):
        mine = jnp.concatenate(gather_direct(columns_at(rows_bf, core, half_width), "ctx"), 0)
        return join_halves(mine, partner(mine), core, 1)

    grad_all = spread(grad_out.astype(bf16))

    def spread_weight(weight):
        padded = jnp.pad(weight[0], ((0, 0), (0, ff_pad)))
        pieces = [columns_at(padded, ctx_rank, ff_block)]
        for step in range(1, ctx_count):
            pieces.append(xor_permute(columns_at(padded, ctx_rank ^ step, ff_block), "ctx", step))
        pairs = gather_halves(place(pieces, ctx_rank, 0), "dp")
        return place([jnp.concatenate(pair, 0) for pair in pairs], dp_rank, 0)

    w_gate = spread_weight(gate_weight)
    w_up = spread_weight(up_weight)
    w_down = spread_weight(down_weight)

    query_pos = ctx_rank * local_len + jnp.arange(local_len, dtype=jnp.int32)
    key_pos = jnp.arange(full_len, dtype=jnp.int32)
    query_seg = lax.dynamic_slice_in_dim(segments, ctx_rank * local_len, local_len, 1)
    allowed = (query_seg[:, :, None] == segments[:, None, :]) & (
        key_pos[None, None, :] <= query_pos[None, :, None]
    )
    cos_tab, sin_tab = rope_tables(positions.reshape(-1))
    cos_tab, sin_tab = cos_tab[:, None, :], sin_tab[:, None, :]
    residual = tokens.astype(f32).reshape(-1, width)
    inv_in, normed_in = norm_forward(residual, gain_in)
    qkv_val = mat_mul(normed_in, w_qkv) + b_qkv
    query_bf = rotate(
        qkv_val[:, :q_cols].reshape(row_count, -1, HEAD_DIM), cos_tab, sin_tab
    ).astype(bf16).reshape(seq_count, -1, kv_local, group_size, HEAD_DIM)
    key_bf = rotate(
        qkv_val[:, q_cols : q_cols + k_cols].reshape(row_count, -1, HEAD_DIM), cos_tab, sin_tab
    ).astype(bf16).reshape(row_count, -1)
    value_bf = qkv_val[:, q_cols + k_cols :].astype(bf16)
    keyval = jnp.concatenate([key_bf, value_bf], 1).reshape(seq_count, local_len, -1)
    keyval_all = place(gather_direct(keyval, "ctx"), ctx_rank, 1)
    keys_all, values_all = keyval_all[..., :k_cols], keyval_all[..., k_cols:]
    attn_bf, log_total = attend_forward(query_bf, keys_all, values_all, allowed)
    attn_flat = attn_bf.reshape(row_count, -1)
    out_part = mat_mul_t(attn_flat, w_out)
    resid_mid = residual + (out_part + partner(out_part))
    inv_mid, normed_mid = norm_forward(resid_mid, gain_mid)

    mid_all = spread(normed_mid)
    gate_pre = mat_mul(mid_all, w_gate)
    up_pre = mat_mul(mid_all, w_up)
    hidden_bf = (jax.nn.silu(gate_pre) * up_pre).astype(bf16)
    grad_hidden = mat_mul(grad_all, w_down)
    sigmoid_gate = jax.nn.sigmoid(gate_pre)
    grad_gate = (
        grad_hidden * up_pre * sigmoid_gate * (1.0 + gate_pre * (1.0 - sigmoid_gate))
    ).astype(bf16)
    grad_up = (grad_hidden * gate_pre * sigmoid_gate).astype(bf16)

    def collect(part):
        part_bf = columns_at(part, 1 - core, half_width).astype(bf16)
        mine = columns_at(part, core, half_width) + partner(part_bf).astype(f32)
        total = scatter_direct(lambda step: mine[step * row_count : (step + 1) * row_count], "ctx")
        return join_halves(total, partner(total), core, 1)

    grad_normed_mid = collect(mat_mul_t(grad_gate, w_gate) + mat_mul_t(grad_up, w_up))

    def owner_weight(left, right):
        blocks = [
            rows_mul(columns_at(left, dp_rank ^ step, group_rows), right)
            for step in range(dp_count)
        ]
        group = scatter_halves(blocks, "dp").astype(bf16)
        pieces = [rows_at(group, ctx_rank, own_rows)]
        for step in range(1, ctx_count):
            pieces.append(xor_permute(rows_at(group, ctx_rank ^ step, own_rows), "ctx", step))
        return place(pieces, ctx_rank, 1)[:, :ff_cols].astype(f32)

    grad_w_down = owner_weight(grad_all, hidden_bf)
    grad_w_gate = owner_weight(mid_all, grad_gate)
    grad_w_up = owner_weight(mid_all, grad_up)

    layer_out = resid_mid + collect(mat_mul_t(hidden_bf, w_down))
    activations = (layer_out * live_rows).reshape(tokens.shape)

    grad_mid_norm, grad_gain_mid = norm_backward(resid_mid, inv_mid, gain_mid, grad_normed_mid)
    grad_mid = grad_out + grad_mid_norm
    grad_mid_bf = grad_mid.astype(bf16)
    grad_attn = mat_mul(grad_mid_bf, w_out).astype(bf16)

    def owner_attn(left, right):
        blocks = [
            rows_mul(columns_at(left, dp_rank ^ step, group_rows), right)
            for step in range(dp_count)
        ]
        group = scatter_halves(blocks, "dp")
        return scatter_direct(lambda step: rows_at(group, ctx_rank ^ step, own_rows), "ctx")

    grad_w_out = owner_attn(grad_mid_bf, attn_flat)
    grad_query, grad_key_all, grad_value_all = attend_backward(
        query_bf, keys_all, values_all, attn_bf, log_total, grad_attn.reshape(attn_bf.shape), allowed
    )
    grad_keyval_all = jnp.concatenate([grad_key_all, grad_value_all], 2)
    grad_keyval = scatter_direct(
        lambda step: lax.dynamic_slice_in_dim(
            grad_keyval_all, (ctx_rank ^ step) * local_len, local_len, 1
        ),
        "ctx",
    ).reshape(row_count, -1)
    grad_query = unrotate(
        grad_query.reshape(row_count, -1, HEAD_DIM), cos_tab, sin_tab
    ).reshape(row_count, -1)
    grad_key = unrotate(
        grad_keyval[:, :k_cols].reshape(row_count, -1, HEAD_DIM), cos_tab, sin_tab
    ).reshape(row_count, -1)
    grad_qkv = jnp.concatenate([grad_query, grad_key, grad_keyval[:, k_cols:]], 1)
    grad_qkv_bf = grad_qkv.astype(bf16)
    grad_w_qkv = owner_attn(normed_in, grad_qkv_bf)
    dot_part = mat_mul_t(grad_qkv_bf, w_qkv)
    grad_normed_in = dot_part + partner(dot_part)
    grad_in_norm, grad_gain_in = norm_backward(residual, inv_in, gain_in, grad_normed_in)
    input_grad = (grad_mid + grad_in_norm).reshape(tokens.shape)

    bias_sum = jnp.sum(grad_qkv, axis=0)
    device_count = dp_count * ctx_count
    grad_small = jnp.concatenate(
        [
            grad_gain_in.reshape(device_count, -1),
            grad_gain_mid.reshape(device_count, -1),
            bias_sum[:q_cols].reshape(kv_local, -1).T.reshape(device_count, -1),
            jnp.concatenate(
                [
                    bias_sum[q_cols : q_cols + k_cols].reshape(kv_local, -1).T,
                    bias_sum[q_cols + k_cols :].reshape(kv_local, -1).T,
                ],
                0,
            ).reshape(device_count, -1),
        ],
        1,
    )
    small_group = scatter_small(
        [rows_at(grad_small, dp_rank ^ step, ctx_count) for step in range(dp_count)], "dp"
    )
    small_own = scatter_small(
        [rows_at(small_group, ctx_rank ^ step, 1) for step in range(ctx_count)], "ctx"
    )
    own = [small_own[:, low:high] for low, high in zip(cuts[:-1], cuts[1:])]
    return (
        activations,
        input_grad,
        own[0],
        grad_w_qkv[None, :, :q_cols],
        own[2].reshape(q_bias.shape),
        grad_w_qkv[None, :, q_cols : q_cols + k_cols],
        grad_w_qkv[None, :, q_cols + k_cols :],
        own[3].reshape(kv_bias.shape),
        grad_w_out[None],
        own[1],
        grad_w_gate[None],
        grad_w_up[None],
        grad_w_down[None],
    )


MESH = pl.DeviceIdType.MESH


def remote(src, dst, send_sem, recv_sem, target):
    return pltpu.make_async_remote_copy(
        src_ref=src, dst_ref=dst, send_sem=send_sem, recv_sem=recv_sem, device_id=target, device_id_type=MESH
    )


def greet(partners):
    barrier = pltpu.get_barrier_semaphore()
    for partner_id in partners:
        pl.semaphore_signal(barrier, inc=1, device_id=partner_id, device_id_type=MESH)
    pl.semaphore_wait(barrier, len(partners))


def spread_row(values, row_cols, period, total):
    left = lax.broadcasted_iota(jnp.int32, (period, total), 0)
    right = lax.broadcasted_iota(jnp.int32, (period, total), 1)
    pick = (lax.rem(right, period) == left).astype(jnp.float32).astype(jnp.bfloat16)
    spread = jnp.dot(values.astype(jnp.bfloat16), pick, preferred_element_type=jnp.float32)
    block = lax.broadcasted_iota(jnp.int32, spread.shape, 0) // 8
    owner = lax.broadcasted_iota(jnp.int32, spread.shape, 1) // period
    return jnp.sum(jnp.where(block == owner, spread, 0.0), axis=0, keepdims=True)


def forward_kernel(
    sizes,
    tok_ref,
    cot_ref,
    attn_own,
    mlp_own,
    small_own,
    cos_ref,
    sin_ref,
    qseg_ref,
    kseg_ref,
    wattn_out,
    e_out,
    b_out,
    h_out,
    a_out,
    q_out,
    kv_out,
    o_out,
    lse_out,
    row_out,
    zgu_out,
    sum_out,
    own_out,
    wattn,
    wmlp,
    e_all,
    b_all,
    h_ref,
    a_ref,
    q_ref,
    kv_ref,
    o_ref,
    lse_ref,
    row_ref,
    small,
    part,
    part_in,
    zgu,
    pair,
    give,
    take,
    done,
    mine,
    zs,
    zr,
    xs,
    xr,
    ys,
    yr,
    fs,
    fr,
    ks,
    kr,
    ps,
    pr,
    bs,
    br,
    us,
    ur,
    ts,
    tr,
    loc,
    out_sem,
):
    dp_count, ctx_count, own, qkv_cols, q_cols, gain_cut = sizes
    dp, ctx, core = lax.axis_index("dp"), lax.axis_index("ctx"), lax.axis_index("tp")
    bf16, f32 = jnp.bfloat16, jnp.float32
    width = tok_ref.shape[1]
    rows = tok_ref.shape[0]
    seqs = cot_ref.shape[0]
    local = cot_ref.shape[1]
    tiles = range(ctx_count)

    def at_x(d):
        return d + 1 - 2 * lax.rem(d, 2)

    def at_y(d):
        return lax.rem(d + 2, 4)

    dpx, dpy = at_x(dp), at_y(dp)
    dpd = at_x(dpy)
    peers = [ctx]
    for step in range(1, ctx_count):
        value = jnp.int32(0)
        for bit in (1, 2, 4, 8):
            if bit < ctx_count:
                digit = lax.rem(ctx // bit, 2)
                value = value + bit * (digit + (1 - 2 * digit) * ((step // bit) % 2))
        peers.append(value)
    other = 1 - core
    to_core = {"tp": other}

    greet(
        [{"dp": dpx}, {"dp": dpy}, {"tp": other}] + [{"ctx": peers[step]} for step in range(1, ctx_count)]
    )
    sent = []

    def start(copy):
        copy.start()
        sent.append(copy)
        return copy

    def block_rows(d, c):
        return pl.ds(pl.multiple_of((d * ctx_count + c) * own, own), own)

    def slot(item, d, c):
        if item == 0:
            return small.at[d * ctx_count + c]
        if item == 1:
            return wattn.at[block_rows(d, c), :]
        return wmlp.at[item - 2, block_rows(d, c), :]

    def source(item, tile):
        if item == 0:
            return small_own
        if item == 1:
            return attn_own
        return mlp_own.at[item - 2, peers[tile]]

    items = range(5)
    local_copies = []
    for item in items:
        copy = pltpu.make_async_copy(source(item, 0), slot(item, dp, ctx), loc.at[item])
        copy.start()
        local_copies.append(copy)
    z_copy = {}

    def z_send(item):
        for tile in range(1, ctx_count):
            z_copy[item, tile] = start(
                remote(source(item, tile), slot(item, dp, ctx), zs.at[item, tile], zr.at[item, tile], {"ctx": peers[tile]})
            )

    x_copy, y_copy, f_copy = {}, {}, {}

    def xy_send(item, tile):
        src = source(item, 0) if tile == 0 else slot(item, dp, peers[tile])
        if tile:
            z_copy[item, tile].wait_recv()
        dst = slot(item, dp, peers[tile])
        x_copy[item, tile] = start(remote(src, dst, xs.at[item, tile], xr.at[item, tile], {"dp": dpx}))
        y_copy[item, tile] = start(remote(src, dst, ys.at[item, tile], yr.at[item, tile], {"dp": dpy}))

    def forward(item, tile):
        if (item + tile) % 2 == 0:
            x_copy[item, tile].wait_recv()
            place_at = slot(item, dpx, peers[tile])
            target = {"dp": dpy}
        else:
            y_copy[item, tile].wait_recv()
            place_at = slot(item, dpy, peers[tile])
            target = {"dp": dpx}
        f_copy[item, tile] = start(remote(place_at, place_at, fs.at[item, tile], fr.at[item, tile], target))

    def settle(item, tile):
        if (item + tile) % 2 == 0:
            y_copy[item, tile].wait_recv()
        else:
            x_copy[item, tile].wait_recv()
        f_copy[item, tile].wait_recv()

    last = ctx_count - 1
    ways = ((1, ctx < last), (-1, ctx > 0))
    relay_sent = []

    def hop(index, buf, way, distance, origin):
        step, _ = ways[way]
        piece = buf.at[origin, core]
        return remote(piece, piece, bs.at[index, way, distance], br.at[index, way, distance], {"ctx": ctx + step})

    def spread_start(index, buf):
        for way in range(2):
            copy = hop(index, buf, way, 0, ctx)

            @pl.when(ways[way][1])
            def _():
                copy.start()

            relay_sent.append((ways[way][1], copy))

    def spread_step(index, buf, distance):
        for way in range(2):
            step, open_end = ways[way]
            origin = ctx - step * distance
            here = (origin >= 0) & (origin <= last)
            safe = jnp.clip(origin, 0, last)
            piece = buf.at[safe, core]
            got = remote(piece, piece, bs.at[index, way, distance - 1], br.at[index, way, distance - 1], to_core)
            share = remote(piece, piece, us.at[index, way, distance], ur.at[index, way, distance], to_core)

            @pl.when(here)
            def _():
                got.wait_recv()
                share.start()

            relay_sent.append((here, share))
            if distance < last:
                copy = hop(index, buf, way, distance, safe)

                @pl.when(here & open_end)
                def _():
                    copy.start()

                relay_sent.append((here & open_end, copy))

    def spread_end(index, buf, distance):
        for way in range(2):
            step, _ = ways[way]
            origin = ctx - step * distance
            piece = buf.at[jnp.clip(origin, 0, last), other]
            got = remote(piece, piece, us.at[index, way, distance], ur.at[index, way, distance], to_core)

            @pl.when((origin >= 0) & (origin <= last))
            def _():
                got.wait_recv()

    z_send(0)
    z_send(1)
    xy_send(0, 0)
    xy_send(1, 0)
    for item in (2, 3):
        z_send(item)
    e_local = pltpu.make_async_copy(cot_ref, e_all.at[ctx], loc.at[5])
    e_local.start()
    kept = []

    def keep_out(src, dst):
        copy = pltpu.make_async_copy(src, dst, out_sem.at[len(kept)])
        copy.start()
        kept.append(copy)

    for tile in range(1, ctx_count):
        xy_send(0, tile)
        xy_send(1, tile)
    for tile in tiles:
        forward(0, tile)
        forward(1, tile)
    for item in (2, 3, 4):
        xy_send(item, 0)
    for tile in tiles:
        settle(0, tile)
    local_copies[0].wait()

    flat = small[...].reshape(dp_count * ctx_count * 8, small.shape[2])
    row_ref[0:1, :] = spread_row(flat[:, gain_cut[0] : gain_cut[1]], None, gain_cut[1] - gain_cut[0], width)
    row_ref[1:2, :] = spread_row(flat[:, gain_cut[1] : gain_cut[2]], None, gain_cut[2] - gain_cut[1], width)
    row_ref[2:3, :q_cols] = spread_row(flat[:, gain_cut[2] : gain_cut[3]], None, gain_cut[3] - gain_cut[2], q_cols)
    row_ref[2:3, q_cols:qkv_cols] = spread_row(
        flat[:, gain_cut[3] : gain_cut[4]], None, gain_cut[4] - gain_cut[3], qkv_cols - q_cols
    )

    step_rows = 32

    def norm_in(index, _):
        piece = pl.ds(index * step_rows, step_rows)
        val = tok_ref[piece, :].astype(f32)
        inv = lax.rsqrt(jnp.mean(val * val, axis=-1, keepdims=True) + norm_eps)
        a_ref[piece, :] = (val * inv * row_ref[0:1, :]).astype(bf16)
        return 0

    lax.fori_loop(0, rows // step_rows, norm_in, 0)
    xy_send(2, 1)
    for tile in tiles:
        settle(1, tile)
    local_copies[1].wait()
    keep_out(wattn, wattn_out)
    keep_out(a_ref, a_out)
    keep_out(row_ref, row_out)

    pending = [(forward, 2, 0), (forward, 3, 0), (xy_send, 3, 1)]
    for tile in (2, 3):
        for item in (2, 3):
            pending.append((xy_send, item, tile))
            pending.append((forward, item, tile - 1))
    pending += [(forward, 4, 0), (forward, 2, 3), (forward, 3, 3)]
    for tile in (1, 2, 3):
        pending.append((xy_send, 4, tile))
    for tile in (1, 2, 3):
        pending.append((forward, 4, tile))

    def pump(count):
        for _ in range(min(count, len(pending))):
            action, item, tile = pending.pop(0)
            action(item, tile)

    own_keys = pl.ds(pl.multiple_of(ctx * local, local), local)
    order = [qkv_cols - 256] + list(range(0, q_cols, 256))
    kv_copies = []
    for low in order:
        val = jnp.dot(a_ref[...], wattn[:, low : low + 256], preferred_element_type=f32) + row_ref[2:3, low : low + 256]
        for head_low in (0, 128):
            head = val[:, head_low : head_low + 128]
            if low + head_low < qkv_cols - 128:
                head = head * cos_ref[...] + pltpu.roll(head, 64, 1) * sin_ref[...]
            head = head.astype(bf16)
            for seq in range(seqs):
                piece = head[seq * local : (seq + 1) * local]
                if low == qkv_cols - 256:
                    kv_ref[seq, head_low // 128, own_keys, :] = piece
                else:
                    q_ref[seq, (low + head_low) // 128] = piece
        if low == qkv_cols - 256:
            for tile in range(1, ctx_count):
                piece = kv_ref.at[:, :, own_keys, :]
                kv_copies.append(start(remote(piece, piece, ks.at[tile], kr.at[tile], {"ctx": peers[tile]})))
            z_send(4)
            e_local.wait()
            spread_start(0, e_all)
        pump(1)
    keep_out(q_ref, q_out)
    pump(1)
    for copy in kv_copies:
        copy.wait_recv()
    keep_out(kv_ref, kv_out)

    keys = kv_ref.shape[2]
    key_no = lax.broadcasted_iota(jnp.int32, (local, keys), 1)
    query_no = lax.broadcasted_iota(jnp.int32, (local, keys), 0) + ctx * local
    for seq in range(seqs):
        seen = (qseg_ref[seq] == kseg_ref[seq]) & (key_no <= query_no)
        hide = jnp.where(seen, 0.0, masked_score)

        def one_head(head, _):
            score = lax.dot_general(
                q_ref[seq, head], kv_ref[seq, 0], (((1,), (1,)), ((), ())), preferred_element_type=f32
            )
            score = jnp.where(hide < 0.0, masked_score, score * HEAD_DIM ** (-0.5))
            top = jnp.max(score, axis=-1, keepdims=True)
            weight = jnp.exp(score - top)
            total = jnp.sum(weight, axis=-1, keepdims=True)
            prob = (weight / total).astype(bf16)
            lse_ref[seq, head] = top + jnp.log(total)
            out = jnp.dot(prob, kv_ref[seq, 1], preferred_element_type=f32)
            o_ref[seq, head] = out.astype(bf16)
            return 0

        lax.fori_loop(0, q_cols // 128, one_head, 0)
        pump(3)
    keep_out(o_ref, o_out)
    keep_out(lse_ref, lse_out)

    o_rows = jnp.concatenate(
        [jnp.concatenate([o_ref[seq, head] for head in range(q_cols // 128)], 1) for seq in range(seqs)], 0
    )
    part_copies = []
    for index in range(width // 256):
        part[index] = lax.dot_general(
            o_rows,
            wattn[index * 256 : (index + 1) * 256, qkv_cols:],
            (((1,), (1,)), ((), ())),
            preferred_element_type=f32,
        )
        part_copies.append(
            start(remote(part.at[index], part_in.at[index], ps.at[index], pr.at[index], {"tp": other}))
        )
    pump(2)
    for index, copy in enumerate(part_copies):
        copy.wait_recv()
        span = slice(index * 256, (index + 1) * 256)
        h_ref[:, span] = tok_ref[:, span].astype(f32) + (part[index] + part_in[index])

    def norm_mid(index, _):
        piece = pl.ds(index * step_rows, step_rows)
        val = h_ref[piece, :]
        inv = lax.rsqrt(jnp.mean(val * val, axis=-1, keepdims=True) + norm_eps)
        per_seq = local // step_rows
        b_all[ctx, index // per_seq, pl.ds(lax.rem(index, per_seq) * step_rows, step_rows), :] = (
            val * inv * row_ref[1:2, :]
        ).astype(bf16)
        return 0

    lax.fori_loop(0, rows // step_rows, norm_mid, 0)
    spread_start(1, b_all)
    keep_out(h_ref, h_out)
    pump(1)
    for distance in range(1, ctx_count):
        spread_step(0, e_all, distance)
        pump(3)
        spread_step(1, b_all, distance)
        pump(2)
    while pending:
        pump(1)
    for item in (2, 3, 4):
        for tile in tiles:
            settle(item, tile)
    for copy in local_copies[2:]:
        copy.wait()
    for distance in range(1, ctx_count):
        spread_end(0, e_all, distance)
        spread_end(1, b_all, distance)
    keep_out(e_all, e_out)
    keep_out(b_all, b_out)

    ff = wmlp.shape[2]
    full_ff = ff // 256 * 256
    nt = (((1,), (1,)), ((), ()))

    def ff_columns(slot, tokens_bf, grads_bf, low, size):
        span = pl.ds(low, size)
        gate = jnp.dot(tokens_bf[...].reshape(rows, width), wmlp[0, :, span], preferred_element_type=f32)
        up = jnp.dot(tokens_bf[...].reshape(rows, width), wmlp[1, :, span], preferred_element_type=f32)
        grad = jnp.dot(grads_bf[...].reshape(rows, width), wmlp[2, :, span], preferred_element_type=f32)
        sig = jax.nn.sigmoid(gate)
        zgu[slot, 0, :, span] = (gate * sig * up).astype(bf16)
        zgu[slot, 1, :, span] = (grad * up * sig * (1.0 + gate * (1.0 - sig))).astype(bf16)
        zgu[slot, 2, :, span] = (grad * gate * sig).astype(bf16)

    zgu_copies, give_copies = {}, {}

    def ff_rows(tile):
        slot = tile % 2
        peer = peers[tile]
        if tile >= 2:
            zgu_copies[tile - 2].wait()

        def columns(index, _):
            ff_columns(slot, b_all.at[peer], e_all.at[peer], pl.multiple_of(index * 256, 256), 256)
            return 0

        lax.fori_loop(0, ff // 256, columns, 0)
        if full_ff < ff:
            ff_columns(slot, b_all.at[peer], e_all.at[peer], full_ff, ff - full_ff)
        zgu_copies[tile] = pltpu.make_async_copy(zgu.at[slot], zgu_out.at[:, peer], loc.at[6 + slot])
        zgu_copies[tile].start()

        def outputs(index, _):
            span = pl.ds(pl.multiple_of(index * 256, 256), 256)
            back = lax.dot_general(zgu[slot, 1], wmlp[0, span, :], nt, preferred_element_type=f32)
            back = back + lax.dot_general(zgu[slot, 2], wmlp[1, span, :], nt, preferred_element_type=f32)
            ahead = lax.dot_general(zgu[slot, 0], wmlp[2, span, :], nt, preferred_element_type=f32)
            for seq in range(seqs):
                pair[slot, 0, seq, :, span] = back[seq * local : (seq + 1) * local]
                pair[slot, 1, seq, :, span] = ahead[seq * local : (seq + 1) * local]
            return 0

        lax.fori_loop(0, width // 256, outputs, 0)
        for item in range(2):

            def convert(index, _):
                piece = pl.ds(index * step_rows, step_rows)
                give[item, tile, piece, :] = pair[slot, item, other, piece, :].astype(bf16)
                return 0

            lax.fori_loop(0, local // step_rows, convert, 0)
            give_copies[tile, item] = start(
                remote(give.at[item, tile], take.at[item, tile], ts.at[item, tile], tr.at[item, tile], to_core)
            )

    def ff_sum(tile):
        slot = tile % 2
        for item in range(2):
            give_copies[tile, item].wait_recv()

            def add(index, _):
                piece = pl.ds(index * step_rows, step_rows)
                total = pair[slot, item, core, piece, :] + take[item, tile, piece, :].astype(f32)
                if tile == 0:
                    mine[item, piece, :] = total
                else:
                    done[item, tile, piece, :] = total.astype(bf16)
                return 0

            lax.fori_loop(0, local // step_rows, add, 0)
            if tile:
                keep_out(done.at[item, tile], sum_out.at[item, peers[tile]])

    for tile in range(ctx_count):
        ff_rows(tile)
        if tile:
            ff_sum(tile - 1)
    ff_sum(ctx_count - 1)
    keep_out(mine, own_out)
    for tile in (ctx_count - 2, ctx_count - 1):
        zgu_copies[tile].wait()
    for copy in kept:
        copy.wait()
    for copy in sent:
        copy.wait_send()
    for here, copy in relay_sent:

        @pl.when(here)
        def _():
            copy.wait_send()


def forward_call(tok, cot, attn_own, mlp_own, small_own, cos, sin, qseg, kseg, qkv_cols, q_cols, gain_cut):
    dp_count, ctx_count = lax.axis_size("dp"), lax.axis_size("ctx")
    own = attn_own.shape[0]
    rows, width = tok.shape
    seqs, local = cot.shape[:2]
    full_rows = own * dp_count * ctx_count
    heads = q_cols // 128
    ff = mlp_own.shape[3]
    bf16, f32 = jnp.bfloat16, jnp.float32
    vmem, hbm = pl.BlockSpec(memory_space=pltpu.VMEM), pl.BlockSpec(memory_space=pl.ANY)
    group = (ctx_count, seqs, local, width)
    kept = [
        ((rows, width), f32),
        ((rows, width), bf16),
        ((seqs, heads, local, 128), bf16),
        ((seqs, 2, local * ctx_count, 128), bf16),
        ((seqs, heads, local, 128), bf16),
        ((seqs, heads, local, 1), f32),
        ((8, width), f32),
    ]
    weights = ((full_rows, attn_own.shape[1]), bf16)
    outs = [weights, (group, bf16), (group, bf16)] + kept
    outs += [((3, ctx_count, rows, ff), bf16), ((2, ctx_count, local, width), bf16), ((2, local, width), f32)]
    chunks = width // 256
    scratch = [weights, ((3, full_rows, ff), bf16), (group, bf16), (group, bf16)] + kept
    scratch += [
        ((dp_count * ctx_count, 8, small_own.shape[1]), f32),
        ((chunks, rows, 256), f32),
        ((chunks, rows, 256), f32),
        ((2, 3, rows, ff), bf16),
        ((2, 2, seqs, local, width), f32),
        ((2, ctx_count, local, width), bf16),
        ((2, ctx_count, local, width), bf16),
        ((2, ctx_count, local, width), bf16),
        ((2, local, width), f32),
    ]
    dma = pltpu.SemaphoreType.DMA
    return pl.pallas_call(
        functools.partial(forward_kernel, (dp_count, ctx_count, own, qkv_cols, q_cols, gain_cut)),
        out_shape=[jax.ShapeDtypeStruct(shape, kind) for shape, kind in outs],
        in_specs=[vmem, hbm, hbm, hbm, hbm, vmem, vmem, vmem, vmem],
        out_specs=[hbm] * len(outs),
        scratch_shapes=[pltpu.VMEM(*entry) for entry in scratch]
        + [dma((5, ctx_count)) for _ in range(8)]
        + [dma((ctx_count,)), dma((ctx_count,)), dma((chunks,)), dma((chunks,))]
        + [dma((2, 2, ctx_count)) for _ in range(4)]
        + [dma((2, ctx_count)), dma((2, ctx_count)), dma((8,)), dma((20,))],
        compiler_params=pltpu.CompilerParams(
            collective_id=0, has_side_effects=True, vmem_limit_bytes=65 * 1024 * 1024 - 65536
        ),
        name="forward_kernel",
    )(tok, cot, attn_own, mlp_own, small_own, cos, sin, qseg, kseg)


def xor_rank(rank, step, count):
    value = jnp.int32(0)
    bit = 1
    while bit < count:
        digit = lax.rem(rank // bit, 2)
        value = value + bit * (digit + (1 - 2 * digit) * ((step // bit) % 2))
        bit *= 2
    return value


def backward_kernel(
    sizes,
    sum_in,
    own_in,
    zgu_in,
    e_in,
    b_in,
    cot_hbm,
    tok_hbm,
    h_hbm,
    a_hbm,
    q_hbm,
    kv_hbm,
    o_hbm,
    lse_hbm,
    wattn_hbm,
    live_ref,
    row_ref,
    cos_ref,
    sin_ref,
    qseg_ref,
    kseg_ref,
    act_ref,
    dx_ref,
    zin,
    gat_ref,
    rows_ref,
    gout,
    zrc,
    fin,
    mine_ref,
    left_ref,
    right_ref,
    block_ref,
    keep,
    r1,
    r2,
    keep_at,
    send_at,
    r1_at,
    r2_at,
    zin_at,
    hb_ref,
    do_ref,
    prob_ref,
    ds_ref,
    dq_ref,
    dkv_ref,
    dkv_bf,
    dkv_in,
    dqkv_ref,
    part,
    part_in,
    zss,
    zrs,
    fs,
    fr,
    ld,
    kd,
    gd,
    s1,
    v1,
    s2,
    v2,
    s3,
    v3,
    ks,
    kr,
    ps,
    pr,
    gs,
    gr,
    acc_ref,
    sm_in,
    sm_sum,
    cot_ref,
    tok_ref,
    h_ref,
    a_ref,
    q_ref,
    kv_ref,
    o_ref,
    lse_ref,
    wattn,
    in_sem,
):
    dp_count, ctx_count, own, qkv_cols, q_cols = sizes
    dp, ctx, core = lax.axis_index("dp"), lax.axis_index("ctx"), lax.axis_index("tp")
    bf16, f32 = jnp.bfloat16, jnp.float32
    seqs, local, width = cot_ref.shape
    loads = []
    for src, dst in (
        (cot_hbm, cot_ref),
        (tok_hbm, tok_ref),
        (h_hbm, h_ref),
        (a_hbm, a_ref),
        (q_hbm, q_ref),
        (kv_hbm, kv_ref),
        (o_hbm, o_ref),
        (lse_hbm, lse_ref),
        (wattn_hbm, wattn),
    ):
        loads.append(pltpu.make_async_copy(src, dst, in_sem.at[len(loads)]))
    group = own * ctx_count
    ff = zgu_in.shape[3]
    heads = q_cols // 128
    other = 1 - core
    peers = [xor_rank(ctx, step, ctx_count) for step in range(ctx_count)]
    nodes = [xor_rank(dp, step, dp_count) for step in range(dp_count)]
    to_x, to_y, to_core = {"dp": nodes[1]}, {"dp": nodes[2]}, {"tp": other}
    greet([to_x, to_y, to_core] + [{"ctx": peers[step]} for step in range(1, ctx_count)])
    sent = []

    def start(copy):
        copy.start()
        sent.append(copy)
        return copy

    def rows_of(count, size, body):
        def one(index, _):
            body(pl.ds(pl.multiple_of(index * size, size), size))
            return 0

        lax.fori_loop(0, count // size, one, 0)

    z_copy, fin_copy = {}, {}

    def collect_start(index):
        for tile in range(1, ctx_count):
            z_copy[index, tile] = start(
                remote(
                    sum_in.at[index, peers[tile]],
                    zrc.at[index, ctx],
                    zss.at[index, tile],
                    zrs.at[index, tile],
                    {"ctx": peers[tile]},
                )
            )

    def collect_fin(index):
        for tile in range(1, ctx_count):
            z_copy[index, tile].wait_recv()

        def add(piece):
            total = mine_ref[index, piece, :]
            for tile in range(1, ctx_count):
                total = total + zrc[index, peers[tile], piece, :].astype(f32)
            fin[index, core, piece, :] = total

        rows_of(local, 32, add)
        fin_copy[index] = remote(fin.at[index, core], fin.at[index, core], fs.at[index], fr.at[index], to_core)
        fin_copy[index].start()

    halves = {}
    for item in range(3):
        cut = (ff // 256 + 1) * 128
        halves[item] = ((0, cut), (cut, ff)) if item != 1 else ((cut, ff), (0, cut))
    middle = qkv_cols + (wattn.shape[1] - qkv_cols) // 2
    halves[3] = ((qkv_cols, middle), (middle, wattn.shape[1]))
    halves[4] = ((0, qkv_cols // 2), (qkv_cols // 2, qkv_cols))
    first_to, second_to = (to_y, to_x), (to_x, to_y)
    first_keys = ((2, 3), (1, 3))
    one_copy, two_copy, three_copy, keep_copy = {}, {}, {}, {}

    def cols(item, half):
        low, high = halves[item][half]
        return slice(low, high)

    def refs(item):
        if item < 3:
            return keep.at[item], r1.at[item], r2.at[item]
        return keep_at, r1_at, r2_at

    def stage_one(item, half):
        span = cols(item, half)
        for slot, key in enumerate(first_keys[half]):
            src = gout.at[item, key, :, span] if item < 3 else send_at.at[slot, :, span]
            one_copy[item, half, slot] = start(
                remote(
                    src,
                    refs(item)[1].at[slot, :, span],
                    s1.at[item, half, slot],
                    v1.at[item, half, slot],
                    first_to[half],
                )
            )

    def stage_two(item, half):
        span = cols(item, half)
        mine, first, second = refs(item)
        if item < 3:
            keep_copy[item, half].wait()
        one_copy[item, half, 1].wait_recv()

        def add(piece):
            mine[1, piece, span] = (mine[1, piece, span].astype(f32) + first[1, piece, span].astype(f32)).astype(bf16)

        rows_of(group, 96, add)
        two_copy[item, half] = start(
            remote(mine.at[1, :, span], second.at[:, span], s2.at[item, half], v2.at[item, half], second_to[half])
        )

    def stage_three(item, half):
        span = cols(item, half)
        mine, first, second = refs(item)
        if item < 3:
            keep_copy[item, 2].wait() if half == 0 else None
        one_copy[item, half, 0].wait_recv()
        two_copy[item, half].wait_recv()

        def total(piece):
            return mine[0, piece, span].astype(f32) + first[0, piece, span].astype(f32) + second[piece, span].astype(f32)

        if item >= 3:
            gat_ref[:, span] = total(pl.ds(pl.multiple_of(ctx * own, own), own))

        def add(piece):
            mine[0, piece, span] = total(piece).astype(bf16)

        rows_of(group, 96, add)
        target = zin.at[item] if item < 3 else zin_at
        for tile in range(1, ctx_count):
            piece = pl.ds(pl.multiple_of(peers[tile] * own, own), own)
            three_copy[item, half, tile] = start(
                remote(
                    mine.at[0, piece, span],
                    target.at[ctx, :, span],
                    s3.at[item, half, tile],
                    v3.at[item, half, tile],
                    {"ctx": peers[tile]},
                )
            )
        if item < 3:
            piece = pl.ds(pl.multiple_of(ctx * own, own), own)
            copy = pltpu.make_async_copy(mine.at[0, piece, span], target.at[ctx, :, span], kd.at[item, 3 + half])
            copy.start()
            three_copy[item, half, 0] = copy

    def stage_four(item, half):
        span = cols(item, half)
        for tile in range(1, ctx_count):
            three_copy[item, half, tile].wait_recv()
        if item < 3:
            three_copy[item, half, 0].wait()
        else:
            total = gat_ref[:, span]
            for tile in range(1, ctx_count):
                total = total + zin_at[peers[tile], :, span].astype(f32)
            gat_ref[:, span] = total

    collect_start(0)
    mine_copy = pltpu.make_async_copy(own_in, mine_ref, ld.at[0])
    mine_copy.start()
    collect_start(1)
    for copy in loads:
        copy.start()

    left_from = (e_in, b_in, b_in)
    right_slot = (0, 1, 2)

    def load_left(count):
        item, key = divmod(count, dp_count)
        key = dp_count - 1 - key
        span = pl.ds(pl.multiple_of(nodes[key] * group, group), group)
        copy = pltpu.make_async_copy(
            left_from[item].at[:, :, :, span], left_ref.at[count % 2], gd.at[count % 2]
        )
        copy.start()
        return copy

    def load_right(item):
        copy = pltpu.make_async_copy(zgu_in.at[right_slot[item]], right_ref, gd.at[2])
        copy.start()
        return copy

    out_copy = {}

    def block(count, left_copy):
        item, key = divmod(count, dp_count)
        key = dp_count - 1 - key
        slot = count % 2
        left_copy.wait()

        def columns(low, size):
            span = pl.ds(low, size)
            val = lax.dot_general(
                left_ref[slot].reshape(-1, group),
                right_ref[:, :, span].reshape(-1, size),
                (((0,), (0,)), ((), ())),
                preferred_element_type=f32,
            )
            block_ref[slot, :, span] = val.astype(bf16)

        def one(index, _):
            columns(pl.multiple_of(index * 256, 256), 256)
            return 0

        lax.fori_loop(0, ff // 256, one, 0)
        if ff % 256:
            columns(ff // 256 * 256, ff % 256)
        out_copy[count] = pltpu.make_async_copy(block_ref.at[slot], gout.at[item, key], gd.at[3 + slot])
        out_copy[count].start()

    def hand_over(count):
        item, key = divmod(count, dp_count)
        key = dp_count - 1 - key
        if key == 2:
            stage_one(item, 0)
        if key == 1:
            stage_one(item, 1)
        if key == 0:
            for half in range(2):
                span = cols(item, half)
                copy = pltpu.make_async_copy(
                    gout.at[item, 1 + half, :, span], keep.at[item, 1, :, span], kd.at[item, half]
                )
                copy.start()
                keep_copy[item, half] = copy
            copy = pltpu.make_async_copy(gout.at[item, 0], keep.at[item, 0], kd.at[item, 2])
            copy.start()
            keep_copy[item, 2] = copy

    right_copy = load_right(0)
    left_copy = load_left(0)
    blocks = 3 * dp_count
    for count in range(blocks):
        following = load_left(count + 1) if count + 1 < blocks else None
        if count % dp_count == 0:
            right_copy.wait()
        block(count, left_copy)
        left_copy = following
        if count % dp_count == dp_count - 1 and count + 1 < blocks:
            right_copy = load_right(count // dp_count + 1)
        if count:
            out_copy[count - 1].wait()
            hand_over(count - 1)
    out_copy[blocks - 1].wait()
    hand_over(blocks - 1)
    mine_copy.wait()
    for copy in loads:
        copy.wait()

    pending = []
    for item in range(3):
        pending += [(stage_two, item, 0), (stage_two, item, 1)]
    for item in range(3):
        pending += [(stage_three, item, 0), (stage_three, item, 1)]

    def pump(count):
        for _ in range(min(count, len(pending))):
            action, item, half = pending.pop(0)
            action(item, half)

    collect_fin(0)
    pump(1)
    fin_copy[0].wait()

    size = 32
    per_seq = local // size

    def split(index):
        return index // per_seq, pl.ds(pl.multiple_of(lax.rem(index, per_seq) * size, size), size)

    acc_ref[...] = jnp.zeros_like(acc_ref)

    def norm_mid(index, total):
        seq, piece = split(index)
        whole = pl.ds(pl.multiple_of(index * size, size), size)
        grad, val = fin[0, seq, piece, :], h_ref[whole, :]
        inv = lax.rsqrt(jnp.mean(val * val, axis=-1, keepdims=True) + norm_eps)
        weighted = grad * row_ref[1:2, :]
        inner = jnp.mean(weighted * val, axis=-1, keepdims=True)
        out = cot_ref[seq, piece, :].astype(f32) + (inv * weighted - val * (inv * inv * inv) * inner)
        dx_ref[seq, piece, :] = out
        hb_ref[whole, :] = out.astype(bf16)
        return total + jnp.sum(grad * val * inv, axis=0, keepdims=True)

    acc_ref[1:2, :] = lax.fori_loop(0, seqs * per_seq, norm_mid, jnp.zeros((1, width), f32))
    pump(1)

    for low in range(0, q_cols, 256):
        val = jnp.dot(hb_ref[...], wattn[:, qkv_cols + low : qkv_cols + low + 256], preferred_element_type=f32).astype(bf16)
        for head_low in (0, 128):
            for seq in range(seqs):
                do_ref[seq, (low + head_low) // 128] = val[seq * local : (seq + 1) * local, head_low : head_low + 128]
    pump(1)

    keys = kv_ref.shape[2]
    key_no = lax.broadcasted_iota(jnp.int32, (local, keys), 1)
    query_no = lax.broadcasted_iota(jnp.int32, (local, keys), 0) + ctx * local
    scale = HEAD_DIM ** (-0.5)
    kv_copies = []
    for seq in range(seqs):
        seen = (qseg_ref[seq] == kseg_ref[seq]) & (key_no <= query_no)
        hide = jnp.where(seen, 0.0, masked_score)

        def one_head(head, _):
            query, grad_out, keys_bf, values_bf = q_ref[seq, head], do_ref[seq, head], kv_ref[seq, 0], kv_ref[seq, 1]
            score = lax.dot_general(query, keys_bf, (((1,), (1,)), ((), ())), preferred_element_type=f32) * scale
            prob = jnp.exp(jnp.where(hide < 0.0, masked_score, score) - lse_ref[seq, head])
            grad_prob = lax.dot_general(grad_out, values_bf, (((1,), (1,)), ((), ())), preferred_element_type=f32)
            row_dot = jnp.sum(grad_out.astype(f32) * o_ref[seq, head].astype(f32), axis=-1, keepdims=True)
            grad_score = (prob * (grad_prob - row_dot) * scale).astype(bf16)
            prob_ref[head] = prob.astype(bf16)
            ds_ref[head] = grad_score
            grad_query = jnp.dot(grad_score, keys_bf, preferred_element_type=f32)
            turned = grad_query * cos_ref[seq * local : (seq + 1) * local, :] + pltpu.roll(
                grad_query * sin_ref[seq * local : (seq + 1) * local, :], 64, 1
            )
            dq_ref[seq, head] = turned
            return 0

        lax.fori_loop(0, heads, one_head, 0)
        stacked = (heads * local, 128)
        dkv_ref[seq, 0] = lax.dot_general(
            ds_ref[...].reshape(heads * local, keys),
            q_ref[seq].reshape(stacked),
            (((0,), (0,)), ((), ())),
            preferred_element_type=f32,
        )
        dkv_ref[seq, 1] = lax.dot_general(
            prob_ref[...].reshape(heads * local, keys),
            do_ref[seq].reshape(stacked),
            (((0,), (0,)), ((), ())),
            preferred_element_type=f32,
        )
        dkv_bf[seq] = dkv_ref[seq].astype(bf16)
        pump(2)
    for tile in range(1, ctx_count):
        piece = pl.ds(pl.multiple_of(peers[tile] * local, local), local)
        kv_copies.append(
            start(remote(dkv_bf.at[:, :, piece, :], dkv_in.at[ctx], ks.at[tile], kr.at[tile], {"ctx": peers[tile]}))
        )

    def weight_blocks(item, left_ref, right, low, high):
        for key in (3, 2, 1, 0):
            left = left_ref[:, pl.ds(pl.multiple_of(nodes[key] * group, group), group)]
            val = lax.dot_general(left, right, (((0,), (0,)), ((), ())), preferred_element_type=f32).astype(bf16)
            for half in range(2):
                span = cols(item, half)
                piece = val[:, span.start - low : span.stop - low]
                if key in first_keys[half]:
                    send_at[first_keys[half].index(key), :, span] = piece
                else:
                    keep_at[0 if key == 0 else 1, :, span] = piece
            if key == 2:
                stage_one(item, 0)
            if key == 1:
                stage_one(item, 1)

    o_rows = jnp.concatenate(
        [jnp.concatenate([o_ref[seq, head] for head in range(heads)], 1) for seq in range(seqs)], 0
    )
    weight_blocks(3, hb_ref, o_rows, qkv_cols, wattn.shape[1])

    for seq in range(seqs):
        for head in range(heads):
            val = dq_ref[seq, head]
            span = slice(head * 128, (head + 1) * 128)
            dqkv_ref[seq * local : (seq + 1) * local, span] = val.astype(bf16)
            acc_ref[2:3, span] = acc_ref[2:3, span] + jnp.sum(val, axis=0, keepdims=True)
    for copy in kv_copies:
        copy.wait_recv()
    own_keys = pl.ds(pl.multiple_of(ctx * local, local), local)
    for seq in range(seqs):
        for part_no in range(2):
            val = dkv_ref[seq, part_no, own_keys, :]
            for tile in range(1, ctx_count):
                val = val + dkv_in[peers[tile], seq, part_no].astype(f32)
            here = slice(seq * local, (seq + 1) * local)
            if part_no == 0:
                val = val * cos_ref[here, :] + pltpu.roll(val * sin_ref[here, :], 64, 1)
            span = slice(q_cols + part_no * 128, q_cols + (part_no + 1) * 128)
            dqkv_ref[here, span] = val.astype(bf16)
            acc_ref[2:3, span] = acc_ref[2:3, span] + jnp.sum(val, axis=0, keepdims=True)
    weight_blocks(4, a_ref, dqkv_ref[...], 0, qkv_cols)

    part_copies = []
    for index in range(width // 256):
        part[index] = lax.dot_general(
            dqkv_ref[...],
            wattn[index * 256 : (index + 1) * 256, :qkv_cols],
            (((1,), (1,)), ((), ())),
            preferred_element_type=f32,
        )
        part_copies.append(
            start(remote(part.at[index], part_in.at[index], ps.at[index], pr.at[index], to_core))
        )
    pump(4)
    for index, copy in enumerate(part_copies):
        copy.wait_recv()
        for seq in range(seqs):
            here = slice(seq * local, (seq + 1) * local)
            fin[0, seq, :, index * 256 : (index + 1) * 256] = part[index, here, :] + part_in[index, here, :]

    def norm_in(index, total):
        seq, piece = split(index)
        whole = pl.ds(pl.multiple_of(index * size, size), size)
        grad, val = fin[0, seq, piece, :], tok_ref[whole, :].astype(f32)
        inv = lax.rsqrt(jnp.mean(val * val, axis=-1, keepdims=True) + norm_eps)
        weighted = grad * row_ref[0:1, :]
        inner = jnp.mean(weighted * val, axis=-1, keepdims=True)
        dx_ref[seq, piece, :] = dx_ref[seq, piece, :] + (inv * weighted - val * (inv * inv * inv) * inner)
        return total + jnp.sum(grad * val * inv, axis=0, keepdims=True)

    acc_ref[0:1, :] = lax.fori_loop(0, seqs * per_seq, norm_in, jnp.zeros((1, width), f32))

    small_copies = [
        start(remote(acc_ref, sm_in.at[tile], gs.at[tile], gr.at[tile], {"ctx": peers[tile]}))
        for tile in range(1, ctx_count)
    ]
    collect_fin(1)
    while pending:
        pump(1)
    for item in (3, 4):
        for half in range(2):
            stage_two(item, half)
    total = acc_ref[...]
    for tile, copy in enumerate(small_copies):
        copy.wait_recv()
        total = total + sm_in[tile + 1]
    sm_sum[0] = total
    for turn, target in ((0, to_x), (1, to_y)):
        slot = ctx_count + turn
        copy = start(remote(sm_sum.at[turn], sm_in.at[slot], gs.at[slot], gr.at[slot], target))
        if turn == 0:
            fin_copy[1].wait()
        copy.wait_recv()
        total = sm_sum[turn] + sm_in[slot]
        if turn == 0:
            sm_sum[1] = total
        else:
            rows_ref[...] = total

    def act_rows(index, _):
        seq, piece = split(index)
        whole = pl.ds(pl.multiple_of(index * size, size), size)
        act_ref[seq, piece, :] = (h_ref[whole, :] + fin[1, seq, piece, :]) * live_ref[seq, piece, :]
        return 0

    lax.fori_loop(0, seqs * per_seq, act_rows, 0)
    for item in (3, 4):
        for half in range(2):
            stage_three(item, half)
    for item in (0, 1, 2, 3, 4):
        for half in range(2):
            stage_four(item, half)
    for copy in sent:
        copy.wait_send()


def backward_call(inputs, sizes):
    dp_count, ctx_count, own, qkv_cols, q_cols = sizes
    bf16, f32 = jnp.bfloat16, jnp.float32
    vmem, hbm = pl.BlockSpec(memory_space=pltpu.VMEM), pl.BlockSpec(memory_space=pl.ANY)
    held = inputs[5:14]
    seqs, local, width = held[0].shape
    ff = inputs[2].shape[3]
    group = own * ctx_count
    rows, keys = seqs * local, local * ctx_count
    heads = q_cols // 128
    attn_cols = held[8].shape[1]
    chunks = width // 256
    outs = [
        ((seqs, local, width), f32, vmem),
        ((seqs, local, width), f32, vmem),
        ((3, ctx_count, own, ff), bf16, hbm),
        ((own, attn_cols), f32, vmem),
        ((8, width), f32, vmem),
        ((3, dp_count, group, ff), bf16, hbm),
    ]
    scratch = [
        ((2, ctx_count, local, width), bf16),
        ((2, seqs, local, width), f32),
        ((2, local, width), f32),
        ((2, ctx_count, seqs, local, group), bf16),
        ((ctx_count, rows, ff), bf16),
        ((2, group, ff), bf16),
        ((3, 2, group, ff), bf16),
        ((3, 2, group, ff), bf16),
        ((3, group, ff), bf16),
        ((2, group, attn_cols), bf16),
        ((2, group, attn_cols), bf16),
        ((2, group, attn_cols), bf16),
        ((group, attn_cols), bf16),
        ((ctx_count, own, attn_cols), bf16),
        ((rows, width), bf16),
        ((seqs, heads, local, 128), bf16),
        ((heads, local, keys), bf16),
        ((heads, local, keys), bf16),
        ((seqs, heads, local, 128), f32),
        ((seqs, 2, keys, 128), f32),
        ((seqs, 2, keys, 128), bf16),
        ((ctx_count, seqs, 2, local, 128), bf16),
        ((rows, qkv_cols), bf16),
        ((chunks, rows, 256), f32),
        ((chunks, rows, 256), f32),
    ]
    dma = pltpu.SemaphoreType.DMA
    sems = [dma((2, ctx_count)), dma((2, ctx_count)), dma((2,)), dma((2,)), dma((2,)), dma((3, 5)), dma((5,))]
    sems += [
        dma(shape)
        for shape in ((5, 2, 2), (5, 2), (5, 2, ctx_count), (ctx_count,), (chunks,), (ctx_count + 2,))
        for _ in range(2)
    ]
    final = [((8, width), f32), ((ctx_count + 2, 8, width), f32), ((2, 8, width), f32)]
    final += [(array.shape, array.dtype) for array in held]
    return pl.pallas_call(
        functools.partial(backward_kernel, sizes),
        out_shape=[jax.ShapeDtypeStruct(shape, kind) for shape, kind, _ in outs],
        in_specs=[hbm] * 14 + [vmem] * (len(inputs) - 14),
        out_specs=[spec for _, _, spec in outs],
        scratch_shapes=[pltpu.VMEM(*entry) for entry in scratch]
        + sems
        + [pltpu.VMEM(*entry) for entry in final]
        + [dma((len(held),))],
        compiler_params=pltpu.CompilerParams(
            collective_id=1, has_side_effects=True, vmem_limit_bytes=65 * 1024 * 1024 - 65536
        ),
        name="backward_kernel",
    )(*inputs)


def on_device_kernels(
    tokens,
    cotangent,
    segments,
    positions,
    counts,
    attn_gain,
    q_weight,
    q_bias,
    k_weight,
    v_weight,
    kv_bias,
    o_weight,
    mlp_gain,
    gate_weight,
    up_weight,
    down_weight,
):
    dp_count, ctx_count = lax.axis_size("dp"), lax.axis_size("ctx")
    dp_rank, ctx_rank, core = lax.axis_index("dp"), lax.axis_index("ctx"), lax.axis_index("tp")
    seq_count, local_len, width = tokens.shape
    full_len = segments.shape[1]
    row_count = seq_count * local_len
    half_width = width // 2
    own_rows = q_weight.shape[1]
    group_rows = own_rows * ctx_count
    q_cols, k_cols, ff_cols = q_weight.shape[2], k_weight.shape[2], gate_weight.shape[2]
    kv_local = k_cols // HEAD_DIM
    group_size = q_cols // k_cols
    qkv_cols = q_cols + 2 * k_cols
    lane = 128
    ff_block = -(-ff_cols // (lane * ctx_count)) * lane
    ff_pad = ff_block * ctx_count - ff_cols
    f32, bf16 = jnp.float32, jnp.bfloat16

    parts = (attn_gain[0], mlp_gain[0], q_bias[0].reshape(-1), kv_bias[0].reshape(-1))
    cuts = [0]
    for part_vec in parts:
        cuts.append(cuts[-1] + part_vec.shape[0])
    small_own = jnp.pad(jnp.concatenate(parts).astype(f32)[None], ((0, 7), (0, 0)))
    attn_own = jnp.concatenate([q_weight[0], k_weight[0], v_weight[0], o_weight[0]], 1)
    mlp_own = jnp.stack(
        [
            jnp.pad(weight[0], ((0, 0), (0, ff_pad))).reshape(own_rows, ctx_count, ff_block).transpose(1, 0, 2)
            for weight in (gate_weight, up_weight, down_weight)
        ]
    )
    live_seq = (jnp.arange(seq_count, dtype=jnp.int32) < counts[0]).astype(f32)
    cot_live = (cotangent.astype(f32) * live_seq[:, None, None]).astype(bf16)
    query_seg = lax.dynamic_slice_in_dim(segments, ctx_rank * local_len, local_len, 1)
    cos_tab, sin_tab = rope_tables(positions.reshape(-1))
    sign = jnp.where(jnp.arange(HEAD_DIM) < HEAD_DIM // 2, -1.0, 1.0)
    (
        w_attn,
        grad_all,
        mid_all,
        resid_mid,
        normed_in,
        query_hm,
        keyval_hm,
        attn_hm,
        log_total,
        small_rows,
        hidden_and_grads,
        part_sums,
        part_own,
    ) = forward_call(
        tokens.reshape(-1, width),
        cot_live,
        attn_own,
        mlp_own,
        small_own,
        cos_tab,
        sin_tab * sign,
        query_seg[:, :, None],
        segments[:, None, :],
        qkv_cols,
        q_cols,
        cuts,
    )
    activations, input_grad, grad_ff, grad_w_attn, rows_sum, _ = backward_call(
        (
            part_sums,
            part_own,
            hidden_and_grads,
            grad_all,
            mid_all,
            cot_live,
            tokens.reshape(-1, width),
            resid_mid,
            normed_in,
            query_hm,
            keyval_hm,
            attn_hm,
            log_total,
            w_attn,
            jnp.broadcast_to(live_seq[:, None, None], (seq_count, local_len, 1)),
            small_rows,
            cos_tab,
            sin_tab * sign,
            query_seg[:, :, None],
            segments[:, None, :],
        ),
        (dp_count, ctx_count, own_rows, qkv_cols, q_cols),
    )
    grad_w_down, grad_w_gate, grad_w_up = (
        jnp.concatenate([grad_ff[item, block] for block in range(ctx_count)], 1)[:, :ff_cols].astype(f32)
        for item in range(3)
    )
    rank = dp_rank * ctx_count + ctx_rank

    def own_part(vector, size):
        return lax.dynamic_slice_in_dim(vector, rank * size, size, 0)

    bias_kv = jnp.concatenate(
        [
            rows_sum[2, q_cols : q_cols + k_cols].reshape(kv_local, -1).T,
            rows_sum[2, q_cols + k_cols : qkv_cols].reshape(kv_local, -1).T,
        ],
        0,
    ).reshape(-1)
    own = [
        own_part(rows_sum[0], own_rows)[None],
        own_part(rows_sum[1], own_rows)[None],
        own_part(rows_sum[2, :q_cols].reshape(kv_local, -1).T.reshape(-1), cuts[3] - cuts[2]),
        own_part(bias_kv, cuts[4] - cuts[3]),
    ]
    grad_w_qkv, grad_w_out = grad_w_attn[:, :qkv_cols], grad_w_attn[:, qkv_cols:]
    return (
        activations.reshape(tokens.shape),
        input_grad.reshape(tokens.shape),
        own[0],
        grad_w_qkv[None, :, :q_cols],
        own[2].reshape(q_bias.shape),
        grad_w_qkv[None, :, q_cols : q_cols + k_cols],
        grad_w_qkv[None, :, q_cols + k_cols :],
        own[3].reshape(kv_bias.shape),
        grad_w_out[None],
        own[1],
        grad_w_gate[None],
        grad_w_up[None],
        grad_w_down[None],
    )


def solution(mesh):
    in_specs = (
        P("dp", "ctx", None),
        P("dp", "ctx", None),
        P("dp", None),
        P("dp", "ctx"),
        P("dp"),
        P(None, ("dp", "ctx")),
        P(None, ("dp", "ctx"), "tp"),
        P(None, ("dp", "ctx"), "tp"),
        P(None, ("dp", "ctx"), "tp"),
        P(None, ("dp", "ctx"), "tp"),
        P(None, ("dp", "ctx"), "tp"),
        P(None, ("dp", "ctx"), "tp"),
        P(None, ("dp", "ctx")),
        P(None, ("dp", "ctx"), "tp"),
        P(None, ("dp", "ctx"), "tp"),
        P(None, ("dp", "ctx"), "tp"),
    )
    out_specs = (
        P("dp", "ctx", None),
        P("dp", "ctx", None),
        P(None, ("dp", "ctx")),
        P(None, ("dp", "ctx"), "tp"),
        P(None, ("dp", "ctx"), "tp"),
        P(None, ("dp", "ctx"), "tp"),
        P(None, ("dp", "ctx"), "tp"),
        P(None, ("dp", "ctx"), "tp"),
        P(None, ("dp", "ctx"), "tp"),
        P(None, ("dp", "ctx")),
        P(None, ("dp", "ctx"), "tp"),
        P(None, ("dp", "ctx"), "tp"),
        P(None, ("dp", "ctx"), "tp"),
    )
    kernels_fit = mesh.shape["dp"] == 4 and mesh.shape["ctx"] == 4 and mesh.shape["tp"] == KV_HEADS
    return jax.shard_map(
        on_device_kernels if kernels_fit else on_device, mesh=mesh, in_specs=in_specs, out_specs=out_specs, check_vma=False
    )
```

```python
import functools

import jax
import jax.numpy as jnp
from jax import lax
from jax.experimental import pallas as pl
from jax.experimental.pallas import tpu as pltpu
from jax.sharding import PartitionSpec as P

HEADS = 12
KV_HEADS = 2
HEAD_DIM = 128
LAYERS = 1


theta_base = 1000000.0
norm_eps = 1e-06
masked_score = -1e30


def mat_mul(left, right):
    return jnp.dot(left, right, preferred_element_type=jnp.float32)


def mat_mul_t(left, right):
    return lax.dot_general(
        left, right, (((1,), (1,)), ((), ())), preferred_element_type=jnp.float32
    )


def rows_mul(left, right):
    return lax.dot_general(
        left, right, (((0,), (0,)), ((), ())), preferred_element_type=jnp.float32
    )


def rope_tables(pos_vals):
    half_dim = HEAD_DIM // 2
    frequency = theta_base ** (-(jnp.arange(half_dim, dtype=jnp.float32) * (2.0 / HEAD_DIM)))
    angles = pos_vals.astype(jnp.float32)[..., None] * frequency
    cos_half = jnp.cos(angles)
    sin_half = jnp.sin(angles)
    return (jnp.concatenate([cos_half, cos_half], -1), jnp.concatenate([sin_half, sin_half], -1))


def rotate(values, cos_tab, sin_tab):
    half_dim = values.shape[-1] // 2
    turned = jnp.concatenate([-values[..., half_dim:], values[..., :half_dim]], -1)
    return values * cos_tab + turned * sin_tab


def unrotate(grad_vals, cos_tab, sin_tab):
    half_dim = grad_vals.shape[-1] // 2
    scaled = grad_vals * sin_tab
    turned = jnp.concatenate([scaled[..., half_dim:], -scaled[..., :half_dim]], -1)
    return grad_vals * cos_tab + turned


def norm_forward(residual, gain_vec):
    inv_rms = lax.rsqrt(jnp.mean(residual * residual, axis=-1, keepdims=True) + norm_eps)
    normed = (residual * inv_rms * gain_vec.astype(jnp.float32)).astype(jnp.bfloat16)
    return (inv_rms, normed)


def norm_backward(residual, inv_rms, gain_vec, grad_normed):
    weighted = grad_normed * gain_vec.astype(jnp.float32)
    inner_mean = jnp.mean(weighted * residual, axis=-1, keepdims=True)
    grad_resid = inv_rms * weighted - residual * (inv_rms * inv_rms * inv_rms) * inner_mean
    grad_gain = jnp.sum(grad_normed * residual * inv_rms, axis=0)
    return (grad_resid, grad_gain)


def split_heads(keys_all, values_all):
    seq_count, full_len, kv_width = keys_all.shape
    kv_local = kv_width // HEAD_DIM
    return (
        keys_all.reshape(seq_count, full_len, kv_local, HEAD_DIM),
        values_all.reshape(seq_count, full_len, kv_local, HEAD_DIM),
    )


def attend_forward(query_bf, keys_all, values_all, allowed):
    key_heads, value_heads = split_heads(keys_all, values_all)
    scores = jnp.einsum(
        "bqkgd,bskd->bkgqs", query_bf, key_heads, preferred_element_type=jnp.float32
    ) * HEAD_DIM ** (-0.5)
    scores = jnp.where(allowed[:, None, None], scores, masked_score)
    top_score = jnp.max(scores, axis=-1, keepdims=True)
    shifted_exp = jnp.exp(scores - top_score)
    totals = jnp.sum(shifted_exp, axis=-1, keepdims=True)
    prob_bf = (shifted_exp / totals).astype(jnp.bfloat16)
    output = jnp.einsum(
        "bkgqs,bskd->bqkgd", prob_bf, value_heads, preferred_element_type=jnp.float32
    )
    return (output.astype(jnp.bfloat16), top_score + jnp.log(totals))


def attend_backward(query_bf, keys_all, values_all, attn_bf, log_total, grad_attn, allowed):
    key_heads, value_heads = split_heads(keys_all, values_all)
    scores = jnp.einsum(
        "bqkgd,bskd->bkgqs", query_bf, key_heads, preferred_element_type=jnp.float32
    ) * HEAD_DIM ** (-0.5)
    prob_full = jnp.exp(jnp.where(allowed[:, None, None], scores, masked_score) - log_total)
    prob_bf = prob_full.astype(jnp.bfloat16)
    grad_value = jnp.einsum(
        "bkgqs,bqkgd->bskd", prob_bf, grad_attn, preferred_element_type=jnp.float32
    )
    grad_prob = jnp.einsum(
        "bqkgd,bskd->bkgqs", grad_attn, value_heads, preferred_element_type=jnp.float32
    )
    row_dot = jnp.sum(grad_attn.astype(jnp.float32) * attn_bf.astype(jnp.float32), axis=-1)
    row_dot = jnp.transpose(row_dot, (0, 2, 3, 1))[..., None]
    grad_score = (prob_full * (grad_prob - row_dot) * HEAD_DIM ** (-0.5)).astype(jnp.bfloat16)
    grad_query = jnp.einsum(
        "bkgqs,bskd->bqkgd", grad_score, key_heads, preferred_element_type=jnp.float32
    )
    grad_key = jnp.einsum(
        "bkgqs,bqkgd->bskd", grad_score, query_bf, preferred_element_type=jnp.float32
    )
    return (grad_query, grad_key.reshape(keys_all.shape), grad_value.reshape(values_all.shape))


def xor_permute(value, axis_name, step):
    count = lax.axis_size(axis_name)
    return lax.ppermute(value, axis_name, [(rank, rank ^ step) for rank in range(count)])


def axis_bits(axis_name):
    return [1 << shift for shift in range(lax.axis_size(axis_name).bit_length() - 1)]


def partner(value):
    return xor_permute(value, "tp", 1)


def place(pieces, rank, dim):
    width = pieces[0].shape[dim]
    whole_shape = list(pieces[0].shape)
    whole_shape[dim] = width * len(pieces)
    whole = jnp.zeros(whole_shape, pieces[0].dtype)
    for offset, piece in enumerate(pieces):
        whole = lax.dynamic_update_slice_in_dim(whole, piece, (rank ^ offset) * width, dim)
    return whole


def join_halves(mine, other, core, dim):
    return jnp.where(
        core == 0, jnp.concatenate([mine, other], dim), jnp.concatenate([other, mine], dim)
    )


def gather_direct(value, axis_name):
    count = lax.axis_size(axis_name)
    return [value] + [xor_permute(value, axis_name, step) for step in range(1, count)]


def gather_halves(value, axis_name):
    rows = value.shape[0]
    half = rows // 2
    bits = axis_bits(axis_name)
    parts = []
    for piece, order in ((value[:half], bits), (value[half:], bits[::-1])):
        held = {0: piece}
        for bit in order:
            for key in list(held):
                held[key | bit] = xor_permute(held[key], axis_name, bit)
        parts.append(held)
    return [(parts[0][key], parts[1][key]) for key in range(len(parts[0]))]


def scatter_halves(blocks, axis_name):
    half = blocks[0].shape[0] // 2
    bits = axis_bits(axis_name)
    done = []
    for low, high, order in ((0, half, bits[::-1]), (half, 2 * half, bits)):
        held = {key: block[low:high] for key, block in enumerate(blocks)}
        for bit in order:
            for key in [key for key in held if key & bit]:
                sent = held.pop(key).astype(jnp.bfloat16)
                held[key ^ bit] = held[key ^ bit] + xor_permute(sent, axis_name, bit).astype(jnp.float32)
        done.append(held[0])
    return jnp.concatenate(done, 0)


def scatter_small(blocks, axis_name):
    held = dict(enumerate(blocks))
    for bit in axis_bits(axis_name)[::-1]:
        for key in [key for key in held if key & bit]:
            held[key ^ bit] = held[key ^ bit] + xor_permute(held.pop(key), axis_name, bit)
    return held[0]


def scatter_direct(block_of, axis_name):
    total = block_of(0)
    for step in range(1, lax.axis_size(axis_name)):
        got = xor_permute(block_of(step).astype(jnp.bfloat16), axis_name, step)
        total = total + got.astype(jnp.float32)
    return total


def rows_at(value, index, size):
    return lax.dynamic_slice_in_dim(value, index * size, size, 0)


def columns_at(value, index, size):
    return lax.dynamic_slice_in_dim(value, index * size, size, 1)


def on_device(
    tokens,
    cotangent,
    segments,
    positions,
    counts,
    attn_gain,
    q_weight,
    q_bias,
    k_weight,
    v_weight,
    kv_bias,
    o_weight,
    mlp_gain,
    gate_weight,
    up_weight,
    down_weight,
):
    dp_count, ctx_count = lax.axis_size("dp"), lax.axis_size("ctx")
    dp_rank, ctx_rank, core = lax.axis_index("dp"), lax.axis_index("ctx"), lax.axis_index("tp")
    seq_count, local_len, width = tokens.shape
    full_len = segments.shape[1]
    row_count = seq_count * local_len
    half_width = width // 2
    own_rows = q_weight.shape[1]
    group_rows = own_rows * ctx_count
    q_cols, k_cols, ff_cols = q_weight.shape[2], k_weight.shape[2], gate_weight.shape[2]
    kv_local = k_cols // HEAD_DIM
    group_size = q_cols // k_cols
    qkv_cols = q_cols + 2 * k_cols
    lane = 128
    ff_block = -(-ff_cols // (lane * ctx_count)) * lane
    ff_pad = ff_block * ctx_count - ff_cols
    f32, bf16 = jnp.float32, jnp.bfloat16

    small = jnp.concatenate(
        [attn_gain[0], mlp_gain[0], q_bias[0].reshape(-1), kv_bias[0].reshape(-1)]
    )[None]
    sizes = (attn_gain.shape[1], mlp_gain.shape[1], q_bias.shape[1] * q_bias.shape[2], kv_bias.shape[1] * kv_bias.shape[2])
    small_ctx = place(gather_direct(small, "ctx"), ctx_rank, 0)[None]
    held = {0: small_ctx}
    for bit in axis_bits("dp"):
        for key in list(held):
            held[key | bit] = xor_permute(held[key], "dp", bit)
    small_all = place([held[key] for key in range(dp_count)], dp_rank, 0)
    small_all = small_all.reshape(dp_count * ctx_count, -1)
    cuts = [0]
    for size in sizes:
        cuts.append(cuts[-1] + size)
    gain_in, gain_mid, b_query, b_keyval = (
        small_all[:, low:high].reshape(-1) for low, high in zip(cuts[:-1], cuts[1:])
    )
    b_query = b_query.reshape(-1, kv_local).T.reshape(-1).astype(f32)
    b_keyval = b_keyval.reshape(-1, kv_local).astype(f32)
    b_qkv = jnp.concatenate(
        [b_query, b_keyval[:HEAD_DIM].T.reshape(-1), b_keyval[HEAD_DIM:].T.reshape(-1)]
    )

    attn_own = jnp.concatenate([q_weight[0], k_weight[0], v_weight[0], o_weight[0]], 1)
    attn_group = place(gather_direct(attn_own, "ctx"), ctx_rank, 0)
    attn_pairs = gather_halves(attn_group, "dp")
    w_attn = place([jnp.concatenate(pair, 0) for pair in attn_pairs], dp_rank, 0)
    w_qkv, w_out = w_attn[:, :qkv_cols], w_attn[:, qkv_cols:]

    live_seq = (jnp.arange(seq_count, dtype=jnp.int32) < counts[0]).astype(f32)
    live_rows = jnp.repeat(live_seq, local_len)[:, None]
    grad_out = cotangent.astype(f32).reshape(-1, width) * live_rows

    def spread(rows_bf):
        mine = jnp.concatenate(gather_direct(columns_at(rows_bf, core, half_width), "ctx"), 0)
        return join_halves(mine, partner(mine), core, 1)

    grad_all = spread(grad_out.astype(bf16))

    def spread_weight(weight):
        padded = jnp.pad(weight[0], ((0, 0), (0, ff_pad)))
        pieces = [columns_at(padded, ctx_rank, ff_block)]
        for step in range(1, ctx_count):
            pieces.append(xor_permute(columns_at(padded, ctx_rank ^ step, ff_block), "ctx", step))
        pairs = gather_halves(place(pieces, ctx_rank, 0), "dp")
        return place([jnp.concatenate(pair, 0) for pair in pairs], dp_rank, 0)

    w_gate = spread_weight(gate_weight)
    w_up = spread_weight(up_weight)
    w_down = spread_weight(down_weight)

    query_pos = ctx_rank * local_len + jnp.arange(local_len, dtype=jnp.int32)
    key_pos = jnp.arange(full_len, dtype=jnp.int32)
    query_seg = lax.dynamic_slice_in_dim(segments, ctx_rank * local_len, local_len, 1)
    allowed = (query_seg[:, :, None] == segments[:, None, :]) & (
        key_pos[None, None, :] <= query_pos[None, :, None]
    )
    cos_tab, sin_tab = rope_tables(positions.reshape(-1))
    cos_tab, sin_tab = cos_tab[:, None, :], sin_tab[:, None, :]
    residual = tokens.astype(f32).reshape(-1, width)
    inv_in, normed_in = norm_forward(residual, gain_in)
    qkv_val = mat_mul(normed_in, w_qkv) + b_qkv
    query_bf = rotate(
        qkv_val[:, :q_cols].reshape(row_count, -1, HEAD_DIM), cos_tab, sin_tab
    ).astype(bf16).reshape(seq_count, -1, kv_local, group_size, HEAD_DIM)
    key_bf = rotate(
        qkv_val[:, q_cols : q_cols + k_cols].reshape(row_count, -1, HEAD_DIM), cos_tab, sin_tab
    ).astype(bf16).reshape(row_count, -1)
    value_bf = qkv_val[:, q_cols + k_cols :].astype(bf16)
    keyval = jnp.concatenate([key_bf, value_bf], 1).reshape(seq_count, local_len, -1)
    keyval_all = place(gather_direct(keyval, "ctx"), ctx_rank, 1)
    keys_all, values_all = keyval_all[..., :k_cols], keyval_all[..., k_cols:]
    attn_bf, log_total = attend_forward(query_bf, keys_all, values_all, allowed)
    attn_flat = attn_bf.reshape(row_count, -1)
    out_part = mat_mul_t(attn_flat, w_out)
    resid_mid = residual + (out_part + partner(out_part))
    inv_mid, normed_mid = norm_forward(resid_mid, gain_mid)

    mid_all = spread(normed_mid)
    gate_pre = mat_mul(mid_all, w_gate)
    up_pre = mat_mul(mid_all, w_up)
    hidden_bf = (jax.nn.silu(gate_pre) * up_pre).astype(bf16)
    grad_hidden = mat_mul(grad_all, w_down)
    sigmoid_gate = jax.nn.sigmoid(gate_pre)
    grad_gate = (
        grad_hidden * up_pre * sigmoid_gate * (1.0 + gate_pre * (1.0 - sigmoid_gate))
    ).astype(bf16)
    grad_up = (grad_hidden * gate_pre * sigmoid_gate).astype(bf16)

    def collect(part):
        part_bf = columns_at(part, 1 - core, half_width).astype(bf16)
        mine = columns_at(part, core, half_width) + partner(part_bf).astype(f32)
        total = scatter_direct(lambda step: mine[step * row_count : (step + 1) * row_count], "ctx")
        return join_halves(total, partner(total), core, 1)

    grad_normed_mid = collect(mat_mul_t(grad_gate, w_gate) + mat_mul_t(grad_up, w_up))

    def owner_weight(left, right):
        blocks = [
            rows_mul(columns_at(left, dp_rank ^ step, group_rows), right)
            for step in range(dp_count)
        ]
        group = scatter_halves(blocks, "dp").astype(bf16)
        pieces = [rows_at(group, ctx_rank, own_rows)]
        for step in range(1, ctx_count):
            pieces.append(xor_permute(rows_at(group, ctx_rank ^ step, own_rows), "ctx", step))
        return place(pieces, ctx_rank, 1)[:, :ff_cols].astype(f32)

    grad_w_down = owner_weight(grad_all, hidden_bf)
    grad_w_gate = owner_weight(mid_all, grad_gate)
    grad_w_up = owner_weight(mid_all, grad_up)

    layer_out = resid_mid + collect(mat_mul_t(hidden_bf, w_down))
    activations = (layer_out * live_rows).reshape(tokens.shape)

    grad_mid_norm, grad_gain_mid = norm_backward(resid_mid, inv_mid, gain_mid, grad_normed_mid)
    grad_mid = grad_out + grad_mid_norm
    grad_mid_bf = grad_mid.astype(bf16)
    grad_attn = mat_mul(grad_mid_bf, w_out).astype(bf16)

    def owner_attn(left, right):
        blocks = [
            rows_mul(columns_at(left, dp_rank ^ step, group_rows), right)
            for step in range(dp_count)
        ]
        group = scatter_halves(blocks, "dp")
        return scatter_direct(lambda step: rows_at(group, ctx_rank ^ step, own_rows), "ctx")

    grad_w_out = owner_attn(grad_mid_bf, attn_flat)
    grad_query, grad_key_all, grad_value_all = attend_backward(
        query_bf, keys_all, values_all, attn_bf, log_total, grad_attn.reshape(attn_bf.shape), allowed
    )
    grad_keyval_all = jnp.concatenate([grad_key_all, grad_value_all], 2)
    grad_keyval = scatter_direct(
        lambda step: lax.dynamic_slice_in_dim(
            grad_keyval_all, (ctx_rank ^ step) * local_len, local_len, 1
        ),
        "ctx",
    ).reshape(row_count, -1)
    grad_query = unrotate(
        grad_query.reshape(row_count, -1, HEAD_DIM), cos_tab, sin_tab
    ).reshape(row_count, -1)
    grad_key = unrotate(
        grad_keyval[:, :k_cols].reshape(row_count, -1, HEAD_DIM), cos_tab, sin_tab
    ).reshape(row_count, -1)
    grad_qkv = jnp.concatenate([grad_query, grad_key, grad_keyval[:, k_cols:]], 1)
    grad_qkv_bf = grad_qkv.astype(bf16)
    grad_w_qkv = owner_attn(normed_in, grad_qkv_bf)
    dot_part = mat_mul_t(grad_qkv_bf, w_qkv)
    grad_normed_in = dot_part + partner(dot_part)
    grad_in_norm, grad_gain_in = norm_backward(residual, inv_in, gain_in, grad_normed_in)
    input_grad = (grad_mid + grad_in_norm).reshape(tokens.shape)

    bias_sum = jnp.sum(grad_qkv, axis=0)
    device_count = dp_count * ctx_count
    grad_small = jnp.concatenate(
        [
            grad_gain_in.reshape(device_count, -1),
            grad_gain_mid.reshape(device_count, -1),
            bias_sum[:q_cols].reshape(kv_local, -1).T.reshape(device_count, -1),
            jnp.concatenate(
                [
                    bias_sum[q_cols : q_cols + k_cols].reshape(kv_local, -1).T,
                    bias_sum[q_cols + k_cols :].reshape(kv_local, -1).T,
                ],
                0,
            ).reshape(device_count, -1),
        ],
        1,
    )
    small_group = scatter_small(
        [rows_at(grad_small, dp_rank ^ step, ctx_count) for step in range(dp_count)], "dp"
    )
    small_own = scatter_small(
        [rows_at(small_group, ctx_rank ^ step, 1) for step in range(ctx_count)], "ctx"
    )
    own = [small_own[:, low:high] for low, high in zip(cuts[:-1], cuts[1:])]
    return (
        activations,
        input_grad,
        own[0],
        grad_w_qkv[None, :, :q_cols],
        own[2].reshape(q_bias.shape),
        grad_w_qkv[None, :, q_cols : q_cols + k_cols],
        grad_w_qkv[None, :, q_cols + k_cols :],
        own[3].reshape(kv_bias.shape),
        grad_w_out[None],
        own[1],
        grad_w_gate[None],
        grad_w_up[None],
        grad_w_down[None],
    )


MESH = pl.DeviceIdType.MESH


def remote(src, dst, send_sem, recv_sem, target):
    return pltpu.make_async_remote_copy(
        src_ref=src, dst_ref=dst, send_sem=send_sem, recv_sem=recv_sem, device_id=target, device_id_type=MESH
    )


def greet(partners):
    barrier = pltpu.get_barrier_semaphore()
    for partner_id in partners:
        pl.semaphore_signal(barrier, inc=1, device_id=partner_id, device_id_type=MESH)
    pl.semaphore_wait(barrier, len(partners))


def spread_row(values, row_cols, period, total):
    left = lax.broadcasted_iota(jnp.int32, (period, total), 0)
    right = lax.broadcasted_iota(jnp.int32, (period, total), 1)
    pick = (lax.rem(right, period) == left).astype(jnp.float32).astype(jnp.bfloat16)
    spread = jnp.dot(values.astype(jnp.bfloat16), pick, preferred_element_type=jnp.float32)
    block = lax.broadcasted_iota(jnp.int32, spread.shape, 0) // 8
    owner = lax.broadcasted_iota(jnp.int32, spread.shape, 1) // period
    return jnp.sum(jnp.where(block == owner, spread, 0.0), axis=0, keepdims=True)


def forward_kernel(
    sizes,
    tok_ref,
    cot_ref,
    attn_own,
    mlp_own,
    small_own,
    cos_ref,
    sin_ref,
    qseg_ref,
    kseg_ref,
    wattn_out,
    e_out,
    b_out,
    h_out,
    a_out,
    q_out,
    kv_out,
    o_out,
    lse_out,
    row_out,
    zgu_out,
    sum_out,
    own_out,
    down_out,
    wattn,
    wmlp,
    e_all,
    b_all,
    h_ref,
    a_ref,
    q_ref,
    kv_ref,
    o_ref,
    lse_ref,
    row_ref,
    small,
    part,
    part_in,
    gu_ref,
    z_ref,
    zgu,
    block_ref,
    pair,
    give,
    take,
    mine,
    zs,
    zr,
    xs,
    xr,
    ys,
    yr,
    fs,
    fr,
    ks,
    kr,
    ps,
    pr,
    bs,
    br,
    us,
    ur,
    ts,
    tr,
    loc,
    out_sem,
    down_sem,
):
    dp_count, ctx_count, own, qkv_cols, q_cols, gain_cut = sizes
    dp, ctx, core = lax.axis_index("dp"), lax.axis_index("ctx"), lax.axis_index("tp")
    bf16, f32 = jnp.bfloat16, jnp.float32
    width = tok_ref.shape[1]
    rows = tok_ref.shape[0]
    seqs = cot_ref.shape[0]
    local = cot_ref.shape[1]
    tiles = range(ctx_count)

    def at_x(d):
        return d + 1 - 2 * lax.rem(d, 2)

    def at_y(d):
        return lax.rem(d + 2, 4)

    dpx, dpy = at_x(dp), at_y(dp)
    dpd = at_x(dpy)
    peers = [ctx]
    for step in range(1, ctx_count):
        value = jnp.int32(0)
        for bit in (1, 2, 4, 8):
            if bit < ctx_count:
                digit = lax.rem(ctx // bit, 2)
                value = value + bit * (digit + (1 - 2 * digit) * ((step // bit) % 2))
        peers.append(value)
    other = 1 - core
    to_core = {"tp": other}

    greet(
        [{"dp": dpx}, {"dp": dpy}, {"tp": other}] + [{"ctx": peers[step]} for step in range(1, ctx_count)]
    )
    sent = []

    def start(copy):
        copy.start()
        sent.append(copy)
        return copy

    def block_rows(d, c):
        return pl.ds(pl.multiple_of((d * ctx_count + c) * own, own), own)

    def slot(item, d, c):
        if item == 0:
            return small.at[d * ctx_count + c]
        if item == 1:
            return wattn.at[block_rows(d, c), :]
        return wmlp.at[item - 2, block_rows(d, c), :]

    def source(item, tile):
        if item == 0:
            return small_own
        if item == 1:
            return attn_own
        return mlp_own.at[item - 2, peers[tile]]

    items = range(5)
    local_copies = []
    for item in items:
        copy = pltpu.make_async_copy(source(item, 0), slot(item, dp, ctx), loc.at[item])
        copy.start()
        local_copies.append(copy)
    z_copy = {}

    def z_send(item):
        for tile in range(1, ctx_count):
            z_copy[item, tile] = start(
                remote(source(item, tile), slot(item, dp, ctx), zs.at[item, tile], zr.at[item, tile], {"ctx": peers[tile]})
            )

    x_copy, y_copy, f_copy = {}, {}, {}

    def xy_send(item, tile):
        src = source(item, 0) if tile == 0 else slot(item, dp, peers[tile])
        if tile:
            z_copy[item, tile].wait_recv()
        dst = slot(item, dp, peers[tile])
        x_copy[item, tile] = start(remote(src, dst, xs.at[item, tile], xr.at[item, tile], {"dp": dpx}))
        y_copy[item, tile] = start(remote(src, dst, ys.at[item, tile], yr.at[item, tile], {"dp": dpy}))

    def forward(item, tile):
        if (item + tile) % 2 == 0:
            x_copy[item, tile].wait_recv()
            place_at = slot(item, dpx, peers[tile])
            target = {"dp": dpy}
        else:
            y_copy[item, tile].wait_recv()
            place_at = slot(item, dpy, peers[tile])
            target = {"dp": dpx}
        f_copy[item, tile] = start(remote(place_at, place_at, fs.at[item, tile], fr.at[item, tile], target))

    def settle(item, tile):
        if (item + tile) % 2 == 0:
            y_copy[item, tile].wait_recv()
        else:
            x_copy[item, tile].wait_recv()
        f_copy[item, tile].wait_recv()

    last = ctx_count - 1
    ways = ((1, ctx < last), (-1, ctx > 0))
    relay_sent = []

    def hop(index, buf, way, distance, origin):
        step, _ = ways[way]
        piece = buf.at[origin, core]
        return remote(piece, piece, bs.at[index, way, distance], br.at[index, way, distance], {"ctx": ctx + step})

    def spread_start(index, buf):
        for way in range(2):
            copy = hop(index, buf, way, 0, ctx)

            @pl.when(ways[way][1])
            def _():
                copy.start()

            relay_sent.append((ways[way][1], copy))

    def spread_step(index, buf, distance):
        for way in range(2):
            step, open_end = ways[way]
            origin = ctx - step * distance
            here = (origin >= 0) & (origin <= last)
            safe = jnp.clip(origin, 0, last)
            piece = buf.at[safe, core]
            got = remote(piece, piece, bs.at[index, way, distance - 1], br.at[index, way, distance - 1], to_core)
            share = remote(piece, piece, us.at[index, way, distance], ur.at[index, way, distance], to_core)

            @pl.when(here)
            def _():
                got.wait_recv()
                share.start()

            relay_sent.append((here, share))
            if distance < last:
                copy = hop(index, buf, way, distance, safe)

                @pl.when(here & open_end)
                def _():
                    copy.start()

                relay_sent.append((here & open_end, copy))

    def spread_end(index, buf, distance):
        for way in range(2):
            step, _ = ways[way]
            origin = ctx - step * distance
            piece = buf.at[jnp.clip(origin, 0, last), other]
            got = remote(piece, piece, us.at[index, way, distance], ur.at[index, way, distance], to_core)

            @pl.when((origin >= 0) & (origin <= last))
            def _():
                got.wait_recv()

    z_send(0)
    z_send(1)
    xy_send(1, 0)
    for item in (2, 3):
        z_send(item)
    e_local = pltpu.make_async_copy(cot_ref, e_all.at[ctx], loc.at[5])
    e_local.start()
    kept = []

    def keep_out(src, dst):
        copy = pltpu.make_async_copy(src, dst, out_sem.at[len(kept)])
        copy.start()
        kept.append(copy)

    for tile in tiles:
        xy_send(0, tile)
    for tile in tiles:
        forward(0, tile)
    for tile in range(1, ctx_count):
        xy_send(1, tile)
    for tile in tiles:
        settle(0, tile)
    local_copies[0].wait()

    flat = small[...].reshape(dp_count * ctx_count * 8, small.shape[2])
    row_ref[0:1, :] = spread_row(flat[:, gain_cut[0] : gain_cut[1]], None, gain_cut[1] - gain_cut[0], width)
    row_ref[1:2, :] = spread_row(flat[:, gain_cut[1] : gain_cut[2]], None, gain_cut[2] - gain_cut[1], width)
    row_ref[2:3, :q_cols] = spread_row(flat[:, gain_cut[2] : gain_cut[3]], None, gain_cut[3] - gain_cut[2], q_cols)
    row_ref[2:3, q_cols:qkv_cols] = spread_row(
        flat[:, gain_cut[3] : gain_cut[4]], None, gain_cut[4] - gain_cut[3], qkv_cols - q_cols
    )

    step_rows = 32

    def norm_in(index, _):
        piece = pl.ds(index * step_rows, step_rows)
        val = tok_ref[piece, :].astype(f32)
        inv = lax.rsqrt(jnp.mean(val * val, axis=-1, keepdims=True) + norm_eps)
        a_ref[piece, :] = (val * inv * row_ref[0:1, :]).astype(bf16)
        return 0

    lax.fori_loop(0, rows // step_rows, norm_in, 0)
    for tile in tiles:
        forward(1, tile)
    for tile in tiles:
        xy_send(2, tile)
    xy_send(3, 0)
    xy_send(4, 0)
    for tile in tiles:
        settle(1, tile)
    local_copies[1].wait()
    keep_out(wattn, wattn_out)
    keep_out(a_ref, a_out)
    keep_out(row_ref, row_out)

    pending = [(forward, 2, tile) for tile in tiles]
    pending += [(xy_send, 3, tile) for tile in tiles if tile]
    pending += [(forward, 3, 0), (forward, 4, 0)]
    pending += [(forward, 3, tile) for tile in tiles if tile]
    pending += [(xy_send, 4, tile) for tile in tiles if tile]
    pending += [(forward, 4, tile) for tile in tiles if tile]

    def pump(count):
        for _ in range(min(count, len(pending))):
            action, item, tile = pending.pop(0)
            action(item, tile)

    own_keys = pl.ds(pl.multiple_of(ctx * local, local), local)
    order = [qkv_cols - 256] + list(range(0, q_cols, 256))
    kv_copies = []
    for low in order:
        val = jnp.dot(a_ref[...], wattn[:, low : low + 256], preferred_element_type=f32) + row_ref[2:3, low : low + 256]
        for head_low in (0, 128):
            head = val[:, head_low : head_low + 128]
            if low + head_low < qkv_cols - 128:
                head = head * cos_ref[...] + pltpu.roll(head, 64, 1) * sin_ref[...]
            head = head.astype(bf16)
            for seq in range(seqs):
                piece = head[seq * local : (seq + 1) * local]
                if low == qkv_cols - 256:
                    kv_ref[seq, head_low // 128, own_keys, :] = piece
                else:
                    q_ref[seq, (low + head_low) // 128] = piece
        if low == qkv_cols - 256:
            for tile in range(1, ctx_count):
                piece = kv_ref.at[:, :, own_keys, :]
                kv_copies.append(start(remote(piece, piece, ks.at[tile], kr.at[tile], {"ctx": peers[tile]})))
    keep_out(q_ref, q_out)
    pump(4)
    for copy in kv_copies:
        copy.wait_recv()
    z_send(4)
    e_local.wait()
    spread_start(0, e_all)
    pump(3)
    keep_out(kv_ref, kv_out)

    keys = kv_ref.shape[2]
    key_no = lax.broadcasted_iota(jnp.int32, (local, keys), 1)
    query_no = lax.broadcasted_iota(jnp.int32, (local, keys), 0) + ctx * local
    for seq in range(seqs):
        seen = (qseg_ref[seq] == kseg_ref[seq]) & (key_no <= query_no)
        hide = jnp.where(seen, 0.0, masked_score)

        def one_head(head, _):
            score = lax.dot_general(
                q_ref[seq, head], kv_ref[seq, 0], (((1,), (1,)), ((), ())), preferred_element_type=f32
            )
            score = jnp.where(hide < 0.0, masked_score, score * HEAD_DIM ** (-0.5))
            top = jnp.max(score, axis=-1, keepdims=True)
            weight = jnp.exp(score - top)
            total = jnp.sum(weight, axis=-1, keepdims=True)
            prob = (weight / total).astype(bf16)
            lse_ref[seq, head] = top + jnp.log(total)
            out = jnp.dot(prob, kv_ref[seq, 1], preferred_element_type=f32)
            o_ref[seq, head] = out.astype(bf16)
            return 0

        lax.fori_loop(0, q_cols // 128, one_head, 0)
        if seq == 0:
            pump(2)
    keep_out(o_ref, o_out)
    keep_out(lse_ref, lse_out)

    o_rows = jnp.concatenate(
        [jnp.concatenate([o_ref[seq, head] for head in range(q_cols // 128)], 1) for seq in range(seqs)], 0
    )
    part_copies = []
    for index in range(width // 256):
        part[index] = lax.dot_general(
            o_rows,
            wattn[index * 256 : (index + 1) * 256, qkv_cols:],
            (((1,), (1,)), ((), ())),
            preferred_element_type=f32,
        )
        part_copies.append(
            start(remote(part.at[index], part_in.at[index], ps.at[index], pr.at[index], {"tp": other}))
        )
    pump(1)
    for index, copy in enumerate(part_copies):
        copy.wait_recv()
        span = slice(index * 256, (index + 1) * 256)
        h_ref[:, span] = tok_ref[:, span].astype(f32) + (part[index] + part_in[index])

    def norm_mid(index, _):
        piece = pl.ds(index * step_rows, step_rows)
        val = h_ref[piece, :]
        inv = lax.rsqrt(jnp.mean(val * val, axis=-1, keepdims=True) + norm_eps)
        per_seq = local // step_rows
        b_all[ctx, index // per_seq, pl.ds(lax.rem(index, per_seq) * step_rows, step_rows), :] = (
            val * inv * row_ref[1:2, :]
        ).astype(bf16)
        return 0

    lax.fori_loop(0, rows // step_rows, norm_mid, 0)
    spread_start(1, b_all)
    keep_out(h_ref, h_out)
    pump(1)
    spread_step(0, e_all, 1)
    spread_step(1, b_all, 1)
    pump(2)
    spread_step(0, e_all, 2)
    spread_step(1, b_all, 2)
    pump(2)

    ff = wmlp.shape[2]
    full_ff = ff // 256 * 256
    nt = (((1,), (1,)), ((), ()))

    def ahead_columns(peer, low, size):
        span = pl.ds(low, size)
        gate = jnp.dot(b_all[peer].reshape(rows, width), wmlp[0, :, span], preferred_element_type=f32)
        up = jnp.dot(b_all[peer].reshape(rows, width), wmlp[1, :, span], preferred_element_type=f32)
        gu_ref[0, peer, :, span] = gate
        gu_ref[1, peer, :, span] = up
        z_ref[peer, :, span] = (gate * jax.nn.sigmoid(gate) * up).astype(bf16)

    def back_columns(slot, peer, low, size):
        span = pl.ds(low, size)
        grad = jnp.dot(e_all[peer].reshape(rows, width), wmlp[2, :, span], preferred_element_type=f32)
        gate, up = gu_ref[0, peer, :, span], gu_ref[1, peer, :, span]
        sig = jax.nn.sigmoid(gate)
        zgu[slot, 0, :, span] = (grad * up * sig * (1.0 + gate * (1.0 - sig))).astype(bf16)
        zgu[slot, 1, :, span] = (grad * gate * sig).astype(bf16)

    def over_columns(body):
        def columns(index, _):
            body(pl.multiple_of(index * 256, 256), 256)
            return 0

        lax.fori_loop(0, ff // 256, columns, 0)
        if full_ff < ff:
            body(full_ff, ff - full_ff)

    def ahead(tile):
        over_columns(lambda low, size: ahead_columns(peers[tile], low, size))

    for item in (2, 3):
        for tile in tiles:
            settle(item, tile)
    local_copies[2].wait()
    local_copies[3].wait()
    ahead(0)
    spread_step(0, e_all, ctx_count - 1)
    spread_step(1, b_all, ctx_count - 1)
    pump(1)
    for distance in range(1, ctx_count):
        spread_end(0, e_all, distance)
        spread_end(1, b_all, distance)
    keep_out(e_all, e_out)
    keep_out(b_all, b_out)
    for tile in range(1, ctx_count):
        ahead(tile)
        pump(1)
    keep_out(z_ref, zgu_out.at[0])

    group = own * ctx_count
    down_copies = {}
    for count, node in enumerate((dpd, dpy, dpx, dp)):
        key = dp_count - 1 - count
        slot = count % 2
        if count >= 2:
            down_copies[count - 2].wait()

        def down_columns(low, size):
            span = pl.ds(low, size)
            left = e_all[:, :, :, pl.ds(pl.multiple_of(node * group, group), group)].reshape(-1, group)
            val = lax.dot_general(
                left, z_ref[:, :, span].reshape(-1, size), (((0,), (0,)), ((), ())), preferred_element_type=f32
            )
            block_ref[slot, :, span] = val.astype(bf16)

        over_columns(down_columns)
        down_copies[count] = pltpu.make_async_copy(block_ref.at[slot], down_out.at[key], down_sem.at[slot])
        down_copies[count].start()
        pump(1)
    while pending:
        pump(1)
    for tile in tiles:
        settle(4, tile)
    local_copies[4].wait()
    down_copies[2].wait()
    down_copies[3].wait()

    zgu_copies, give_copies = {}, {}

    def ff_rows(tile):
        slot = tile % 2
        peer = peers[tile]
        if tile >= 2:
            zgu_copies[tile - 2].wait()
        over_columns(lambda low, size: back_columns(slot, peer, low, size))
        zgu_copies[tile] = pltpu.make_async_copy(zgu.at[slot], zgu_out.at[1:3, peer], loc.at[6 + slot])
        zgu_copies[tile].start()

        def outputs(index, _):
            span = pl.ds(pl.multiple_of(index * 256, 256), 256)
            back = lax.dot_general(zgu[slot, 0], wmlp[0, span, :], nt, preferred_element_type=f32)
            back = back + lax.dot_general(zgu[slot, 1], wmlp[1, span, :], nt, preferred_element_type=f32)
            ahead_part = lax.dot_general(z_ref[peer], wmlp[2, span, :], nt, preferred_element_type=f32)
            for seq in range(seqs):
                pair[slot, 0, seq, :, span] = back[seq * local : (seq + 1) * local]
                pair[slot, 1, seq, :, span] = ahead_part[seq * local : (seq + 1) * local]
            return 0

        lax.fori_loop(0, width // 256, outputs, 0)
        for item in range(2):

            def convert(index, _):
                piece = pl.ds(index * step_rows, step_rows)
                give[item, tile, piece, :] = pair[slot, item, other, piece, :].astype(bf16)
                return 0

            lax.fori_loop(0, local // step_rows, convert, 0)
            give_copies[tile, item] = start(
                remote(give.at[item, tile], take.at[item, tile], ts.at[item, tile], tr.at[item, tile], to_core)
            )

    def ff_sum(tile):
        slot = tile % 2
        for item in range(2):
            give_copies[tile, item].wait_recv()

            def add(index, _):
                piece = pl.ds(index * step_rows, step_rows)
                total = pair[slot, item, core, piece, :] + take[item, tile, piece, :].astype(f32)
                if tile == 0:
                    mine[item, piece, :] = total
                else:
                    take[item, tile, piece, :] = total.astype(bf16)
                return 0

            lax.fori_loop(0, local // step_rows, add, 0)
            if tile:
                keep_out(take.at[item, tile], sum_out.at[item, peers[tile]])

    for tile in range(ctx_count):
        ff_rows(tile)
        if tile:
            ff_sum(tile - 1)
    ff_sum(ctx_count - 1)
    keep_out(mine, own_out)
    for tile in (ctx_count - 2, ctx_count - 1):
        zgu_copies[tile].wait()
    for copy in kept:
        copy.wait()
    for copy in sent:
        copy.wait_send()
    for here, copy in relay_sent:

        @pl.when(here)
        def _():
            copy.wait_send()


def forward_call(tok, cot, attn_own, mlp_own, small_own, cos, sin, qseg, kseg, qkv_cols, q_cols, gain_cut):
    dp_count, ctx_count = lax.axis_size("dp"), lax.axis_size("ctx")
    own = attn_own.shape[0]
    rows, width = tok.shape
    seqs, local = cot.shape[:2]
    full_rows = own * dp_count * ctx_count
    heads = q_cols // 128
    ff = mlp_own.shape[3]
    bf16, f32 = jnp.bfloat16, jnp.float32
    vmem, hbm = pl.BlockSpec(memory_space=pltpu.VMEM), pl.BlockSpec(memory_space=pl.ANY)
    group = (ctx_count, seqs, local, width)
    kept = [
        ((rows, width), f32),
        ((rows, width), bf16),
        ((seqs, heads, local, 128), bf16),
        ((seqs, 2, local * ctx_count, 128), bf16),
        ((seqs, heads, local, 128), bf16),
        ((seqs, heads, local, 1), f32),
        ((8, width), f32),
    ]
    weights = ((full_rows, attn_own.shape[1]), bf16)
    outs = [weights, (group, bf16), (group, bf16)] + kept
    outs += [((3, ctx_count, rows, ff), bf16), ((2, ctx_count, local, width), bf16), ((2, local, width), f32)]
    outs += [((dp_count, own * ctx_count, ff), bf16)]
    chunks = width // 256
    scratch = [weights, ((3, full_rows, ff), bf16), (group, bf16), (group, bf16)] + kept
    scratch += [
        ((dp_count * ctx_count, 8, small_own.shape[1]), f32),
        ((chunks, rows, 256), f32),
        ((chunks, rows, 256), f32),
        ((2, ctx_count, rows, ff), f32),
        ((ctx_count, rows, ff), bf16),
        ((2, 2, rows, ff), bf16),
        ((2, own * ctx_count, ff), bf16),
        ((2, 2, seqs, local, width), f32),
        ((2, ctx_count, local, width), bf16),
        ((2, ctx_count, local, width), bf16),
        ((2, local, width), f32),
    ]
    dma = pltpu.SemaphoreType.DMA
    return pl.pallas_call(
        functools.partial(forward_kernel, (dp_count, ctx_count, own, qkv_cols, q_cols, gain_cut)),
        out_shape=[jax.ShapeDtypeStruct(shape, kind) for shape, kind in outs],
        in_specs=[vmem, hbm, hbm, hbm, hbm, vmem, vmem, vmem, vmem],
        out_specs=[hbm] * len(outs),
        scratch_shapes=[pltpu.VMEM(*entry) for entry in scratch]
        + [dma((5, ctx_count)) for _ in range(8)]
        + [dma((ctx_count,)), dma((ctx_count,)), dma((chunks,)), dma((chunks,))]
        + [dma((2, 2, ctx_count)) for _ in range(4)]
        + [dma((2, ctx_count)), dma((2, ctx_count)), dma((8,)), dma((20,)), dma((2,))],
        compiler_params=pltpu.CompilerParams(
            collective_id=0, has_side_effects=True, vmem_limit_bytes=65 * 1024 * 1024 - 65536
        ),
        name="forward_kernel",
    )(tok, cot, attn_own, mlp_own, small_own, cos, sin, qseg, kseg)


def xor_rank(rank, step, count):
    value = jnp.int32(0)
    bit = 1
    while bit < count:
        digit = lax.rem(rank // bit, 2)
        value = value + bit * (digit + (1 - 2 * digit) * ((step // bit) % 2))
        bit *= 2
    return value


def backward_kernel(
    sizes,
    sum_in,
    own_in,
    zgu_in,
    b_in,
    down_in,
    cot_hbm,
    tok_hbm,
    h_hbm,
    a_hbm,
    q_hbm,
    kv_hbm,
    o_hbm,
    lse_hbm,
    wattn_hbm,
    live_ref,
    row_ref,
    cos_ref,
    sin_ref,
    qseg_ref,
    kseg_ref,
    act_ref,
    dx_ref,
    zin,
    gat_ref,
    rows_ref,
    gout,
    lin,
    sum_v,
    fin,
    left_ref,
    right_ref,
    block_ref,
    keep,
    r1,
    r2,
    keep_at,
    send_at,
    r1_at,
    r2_at,
    zin_at,
    hb_ref,
    do_ref,
    prob_ref,
    ds_ref,
    dkv_ref,
    dkv_bf,
    dkv_in,
    dqkv_ref,
    part,
    part_in,
    zss,
    zrs,
    fs,
    fr,
    ld,
    kd,
    gd,
    s1,
    v1,
    s2,
    v2,
    s3,
    v3,
    ks,
    kr,
    ps,
    pr,
    gs,
    gr,
    acc_ref,
    sm_in,
    sm_sum,
    cot_ref,
    tok_ref,
    h_ref,
    a_ref,
    q_ref,
    kv_ref,
    o_ref,
    lse_ref,
    wattn,
    in_sem,
):
    dp_count, ctx_count, own, qkv_cols, q_cols = sizes
    dp, ctx, core = lax.axis_index("dp"), lax.axis_index("ctx"), lax.axis_index("tp")
    bf16, f32 = jnp.bfloat16, jnp.float32
    seqs, local, width = cot_ref.shape
    loads = []
    for src, dst in (
        (cot_hbm, cot_ref),
        (tok_hbm, tok_ref),
        (h_hbm, h_ref),
        (a_hbm, a_ref),
        (q_hbm, q_ref),
        (kv_hbm, kv_ref),
        (o_hbm, o_ref),
        (lse_hbm, lse_ref),
        (wattn_hbm, wattn),
    ):
        loads.append(pltpu.make_async_copy(src, dst, in_sem.at[len(loads)]))
    group = own * ctx_count
    ff = zgu_in.shape[3]
    heads = q_cols // 128
    other = 1 - core
    peers = [xor_rank(ctx, step, ctx_count) for step in range(ctx_count)]
    nodes = [xor_rank(dp, step, dp_count) for step in range(dp_count)]
    to_x, to_y, to_core = {"dp": nodes[1]}, {"dp": nodes[2]}, {"tp": other}
    greet([to_x, to_y, to_core] + [{"ctx": peers[step]} for step in range(1, ctx_count)])
    sent = []

    def start(copy):
        copy.start()
        sent.append(copy)
        return copy

    def rows_of(count, size, body):
        def one(index, _):
            body(pl.ds(pl.multiple_of(index * size, size), size))
            return 0

        lax.fori_loop(0, count // size, one, 0)

    last = ctx_count - 1
    ends = (ctx == 0, ctx == last)
    fin_copy, relay_sent = {}, []
    sums_of = (fin, act_ref)

    def line_step(index, turn):
        for way, step in ((0, 1), (1, -1)):
            owner = ctx + step * (ctx_count - turn)
            active = (owner >= 0) & (owner <= last)
            safe = jnp.clip(owner, 0, last)
            target = {"ctx": ctx + step}

            def message(src):
                return remote(
                    src,
                    lin.at[index, way, turn - 1],
                    zss.at[index, way, turn - 1],
                    zrs.at[index, way, turn - 1],
                    target,
                )

            fresh = message(sum_v.at[index, safe])

            @pl.when(active & ends[way])
            def _():
                fresh.start()

            relay_sent.append((active, fresh))
            if turn > 1:
                held = lin.at[index, way, turn - 2]
                got = remote(
                    held, held, zss.at[index, way, turn - 2], zrs.at[index, way, turn - 2], target
                )

                @pl.when(active & jnp.logical_not(ends[way]))
                def _():
                    got.wait_recv()

                    def add(piece):
                        lin[index, way, turn - 2, piece, :] = (
                            lin[index, way, turn - 2, piece, :].astype(f32) + sum_v[index, safe, piece, :].astype(f32)
                        ).astype(bf16)

                    rows_of(local, 32, add)
                    message(held).start()

    def collect_fin(index):
        into = sums_of[index]
        for way, step in ((0, 1), (1, -1)):
            held = lin.at[index, way, last - 1]
            got = remote(
                held, held, zss.at[index, way, last - 1], zrs.at[index, way, last - 1], {"ctx": ctx + step}
            )

            @pl.when(jnp.logical_not(ends[way]))
            def _():
                got.wait_recv()

                def add(piece):
                    into[core, piece, :] = into[core, piece, :] + lin[index, way, last - 1, piece, :].astype(f32)

                rows_of(local, 32, add)

        fin_copy[index] = remote(into.at[core], into.at[core], fs.at[index], fr.at[index], to_core)
        fin_copy[index].start()

    halves = {}
    for item in range(3):
        cut = (ff // 256 + 1) * 128
        halves[item] = ((0, cut), (cut, ff)) if item != 1 else ((cut, ff), (0, cut))
    middle = qkv_cols + (wattn.shape[1] - qkv_cols) // 2
    halves[3] = ((qkv_cols, middle), (middle, wattn.shape[1]))
    halves[4] = ((0, qkv_cols // 2), (qkv_cols // 2, qkv_cols))
    first_to, second_to = (to_y, to_x), (to_x, to_y)
    first_keys = ((2, 3), (1, 3))
    one_copy, two_copy, three_copy, keep_copy = {}, {}, {}, {}

    def cols(item, half):
        low, high = halves[item][half]
        return slice(low, high)

    def refs(item):
        if item < 3:
            return keep.at[item], r1.at[item], r2.at[item]
        return keep_at, r1_at, r2_at

    def block_of(item, key):
        return down_in.at[key] if item == 0 else gout.at[item - 1, key]

    def stage_one(item, half):
        span = cols(item, half)
        for slot, key in enumerate(first_keys[half]):
            src = block_of(item, key).at[:, span] if item < 3 else send_at.at[slot, :, span]
            one_copy[item, half, slot] = start(
                remote(
                    src,
                    refs(item)[1].at[slot, :, span],
                    s1.at[item, half, slot],
                    v1.at[item, half, slot],
                    first_to[half],
                )
            )

    def stage_two(item, half):
        span = cols(item, half)
        mine, first, second = refs(item)
        if item < 3:
            keep_copy[item, half].wait()
        one_copy[item, half, 1].wait_recv()

        def add(piece):
            mine[1, piece, span] = (mine[1, piece, span].astype(f32) + first[1, piece, span].astype(f32)).astype(bf16)

        rows_of(group, 96, add)
        two_copy[item, half] = start(
            remote(mine.at[1, :, span], second.at[:, span], s2.at[item, half], v2.at[item, half], second_to[half])
        )

    def stage_three(item, half):
        span = cols(item, half)
        mine, first, second = refs(item)
        if item < 3:
            keep_copy[item, 2].wait() if half == 0 else None
        one_copy[item, half, 0].wait_recv()
        two_copy[item, half].wait_recv()

        def total(piece):
            return mine[0, piece, span].astype(f32) + first[0, piece, span].astype(f32) + second[piece, span].astype(f32)

        if item >= 3:
            gat_ref[:, span] = total(pl.ds(pl.multiple_of(ctx * own, own), own))

        def add(piece):
            mine[0, piece, span] = total(piece).astype(bf16)

        rows_of(group, 96, add)
        target = zin.at[item] if item < 3 else zin_at
        for tile in range(1, ctx_count):
            piece = pl.ds(pl.multiple_of(peers[tile] * own, own), own)
            three_copy[item, half, tile] = start(
                remote(
                    mine.at[0, piece, span],
                    target.at[ctx, :, span],
                    s3.at[item, half, tile],
                    v3.at[item, half, tile],
                    {"ctx": peers[tile]},
                )
            )
        if item < 3:
            piece = pl.ds(pl.multiple_of(ctx * own, own), own)
            copy = pltpu.make_async_copy(mine.at[0, piece, span], target.at[ctx, :, span], kd.at[item, 3 + half])
            copy.start()
            three_copy[item, half, 0] = copy

    def stage_four(item, half):
        span = cols(item, half)
        for tile in range(1, ctx_count):
            three_copy[item, half, tile].wait_recv()
        if item < 3:
            three_copy[item, half, 0].wait()
        else:
            total = gat_ref[:, span]
            for tile in range(1, ctx_count):
                total = total + zin_at[peers[tile], :, span].astype(f32)
            gat_ref[:, span] = total

    def keep_load(item):
        for half in range(2):
            span = cols(item, half)
            copy = pltpu.make_async_copy(
                block_of(item, 1 + half).at[:, span], keep.at[item, 1, :, span], kd.at[item, half]
            )
            copy.start()
            keep_copy[item, half] = copy
        copy = pltpu.make_async_copy(block_of(item, 0), keep.at[item, 0], kd.at[item, 2])
        copy.start()
        keep_copy[item, 2] = copy

    stage_one(0, 0)
    stage_one(0, 1)
    sum_copy = pltpu.make_async_copy(sum_in, sum_v, ld.at[1])
    sum_copy.start()

    def load_left(count):
        span = pl.ds(pl.multiple_of(nodes[dp_count - 1 - count % dp_count] * group, group), group)
        copy = pltpu.make_async_copy(b_in.at[:, :, :, span], left_ref.at[count % 2], gd.at[count % 2])
        copy.start()
        return copy

    def load_right(item):
        copy = pltpu.make_async_copy(zgu_in.at[item], right_ref, gd.at[2])
        copy.start()
        return copy

    right_copy = load_right(1)
    left_copy = load_left(0)
    mine_copies = [
        pltpu.make_async_copy(own_in.at[0], fin.at[core], ld.at[0]),
        pltpu.make_async_copy(own_in.at[1], act_ref.at[core], ld.at[2]),
    ]
    for copy in mine_copies:
        copy.start()
    keep_load(0)
    for copy in loads:
        copy.start()
    sum_copy.wait()
    line_step(0, 1)

    out_copy = {}

    def block(count, left_copy):
        slot = count % 2
        left_copy.wait()

        def columns(low, size):
            span = pl.ds(low, size)
            val = lax.dot_general(
                left_ref[slot].reshape(-1, group),
                right_ref[:, :, span].reshape(-1, size),
                (((0,), (0,)), ((), ())),
                preferred_element_type=f32,
            )
            block_ref[slot, :, span] = val.astype(bf16)

        def one(index, _):
            columns(pl.multiple_of(index * 256, 256), 256)
            return 0

        lax.fori_loop(0, ff // 256, one, 0)
        if ff % 256:
            columns(ff // 256 * 256, ff % 256)
        item, key = count // dp_count, dp_count - 1 - count % dp_count
        out_copy[count] = pltpu.make_async_copy(block_ref.at[slot], gout.at[item, key], gd.at[3 + slot])
        out_copy[count].start()

    def hand_over(count):
        out_copy[count].wait()
        item, key = 1 + count // dp_count, dp_count - 1 - count % dp_count
        if key == 2:
            stage_one(item, 0)
        if key == 1:
            stage_one(item, 1)
        if key == 0:
            keep_load(item)

    blocks = 2 * dp_count
    for count in range(blocks):
        following = load_left(count + 1) if count + 1 < blocks else None
        if count % dp_count == 0:
            right_copy.wait()
        block(count, left_copy)
        left_copy = following
        if count == dp_count - 1:
            right_copy = load_right(2)
        if count:
            hand_over(count - 1)
        if count == blocks // 2:
            line_step(0, 2)
    hand_over(blocks - 1)
    for copy in mine_copies:
        copy.wait()
    line_step(0, 3)
    line_step(1, 1)
    for copy in loads:
        copy.wait()

    pending = [(stage_two, 0, 0), (stage_two, 0, 1), (stage_two, 1, 0), (stage_two, 1, 1)]
    pending += [(stage_three, 0, 0), (stage_three, 0, 1), (stage_two, 2, 0), (stage_two, 2, 1)]
    pending += [(stage_three, 1, 0), (stage_three, 1, 1), (stage_three, 2, 0), (stage_three, 2, 1)]

    def pump(count):
        for _ in range(min(count, len(pending))):
            action, item, half = pending.pop(0)
            action(item, half)

    pump(2)
    collect_fin(0)
    fin_copy[0].wait()

    size = 32
    per_seq = local // size

    def split(index):
        return index // per_seq, pl.ds(pl.multiple_of(lax.rem(index, per_seq) * size, size), size)

    acc_ref[...] = jnp.zeros_like(acc_ref)

    def norm_mid(index, total):
        seq, piece = split(index)
        whole = pl.ds(pl.multiple_of(index * size, size), size)
        grad, val = fin[seq, piece, :], h_ref[whole, :]
        inv = lax.rsqrt(jnp.mean(val * val, axis=-1, keepdims=True) + norm_eps)
        weighted = grad * row_ref[1:2, :]
        inner = jnp.mean(weighted * val, axis=-1, keepdims=True)
        out = cot_ref[seq, piece, :].astype(f32) + (inv * weighted - val * (inv * inv * inv) * inner)
        dx_ref[seq, piece, :] = out
        hb_ref[whole, :] = out.astype(bf16)
        return total + jnp.sum(grad * val * inv, axis=0, keepdims=True)

    acc_ref[1:2, :] = lax.fori_loop(0, seqs * per_seq, norm_mid, jnp.zeros((1, width), f32))
    line_step(1, 2)

    for low in range(0, q_cols, 256):
        val = jnp.dot(hb_ref[...], wattn[:, qkv_cols + low : qkv_cols + low + 256], preferred_element_type=f32).astype(bf16)
        for head_low in (0, 128):
            for seq in range(seqs):
                do_ref[seq, (low + head_low) // 128] = val[seq * local : (seq + 1) * local, head_low : head_low + 128]

    keys = kv_ref.shape[2]
    key_no = lax.broadcasted_iota(jnp.int32, (local, keys), 1)
    query_no = lax.broadcasted_iota(jnp.int32, (local, keys), 0) + ctx * local
    scale = HEAD_DIM ** (-0.5)
    kv_copies = []
    for seq in range(seqs):
        seen = (qseg_ref[seq] == kseg_ref[seq]) & (key_no <= query_no)
        hide = jnp.where(seen, 0.0, masked_score)

        def one_head(head, _):
            query, grad_out, keys_bf, values_bf = q_ref[seq, head], do_ref[seq, head], kv_ref[seq, 0], kv_ref[seq, 1]
            score = lax.dot_general(query, keys_bf, (((1,), (1,)), ((), ())), preferred_element_type=f32) * scale
            prob = jnp.exp(jnp.where(hide < 0.0, masked_score, score) - lse_ref[seq, head])
            grad_prob = lax.dot_general(grad_out, values_bf, (((1,), (1,)), ((), ())), preferred_element_type=f32)
            row_dot = jnp.sum(grad_out.astype(f32) * o_ref[seq, head].astype(f32), axis=-1, keepdims=True)
            grad_score = (prob * (grad_prob - row_dot) * scale).astype(bf16)
            prob_ref[head] = prob.astype(bf16)
            ds_ref[head] = grad_score
            grad_query = jnp.dot(grad_score, keys_bf, preferred_element_type=f32)
            turned = grad_query * cos_ref[seq * local : (seq + 1) * local, :] + pltpu.roll(
                grad_query * sin_ref[seq * local : (seq + 1) * local, :], 64, 1
            )
            span = pl.ds(pl.multiple_of(head * 128, 128), 128)
            dqkv_ref[seq * local : (seq + 1) * local, span] = turned.astype(bf16)
            acc_ref[2:3, span] = acc_ref[2:3, span] + jnp.sum(turned, axis=0, keepdims=True)
            return 0

        lax.fori_loop(0, heads, one_head, 0)
        stacked = (heads * local, 128)
        dkv_ref[seq, 0] = lax.dot_general(
            ds_ref[...].reshape(heads * local, keys),
            q_ref[seq].reshape(stacked),
            (((0,), (0,)), ((), ())),
            preferred_element_type=f32,
        )
        dkv_ref[seq, 1] = lax.dot_general(
            prob_ref[...].reshape(heads * local, keys),
            do_ref[seq].reshape(stacked),
            (((0,), (0,)), ((), ())),
            preferred_element_type=f32,
        )
        dkv_bf[seq] = dkv_ref[seq].astype(bf16)
        if seq == 0:
            line_step(1, 3)
            pump(2)
    for tile in range(1, ctx_count):
        piece = pl.ds(pl.multiple_of(peers[tile] * local, local), local)
        kv_copies.append(
            start(remote(dkv_bf.at[:, :, piece, :], dkv_in.at[ctx], ks.at[tile], kr.at[tile], {"ctx": peers[tile]}))
        )

    def weight_blocks(item, left_ref, right, low, high):
        for key in (3, 2, 1, 0):
            left = left_ref[:, pl.ds(pl.multiple_of(nodes[key] * group, group), group)]
            val = lax.dot_general(left, right, (((0,), (0,)), ((), ())), preferred_element_type=f32).astype(bf16)
            for half in range(2):
                span = cols(item, half)
                piece = val[:, span.start - low : span.stop - low]
                if key in first_keys[half]:
                    send_at[first_keys[half].index(key), :, span] = piece
                else:
                    keep_at[0 if key == 0 else 1, :, span] = piece
            if key == 2:
                stage_one(item, 0)
            if key == 1:
                stage_one(item, 1)

    o_rows = jnp.concatenate(
        [jnp.concatenate([o_ref[seq, head] for head in range(heads)], 1) for seq in range(seqs)], 0
    )
    weight_blocks(3, hb_ref, o_rows, qkv_cols, wattn.shape[1])

    pump(2)

    pump(2)
    for copy in kv_copies:
        copy.wait_recv()
    own_keys = pl.ds(pl.multiple_of(ctx * local, local), local)
    for seq in range(seqs):
        for part_no in range(2):
            val = dkv_ref[seq, part_no, own_keys, :]
            for tile in range(1, ctx_count):
                val = val + dkv_in[peers[tile], seq, part_no].astype(f32)
            here = slice(seq * local, (seq + 1) * local)
            if part_no == 0:
                val = val * cos_ref[here, :] + pltpu.roll(val * sin_ref[here, :], 64, 1)
            span = slice(q_cols + part_no * 128, q_cols + (part_no + 1) * 128)
            dqkv_ref[here, span] = val.astype(bf16)
            acc_ref[2:3, span] = acc_ref[2:3, span] + jnp.sum(val, axis=0, keepdims=True)
    weight_blocks(4, a_ref, dqkv_ref[...], 0, qkv_cols)

    part_copies = []
    for index in range(width // 256):
        part[index] = lax.dot_general(
            dqkv_ref[...],
            wattn[index * 256 : (index + 1) * 256, :qkv_cols],
            (((1,), (1,)), ((), ())),
            preferred_element_type=f32,
        )
        part_copies.append(
            start(remote(part.at[index], part_in.at[index], ps.at[index], pr.at[index], to_core))
        )
    pump(2)
    for index, copy in enumerate(part_copies):
        copy.wait_recv()
        for seq in range(seqs):
            here = slice(seq * local, (seq + 1) * local)
            fin[seq, :, index * 256 : (index + 1) * 256] = part[index, here, :] + part_in[index, here, :]

    def norm_in(index, total):
        seq, piece = split(index)
        whole = pl.ds(pl.multiple_of(index * size, size), size)
        grad, val = fin[seq, piece, :], tok_ref[whole, :].astype(f32)
        inv = lax.rsqrt(jnp.mean(val * val, axis=-1, keepdims=True) + norm_eps)
        weighted = grad * row_ref[0:1, :]
        inner = jnp.mean(weighted * val, axis=-1, keepdims=True)
        dx_ref[seq, piece, :] = dx_ref[seq, piece, :] + (inv * weighted - val * (inv * inv * inv) * inner)
        return total + jnp.sum(grad * val * inv, axis=0, keepdims=True)

    acc_ref[0:1, :] = lax.fori_loop(0, seqs * per_seq, norm_in, jnp.zeros((1, width), f32))

    small_copies = [
        start(remote(acc_ref, sm_in.at[tile], gs.at[tile], gr.at[tile], {"ctx": peers[tile]}))
        for tile in range(1, ctx_count)
    ]
    while pending:
        pump(1)
    for half in range(2):
        stage_two(3, half)
    collect_fin(1)
    for half in range(2):
        stage_two(4, half)
    for half in range(2):
        stage_three(3, half)
    total = acc_ref[...]
    for tile, copy in enumerate(small_copies):
        copy.wait_recv()
        total = total + sm_in[tile + 1]
    sm_sum[0] = total
    small_turns = [
        remote(sm_sum.at[turn], sm_in.at[ctx_count + turn], gs.at[ctx_count + turn], gr.at[ctx_count + turn], target)
        for turn, target in ((0, to_x), (1, to_y))
    ]
    start(small_turns[0])
    fin_copy[1].wait()

    def act_rows(index, _):
        seq, piece = split(index)
        whole = pl.ds(pl.multiple_of(index * size, size), size)
        act_ref[seq, piece, :] = (h_ref[whole, :] + act_ref[seq, piece, :]) * live_ref[seq, piece, :]
        return 0

    lax.fori_loop(0, seqs * per_seq, act_rows, 0)
    small_turns[0].wait_recv()
    sm_sum[1] = sm_sum[0] + sm_in[ctx_count]
    start(small_turns[1])
    for half in range(2):
        stage_three(4, half)
    small_turns[1].wait_recv()
    rows_ref[...] = sm_sum[1] + sm_in[ctx_count + 1]
    for item in (0, 1, 2, 3, 4):
        for half in range(2):
            stage_four(item, half)
    for copy in sent:
        copy.wait_send()
    for here, copy in relay_sent:

        @pl.when(here)
        def _():
            copy.wait_send()


def backward_call(inputs, sizes):
    dp_count, ctx_count, own, qkv_cols, q_cols = sizes
    bf16, f32 = jnp.bfloat16, jnp.float32
    vmem, hbm = pl.BlockSpec(memory_space=pltpu.VMEM), pl.BlockSpec(memory_space=pl.ANY)
    held = inputs[5:14]
    seqs, local, width = held[0].shape
    ff = inputs[2].shape[3]
    group = own * ctx_count
    rows, keys = seqs * local, local * ctx_count
    heads = q_cols // 128
    attn_cols = held[8].shape[1]
    chunks = width // 256
    outs = [
        ((seqs, local, width), f32, vmem),
        ((seqs, local, width), f32, vmem),
        ((3, ctx_count, own, ff), bf16, hbm),
        ((own, attn_cols), f32, vmem),
        ((8, width), f32, vmem),
        ((2, dp_count, group, ff), bf16, hbm),
    ]
    scratch = [
        ((2, 2, ctx_count - 1, local, width), bf16),
        ((2, ctx_count, local, width), bf16),
        ((seqs, local, width), f32),
        ((2, ctx_count, seqs, local, group), bf16),
        ((ctx_count, rows, ff), bf16),
        ((2, group, ff), bf16),
        ((3, 2, group, ff), bf16),
        ((3, 2, group, ff), bf16),
        ((3, group, ff), bf16),
        ((2, group, attn_cols), bf16),
        ((2, group, attn_cols), bf16),
        ((2, group, attn_cols), bf16),
        ((group, attn_cols), bf16),
        ((ctx_count, own, attn_cols), bf16),
        ((rows, width), bf16),
        ((seqs, heads, local, 128), bf16),
        ((heads, local, keys), bf16),
        ((heads, local, keys), bf16),
        ((seqs, 2, keys, 128), f32),
        ((seqs, 2, keys, 128), bf16),
        ((ctx_count, seqs, 2, local, 128), bf16),
        ((rows, qkv_cols), bf16),
        ((chunks, rows, 256), f32),
        ((chunks, rows, 256), f32),
    ]
    dma = pltpu.SemaphoreType.DMA
    sems = [dma((2, 2, ctx_count)), dma((2, 2, ctx_count)), dma((2,)), dma((2,)), dma((3,)), dma((3, 5)), dma((5,))]
    sems += [
        dma(shape)
        for shape in ((5, 2, 2), (5, 2), (5, 2, ctx_count), (ctx_count,), (chunks,), (ctx_count + 2,))
        for _ in range(2)
    ]
    final = [((8, width), f32), ((ctx_count + 2, 8, width), f32), ((2, 8, width), f32)]
    final += [(array.shape, array.dtype) for array in held]
    return pl.pallas_call(
        functools.partial(backward_kernel, sizes),
        out_shape=[jax.ShapeDtypeStruct(shape, kind) for shape, kind, _ in outs],
        in_specs=[hbm] * 14 + [vmem] * (len(inputs) - 14),
        out_specs=[spec for _, _, spec in outs],
        scratch_shapes=[pltpu.VMEM(*entry) for entry in scratch]
        + sems
        + [pltpu.VMEM(*entry) for entry in final]
        + [dma((len(held),))],
        compiler_params=pltpu.CompilerParams(
            collective_id=1, has_side_effects=True, vmem_limit_bytes=65 * 1024 * 1024 - 65536
        ),
        name="backward_kernel",
    )(*inputs)


def on_device_kernels(
    tokens,
    cotangent,
    segments,
    positions,
    counts,
    attn_gain,
    q_weight,
    q_bias,
    k_weight,
    v_weight,
    kv_bias,
    o_weight,
    mlp_gain,
    gate_weight,
    up_weight,
    down_weight,
):
    dp_count, ctx_count = lax.axis_size("dp"), lax.axis_size("ctx")
    dp_rank, ctx_rank, core = lax.axis_index("dp"), lax.axis_index("ctx"), lax.axis_index("tp")
    seq_count, local_len, width = tokens.shape
    full_len = segments.shape[1]
    row_count = seq_count * local_len
    half_width = width // 2
    own_rows = q_weight.shape[1]
    group_rows = own_rows * ctx_count
    q_cols, k_cols, ff_cols = q_weight.shape[2], k_weight.shape[2], gate_weight.shape[2]
    kv_local = k_cols // HEAD_DIM
    group_size = q_cols // k_cols
    qkv_cols = q_cols + 2 * k_cols
    lane = 128
    ff_block = -(-ff_cols // (lane * ctx_count)) * lane
    ff_pad = ff_block * ctx_count - ff_cols
    f32, bf16 = jnp.float32, jnp.bfloat16

    parts = (attn_gain[0], mlp_gain[0], q_bias[0].reshape(-1), kv_bias[0].reshape(-1))
    cuts = [0]
    for part_vec in parts:
        cuts.append(cuts[-1] + part_vec.shape[0])
    small_own = jnp.pad(jnp.concatenate(parts).astype(f32)[None], ((0, 7), (0, 0)))
    attn_own = jnp.concatenate([q_weight[0], k_weight[0], v_weight[0], o_weight[0]], 1)
    mlp_own = jnp.stack(
        [
            jnp.pad(weight[0], ((0, 0), (0, ff_pad))).reshape(own_rows, ctx_count, ff_block).transpose(1, 0, 2)
            for weight in (gate_weight, up_weight, down_weight)
        ]
    )
    live_seq = (jnp.arange(seq_count, dtype=jnp.int32) < counts[0]).astype(f32)
    cot_live = (cotangent.astype(f32) * live_seq[:, None, None]).astype(bf16)
    query_seg = lax.dynamic_slice_in_dim(segments, ctx_rank * local_len, local_len, 1)
    cos_tab, sin_tab = rope_tables(positions.reshape(-1))
    sign = jnp.where(jnp.arange(HEAD_DIM) < HEAD_DIM // 2, -1.0, 1.0)
    (
        w_attn,
        _,
        mid_all,
        resid_mid,
        normed_in,
        query_hm,
        keyval_hm,
        attn_hm,
        log_total,
        small_rows,
        hidden_and_grads,
        part_sums,
        part_own,
        grad_down,
    ) = forward_call(
        tokens.reshape(-1, width),
        cot_live,
        attn_own,
        mlp_own,
        small_own,
        cos_tab,
        sin_tab * sign,
        query_seg[:, :, None],
        segments[:, None, :],
        qkv_cols,
        q_cols,
        cuts,
    )
    activations, input_grad, grad_ff, grad_w_attn, rows_sum, _ = backward_call(
        (
            part_sums,
            part_own,
            hidden_and_grads,
            mid_all,
            grad_down,
            cot_live,
            tokens.reshape(-1, width),
            resid_mid,
            normed_in,
            query_hm,
            keyval_hm,
            attn_hm,
            log_total,
            w_attn,
            jnp.broadcast_to(live_seq[:, None, None], (seq_count, local_len, 1)),
            small_rows,
            cos_tab,
            sin_tab * sign,
            query_seg[:, :, None],
            segments[:, None, :],
        ),
        (dp_count, ctx_count, own_rows, qkv_cols, q_cols),
    )
    grad_w_down, grad_w_gate, grad_w_up = (
        jnp.concatenate([grad_ff[item, block] for block in range(ctx_count)], 1)[:, :ff_cols].astype(f32)
        for item in range(3)
    )
    rank = dp_rank * ctx_count + ctx_rank

    def own_part(vector, size):
        return lax.dynamic_slice_in_dim(vector, rank * size, size, 0)

    bias_kv = jnp.concatenate(
        [
            rows_sum[2, q_cols : q_cols + k_cols].reshape(kv_local, -1).T,
            rows_sum[2, q_cols + k_cols : qkv_cols].reshape(kv_local, -1).T,
        ],
        0,
    ).reshape(-1)
    own = [
        own_part(rows_sum[0], own_rows)[None],
        own_part(rows_sum[1], own_rows)[None],
        own_part(rows_sum[2, :q_cols].reshape(kv_local, -1).T.reshape(-1), cuts[3] - cuts[2]),
        own_part(bias_kv, cuts[4] - cuts[3]),
    ]
    grad_w_qkv, grad_w_out = grad_w_attn[:, :qkv_cols], grad_w_attn[:, qkv_cols:]
    return (
        activations.reshape(tokens.shape),
        input_grad.reshape(tokens.shape),
        own[0],
        grad_w_qkv[None, :, :q_cols],
        own[2].reshape(q_bias.shape),
        grad_w_qkv[None, :, q_cols : q_cols + k_cols],
        grad_w_qkv[None, :, q_cols + k_cols :],
        own[3].reshape(kv_bias.shape),
        grad_w_out[None],
        own[1],
        grad_w_gate[None],
        grad_w_up[None],
        grad_w_down[None],
    )


def solution(mesh):
    in_specs = (
        P("dp", "ctx", None),
        P("dp", "ctx", None),
        P("dp", None),
        P("dp", "ctx"),
        P("dp"),
        P(None, ("dp", "ctx")),
        P(None, ("dp", "ctx"), "tp"),
        P(None, ("dp", "ctx"), "tp"),
        P(None, ("dp", "ctx"), "tp"),
        P(None, ("dp", "ctx"), "tp"),
        P(None, ("dp", "ctx"), "tp"),
        P(None, ("dp", "ctx"), "tp"),
        P(None, ("dp", "ctx")),
        P(None, ("dp", "ctx"), "tp"),
        P(None, ("dp", "ctx"), "tp"),
        P(None, ("dp", "ctx"), "tp"),
    )
    out_specs = (
        P("dp", "ctx", None),
        P("dp", "ctx", None),
        P(None, ("dp", "ctx")),
        P(None, ("dp", "ctx"), "tp"),
        P(None, ("dp", "ctx"), "tp"),
        P(None, ("dp", "ctx"), "tp"),
        P(None, ("dp", "ctx"), "tp"),
        P(None, ("dp", "ctx"), "tp"),
        P(None, ("dp", "ctx"), "tp"),
        P(None, ("dp", "ctx")),
        P(None, ("dp", "ctx"), "tp"),
        P(None, ("dp", "ctx"), "tp"),
        P(None, ("dp", "ctx"), "tp"),
    )
    kernels_fit = mesh.shape["dp"] == 4 and mesh.shape["ctx"] == 4 and mesh.shape["tp"] == KV_HEADS
    return jax.shard_map(
        on_device_kernels if kernels_fit else on_device, mesh=mesh, in_specs=in_specs, out_specs=out_specs, check_vma=False
    )
```

```python
import functools

import jax
import jax.numpy as jnp
from jax import lax
from jax.experimental import pallas as pl
from jax.experimental.pallas import tpu as pltpu
from jax.sharding import PartitionSpec as P

HEADS = 12
KV_HEADS = 2
HEAD_DIM = 128
LAYERS = 1


theta_base = 1000000.0
norm_eps = 1e-06
masked_score = -1e30


def mat_mul(left, right):
    return jnp.dot(left, right, preferred_element_type=jnp.float32)


def mat_mul_t(left, right):
    return lax.dot_general(
        left, right, (((1,), (1,)), ((), ())), preferred_element_type=jnp.float32
    )


def rows_mul(left, right):
    return lax.dot_general(
        left, right, (((0,), (0,)), ((), ())), preferred_element_type=jnp.float32
    )


def rope_tables(pos_vals):
    half_dim = HEAD_DIM // 2
    frequency = theta_base ** (-(jnp.arange(half_dim, dtype=jnp.float32) * (2.0 / HEAD_DIM)))
    angles = pos_vals.astype(jnp.float32)[..., None] * frequency
    cos_half = jnp.cos(angles)
    sin_half = jnp.sin(angles)
    return (jnp.concatenate([cos_half, cos_half], -1), jnp.concatenate([sin_half, sin_half], -1))


def rotate(values, cos_tab, sin_tab):
    half_dim = values.shape[-1] // 2
    turned = jnp.concatenate([-values[..., half_dim:], values[..., :half_dim]], -1)
    return values * cos_tab + turned * sin_tab


def unrotate(grad_vals, cos_tab, sin_tab):
    half_dim = grad_vals.shape[-1] // 2
    scaled = grad_vals * sin_tab
    turned = jnp.concatenate([scaled[..., half_dim:], -scaled[..., :half_dim]], -1)
    return grad_vals * cos_tab + turned


def norm_forward(residual, gain_vec):
    inv_rms = lax.rsqrt(jnp.mean(residual * residual, axis=-1, keepdims=True) + norm_eps)
    normed = (residual * inv_rms * gain_vec.astype(jnp.float32)).astype(jnp.bfloat16)
    return (inv_rms, normed)


def norm_backward(residual, inv_rms, gain_vec, grad_normed):
    weighted = grad_normed * gain_vec.astype(jnp.float32)
    inner_mean = jnp.mean(weighted * residual, axis=-1, keepdims=True)
    grad_resid = inv_rms * weighted - residual * (inv_rms * inv_rms * inv_rms) * inner_mean
    grad_gain = jnp.sum(grad_normed * residual * inv_rms, axis=0)
    return (grad_resid, grad_gain)


def split_heads(keys_all, values_all):
    seq_count, full_len, kv_width = keys_all.shape
    kv_local = kv_width // HEAD_DIM
    return (
        keys_all.reshape(seq_count, full_len, kv_local, HEAD_DIM),
        values_all.reshape(seq_count, full_len, kv_local, HEAD_DIM),
    )


def attend_forward(query_bf, keys_all, values_all, allowed):
    key_heads, value_heads = split_heads(keys_all, values_all)
    scores = jnp.einsum(
        "bqkgd,bskd->bkgqs", query_bf, key_heads, preferred_element_type=jnp.float32
    ) * HEAD_DIM ** (-0.5)
    scores = jnp.where(allowed[:, None, None], scores, masked_score)
    top_score = jnp.max(scores, axis=-1, keepdims=True)
    shifted_exp = jnp.exp(scores - top_score)
    totals = jnp.sum(shifted_exp, axis=-1, keepdims=True)
    prob_bf = (shifted_exp / totals).astype(jnp.bfloat16)
    output = jnp.einsum(
        "bkgqs,bskd->bqkgd", prob_bf, value_heads, preferred_element_type=jnp.float32
    )
    return (output.astype(jnp.bfloat16), top_score + jnp.log(totals))


def attend_backward(query_bf, keys_all, values_all, attn_bf, log_total, grad_attn, allowed):
    key_heads, value_heads = split_heads(keys_all, values_all)
    scores = jnp.einsum(
        "bqkgd,bskd->bkgqs", query_bf, key_heads, preferred_element_type=jnp.float32
    ) * HEAD_DIM ** (-0.5)
    prob_full = jnp.exp(jnp.where(allowed[:, None, None], scores, masked_score) - log_total)
    prob_bf = prob_full.astype(jnp.bfloat16)
    grad_value = jnp.einsum(
        "bkgqs,bqkgd->bskd", prob_bf, grad_attn, preferred_element_type=jnp.float32
    )
    grad_prob = jnp.einsum(
        "bqkgd,bskd->bkgqs", grad_attn, value_heads, preferred_element_type=jnp.float32
    )
    row_dot = jnp.sum(grad_attn.astype(jnp.float32) * attn_bf.astype(jnp.float32), axis=-1)
    row_dot = jnp.transpose(row_dot, (0, 2, 3, 1))[..., None]
    grad_score = (prob_full * (grad_prob - row_dot) * HEAD_DIM ** (-0.5)).astype(jnp.bfloat16)
    grad_query = jnp.einsum(
        "bkgqs,bskd->bqkgd", grad_score, key_heads, preferred_element_type=jnp.float32
    )
    grad_key = jnp.einsum(
        "bkgqs,bqkgd->bskd", grad_score, query_bf, preferred_element_type=jnp.float32
    )
    return (grad_query, grad_key.reshape(keys_all.shape), grad_value.reshape(values_all.shape))


def xor_permute(value, axis_name, step):
    count = lax.axis_size(axis_name)
    return lax.ppermute(value, axis_name, [(rank, rank ^ step) for rank in range(count)])


def axis_bits(axis_name):
    return [1 << shift for shift in range(lax.axis_size(axis_name).bit_length() - 1)]


def partner(value):
    return xor_permute(value, "tp", 1)


def place(pieces, rank, dim):
    width = pieces[0].shape[dim]
    whole_shape = list(pieces[0].shape)
    whole_shape[dim] = width * len(pieces)
    whole = jnp.zeros(whole_shape, pieces[0].dtype)
    for offset, piece in enumerate(pieces):
        whole = lax.dynamic_update_slice_in_dim(whole, piece, (rank ^ offset) * width, dim)
    return whole


def join_halves(mine, other, core, dim):
    return jnp.where(
        core == 0, jnp.concatenate([mine, other], dim), jnp.concatenate([other, mine], dim)
    )


def gather_direct(value, axis_name):
    count = lax.axis_size(axis_name)
    return [value] + [xor_permute(value, axis_name, step) for step in range(1, count)]


def gather_halves(value, axis_name):
    rows = value.shape[0]
    half = rows // 2
    bits = axis_bits(axis_name)
    parts = []
    for piece, order in ((value[:half], bits), (value[half:], bits[::-1])):
        held = {0: piece}
        for bit in order:
            for key in list(held):
                held[key | bit] = xor_permute(held[key], axis_name, bit)
        parts.append(held)
    return [(parts[0][key], parts[1][key]) for key in range(len(parts[0]))]


def scatter_halves(blocks, axis_name):
    half = blocks[0].shape[0] // 2
    bits = axis_bits(axis_name)
    done = []
    for low, high, order in ((0, half, bits[::-1]), (half, 2 * half, bits)):
        held = {key: block[low:high] for key, block in enumerate(blocks)}
        for bit in order:
            for key in [key for key in held if key & bit]:
                sent = held.pop(key).astype(jnp.bfloat16)
                held[key ^ bit] = held[key ^ bit] + xor_permute(sent, axis_name, bit).astype(jnp.float32)
        done.append(held[0])
    return jnp.concatenate(done, 0)


def scatter_small(blocks, axis_name):
    held = dict(enumerate(blocks))
    for bit in axis_bits(axis_name)[::-1]:
        for key in [key for key in held if key & bit]:
            held[key ^ bit] = held[key ^ bit] + xor_permute(held.pop(key), axis_name, bit)
    return held[0]


def scatter_direct(block_of, axis_name):
    total = block_of(0)
    for step in range(1, lax.axis_size(axis_name)):
        got = xor_permute(block_of(step).astype(jnp.bfloat16), axis_name, step)
        total = total + got.astype(jnp.float32)
    return total


def rows_at(value, index, size):
    return lax.dynamic_slice_in_dim(value, index * size, size, 0)


def columns_at(value, index, size):
    return lax.dynamic_slice_in_dim(value, index * size, size, 1)


def on_device(
    tokens,
    cotangent,
    segments,
    positions,
    counts,
    attn_gain,
    q_weight,
    q_bias,
    k_weight,
    v_weight,
    kv_bias,
    o_weight,
    mlp_gain,
    gate_weight,
    up_weight,
    down_weight,
):
    dp_count, ctx_count = lax.axis_size("dp"), lax.axis_size("ctx")
    dp_rank, ctx_rank, core = lax.axis_index("dp"), lax.axis_index("ctx"), lax.axis_index("tp")
    seq_count, local_len, width = tokens.shape
    full_len = segments.shape[1]
    row_count = seq_count * local_len
    half_width = width // 2
    own_rows = q_weight.shape[1]
    group_rows = own_rows * ctx_count
    q_cols, k_cols, ff_cols = q_weight.shape[2], k_weight.shape[2], gate_weight.shape[2]
    kv_local = k_cols // HEAD_DIM
    group_size = q_cols // k_cols
    qkv_cols = q_cols + 2 * k_cols
    lane = 128
    ff_block = -(-ff_cols // (lane * ctx_count)) * lane
    ff_pad = ff_block * ctx_count - ff_cols
    f32, bf16 = jnp.float32, jnp.bfloat16

    small = jnp.concatenate(
        [attn_gain[0], mlp_gain[0], q_bias[0].reshape(-1), kv_bias[0].reshape(-1)]
    )[None]
    sizes = (attn_gain.shape[1], mlp_gain.shape[1], q_bias.shape[1] * q_bias.shape[2], kv_bias.shape[1] * kv_bias.shape[2])
    small_ctx = place(gather_direct(small, "ctx"), ctx_rank, 0)[None]
    held = {0: small_ctx}
    for bit in axis_bits("dp"):
        for key in list(held):
            held[key | bit] = xor_permute(held[key], "dp", bit)
    small_all = place([held[key] for key in range(dp_count)], dp_rank, 0)
    small_all = small_all.reshape(dp_count * ctx_count, -1)
    cuts = [0]
    for size in sizes:
        cuts.append(cuts[-1] + size)
    gain_in, gain_mid, b_query, b_keyval = (
        small_all[:, low:high].reshape(-1) for low, high in zip(cuts[:-1], cuts[1:])
    )
    b_query = b_query.reshape(-1, kv_local).T.reshape(-1).astype(f32)
    b_keyval = b_keyval.reshape(-1, kv_local).astype(f32)
    b_qkv = jnp.concatenate(
        [b_query, b_keyval[:HEAD_DIM].T.reshape(-1), b_keyval[HEAD_DIM:].T.reshape(-1)]
    )

    attn_own = jnp.concatenate([q_weight[0], k_weight[0], v_weight[0], o_weight[0]], 1)
    attn_group = place(gather_direct(attn_own, "ctx"), ctx_rank, 0)
    attn_pairs = gather_halves(attn_group, "dp")
    w_attn = place([jnp.concatenate(pair, 0) for pair in attn_pairs], dp_rank, 0)
    w_qkv, w_out = w_attn[:, :qkv_cols], w_attn[:, qkv_cols:]

    live_seq = (jnp.arange(seq_count, dtype=jnp.int32) < counts[0]).astype(f32)
    live_rows = jnp.repeat(live_seq, local_len)[:, None]
    grad_out = cotangent.astype(f32).reshape(-1, width) * live_rows

    def spread(rows_bf):
        mine = jnp.concatenate(gather_direct(columns_at(rows_bf, core, half_width), "ctx"), 0)
        return join_halves(mine, partner(mine), core, 1)

    grad_all = spread(grad_out.astype(bf16))

    def spread_weight(weight):
        padded = jnp.pad(weight[0], ((0, 0), (0, ff_pad)))
        pieces = [columns_at(padded, ctx_rank, ff_block)]
        for step in range(1, ctx_count):
            pieces.append(xor_permute(columns_at(padded, ctx_rank ^ step, ff_block), "ctx", step))
        pairs = gather_halves(place(pieces, ctx_rank, 0), "dp")
        return place([jnp.concatenate(pair, 0) for pair in pairs], dp_rank, 0)

    w_gate = spread_weight(gate_weight)
    w_up = spread_weight(up_weight)
    w_down = spread_weight(down_weight)

    query_pos = ctx_rank * local_len + jnp.arange(local_len, dtype=jnp.int32)
    key_pos = jnp.arange(full_len, dtype=jnp.int32)
    query_seg = lax.dynamic_slice_in_dim(segments, ctx_rank * local_len, local_len, 1)
    allowed = (query_seg[:, :, None] == segments[:, None, :]) & (
        key_pos[None, None, :] <= query_pos[None, :, None]
    )
    cos_tab, sin_tab = rope_tables(positions.reshape(-1))
    cos_tab, sin_tab = cos_tab[:, None, :], sin_tab[:, None, :]
    residual = tokens.astype(f32).reshape(-1, width)
    inv_in, normed_in = norm_forward(residual, gain_in)
    qkv_val = mat_mul(normed_in, w_qkv) + b_qkv
    query_bf = rotate(
        qkv_val[:, :q_cols].reshape(row_count, -1, HEAD_DIM), cos_tab, sin_tab
    ).astype(bf16).reshape(seq_count, -1, kv_local, group_size, HEAD_DIM)
    key_bf = rotate(
        qkv_val[:, q_cols : q_cols + k_cols].reshape(row_count, -1, HEAD_DIM), cos_tab, sin_tab
    ).astype(bf16).reshape(row_count, -1)
    value_bf = qkv_val[:, q_cols + k_cols :].astype(bf16)
    keyval = jnp.concatenate([key_bf, value_bf], 1).reshape(seq_count, local_len, -1)
    keyval_all = place(gather_direct(keyval, "ctx"), ctx_rank, 1)
    keys_all, values_all = keyval_all[..., :k_cols], keyval_all[..., k_cols:]
    attn_bf, log_total = attend_forward(query_bf, keys_all, values_all, allowed)
    attn_flat = attn_bf.reshape(row_count, -1)
    out_part = mat_mul_t(attn_flat, w_out)
    resid_mid = residual + (out_part + partner(out_part))
    inv_mid, normed_mid = norm_forward(resid_mid, gain_mid)

    mid_all = spread(normed_mid)
    gate_pre = mat_mul(mid_all, w_gate)
    up_pre = mat_mul(mid_all, w_up)
    hidden_bf = (jax.nn.silu(gate_pre) * up_pre).astype(bf16)
    grad_hidden = mat_mul(grad_all, w_down)
    sigmoid_gate = jax.nn.sigmoid(gate_pre)
    grad_gate = (
        grad_hidden * up_pre * sigmoid_gate * (1.0 + gate_pre * (1.0 - sigmoid_gate))
    ).astype(bf16)
    grad_up = (grad_hidden * gate_pre * sigmoid_gate).astype(bf16)

    def collect(part):
        part_bf = columns_at(part, 1 - core, half_width).astype(bf16)
        mine = columns_at(part, core, half_width) + partner(part_bf).astype(f32)
        total = scatter_direct(lambda step: mine[step * row_count : (step + 1) * row_count], "ctx")
        return join_halves(total, partner(total), core, 1)

    grad_normed_mid = collect(mat_mul_t(grad_gate, w_gate) + mat_mul_t(grad_up, w_up))

    def owner_weight(left, right):
        blocks = [
            rows_mul(columns_at(left, dp_rank ^ step, group_rows), right)
            for step in range(dp_count)
        ]
        group = scatter_halves(blocks, "dp").astype(bf16)
        pieces = [rows_at(group, ctx_rank, own_rows)]
        for step in range(1, ctx_count):
            pieces.append(xor_permute(rows_at(group, ctx_rank ^ step, own_rows), "ctx", step))
        return place(pieces, ctx_rank, 1)[:, :ff_cols].astype(f32)

    grad_w_down = owner_weight(grad_all, hidden_bf)
    grad_w_gate = owner_weight(mid_all, grad_gate)
    grad_w_up = owner_weight(mid_all, grad_up)

    layer_out = resid_mid + collect(mat_mul_t(hidden_bf, w_down))
    activations = (layer_out * live_rows).reshape(tokens.shape)

    grad_mid_norm, grad_gain_mid = norm_backward(resid_mid, inv_mid, gain_mid, grad_normed_mid)
    grad_mid = grad_out + grad_mid_norm
    grad_mid_bf = grad_mid.astype(bf16)
    grad_attn = mat_mul(grad_mid_bf, w_out).astype(bf16)

    def owner_attn(left, right):
        blocks = [
            rows_mul(columns_at(left, dp_rank ^ step, group_rows), right)
            for step in range(dp_count)
        ]
        group = scatter_halves(blocks, "dp")
        return scatter_direct(lambda step: rows_at(group, ctx_rank ^ step, own_rows), "ctx")

    grad_w_out = owner_attn(grad_mid_bf, attn_flat)
    grad_query, grad_key_all, grad_value_all = attend_backward(
        query_bf, keys_all, values_all, attn_bf, log_total, grad_attn.reshape(attn_bf.shape), allowed
    )
    grad_keyval_all = jnp.concatenate([grad_key_all, grad_value_all], 2)
    grad_keyval = scatter_direct(
        lambda step: lax.dynamic_slice_in_dim(
            grad_keyval_all, (ctx_rank ^ step) * local_len, local_len, 1
        ),
        "ctx",
    ).reshape(row_count, -1)
    grad_query = unrotate(
        grad_query.reshape(row_count, -1, HEAD_DIM), cos_tab, sin_tab
    ).reshape(row_count, -1)
    grad_key = unrotate(
        grad_keyval[:, :k_cols].reshape(row_count, -1, HEAD_DIM), cos_tab, sin_tab
    ).reshape(row_count, -1)
    grad_qkv = jnp.concatenate([grad_query, grad_key, grad_keyval[:, k_cols:]], 1)
    grad_qkv_bf = grad_qkv.astype(bf16)
    grad_w_qkv = owner_attn(normed_in, grad_qkv_bf)
    dot_part = mat_mul_t(grad_qkv_bf, w_qkv)
    grad_normed_in = dot_part + partner(dot_part)
    grad_in_norm, grad_gain_in = norm_backward(residual, inv_in, gain_in, grad_normed_in)
    input_grad = (grad_mid + grad_in_norm).reshape(tokens.shape)

    bias_sum = jnp.sum(grad_qkv, axis=0)
    device_count = dp_count * ctx_count
    grad_small = jnp.concatenate(
        [
            grad_gain_in.reshape(device_count, -1),
            grad_gain_mid.reshape(device_count, -1),
            bias_sum[:q_cols].reshape(kv_local, -1).T.reshape(device_count, -1),
            jnp.concatenate(
                [
                    bias_sum[q_cols : q_cols + k_cols].reshape(kv_local, -1).T,
                    bias_sum[q_cols + k_cols :].reshape(kv_local, -1).T,
                ],
                0,
            ).reshape(device_count, -1),
        ],
        1,
    )
    small_group = scatter_small(
        [rows_at(grad_small, dp_rank ^ step, ctx_count) for step in range(dp_count)], "dp"
    )
    small_own = scatter_small(
        [rows_at(small_group, ctx_rank ^ step, 1) for step in range(ctx_count)], "ctx"
    )
    own = [small_own[:, low:high] for low, high in zip(cuts[:-1], cuts[1:])]
    return (
        activations,
        input_grad,
        own[0],
        grad_w_qkv[None, :, :q_cols],
        own[2].reshape(q_bias.shape),
        grad_w_qkv[None, :, q_cols : q_cols + k_cols],
        grad_w_qkv[None, :, q_cols + k_cols :],
        own[3].reshape(kv_bias.shape),
        grad_w_out[None],
        own[1],
        grad_w_gate[None],
        grad_w_up[None],
        grad_w_down[None],
    )


MESH = pl.DeviceIdType.MESH


def remote(src, dst, send_sem, recv_sem, target):
    return pltpu.make_async_remote_copy(
        src_ref=src, dst_ref=dst, send_sem=send_sem, recv_sem=recv_sem, device_id=target, device_id_type=MESH
    )


def greet(partners):
    barrier = pltpu.get_barrier_semaphore()
    for partner_id in partners:
        pl.semaphore_signal(barrier, inc=1, device_id=partner_id, device_id_type=MESH)
    pl.semaphore_wait(barrier, len(partners))


def spread_row(values, row_cols, period, total):
    left = lax.broadcasted_iota(jnp.int32, (period, total), 0)
    right = lax.broadcasted_iota(jnp.int32, (period, total), 1)
    pick = (lax.rem(right, period) == left).astype(jnp.float32).astype(jnp.bfloat16)
    spread = jnp.dot(values.astype(jnp.bfloat16), pick, preferred_element_type=jnp.float32)
    block = lax.broadcasted_iota(jnp.int32, spread.shape, 0) // 8
    owner = lax.broadcasted_iota(jnp.int32, spread.shape, 1) // period
    return jnp.sum(jnp.where(block == owner, spread, 0.0), axis=0, keepdims=True)


def same_document(seg_ref, seq, ctx, local):
    row = seg_ref[seq : seq + 1, pl.ds(pl.multiple_of(ctx * local, local), local)].astype(jnp.float32)
    down = lax.broadcasted_iota(jnp.int32, (local, local), 0)
    across = lax.broadcasted_iota(jnp.int32, (local, local), 1)
    column = jnp.sum(jnp.where(down == across, row, 0.0), axis=1, keepdims=True)
    return column == seg_ref[seq : seq + 1, :].astype(jnp.float32)


def forward_kernel(
    sizes,
    tok_ref,
    cot_ref,
    attn_own,
    gate_own,
    up_own,
    down_own,
    small_own,
    cos_ref,
    sin_ref,
    seg_ref,
    live_ref,
    wattn_out,
    b_out,
    h_out,
    a_out,
    q_out,
    kv_out,
    o_out,
    lse_out,
    row_out,
    zgu_out,
    sum_out,
    own_out,
    down_out,
    wattn,
    wmlp,
    e_all,
    b_all,
    h_ref,
    a_ref,
    q_ref,
    kv_ref,
    o_ref,
    lse_ref,
    row_ref,
    small,
    part,
    part_in,
    gu_ref,
    z_ref,
    zgu,
    block_ref,
    pair,
    give,
    take,
    done,
    mine,
    zs,
    zr,
    xs,
    xr,
    ys,
    yr,
    fs,
    fr,
    ks,
    kr,
    ps,
    pr,
    bs,
    br,
    us,
    ur,
    ts,
    tr,
    loc,
    out_sem,
    down_sem,
):
    dp_count, ctx_count, own, qkv_cols, q_cols, gain_cut = sizes
    dp, ctx, core = lax.axis_index("dp"), lax.axis_index("ctx"), lax.axis_index("tp")
    bf16, f32 = jnp.bfloat16, jnp.float32
    width = tok_ref.shape[1]
    rows = tok_ref.shape[0]
    seqs = cot_ref.shape[0]
    local = cot_ref.shape[1]
    tiles = range(ctx_count)

    def at_x(d):
        return d + 1 - 2 * lax.rem(d, 2)

    def at_y(d):
        return lax.rem(d + 2, 4)

    dpx, dpy = at_x(dp), at_y(dp)
    dpd = at_x(dpy)
    peers = [ctx]
    for step in range(1, ctx_count):
        value = jnp.int32(0)
        for bit in (1, 2, 4, 8):
            if bit < ctx_count:
                digit = lax.rem(ctx // bit, 2)
                value = value + bit * (digit + (1 - 2 * digit) * ((step // bit) % 2))
        peers.append(value)
    other = 1 - core
    to_core = {"tp": other}

    greet(
        [{"dp": dpx}, {"dp": dpy}, {"tp": other}] + [{"ctx": peers[step]} for step in range(1, ctx_count)]
    )
    sent = []

    def start(copy):
        copy.start()
        sent.append(copy)
        return copy

    def block_rows(d, c):
        return pl.ds(pl.multiple_of((d * ctx_count + c) * own, own), own)

    def slot(item, d, c):
        if item == 0:
            return small.at[d * ctx_count + c]
        if item == 1:
            return wattn.at[block_rows(d, c), :]
        return wmlp.at[item - 2, block_rows(d, c), :]

    def source(item):
        return small_own if item == 0 else attn_own

    ff_block = wmlp.shape[2]
    top = ctx_count - 1
    ff_tail = gate_own.shape[1] - top * ff_block

    class Either:
        def __init__(self, full_there, full_here, wide, slim):
            self.there, self.here, self.wide, self.slim = full_there, full_here, wide, slim

        def pick(self, full, name):
            @pl.when(full)
            def _():
                getattr(self.wide, name)()

            @pl.when(jnp.logical_not(full))
            def _():
                getattr(self.slim, name)()

        def start(self):
            self.pick(self.there, "start")

        def wait_send(self):
            self.pick(self.there, "wait_send")

        def wait_recv(self):
            self.pick(self.here, "wait_recv")

        def wait(self):
            self.pick(self.here, "wait")

    def column_copy(item, tile, make):
        own_weight = (gate_own, up_own, down_own)[item - 2]
        peer = peers[tile]
        wide_from = own_weight.at[:, pl.ds(pl.multiple_of(jnp.minimum(peer, top - 1) * ff_block, 128), ff_block)]
        slim_from = own_weight.at[:, top * ff_block :]
        place_at = block_rows(dp, ctx)
        return Either(
            peer != top,
            ctx != top,
            make(wide_from, wmlp.at[item - 2, place_at, :]),
            make(slim_from, wmlp.at[item - 2, place_at, 0:ff_tail]),
        )

    if ff_tail < ff_block:

        @pl.when(ctx == top)
        def _():
            fill = pl.ds(pl.multiple_of(dp * own * ctx_count, own), own * ctx_count)
            for item in range(3):
                wmlp[item, fill, ff_tail:] = jnp.zeros((own * ctx_count, ff_block - ff_tail), bf16)


    items = range(5)
    local_copies = []
    for item in items:
        if item < 2:
            copy = pltpu.make_async_copy(source(item), slot(item, dp, ctx), loc.at[item])
        else:
            copy = column_copy(item, 0, lambda src, dst: pltpu.make_async_copy(src, dst, loc.at[item]))
        copy.start()
        local_copies.append(copy)
    z_copy = {}

    def z_send(item):
        for tile in range(1, ctx_count):

            def make(src, dst):
                return remote(src, dst, zs.at[item, tile], zr.at[item, tile], {"ctx": peers[tile]})

            if item < 2:
                z_copy[item, tile] = start(make(source(item), slot(item, dp, ctx)))
            else:
                z_copy[item, tile] = start(column_copy(item, tile, make))

    x_copy, y_copy, f_copy = {}, {}, {}

    def xy_send(item, tile):
        src = source(item) if tile == 0 and item < 2 else slot(item, dp, peers[tile])
        if tile:
            z_copy[item, tile].wait_recv()
        elif item >= 2:
            local_copies[item].wait()
        dst = slot(item, dp, peers[tile])
        x_copy[item, tile] = start(remote(src, dst, xs.at[item, tile], xr.at[item, tile], {"dp": dpx}))
        y_copy[item, tile] = start(remote(src, dst, ys.at[item, tile], yr.at[item, tile], {"dp": dpy}))

    def forward(item, tile):
        if (item + tile) % 2 == 0:
            x_copy[item, tile].wait_recv()
            place_at = slot(item, dpx, peers[tile])
            target = {"dp": dpy}
        else:
            y_copy[item, tile].wait_recv()
            place_at = slot(item, dpy, peers[tile])
            target = {"dp": dpx}
        f_copy[item, tile] = start(remote(place_at, place_at, fs.at[item, tile], fr.at[item, tile], target))

    def settle(item, tile):
        if (item + tile) % 2 == 0:
            y_copy[item, tile].wait_recv()
        else:
            x_copy[item, tile].wait_recv()
        f_copy[item, tile].wait_recv()

    last = ctx_count - 1
    ways = ((1, ctx < last), (-1, ctx > 0))
    relay_sent = []

    def hop(index, buf, way, distance, origin):
        step, _ = ways[way]
        piece = buf.at[origin, core]
        return remote(piece, piece, bs.at[index, way, distance], br.at[index, way, distance], {"ctx": ctx + step})

    def spread_start(index, buf):
        for way in range(2):
            copy = hop(index, buf, way, 0, ctx)

            @pl.when(ways[way][1])
            def _():
                copy.start()

            relay_sent.append((ways[way][1], copy))

    def spread_step(index, buf, distance):
        for way in range(2):
            step, open_end = ways[way]
            origin = ctx - step * distance
            here = (origin >= 0) & (origin <= last)
            safe = jnp.clip(origin, 0, last)
            piece = buf.at[safe, core]
            got = remote(piece, piece, bs.at[index, way, distance - 1], br.at[index, way, distance - 1], to_core)
            share = remote(piece, piece, us.at[index, way, distance], ur.at[index, way, distance], to_core)

            @pl.when(here)
            def _():
                got.wait_recv()
                share.start()

            relay_sent.append((here, share))
            if distance < last:
                copy = hop(index, buf, way, distance, safe)

                @pl.when(here & open_end)
                def _():
                    copy.start()

                relay_sent.append((here & open_end, copy))

    def spread_end(index, buf, distance):
        for way in range(2):
            step, _ = ways[way]
            origin = ctx - step * distance
            piece = buf.at[jnp.clip(origin, 0, last), other]
            got = remote(piece, piece, us.at[index, way, distance], ur.at[index, way, distance], to_core)

            @pl.when((origin >= 0) & (origin <= last))
            def _():
                got.wait_recv()

    z_send(0)
    z_send(1)
    xy_send(1, 0)
    for item in (2, 3):
        z_send(item)
    e_local = pltpu.make_async_copy(cot_ref, e_all.at[ctx], loc.at[5])
    e_local.start()
    kept = []

    def keep_out(src, dst):
        copy = pltpu.make_async_copy(src, dst, out_sem.at[len(kept)])
        copy.start()
        kept.append(copy)

    for tile in tiles:
        xy_send(0, tile)
    for tile in tiles:
        forward(0, tile)
    for tile in range(1, ctx_count):
        xy_send(1, tile)
    for tile in tiles:
        settle(0, tile)
    local_copies[0].wait()

    flat = small[...].reshape(dp_count * ctx_count * 8, small.shape[2])
    row_ref[0:1, :] = spread_row(flat[:, gain_cut[0] : gain_cut[1]], None, gain_cut[1] - gain_cut[0], width)
    row_ref[1:2, :] = spread_row(flat[:, gain_cut[1] : gain_cut[2]], None, gain_cut[2] - gain_cut[1], width)
    row_ref[2:3, :q_cols] = spread_row(flat[:, gain_cut[2] : gain_cut[3]], None, gain_cut[3] - gain_cut[2], q_cols)
    row_ref[2:3, q_cols:qkv_cols] = spread_row(
        flat[:, gain_cut[3] : gain_cut[4]], None, gain_cut[4] - gain_cut[3], qkv_cols - q_cols
    )

    step_rows = 32

    def norm_in(index, _):
        piece = pl.ds(index * step_rows, step_rows)
        val = tok_ref[piece, :].astype(f32)
        inv = lax.rsqrt(jnp.mean(val * val, axis=-1, keepdims=True) + norm_eps)
        a_ref[piece, :] = (val * inv * row_ref[0:1, :]).astype(bf16)
        return 0

    lax.fori_loop(0, rows // step_rows, norm_in, 0)
    e_local.wait()

    def mask_rows(index, _):
        per_seq = local // step_rows
        seq = index // per_seq
        piece = pl.ds(pl.multiple_of(lax.rem(index, per_seq) * step_rows, step_rows), step_rows)
        e_all[ctx, seq, piece, :] = (e_all[ctx, seq, piece, :].astype(f32) * live_ref[seq][:, 0:1]).astype(bf16)
        return 0

    lax.fori_loop(0, rows // step_rows, mask_rows, 0)
    for tile in tiles:
        forward(1, tile)
    for item in (2, 3, 4):
        xy_send(item, 0)
    for tile in tiles:
        if tile:
            xy_send(2, tile)
    for tile in tiles:
        settle(1, tile)
    local_copies[1].wait()
    keep_out(wattn, wattn_out)
    keep_out(a_ref, a_out)
    keep_out(row_ref, row_out)

    pending = [(forward, 2, 0), (forward, 3, 0), (forward, 4, 0)]
    pending += [(xy_send, 3, tile) for tile in tiles if tile]
    pending += [(forward, 2, tile) for tile in tiles if tile]
    pending += [(forward, 3, 1)] + [(xy_send, 4, tile) for tile in tiles if tile]
    pending += [(forward, 3, 2), (forward, 3, 3)]
    pending += [(forward, 4, tile) for tile in tiles if tile]

    def pump(count):
        for _ in range(min(count, len(pending))):
            action, item, tile = pending.pop(0)
            action(item, tile)

    own_keys = pl.ds(pl.multiple_of(ctx * local, local), local)
    order = [qkv_cols - 256] + list(range(0, q_cols, 256))
    kv_copies = []
    for low in order:
        val = jnp.dot(a_ref[...], wattn[:, low : low + 256], preferred_element_type=f32) + row_ref[2:3, low : low + 256]
        for head_low in (0, 128):
            head = val[:, head_low : head_low + 128]
            if low + head_low < qkv_cols - 128:
                head = head * cos_ref[...] + pltpu.roll(head, 64, 1) * sin_ref[...]
            head = head.astype(bf16)
            for seq in range(seqs):
                piece = head[seq * local : (seq + 1) * local]
                if low == qkv_cols - 256:
                    kv_ref[seq, head_low // 128, own_keys, :] = piece
                else:
                    q_ref[seq, (low + head_low) // 128] = piece
        if low == qkv_cols - 256:
            for tile in range(1, ctx_count):
                piece = kv_ref.at[:, :, own_keys, :]
                kv_copies.append(start(remote(piece, piece, ks.at[tile], kr.at[tile], {"ctx": peers[tile]})))
    keep_out(q_ref, q_out)
    pump(1)
    for copy in kv_copies:
        copy.wait_recv()
    z_send(4)
    pump(5)
    keep_out(kv_ref, kv_out)

    keys = kv_ref.shape[2]
    key_no = lax.broadcasted_iota(jnp.int32, (local, keys), 1)
    query_no = lax.broadcasted_iota(jnp.int32, (local, keys), 0) + ctx * local
    for seq in range(seqs):
        seen = same_document(seg_ref, seq, ctx, local) & (key_no <= query_no)
        hide = jnp.where(seen, 0.0, masked_score)

        def one_head(head, _):
            score = lax.dot_general(
                q_ref[seq, head], kv_ref[seq, 0], (((1,), (1,)), ((), ())), preferred_element_type=f32
            )
            score = jnp.where(hide < 0.0, masked_score, score * HEAD_DIM ** (-0.5))
            top = jnp.max(score, axis=-1, keepdims=True)
            weight = jnp.exp(score - top)
            total = jnp.sum(weight, axis=-1, keepdims=True)
            prob = (weight / total).astype(bf16)
            lse_ref[seq, head] = top + jnp.log(total)
            out = jnp.dot(prob, kv_ref[seq, 1], preferred_element_type=f32)
            o_ref[seq, head] = out.astype(bf16)
            return 0

        lax.fori_loop(0, q_cols // 128, one_head, 0)
        pump(2 - seq)
    keep_out(o_ref, o_out)
    keep_out(lse_ref, lse_out)

    o_rows = jnp.concatenate(
        [jnp.concatenate([o_ref[seq, head] for head in range(q_cols // 128)], 1) for seq in range(seqs)], 0
    )
    part_copies = []
    for index in range(width // 256):
        part[index] = lax.dot_general(
            o_rows,
            wattn[index * 256 : (index + 1) * 256, qkv_cols:],
            (((1,), (1,)), ((), ())),
            preferred_element_type=f32,
        )
        part_copies.append(
            start(remote(part.at[index], part_in.at[index], ps.at[index], pr.at[index], {"tp": other}))
        )
    for index, copy in enumerate(part_copies):
        copy.wait_recv()
        span = slice(index * 256, (index + 1) * 256)
        h_ref[:, span] = tok_ref[:, span].astype(f32) + (part[index] + part_in[index])

    def norm_mid(index, _):
        piece = pl.ds(index * step_rows, step_rows)
        val = h_ref[piece, :]
        inv = lax.rsqrt(jnp.mean(val * val, axis=-1, keepdims=True) + norm_eps)
        per_seq = local // step_rows
        b_all[ctx, index // per_seq, pl.ds(lax.rem(index, per_seq) * step_rows, step_rows), :] = (
            val * inv * row_ref[1:2, :]
        ).astype(bf16)
        return 0

    lax.fori_loop(0, rows // step_rows, norm_mid, 0)
    spread_start(1, b_all)
    keep_out(h_ref, h_out)
    pump(4)
    spread_step(1, b_all, 1)
    pump(2)
    spread_step(1, b_all, 2)
    spread_start(0, e_all)

    ff = wmlp.shape[2]
    full_ff = ff // 256 * 256
    nt = (((1,), (1,)), ((), ()))

    def ahead_columns(peer, low, size):
        span = pl.ds(low, size)
        gate = jnp.dot(b_all[peer].reshape(rows, width), wmlp[0, :, span], preferred_element_type=f32)
        up = jnp.dot(b_all[peer].reshape(rows, width), wmlp[1, :, span], preferred_element_type=f32)
        gu_ref[0, peer, :, span] = gate
        gu_ref[1, peer, :, span] = up
        z_ref[peer, :, span] = (gate * jax.nn.sigmoid(gate) * up).astype(bf16)

    def back_columns(tile, low, size):
        span, peer = pl.ds(low, size), peers[tile]
        grad = jnp.dot(e_all[peer].reshape(rows, width), wmlp[2, :, span], preferred_element_type=f32)
        gate, up = gu_ref[0, peer, :, span], gu_ref[1, peer, :, span]
        sig = jax.nn.sigmoid(gate)
        zgu[0, peer, :, span] = (grad * up * sig * (1.0 + gate * (1.0 - sig))).astype(bf16)
        zgu[1, peer, :, span] = (grad * gate * sig).astype(bf16)

    def over_columns(body):
        def columns(index, _):
            body(pl.multiple_of(index * 256, 256), 256)
            return 0

        lax.fori_loop(0, ff // 256, columns, 0)
        if full_ff < ff:
            body(full_ff, ff - full_ff)

    def ahead(tile):
        over_columns(lambda low, size: ahead_columns(peers[tile], low, size))

    for item in (2, 3):
        for tile in tiles:
            settle(item, tile)
    ahead(0)
    spread_step(1, b_all, ctx_count - 1)
    pump(1)
    for distance in range(1, ctx_count):
        spread_end(1, b_all, distance)
    keep_out(b_all, b_out)
    ahead(1)
    pump(1)
    ahead(2)
    spread_step(0, e_all, 1)
    pump(1)
    ahead(3)
    keep_out(z_ref, zgu_out.at[0])

    while pending:
        pump(1)
    for tile in tiles:
        settle(4, tile)

    group = own * ctx_count
    down_copies = {}
    nodes_down = (dpd, dpy, dpx, dp)

    def down_block(count):
        node = nodes_down[count]
        key = dp_count - 1 - count
        slot = count % 2
        if count >= 2:
            down_copies[count - 2].wait()

        def down_columns(low, size):
            span = pl.ds(low, size)
            left = e_all[:, :, :, pl.ds(pl.multiple_of(node * group, group), group)].reshape(-1, group)
            val = lax.dot_general(
                left, z_ref[:, :, span].reshape(-1, size), (((0,), (0,)), ((), ())), preferred_element_type=f32
            )
            block_ref[slot, :, span] = val.astype(bf16)

        over_columns(down_columns)
        down_copies[count] = pltpu.make_async_copy(block_ref.at[slot], down_out.at[key], down_sem.at[slot])
        down_copies[count].start()
    give_copies = {}
    tokens_all = ctx_count * rows
    sums = width // 256

    def emit(item, index, val):
        val = val.reshape(ctx_count, seqs, local, 256)
        ours = jnp.where(core == 0, val[:, 0], val[:, 1])
        theirs = jnp.where(core == 0, val[:, 1], val[:, 0])
        span = pl.ds(pl.multiple_of(index * 256, 256), 256)
        pair[:, :, span] = ours
        give[item, index] = theirs.astype(bf16)

    def emit_send(item, index):
        give_copies[item, index] = start(
            remote(give.at[item, index], take.at[item, index], ts.at[item, index], tr.at[item, index], to_core)
        )

    def gather(item):
        for index in range(sums):
            give_copies[item, index].wait_recv()
            span = slice(index * 256, (index + 1) * 256)

            def add(tile, _):
                total = pair[tile, :, span] + take[item, index, tile].astype(f32)
                done[item, tile, :, span] = total.astype(bf16)
                return 0

            lax.fori_loop(0, ctx_count, add, 0)
            mine[item, :, span] = pair[ctx, :, span] + take[item, index, ctx].astype(f32)
        keep_out(done.at[item], sum_out.at[item])

    def wide_dot(left, right):
        return lax.dot_general(left, right, nt, preferred_element_type=f32)

    def out_sum(index, _):
        span = pl.ds(pl.multiple_of(index * 256, 256), 256)
        emit(1, index, wide_dot(z_ref[...].reshape(tokens_all, ff), wmlp[2, span, :]))
        return 0

    def back_sum(index, _):
        span = pl.ds(pl.multiple_of(index * 256, 256), 256)
        val = wide_dot(zgu[0].reshape(tokens_all, ff), wmlp[0, span, :])
        emit(0, index, val + wide_dot(zgu[1].reshape(tokens_all, ff), wmlp[1, span, :]))
        return 0

    lax.fori_loop(0, sums, out_sum, 0)
    for index in range(sums):
        emit_send(1, index)
    spread_step(0, e_all, 2)
    over_columns(lambda low, size: back_columns(0, low, size))
    gather(1)
    for tile in range(1, ctx_count):
        if tile == ctx_count - 1:
            spread_step(0, e_all, tile)
        spread_end(0, e_all, tile)
        over_columns(lambda low, size: back_columns(tile, low, size))
    keep_out(zgu, zgu_out.at[1:3])
    lax.fori_loop(0, sums, back_sum, 0)
    for index in range(sums):
        emit_send(0, index)
    for count in range(dp_count):
        down_block(count)
    gather(0)
    keep_out(mine, own_out)
    down_copies[2].wait()
    down_copies[3].wait()
    for copy in kept:
        copy.wait()
    for copy in sent:
        copy.wait_send()
    for here, copy in relay_sent:

        @pl.when(here)
        def _():
            copy.wait_send()


def forward_call(tok, cot, attn_own, mlp_own, small_own, cos, sin, seg, live, qkv_cols, q_cols, gain_cut):
    dp_count, ctx_count = lax.axis_size("dp"), lax.axis_size("ctx")
    own = attn_own.shape[0]
    rows, width = tok.shape
    seqs, local = cot.shape[:2]
    full_rows = own * dp_count * ctx_count
    heads = q_cols // 128
    lanes = 128 * ctx_count
    ff = -(-mlp_own[0].shape[1] // lanes) * 128
    bf16, f32 = jnp.bfloat16, jnp.float32
    vmem, hbm = pl.BlockSpec(memory_space=pltpu.VMEM), pl.BlockSpec(memory_space=pl.ANY)
    group = (ctx_count, seqs, local, width)
    kept = [
        ((rows, width), f32),
        ((rows, width), bf16),
        ((seqs, heads, local, 128), bf16),
        ((seqs, 2, local * ctx_count, 128), bf16),
        ((seqs, heads, local, 128), bf16),
        ((seqs, heads, local, 1), f32),
        ((8, width), f32),
    ]
    weights = ((full_rows, attn_own.shape[1]), bf16)
    outs = [weights, (group, bf16)] + kept
    outs += [((3, ctx_count, rows, ff), bf16), ((2, ctx_count, local, width), bf16), ((2, local, width), f32)]
    outs += [((dp_count, own * ctx_count, ff), bf16)]
    chunks = width // 256
    scratch = [weights, ((3, full_rows, ff), bf16), (group, bf16), (group, bf16)] + kept
    scratch += [
        ((dp_count * ctx_count, 8, small_own.shape[1]), f32),
        ((chunks, rows, 256), f32),
        ((chunks, rows, 256), f32),
        ((2, ctx_count, rows, ff), f32),
        ((ctx_count, rows, ff), bf16),
        ((2, ctx_count, rows, ff), bf16),
        ((2, own * ctx_count, ff), bf16),
        ((ctx_count, local, width), f32),
        ((2, chunks, ctx_count, local, 256), bf16),
        ((2, chunks, ctx_count, local, 256), bf16),
        ((2, ctx_count, local, width), bf16),
        ((2, local, width), f32),
    ]
    dma = pltpu.SemaphoreType.DMA
    return pl.pallas_call(
        functools.partial(forward_kernel, (dp_count, ctx_count, own, qkv_cols, q_cols, gain_cut)),
        out_shape=[jax.ShapeDtypeStruct(shape, kind) for shape, kind in outs],
        in_specs=[vmem] + [hbm] * 6 + [vmem] * 4,
        out_specs=[hbm] * len(outs),
        scratch_shapes=[pltpu.VMEM(*entry) for entry in scratch]
        + [dma((5, ctx_count)) for _ in range(8)]
        + [dma((ctx_count,)), dma((ctx_count,)), dma((chunks,)), dma((chunks,))]
        + [dma((2, 2, ctx_count)) for _ in range(4)]
        + [dma((2, chunks)), dma((2, chunks)), dma((8,)), dma((20,)), dma((2,))],
        compiler_params=pltpu.CompilerParams(
            collective_id=0, has_side_effects=True, vmem_limit_bytes=65 * 1024 * 1024 - 65536
        ),
        name="forward_kernel",
    )(tok, cot, attn_own, *mlp_own, small_own, cos, sin, seg, live)


def xor_rank(rank, step, count):
    value = jnp.int32(0)
    bit = 1
    while bit < count:
        digit = lax.rem(rank // bit, 2)
        value = value + bit * (digit + (1 - 2 * digit) * ((step // bit) % 2))
        bit *= 2
    return value


def backward_kernel(
    sizes,
    sum_in,
    own_in,
    zgu_in,
    b_in,
    down_in,
    cot_hbm,
    tok_hbm,
    h_hbm,
    a_hbm,
    q_hbm,
    kv_hbm,
    o_hbm,
    lse_hbm,
    wattn_hbm,
    live_ref,
    row_ref,
    cos_ref,
    sin_ref,
    seg_ref,
    act_ref,
    dx_ref,
    zin,
    gat_ref,
    rows_ref,
    gout,
    lin,
    sum_v,
    fin,
    left_ref,
    right_ref,
    block_ref,
    keep,
    r1,
    r2,
    keep_at,
    send_at,
    r1_at,
    r2_at,
    zin_at,
    hb_ref,
    do_ref,
    prob_ref,
    ds_ref,
    dkv_ref,
    dkv_bf,
    dkv_in,
    dqkv_ref,
    part,
    part_in,
    zss,
    zrs,
    fs,
    fr,
    ld,
    kd,
    gd,
    s1,
    v1,
    s2,
    v2,
    s3,
    v3,
    ks,
    kr,
    ps,
    pr,
    gs,
    gr,
    acc_ref,
    sm_in,
    sm_sum,
    cot_ref,
    tok_ref,
    h_ref,
    a_ref,
    q_ref,
    kv_ref,
    o_ref,
    lse_ref,
    wattn,
    in_sem,
):
    dp_count, ctx_count, own, qkv_cols, q_cols = sizes
    dp, ctx, core = lax.axis_index("dp"), lax.axis_index("ctx"), lax.axis_index("tp")
    bf16, f32 = jnp.bfloat16, jnp.float32
    seqs, local, width = cot_ref.shape
    loads = []
    for src, dst in (
        (cot_hbm, cot_ref),
        (tok_hbm, tok_ref),
        (h_hbm, h_ref),
        (a_hbm, a_ref),
        (q_hbm, q_ref),
        (kv_hbm, kv_ref),
        (o_hbm, o_ref),
        (lse_hbm, lse_ref),
        (wattn_hbm, wattn),
    ):
        loads.append(pltpu.make_async_copy(src, dst, in_sem.at[len(loads)]))
    group = own * ctx_count
    ff = zgu_in.shape[3]
    heads = q_cols // 128
    other = 1 - core
    peers = [xor_rank(ctx, step, ctx_count) for step in range(ctx_count)]
    nodes = [xor_rank(dp, step, dp_count) for step in range(dp_count)]
    to_x, to_y, to_core = {"dp": nodes[1]}, {"dp": nodes[2]}, {"tp": other}
    greet([to_x, to_y, to_core] + [{"ctx": peers[step]} for step in range(1, ctx_count)])
    sent = []

    def start(copy):
        copy.start()
        sent.append(copy)
        return copy

    def rows_of(count, size, body):
        def one(index, _):
            body(pl.ds(pl.multiple_of(index * size, size), size))
            return 0

        lax.fori_loop(0, count // size, one, 0)

    last = ctx_count - 1
    ends = (ctx == 0, ctx == last)
    fin_copy, relay_sent = {}, []
    sums_of = (fin, act_ref)

    def line_step(index, turn):
        for way, step in ((0, 1), (1, -1)):
            owner = ctx + step * (ctx_count - turn)
            active = (owner >= 0) & (owner <= last)
            safe = jnp.clip(owner, 0, last)
            target = {"ctx": ctx + step}

            def message(src):
                return remote(
                    src,
                    lin.at[index, way, turn - 1],
                    zss.at[index, way, turn - 1],
                    zrs.at[index, way, turn - 1],
                    target,
                )

            fresh = message(sum_v.at[index, safe])

            @pl.when(active & ends[way])
            def _():
                fresh.start()

            relay_sent.append((active, fresh))
            if turn > 1:
                held = lin.at[index, way, turn - 2]
                got = remote(
                    held, held, zss.at[index, way, turn - 2], zrs.at[index, way, turn - 2], target
                )

                @pl.when(active & jnp.logical_not(ends[way]))
                def _():
                    got.wait_recv()

                    def add(piece):
                        lin[index, way, turn - 2, piece, :] = (
                            lin[index, way, turn - 2, piece, :].astype(f32) + sum_v[index, safe, piece, :].astype(f32)
                        ).astype(bf16)

                    rows_of(local, 32, add)
                    message(held).start()

    def collect_fin(index):
        into = sums_of[index]
        for way, step in ((0, 1), (1, -1)):
            held = lin.at[index, way, last - 1]
            got = remote(
                held, held, zss.at[index, way, last - 1], zrs.at[index, way, last - 1], {"ctx": ctx + step}
            )

            @pl.when(jnp.logical_not(ends[way]))
            def _():
                got.wait_recv()

                def add(piece):
                    into[core, piece, :] = into[core, piece, :] + lin[index, way, last - 1, piece, :].astype(f32)

                rows_of(local, 32, add)

        fin_copy[index] = remote(into.at[core], into.at[core], fs.at[index], fr.at[index], to_core)
        fin_copy[index].start()

    halves = {}
    for item in range(3):
        cut = (ff // 256 + 1) * 128
        halves[item] = ((0, cut), (cut, ff)) if item != 1 else ((cut, ff), (0, cut))
    middle = qkv_cols + (wattn.shape[1] - qkv_cols) // 2
    halves[3] = ((qkv_cols, middle), (middle, wattn.shape[1]))
    quarter = qkv_cols // 4
    halves[4] = ((0, quarter), (quarter, 2 * quarter))
    halves[5] = ((2 * quarter, 3 * quarter), (3 * quarter, qkv_cols))
    first_to, second_to = (to_y, to_x), (to_x, to_y)
    first_keys = ((2, 3), (1, 3))
    one_copy, two_copy, three_copy, keep_copy = {}, {}, {}, {}

    def cols(item, half):
        low, high = halves[item][half]
        return slice(low, high)

    def refs(item):
        if item < 3:
            return keep.at[item], r1.at[item], r2.at[item]
        return keep_at, r1_at, r2_at

    def block_of(item, key):
        return down_in.at[key] if item == 0 else gout.at[item - 1, key]

    def stage_one(item, half):
        span = cols(item, half)
        for slot, key in enumerate(first_keys[half]):
            src = block_of(item, key).at[:, span] if item < 3 else send_at.at[slot, :, span]
            one_copy[item, half, slot] = start(
                remote(
                    src,
                    refs(item)[1].at[slot, :, span],
                    s1.at[item, half, slot],
                    v1.at[item, half, slot],
                    first_to[half],
                )
            )

    def stage_two(item, half):
        span = cols(item, half)
        mine, first, second = refs(item)
        if item < 3:
            keep_copy[item, half].wait()
        one_copy[item, half, 1].wait_recv()

        def add(piece):
            mine[1, piece, span] = (mine[1, piece, span].astype(f32) + first[1, piece, span].astype(f32)).astype(bf16)

        rows_of(group, 96, add)
        two_copy[item, half] = start(
            remote(mine.at[1, :, span], second.at[:, span], s2.at[item, half], v2.at[item, half], second_to[half])
        )

    def stage_three(item, half):
        span = cols(item, half)
        mine, first, second = refs(item)
        if item < 3:
            keep_copy[item, 2].wait() if half == 0 else None
        one_copy[item, half, 0].wait_recv()
        two_copy[item, half].wait_recv()

        def total(piece):
            return mine[0, piece, span].astype(f32) + first[0, piece, span].astype(f32) + second[piece, span].astype(f32)

        if item >= 3:
            gat_ref[:, span] = total(pl.ds(pl.multiple_of(ctx * own, own), own))

        def add(piece):
            mine[0, piece, span] = total(piece).astype(bf16)

        rows_of(group, 96, add)
        if item < 3:
            there = zin.at[item, :, pl.ds(pl.multiple_of(ctx * ff + span.start, 128), span.stop - span.start)]
        else:
            there = zin_at.at[ctx, :, span]
        for tile in range(1, ctx_count):
            piece = pl.ds(pl.multiple_of(peers[tile] * own, own), own)
            three_copy[item, half, tile] = start(
                remote(
                    mine.at[0, piece, span],
                    there,
                    s3.at[item, half, tile],
                    v3.at[item, half, tile],
                    {"ctx": peers[tile]},
                )
            )
        if item < 3:
            piece = pl.ds(pl.multiple_of(ctx * own, own), own)
            copy = pltpu.make_async_copy(mine.at[0, piece, span], there, kd.at[item, 3 + half])
            copy.start()
            three_copy[item, half, 0] = copy

    def stage_four(item, half):
        span = cols(item, half)
        for tile in range(1, ctx_count):
            three_copy[item, half, tile].wait_recv()
        if item < 3:
            three_copy[item, half, 0].wait()
        else:
            total = gat_ref[:, span]
            for tile in range(1, ctx_count):
                total = total + zin_at[peers[tile], :, span].astype(f32)
            gat_ref[:, span] = total

    def keep_load(item):
        for half in range(2):
            span = cols(item, half)
            copy = pltpu.make_async_copy(
                block_of(item, 1 + half).at[:, span], keep.at[item, 1, :, span], kd.at[item, half]
            )
            copy.start()
            keep_copy[item, half] = copy
        copy = pltpu.make_async_copy(block_of(item, 0), keep.at[item, 0], kd.at[item, 2])
        copy.start()
        keep_copy[item, 2] = copy

    stage_one(0, 0)
    stage_one(0, 1)
    sum_copy = pltpu.make_async_copy(sum_in, sum_v, ld.at[1])
    sum_copy.start()

    def load_left(count):
        span = pl.ds(pl.multiple_of(nodes[dp_count - 1 - count % dp_count] * group, group), group)
        copy = pltpu.make_async_copy(b_in.at[:, :, :, span], left_ref.at[count % 2], gd.at[count % 2])
        copy.start()
        return copy

    def load_right(item):
        copy = pltpu.make_async_copy(zgu_in.at[item], right_ref, gd.at[2])
        copy.start()
        return copy

    right_copy = load_right(1)
    left_copy = load_left(0)
    mine_copies = [
        pltpu.make_async_copy(own_in.at[0], fin.at[core], ld.at[0]),
        pltpu.make_async_copy(own_in.at[1], act_ref.at[core], ld.at[2]),
    ]
    for copy in mine_copies:
        copy.start()
    keep_load(0)
    for copy in loads:
        copy.start()
    sum_copy.wait()
    line_step(0, 1)

    out_copy = {}

    def block(count, left_copy):
        slot = count % 2
        left_copy.wait()

        def columns(low, size):
            span = pl.ds(low, size)
            val = lax.dot_general(
                left_ref[slot].reshape(-1, group),
                right_ref[:, :, span].reshape(-1, size),
                (((0,), (0,)), ((), ())),
                preferred_element_type=f32,
            )
            block_ref[slot, :, span] = val.astype(bf16)

        def one(index, _):
            columns(pl.multiple_of(index * 256, 256), 256)
            return 0

        lax.fori_loop(0, ff // 256, one, 0)
        if ff % 256:
            columns(ff // 256 * 256, ff % 256)
        item, key = count // dp_count, dp_count - 1 - count % dp_count
        out_copy[count] = pltpu.make_async_copy(block_ref.at[slot], gout.at[item, key], gd.at[3 + slot])
        out_copy[count].start()

    def hand_over(count):
        out_copy[count].wait()
        item, key = 1 + count // dp_count, dp_count - 1 - count % dp_count
        if key == 2 and item == 1:
            stage_one(item, 0)
        if key == 1 and item == 1:
            stage_one(item, 1)
        if key == 0:
            keep_load(item)

    blocks = 2 * dp_count
    for count in range(blocks):
        following = load_left(count + 1) if count + 1 < blocks else None
        if count % dp_count == 0:
            right_copy.wait()
        block(count, left_copy)
        left_copy = following
        if count == dp_count - 1:
            right_copy = load_right(2)
        if count:
            hand_over(count - 1)
        if count == blocks // 2 - 1:
            line_step(0, 2)
    hand_over(blocks - 1)
    for copy in mine_copies:
        copy.wait()
    line_step(0, 3)
    line_step(1, 1)
    for half in range(2):
        stage_two(0, half)
    for half in range(2):
        stage_one(2, half)
    for copy in loads:
        copy.wait()

    pending = [(stage_two, 1, 0), (stage_two, 1, 1)]
    pending += [(stage_three, item, half) for item in (1, 2) for half in range(2)]

    def pump(count):
        for _ in range(min(count, len(pending))):
            action, item, half = pending.pop(0)
            action(item, half)

    collect_fin(0)
    fin_copy[0].wait()

    size = 32
    per_seq = local // size

    def split(index):
        return index // per_seq, pl.ds(pl.multiple_of(lax.rem(index, per_seq) * size, size), size)

    acc_ref[...] = jnp.zeros_like(acc_ref)

    def norm_mid(index, total):
        seq, piece = split(index)
        whole = pl.ds(pl.multiple_of(index * size, size), size)
        grad, val = fin[seq, piece, :], h_ref[whole, :]
        inv = lax.rsqrt(jnp.mean(val * val, axis=-1, keepdims=True) + norm_eps)
        weighted = grad * row_ref[1:2, :]
        inner = jnp.mean(weighted * val, axis=-1, keepdims=True)
        out = cot_ref[seq, piece, :].astype(f32) * live_ref[seq][:, 0:1] + (inv * weighted - val * (inv * inv * inv) * inner)
        dx_ref[seq, piece, :] = out
        hb_ref[whole, :] = out.astype(bf16)
        return total + jnp.sum(grad * val * inv, axis=0, keepdims=True)

    acc_ref[1:2, :] = lax.fori_loop(0, seqs * per_seq, norm_mid, jnp.zeros((1, width), f32))
    line_step(1, 2)

    for low in range(0, q_cols, 256):
        val = jnp.dot(hb_ref[...], wattn[:, qkv_cols + low : qkv_cols + low + 256], preferred_element_type=f32).astype(bf16)
        for head_low in (0, 128):
            for seq in range(seqs):
                do_ref[seq, (low + head_low) // 128] = val[seq * local : (seq + 1) * local, head_low : head_low + 128]

    pump(2)

    keys = kv_ref.shape[2]
    key_no = lax.broadcasted_iota(jnp.int32, (local, keys), 1)
    query_no = lax.broadcasted_iota(jnp.int32, (local, keys), 0) + ctx * local
    scale = HEAD_DIM ** (-0.5)
    kv_copies = []
    for seq in range(seqs):
        seen = same_document(seg_ref, seq, ctx, local) & (key_no <= query_no)
        hide = jnp.where(seen, 0.0, masked_score)

        def one_head(head, _):
            query, grad_out, keys_bf, values_bf = q_ref[seq, head], do_ref[seq, head], kv_ref[seq, 0], kv_ref[seq, 1]
            score = lax.dot_general(query, keys_bf, (((1,), (1,)), ((), ())), preferred_element_type=f32) * scale
            prob = jnp.exp(jnp.where(hide < 0.0, masked_score, score) - lse_ref[seq, head])
            grad_prob = lax.dot_general(grad_out, values_bf, (((1,), (1,)), ((), ())), preferred_element_type=f32)
            row_dot = jnp.sum(grad_out.astype(f32) * o_ref[seq, head].astype(f32), axis=-1, keepdims=True)
            grad_score = (prob * (grad_prob - row_dot) * scale).astype(bf16)
            prob_ref[head] = prob.astype(bf16)
            ds_ref[head] = grad_score
            grad_query = jnp.dot(grad_score, keys_bf, preferred_element_type=f32)
            turned = grad_query * cos_ref[seq * local : (seq + 1) * local, :] + pltpu.roll(
                grad_query * sin_ref[seq * local : (seq + 1) * local, :], 64, 1
            )
            span = pl.ds(pl.multiple_of(head * 128, 128), 128)
            dqkv_ref[seq * local : (seq + 1) * local, span] = turned.astype(bf16)
            acc_ref[2:3, span] = acc_ref[2:3, span] + jnp.sum(turned, axis=0, keepdims=True)
            return 0

        lax.fori_loop(0, heads, one_head, 0)
        stacked = (heads * local, 128)
        dkv_ref[seq, 0] = lax.dot_general(
            ds_ref[...].reshape(heads * local, keys),
            q_ref[seq].reshape(stacked),
            (((0,), (0,)), ((), ())),
            preferred_element_type=f32,
        )
        dkv_ref[seq, 1] = lax.dot_general(
            prob_ref[...].reshape(heads * local, keys),
            do_ref[seq].reshape(stacked),
            (((0,), (0,)), ((), ())),
            preferred_element_type=f32,
        )
        dkv_bf[seq] = dkv_ref[seq].astype(bf16)
    for tile in range(1, ctx_count):
        piece = pl.ds(pl.multiple_of(peers[tile] * local, local), local)
        kv_copies.append(
            start(remote(dkv_bf.at[:, :, piece, :], dkv_in.at[ctx], ks.at[tile], kr.at[tile], {"ctx": peers[tile]}))
        )

    def weight_blocks(items, left_ref, right, low, high):
        for key in (3, 2, 1, 0):
            left = left_ref[:, pl.ds(pl.multiple_of(nodes[key] * group, group), group)]
            val = lax.dot_general(left, right, (((0,), (0,)), ((), ())), preferred_element_type=f32).astype(bf16)
            for item in items:
                for half in range(2):
                    span = cols(item, half)
                    piece = val[:, span.start - low : span.stop - low]
                    if key in first_keys[half]:
                        send_at[first_keys[half].index(key), :, span] = piece
                    else:
                        keep_at[0 if key == 0 else 1, :, span] = piece

    o_rows = jnp.concatenate(
        [jnp.concatenate([o_ref[seq, head] for head in range(heads)], 1) for seq in range(seqs)], 0
    )
    line_step(1, 3)
    weight_blocks((3,), hb_ref, o_rows, qkv_cols, wattn.shape[1])
    for half in range(2):
        stage_three(0, half)
    for copy in kv_copies:
        copy.wait_recv()
    own_keys = pl.ds(pl.multiple_of(ctx * local, local), local)
    for seq in range(seqs):
        for part_no in range(2):
            val = dkv_ref[seq, part_no, own_keys, :]
            for tile in range(1, ctx_count):
                val = val + dkv_in[peers[tile], seq, part_no].astype(f32)
            here = slice(seq * local, (seq + 1) * local)
            if part_no == 0:
                val = val * cos_ref[here, :] + pltpu.roll(val * sin_ref[here, :], 64, 1)
            span = slice(q_cols + part_no * 128, q_cols + (part_no + 1) * 128)
            dqkv_ref[here, span] = val.astype(bf16)
            acc_ref[2:3, span] = acc_ref[2:3, span] + jnp.sum(val, axis=0, keepdims=True)
    for half in range(2):
        stage_two(2, half)
    for half in range(2):
        stage_one(3, half)
    weight_blocks((4, 5), a_ref, dqkv_ref[...], 0, qkv_cols)
    for item in (4, 5):
        for half in range(2):
            stage_one(item, half)

    part_copies = []
    for index in range(width // 256):
        part[index] = lax.dot_general(
            dqkv_ref[...],
            wattn[index * 256 : (index + 1) * 256, :qkv_cols],
            (((1,), (1,)), ((), ())),
            preferred_element_type=f32,
        )
        part_copies.append(
            start(remote(part.at[index], part_in.at[index], ps.at[index], pr.at[index], to_core))
        )
    for index, copy in enumerate(part_copies):
        copy.wait_recv()
        for seq in range(seqs):
            here = slice(seq * local, (seq + 1) * local)
            fin[seq, :, index * 256 : (index + 1) * 256] = part[index, here, :] + part_in[index, here, :]

    def norm_in(index, total):
        seq, piece = split(index)
        whole = pl.ds(pl.multiple_of(index * size, size), size)
        grad, val = fin[seq, piece, :], tok_ref[whole, :].astype(f32)
        inv = lax.rsqrt(jnp.mean(val * val, axis=-1, keepdims=True) + norm_eps)
        weighted = grad * row_ref[0:1, :]
        inner = jnp.mean(weighted * val, axis=-1, keepdims=True)
        dx_ref[seq, piece, :] = dx_ref[seq, piece, :] + (inv * weighted - val * (inv * inv * inv) * inner)
        return total + jnp.sum(grad * val * inv, axis=0, keepdims=True)

    acc_ref[0:1, :] = lax.fori_loop(0, seqs * per_seq, norm_in, jnp.zeros((1, width), f32))

    small_copies = [
        start(remote(acc_ref, sm_in.at[tile], gs.at[tile], gr.at[tile], {"ctx": peers[tile]}))
        for tile in range(1, ctx_count)
    ]
    collect_fin(1)
    fin_copy[1].wait()

    def act_rows(index, _):
        seq, piece = split(index)
        whole = pl.ds(pl.multiple_of(index * size, size), size)
        act_ref[seq, piece, :] = (h_ref[whole, :] + act_ref[seq, piece, :]) * live_ref[seq][:, 0:1]
        return 0

    lax.fori_loop(0, seqs * per_seq, act_rows, 0)
    pump(2)
    for half in range(2):
        stage_two(3, half)
    while pending:
        pump(1)
    for half in range(2):
        stage_two(4, half)
    for half in range(2):
        stage_three(3, half)
    for half in range(2):
        stage_two(5, half)
    total = acc_ref[...]
    for tile, copy in enumerate(small_copies):
        copy.wait_recv()
        total = total + sm_in[tile + 1]
    sm_sum[0] = total
    small_turns = [
        remote(sm_sum.at[turn], sm_in.at[ctx_count + turn], gs.at[ctx_count + turn], gr.at[ctx_count + turn], target)
        for turn, target in ((0, to_x), (1, to_y))
    ]
    start(small_turns[0])
    for half in range(2):
        stage_three(4, half)
    small_turns[0].wait_recv()
    sm_sum[1] = sm_sum[0] + sm_in[ctx_count]
    start(small_turns[1])
    for half in range(2):
        stage_three(5, half)
    small_turns[1].wait_recv()
    rows_ref[...] = sm_sum[1] + sm_in[ctx_count + 1]
    for item in range(6):
        for half in range(2):
            stage_four(item, half)
    for copy in sent:
        copy.wait_send()
    for here, copy in relay_sent:

        @pl.when(here)
        def _():
            copy.wait_send()


def backward_call(inputs, sizes):
    dp_count, ctx_count, own, qkv_cols, q_cols = sizes
    bf16, f32 = jnp.bfloat16, jnp.float32
    vmem, hbm = pl.BlockSpec(memory_space=pltpu.VMEM), pl.BlockSpec(memory_space=pl.ANY)
    held = inputs[5:14]
    seqs, local, width = held[0].shape
    ff = inputs[2].shape[3]
    group = own * ctx_count
    rows, keys = seqs * local, local * ctx_count
    heads = q_cols // 128
    attn_cols = held[8].shape[1]
    chunks = width // 256
    outs = [
        ((seqs, local, width), f32, vmem),
        ((seqs, local, width), f32, vmem),
        ((3, own, ctx_count * ff), bf16, hbm),
        ((own, attn_cols), f32, vmem),
        ((8, width), f32, vmem),
        ((2, dp_count, group, ff), bf16, hbm),
    ]
    scratch = [
        ((2, 2, ctx_count - 1, local, width), bf16),
        ((2, ctx_count, local, width), bf16),
        ((seqs, local, width), f32),
        ((2, ctx_count, seqs, local, group), bf16),
        ((ctx_count, rows, ff), bf16),
        ((2, group, ff), bf16),
        ((3, 2, group, ff), bf16),
        ((3, 2, group, ff), bf16),
        ((3, group, ff), bf16),
        ((2, group, attn_cols), bf16),
        ((2, group, attn_cols), bf16),
        ((2, group, attn_cols), bf16),
        ((group, attn_cols), bf16),
        ((ctx_count, own, attn_cols), bf16),
        ((rows, width), bf16),
        ((seqs, heads, local, 128), bf16),
        ((heads, local, keys), bf16),
        ((heads, local, keys), bf16),
        ((seqs, 2, keys, 128), f32),
        ((seqs, 2, keys, 128), bf16),
        ((ctx_count, seqs, 2, local, 128), bf16),
        ((rows, qkv_cols), bf16),
        ((chunks, rows, 256), f32),
        ((chunks, rows, 256), f32),
    ]
    dma = pltpu.SemaphoreType.DMA
    sems = [dma((2, 2, ctx_count)), dma((2, 2, ctx_count)), dma((2,)), dma((2,)), dma((3,)), dma((3, 5)), dma((5,))]
    sems += [
        dma(shape)
        for shape in ((6, 2, 2), (6, 2), (6, 2, ctx_count), (ctx_count,), (chunks,), (ctx_count + 2,))
        for _ in range(2)
    ]
    final = [((8, width), f32), ((ctx_count + 2, 8, width), f32), ((2, 8, width), f32)]
    final += [(array.shape, array.dtype) for array in held]
    return pl.pallas_call(
        functools.partial(backward_kernel, sizes),
        out_shape=[jax.ShapeDtypeStruct(shape, kind) for shape, kind, _ in outs],
        in_specs=[hbm] * 14 + [vmem] * (len(inputs) - 14),
        out_specs=[spec for _, _, spec in outs],
        scratch_shapes=[pltpu.VMEM(*entry) for entry in scratch]
        + sems
        + [pltpu.VMEM(*entry) for entry in final]
        + [dma((len(held),))],
        compiler_params=pltpu.CompilerParams(
            collective_id=1, has_side_effects=True, vmem_limit_bytes=65 * 1024 * 1024 - 65536
        ),
        name="backward_kernel",
    )(*inputs)


def on_device_kernels(
    tokens,
    cotangent,
    segments,
    positions,
    counts,
    attn_gain,
    q_weight,
    q_bias,
    k_weight,
    v_weight,
    kv_bias,
    o_weight,
    mlp_gain,
    gate_weight,
    up_weight,
    down_weight,
):
    dp_count, ctx_count = lax.axis_size("dp"), lax.axis_size("ctx")
    dp_rank, ctx_rank, core = lax.axis_index("dp"), lax.axis_index("ctx"), lax.axis_index("tp")
    seq_count, local_len, width = tokens.shape
    full_len = segments.shape[1]
    row_count = seq_count * local_len
    own_rows = q_weight.shape[1]
    group_rows = own_rows * ctx_count
    q_cols, k_cols, ff_cols = q_weight.shape[2], k_weight.shape[2], gate_weight.shape[2]
    kv_local = k_cols // HEAD_DIM
    group_size = q_cols // k_cols
    qkv_cols = q_cols + 2 * k_cols
    lane = 128
    ff_block = -(-ff_cols // (lane * ctx_count)) * lane
    ff_pad = ff_block * ctx_count - ff_cols
    f32, bf16 = jnp.float32, jnp.bfloat16

    parts = (attn_gain[0], mlp_gain[0], q_bias[0].reshape(-1), kv_bias[0].reshape(-1))
    cuts = [0]
    for part_vec in parts:
        cuts.append(cuts[-1] + part_vec.shape[0])
    small_own = jnp.pad(jnp.concatenate(parts).astype(f32)[None], ((0, 7), (0, 0)))
    attn_own = jnp.concatenate([q_weight[0], k_weight[0], v_weight[0], o_weight[0]], 1)
    live_seq = (jnp.arange(seq_count, dtype=jnp.int32) < counts[0]).astype(f32)
    live = jnp.broadcast_to(live_seq[:, None, None], (seq_count, 1, 128))
    cos_tab, sin_tab = rope_tables(positions.reshape(-1))
    sign = jnp.where(jnp.arange(HEAD_DIM) < HEAD_DIM // 2, -1.0, 1.0)
    (
        w_attn,
        mid_all,
        resid_mid,
        normed_in,
        query_hm,
        keyval_hm,
        attn_hm,
        log_total,
        small_rows,
        hidden_and_grads,
        part_sums,
        part_own,
        grad_down,
    ) = forward_call(
        tokens.reshape(-1, width),
        cotangent,
        attn_own,
        (gate_weight[0], up_weight[0], down_weight[0]),
        small_own,
        cos_tab,
        sin_tab * sign,
        segments,
        live,
        qkv_cols,
        q_cols,
        cuts,
    )
    activations, input_grad, grad_ff, grad_w_attn, rows_sum, _ = backward_call(
        (
            part_sums,
            part_own,
            hidden_and_grads,
            mid_all,
            grad_down,
            cotangent,
            tokens.reshape(-1, width),
            resid_mid,
            normed_in,
            query_hm,
            keyval_hm,
            attn_hm,
            log_total,
            w_attn,
            live,
            small_rows,
            cos_tab,
            sin_tab * sign,
            segments,
        ),
        (dp_count, ctx_count, own_rows, qkv_cols, q_cols),
    )
    grad_w_down, grad_w_gate, grad_w_up = (grad_ff[item, :, :ff_cols].astype(f32) for item in range(3))
    rank = dp_rank * ctx_count + ctx_rank

    def own_part(vector, size):
        return lax.dynamic_slice_in_dim(vector, rank * size, size, 0)

    bias_kv = jnp.concatenate(
        [
            rows_sum[2, q_cols : q_cols + k_cols].reshape(kv_local, -1).T,
            rows_sum[2, q_cols + k_cols : qkv_cols].reshape(kv_local, -1).T,
        ],
        0,
    ).reshape(-1)
    own = [
        own_part(rows_sum[0], own_rows)[None],
        own_part(rows_sum[1], own_rows)[None],
        own_part(rows_sum[2, :q_cols].reshape(kv_local, -1).T.reshape(-1), cuts[3] - cuts[2]),
        own_part(bias_kv, cuts[4] - cuts[3]),
    ]
    grad_w_qkv, grad_w_out = grad_w_attn[:, :qkv_cols], grad_w_attn[:, qkv_cols:]
    return (
        activations.reshape(tokens.shape),
        input_grad.reshape(tokens.shape),
        own[0],
        grad_w_qkv[None, :, :q_cols],
        own[2].reshape(q_bias.shape),
        grad_w_qkv[None, :, q_cols : q_cols + k_cols],
        grad_w_qkv[None, :, q_cols + k_cols :],
        own[3].reshape(kv_bias.shape),
        grad_w_out[None],
        own[1],
        grad_w_gate[None],
        grad_w_up[None],
        grad_w_down[None],
    )


def solution(mesh):
    in_specs = (
        P("dp", "ctx", None),
        P("dp", "ctx", None),
        P("dp", None),
        P("dp", "ctx"),
        P("dp"),
        P(None, ("dp", "ctx")),
        P(None, ("dp", "ctx"), "tp"),
        P(None, ("dp", "ctx"), "tp"),
        P(None, ("dp", "ctx"), "tp"),
        P(None, ("dp", "ctx"), "tp"),
        P(None, ("dp", "ctx"), "tp"),
        P(None, ("dp", "ctx"), "tp"),
        P(None, ("dp", "ctx")),
        P(None, ("dp", "ctx"), "tp"),
        P(None, ("dp", "ctx"), "tp"),
        P(None, ("dp", "ctx"), "tp"),
    )
    out_specs = (
        P("dp", "ctx", None),
        P("dp", "ctx", None),
        P(None, ("dp", "ctx")),
        P(None, ("dp", "ctx"), "tp"),
        P(None, ("dp", "ctx"), "tp"),
        P(None, ("dp", "ctx"), "tp"),
        P(None, ("dp", "ctx"), "tp"),
        P(None, ("dp", "ctx"), "tp"),
        P(None, ("dp", "ctx"), "tp"),
        P(None, ("dp", "ctx")),
        P(None, ("dp", "ctx"), "tp"),
        P(None, ("dp", "ctx"), "tp"),
        P(None, ("dp", "ctx"), "tp"),
    )
    kernels_fit = mesh.shape["dp"] == 4 and mesh.shape["ctx"] == 4 and mesh.shape["tp"] == KV_HEADS
    return jax.shard_map(
        on_device_kernels if kernels_fit else on_device, mesh=mesh, in_specs=in_specs, out_specs=out_specs, check_vma=False
    )
```

```python
import functools

import jax
import jax.numpy as jnp
from jax import lax
from jax.experimental import pallas as pl
from jax.experimental.pallas import tpu as pltpu
from jax.sharding import PartitionSpec as P

HEADS = 12
KV_HEADS = 2
HEAD_DIM = 128
LAYERS = 1


theta_base = 1000000.0
norm_eps = 1e-06
masked_score = -1e30


def mat_mul(left, right):
    return jnp.dot(left, right, preferred_element_type=jnp.float32)


def mat_mul_t(left, right):
    return lax.dot_general(
        left, right, (((1,), (1,)), ((), ())), preferred_element_type=jnp.float32
    )


def rows_mul(left, right):
    return lax.dot_general(
        left, right, (((0,), (0,)), ((), ())), preferred_element_type=jnp.float32
    )


def rope_tables(pos_vals):
    half_dim = HEAD_DIM // 2
    frequency = theta_base ** (-(jnp.arange(half_dim, dtype=jnp.float32) * (2.0 / HEAD_DIM)))
    angles = pos_vals.astype(jnp.float32)[..., None] * frequency
    cos_half = jnp.cos(angles)
    sin_half = jnp.sin(angles)
    return (jnp.concatenate([cos_half, cos_half], -1), jnp.concatenate([sin_half, sin_half], -1))


def rotate(values, cos_tab, sin_tab):
    half_dim = values.shape[-1] // 2
    turned = jnp.concatenate([-values[..., half_dim:], values[..., :half_dim]], -1)
    return values * cos_tab + turned * sin_tab


def unrotate(grad_vals, cos_tab, sin_tab):
    half_dim = grad_vals.shape[-1] // 2
    scaled = grad_vals * sin_tab
    turned = jnp.concatenate([scaled[..., half_dim:], -scaled[..., :half_dim]], -1)
    return grad_vals * cos_tab + turned


def norm_forward(residual, gain_vec):
    inv_rms = lax.rsqrt(jnp.mean(residual * residual, axis=-1, keepdims=True) + norm_eps)
    normed = (residual * inv_rms * gain_vec.astype(jnp.float32)).astype(jnp.bfloat16)
    return (inv_rms, normed)


def norm_backward(residual, inv_rms, gain_vec, grad_normed):
    weighted = grad_normed * gain_vec.astype(jnp.float32)
    inner_mean = jnp.mean(weighted * residual, axis=-1, keepdims=True)
    grad_resid = inv_rms * weighted - residual * (inv_rms * inv_rms * inv_rms) * inner_mean
    grad_gain = jnp.sum(grad_normed * residual * inv_rms, axis=0)
    return (grad_resid, grad_gain)


def split_heads(keys_all, values_all):
    seq_count, full_len, kv_width = keys_all.shape
    kv_local = kv_width // HEAD_DIM
    return (
        keys_all.reshape(seq_count, full_len, kv_local, HEAD_DIM),
        values_all.reshape(seq_count, full_len, kv_local, HEAD_DIM),
    )


def attend_forward(query_bf, keys_all, values_all, allowed):
    key_heads, value_heads = split_heads(keys_all, values_all)
    scores = jnp.einsum(
        "bqkgd,bskd->bkgqs", query_bf, key_heads, preferred_element_type=jnp.float32
    ) * HEAD_DIM ** (-0.5)
    scores = jnp.where(allowed[:, None, None], scores, masked_score)
    top_score = jnp.max(scores, axis=-1, keepdims=True)
    shifted_exp = jnp.exp(scores - top_score)
    totals = jnp.sum(shifted_exp, axis=-1, keepdims=True)
    prob_bf = (shifted_exp / totals).astype(jnp.bfloat16)
    output = jnp.einsum(
        "bkgqs,bskd->bqkgd", prob_bf, value_heads, preferred_element_type=jnp.float32
    )
    return (output.astype(jnp.bfloat16), top_score + jnp.log(totals))


def attend_backward(query_bf, keys_all, values_all, attn_bf, log_total, grad_attn, allowed):
    key_heads, value_heads = split_heads(keys_all, values_all)
    scores = jnp.einsum(
        "bqkgd,bskd->bkgqs", query_bf, key_heads, preferred_element_type=jnp.float32
    ) * HEAD_DIM ** (-0.5)
    prob_full = jnp.exp(jnp.where(allowed[:, None, None], scores, masked_score) - log_total)
    prob_bf = prob_full.astype(jnp.bfloat16)
    grad_value = jnp.einsum(
        "bkgqs,bqkgd->bskd", prob_bf, grad_attn, preferred_element_type=jnp.float32
    )
    grad_prob = jnp.einsum(
        "bqkgd,bskd->bkgqs", grad_attn, value_heads, preferred_element_type=jnp.float32
    )
    row_dot = jnp.sum(grad_attn.astype(jnp.float32) * attn_bf.astype(jnp.float32), axis=-1)
    row_dot = jnp.transpose(row_dot, (0, 2, 3, 1))[..., None]
    grad_score = (prob_full * (grad_prob - row_dot) * HEAD_DIM ** (-0.5)).astype(jnp.bfloat16)
    grad_query = jnp.einsum(
        "bkgqs,bskd->bqkgd", grad_score, key_heads, preferred_element_type=jnp.float32
    )
    grad_key = jnp.einsum(
        "bkgqs,bqkgd->bskd", grad_score, query_bf, preferred_element_type=jnp.float32
    )
    return (grad_query, grad_key.reshape(keys_all.shape), grad_value.reshape(values_all.shape))


def xor_permute(value, axis_name, step):
    count = lax.axis_size(axis_name)
    return lax.ppermute(value, axis_name, [(rank, rank ^ step) for rank in range(count)])


def axis_bits(axis_name):
    return [1 << shift for shift in range(lax.axis_size(axis_name).bit_length() - 1)]


def partner(value):
    return xor_permute(value, "tp", 1)


def place(pieces, rank, dim):
    width = pieces[0].shape[dim]
    whole_shape = list(pieces[0].shape)
    whole_shape[dim] = width * len(pieces)
    whole = jnp.zeros(whole_shape, pieces[0].dtype)
    for offset, piece in enumerate(pieces):
        whole = lax.dynamic_update_slice_in_dim(whole, piece, (rank ^ offset) * width, dim)
    return whole


def join_halves(mine, other, core, dim):
    return jnp.where(
        core == 0, jnp.concatenate([mine, other], dim), jnp.concatenate([other, mine], dim)
    )


def gather_direct(value, axis_name):
    count = lax.axis_size(axis_name)
    return [value] + [xor_permute(value, axis_name, step) for step in range(1, count)]


def gather_halves(value, axis_name):
    rows = value.shape[0]
    half = rows // 2
    bits = axis_bits(axis_name)
    parts = []
    for piece, order in ((value[:half], bits), (value[half:], bits[::-1])):
        held = {0: piece}
        for bit in order:
            for key in list(held):
                held[key | bit] = xor_permute(held[key], axis_name, bit)
        parts.append(held)
    return [(parts[0][key], parts[1][key]) for key in range(len(parts[0]))]


def scatter_halves(blocks, axis_name):
    half = blocks[0].shape[0] // 2
    bits = axis_bits(axis_name)
    done = []
    for low, high, order in ((0, half, bits[::-1]), (half, 2 * half, bits)):
        held = {key: block[low:high] for key, block in enumerate(blocks)}
        for bit in order:
            for key in [key for key in held if key & bit]:
                sent = held.pop(key).astype(jnp.bfloat16)
                held[key ^ bit] = held[key ^ bit] + xor_permute(sent, axis_name, bit).astype(jnp.float32)
        done.append(held[0])
    return jnp.concatenate(done, 0)


def scatter_small(blocks, axis_name):
    held = dict(enumerate(blocks))
    for bit in axis_bits(axis_name)[::-1]:
        for key in [key for key in held if key & bit]:
            held[key ^ bit] = held[key ^ bit] + xor_permute(held.pop(key), axis_name, bit)
    return held[0]


def scatter_direct(block_of, axis_name):
    total = block_of(0)
    for step in range(1, lax.axis_size(axis_name)):
        got = xor_permute(block_of(step).astype(jnp.bfloat16), axis_name, step)
        total = total + got.astype(jnp.float32)
    return total


def rows_at(value, index, size):
    return lax.dynamic_slice_in_dim(value, index * size, size, 0)


def columns_at(value, index, size):
    return lax.dynamic_slice_in_dim(value, index * size, size, 1)


def on_device(
    tokens,
    cotangent,
    segments,
    positions,
    counts,
    attn_gain,
    q_weight,
    q_bias,
    k_weight,
    v_weight,
    kv_bias,
    o_weight,
    mlp_gain,
    gate_weight,
    up_weight,
    down_weight,
):
    dp_count, ctx_count = lax.axis_size("dp"), lax.axis_size("ctx")
    dp_rank, ctx_rank, core = lax.axis_index("dp"), lax.axis_index("ctx"), lax.axis_index("tp")
    seq_count, local_len, width = tokens.shape
    full_len = segments.shape[1]
    row_count = seq_count * local_len
    half_width = width // 2
    own_rows = q_weight.shape[1]
    group_rows = own_rows * ctx_count
    q_cols, k_cols, ff_cols = q_weight.shape[2], k_weight.shape[2], gate_weight.shape[2]
    kv_local = k_cols // HEAD_DIM
    group_size = q_cols // k_cols
    qkv_cols = q_cols + 2 * k_cols
    lane = 128
    ff_block = -(-ff_cols // (lane * ctx_count)) * lane
    ff_pad = ff_block * ctx_count - ff_cols
    f32, bf16 = jnp.float32, jnp.bfloat16

    small = jnp.concatenate(
        [attn_gain[0], mlp_gain[0], q_bias[0].reshape(-1), kv_bias[0].reshape(-1)]
    )[None]
    sizes = (attn_gain.shape[1], mlp_gain.shape[1], q_bias.shape[1] * q_bias.shape[2], kv_bias.shape[1] * kv_bias.shape[2])
    small_ctx = place(gather_direct(small, "ctx"), ctx_rank, 0)[None]
    held = {0: small_ctx}
    for bit in axis_bits("dp"):
        for key in list(held):
            held[key | bit] = xor_permute(held[key], "dp", bit)
    small_all = place([held[key] for key in range(dp_count)], dp_rank, 0)
    small_all = small_all.reshape(dp_count * ctx_count, -1)
    cuts = [0]
    for size in sizes:
        cuts.append(cuts[-1] + size)
    gain_in, gain_mid, b_query, b_keyval = (
        small_all[:, low:high].reshape(-1) for low, high in zip(cuts[:-1], cuts[1:])
    )
    b_query = b_query.reshape(-1, kv_local).T.reshape(-1).astype(f32)
    b_keyval = b_keyval.reshape(-1, kv_local).astype(f32)
    b_qkv = jnp.concatenate(
        [b_query, b_keyval[:HEAD_DIM].T.reshape(-1), b_keyval[HEAD_DIM:].T.reshape(-1)]
    )

    attn_own = jnp.concatenate([q_weight[0], k_weight[0], v_weight[0], o_weight[0]], 1)
    attn_group = place(gather_direct(attn_own, "ctx"), ctx_rank, 0)
    attn_pairs = gather_halves(attn_group, "dp")
    w_attn = place([jnp.concatenate(pair, 0) for pair in attn_pairs], dp_rank, 0)
    w_qkv, w_out = w_attn[:, :qkv_cols], w_attn[:, qkv_cols:]

    live_seq = (jnp.arange(seq_count, dtype=jnp.int32) < counts[0]).astype(f32)
    live_rows = jnp.repeat(live_seq, local_len)[:, None]
    grad_out = cotangent.astype(f32).reshape(-1, width) * live_rows

    def spread(rows_bf):
        mine = jnp.concatenate(gather_direct(columns_at(rows_bf, core, half_width), "ctx"), 0)
        return join_halves(mine, partner(mine), core, 1)

    grad_all = spread(grad_out.astype(bf16))

    def spread_weight(weight):
        padded = jnp.pad(weight[0], ((0, 0), (0, ff_pad)))
        pieces = [columns_at(padded, ctx_rank, ff_block)]
        for step in range(1, ctx_count):
            pieces.append(xor_permute(columns_at(padded, ctx_rank ^ step, ff_block), "ctx", step))
        pairs = gather_halves(place(pieces, ctx_rank, 0), "dp")
        return place([jnp.concatenate(pair, 0) for pair in pairs], dp_rank, 0)

    w_gate = spread_weight(gate_weight)
    w_up = spread_weight(up_weight)
    w_down = spread_weight(down_weight)

    query_pos = ctx_rank * local_len + jnp.arange(local_len, dtype=jnp.int32)
    key_pos = jnp.arange(full_len, dtype=jnp.int32)
    query_seg = lax.dynamic_slice_in_dim(segments, ctx_rank * local_len, local_len, 1)
    allowed = (query_seg[:, :, None] == segments[:, None, :]) & (
        key_pos[None, None, :] <= query_pos[None, :, None]
    )
    cos_tab, sin_tab = rope_tables(positions.reshape(-1))
    cos_tab, sin_tab = cos_tab[:, None, :], sin_tab[:, None, :]
    residual = tokens.astype(f32).reshape(-1, width)
    inv_in, normed_in = norm_forward(residual, gain_in)
    qkv_val = mat_mul(normed_in, w_qkv) + b_qkv
    query_bf = rotate(
        qkv_val[:, :q_cols].reshape(row_count, -1, HEAD_DIM), cos_tab, sin_tab
    ).astype(bf16).reshape(seq_count, -1, kv_local, group_size, HEAD_DIM)
    key_bf = rotate(
        qkv_val[:, q_cols : q_cols + k_cols].reshape(row_count, -1, HEAD_DIM), cos_tab, sin_tab
    ).astype(bf16).reshape(row_count, -1)
    value_bf = qkv_val[:, q_cols + k_cols :].astype(bf16)
    keyval = jnp.concatenate([key_bf, value_bf], 1).reshape(seq_count, local_len, -1)
    keyval_all = place(gather_direct(keyval, "ctx"), ctx_rank, 1)
    keys_all, values_all = keyval_all[..., :k_cols], keyval_all[..., k_cols:]
    attn_bf, log_total = attend_forward(query_bf, keys_all, values_all, allowed)
    attn_flat = attn_bf.reshape(row_count, -1)
    out_part = mat_mul_t(attn_flat, w_out)
    resid_mid = residual + (out_part + partner(out_part))
    inv_mid, normed_mid = norm_forward(resid_mid, gain_mid)

    mid_all = spread(normed_mid)
    gate_pre = mat_mul(mid_all, w_gate)
    up_pre = mat_mul(mid_all, w_up)
    hidden_bf = (jax.nn.silu(gate_pre) * up_pre).astype(bf16)
    grad_hidden = mat_mul(grad_all, w_down)
    sigmoid_gate = jax.nn.sigmoid(gate_pre)
    grad_gate = (
        grad_hidden * up_pre * sigmoid_gate * (1.0 + gate_pre * (1.0 - sigmoid_gate))
    ).astype(bf16)
    grad_up = (grad_hidden * gate_pre * sigmoid_gate).astype(bf16)

    def collect(part):
        part_bf = columns_at(part, 1 - core, half_width).astype(bf16)
        mine = columns_at(part, core, half_width) + partner(part_bf).astype(f32)
        total = scatter_direct(lambda step: mine[step * row_count : (step + 1) * row_count], "ctx")
        return join_halves(total, partner(total), core, 1)

    grad_normed_mid = collect(mat_mul_t(grad_gate, w_gate) + mat_mul_t(grad_up, w_up))

    def owner_weight(left, right):
        blocks = [
            rows_mul(columns_at(left, dp_rank ^ step, group_rows), right)
            for step in range(dp_count)
        ]
        group = scatter_halves(blocks, "dp").astype(bf16)
        pieces = [rows_at(group, ctx_rank, own_rows)]
        for step in range(1, ctx_count):
            pieces.append(xor_permute(rows_at(group, ctx_rank ^ step, own_rows), "ctx", step))
        return place(pieces, ctx_rank, 1)[:, :ff_cols].astype(f32)

    grad_w_down = owner_weight(grad_all, hidden_bf)
    grad_w_gate = owner_weight(mid_all, grad_gate)
    grad_w_up = owner_weight(mid_all, grad_up)

    layer_out = resid_mid + collect(mat_mul_t(hidden_bf, w_down))
    activations = (layer_out * live_rows).reshape(tokens.shape)

    grad_mid_norm, grad_gain_mid = norm_backward(resid_mid, inv_mid, gain_mid, grad_normed_mid)
    grad_mid = grad_out + grad_mid_norm
    grad_mid_bf = grad_mid.astype(bf16)
    grad_attn = mat_mul(grad_mid_bf, w_out).astype(bf16)

    def owner_attn(left, right):
        blocks = [
            rows_mul(columns_at(left, dp_rank ^ step, group_rows), right)
            for step in range(dp_count)
        ]
        group = scatter_halves(blocks, "dp")
        return scatter_direct(lambda step: rows_at(group, ctx_rank ^ step, own_rows), "ctx")

    grad_w_out = owner_attn(grad_mid_bf, attn_flat)
    grad_query, grad_key_all, grad_value_all = attend_backward(
        query_bf, keys_all, values_all, attn_bf, log_total, grad_attn.reshape(attn_bf.shape), allowed
    )
    grad_keyval_all = jnp.concatenate([grad_key_all, grad_value_all], 2)
    grad_keyval = scatter_direct(
        lambda step: lax.dynamic_slice_in_dim(
            grad_keyval_all, (ctx_rank ^ step) * local_len, local_len, 1
        ),
        "ctx",
    ).reshape(row_count, -1)
    grad_query = unrotate(
        grad_query.reshape(row_count, -1, HEAD_DIM), cos_tab, sin_tab
    ).reshape(row_count, -1)
    grad_key = unrotate(
        grad_keyval[:, :k_cols].reshape(row_count, -1, HEAD_DIM), cos_tab, sin_tab
    ).reshape(row_count, -1)
    grad_qkv = jnp.concatenate([grad_query, grad_key, grad_keyval[:, k_cols:]], 1)
    grad_qkv_bf = grad_qkv.astype(bf16)
    grad_w_qkv = owner_attn(normed_in, grad_qkv_bf)
    dot_part = mat_mul_t(grad_qkv_bf, w_qkv)
    grad_normed_in = dot_part + partner(dot_part)
    grad_in_norm, grad_gain_in = norm_backward(residual, inv_in, gain_in, grad_normed_in)
    input_grad = (grad_mid + grad_in_norm).reshape(tokens.shape)

    bias_sum = jnp.sum(grad_qkv, axis=0)
    device_count = dp_count * ctx_count
    grad_small = jnp.concatenate(
        [
            grad_gain_in.reshape(device_count, -1),
            grad_gain_mid.reshape(device_count, -1),
            bias_sum[:q_cols].reshape(kv_local, -1).T.reshape(device_count, -1),
            jnp.concatenate(
                [
                    bias_sum[q_cols : q_cols + k_cols].reshape(kv_local, -1).T,
                    bias_sum[q_cols + k_cols :].reshape(kv_local, -1).T,
                ],
                0,
            ).reshape(device_count, -1),
        ],
        1,
    )
    small_group = scatter_small(
        [rows_at(grad_small, dp_rank ^ step, ctx_count) for step in range(dp_count)], "dp"
    )
    small_own = scatter_small(
        [rows_at(small_group, ctx_rank ^ step, 1) for step in range(ctx_count)], "ctx"
    )
    own = [small_own[:, low:high] for low, high in zip(cuts[:-1], cuts[1:])]
    return (
        activations,
        input_grad,
        own[0],
        grad_w_qkv[None, :, :q_cols],
        own[2].reshape(q_bias.shape),
        grad_w_qkv[None, :, q_cols : q_cols + k_cols],
        grad_w_qkv[None, :, q_cols + k_cols :],
        own[3].reshape(kv_bias.shape),
        grad_w_out[None],
        own[1],
        grad_w_gate[None],
        grad_w_up[None],
        grad_w_down[None],
    )


MESH = pl.DeviceIdType.MESH


def remote(src, dst, send_sem, recv_sem, target):
    return pltpu.make_async_remote_copy(
        src_ref=src, dst_ref=dst, send_sem=send_sem, recv_sem=recv_sem, device_id=target, device_id_type=MESH
    )


def greet(partners):
    barrier = pltpu.get_barrier_semaphore()
    for partner_id in partners:
        pl.semaphore_signal(barrier, inc=1, device_id=partner_id, device_id_type=MESH)
    pl.semaphore_wait(barrier, len(partners))


def spread_row(values, row_cols, period, total):
    left = lax.broadcasted_iota(jnp.int32, (period, total), 0)
    right = lax.broadcasted_iota(jnp.int32, (period, total), 1)
    pick = (lax.rem(right, period) == left).astype(jnp.float32).astype(jnp.bfloat16)
    spread = jnp.dot(values.astype(jnp.bfloat16), pick, preferred_element_type=jnp.float32)
    block = lax.broadcasted_iota(jnp.int32, spread.shape, 0) // 8
    owner = lax.broadcasted_iota(jnp.int32, spread.shape, 1) // period
    return jnp.sum(jnp.where(block == owner, spread, 0.0), axis=0, keepdims=True)


def same_document(seg_ref, seq, ctx, local):
    row = seg_ref[seq : seq + 1, pl.ds(pl.multiple_of(ctx * local, local), local)].astype(jnp.float32)
    down = lax.broadcasted_iota(jnp.int32, (local, local), 0)
    across = lax.broadcasted_iota(jnp.int32, (local, local), 1)
    column = jnp.sum(jnp.where(down == across, row, 0.0), axis=1, keepdims=True)
    return column == seg_ref[seq : seq + 1, :].astype(jnp.float32)


def forward_kernel(
    sizes,
    tok_ref,
    cot_ref,
    attn_own,
    gate_own,
    up_own,
    down_own,
    small_own,
    cos_ref,
    sin_ref,
    seg_ref,
    live_ref,
    wattn_out,
    b_out,
    h_out,
    a_out,
    q_out,
    kv_out,
    o_out,
    lse_out,
    row_out,
    zgu_out,
    sum_out,
    own_out,
    e_out,
    wattn,
    wmlp,
    e_all,
    b_all,
    h_ref,
    a_ref,
    q_ref,
    kv_ref,
    o_ref,
    lse_ref,
    row_ref,
    small,
    part,
    part_in,
    gu_ref,
    z_ref,
    zgu,
    pair,
    give,
    take,
    done,
    mine,
    zs,
    zr,
    xs,
    xr,
    ys,
    yr,
    fs,
    fr,
    ks,
    kr,
    ps,
    pr,
    bs,
    br,
    us,
    ur,
    ts,
    tr,
    loc,
    out_sem,
):
    dp_count, ctx_count, own, qkv_cols, q_cols, gain_cut = sizes
    dp, ctx, core = lax.axis_index("dp"), lax.axis_index("ctx"), lax.axis_index("tp")
    bf16, f32 = jnp.bfloat16, jnp.float32
    width = tok_ref.shape[1]
    rows = tok_ref.shape[0]
    seqs = cot_ref.shape[0]
    local = cot_ref.shape[1]
    tiles = range(ctx_count)

    def at_x(d):
        return d + 1 - 2 * lax.rem(d, 2)

    def at_y(d):
        return lax.rem(d + 2, 4)

    dpx, dpy = at_x(dp), at_y(dp)
    dpd = at_x(dpy)
    peers = [ctx]
    for step in range(1, ctx_count):
        value = jnp.int32(0)
        for bit in (1, 2, 4, 8):
            if bit < ctx_count:
                digit = lax.rem(ctx // bit, 2)
                value = value + bit * (digit + (1 - 2 * digit) * ((step // bit) % 2))
        peers.append(value)
    other = 1 - core
    to_core = {"tp": other}

    greet(
        [{"dp": dpx}, {"dp": dpy}, {"tp": other}] + [{"ctx": peers[step]} for step in range(1, ctx_count)]
    )
    sent = []

    def start(copy):
        copy.start()
        sent.append(copy)
        return copy

    def block_rows(d, c):
        return pl.ds(pl.multiple_of((d * ctx_count + c) * own, own), own)

    def slot(item, d, c):
        if item == 0:
            return small.at[d * ctx_count + c]
        if item == 1:
            return wattn.at[block_rows(d, c), :]
        return wmlp.at[item - 2, block_rows(d, c), :]

    def source(item):
        return small_own if item == 0 else attn_own

    ff_block = wmlp.shape[2]
    top = ctx_count - 1
    ff_tail = gate_own.shape[1] - top * ff_block

    class Either:
        def __init__(self, full_there, full_here, wide, slim):
            self.there, self.here, self.wide, self.slim = full_there, full_here, wide, slim

        def pick(self, full, name):
            @pl.when(full)
            def _():
                getattr(self.wide, name)()

            @pl.when(jnp.logical_not(full))
            def _():
                getattr(self.slim, name)()

        def start(self):
            self.pick(self.there, "start")

        def wait_send(self):
            self.pick(self.there, "wait_send")

        def wait_recv(self):
            self.pick(self.here, "wait_recv")

        def wait(self):
            self.pick(self.here, "wait")

    def column_copy(item, tile, make):
        own_weight = (gate_own, up_own, down_own)[item - 2]
        peer = peers[tile]
        wide_from = own_weight.at[:, pl.ds(pl.multiple_of(jnp.minimum(peer, top - 1) * ff_block, 128), ff_block)]
        slim_from = own_weight.at[:, top * ff_block :]
        place_at = block_rows(dp, ctx)
        return Either(
            peer != top,
            ctx != top,
            make(wide_from, wmlp.at[item - 2, place_at, :]),
            make(slim_from, wmlp.at[item - 2, place_at, 0:ff_tail]),
        )

    if ff_tail < ff_block:

        @pl.when(ctx == top)
        def _():
            fill = pl.ds(pl.multiple_of(dp * own * ctx_count, own), own * ctx_count)
            for item in range(3):
                wmlp[item, fill, ff_tail:] = jnp.zeros((own * ctx_count, ff_block - ff_tail), bf16)


    items = range(5)
    local_copies = []
    for item in items:
        if item < 2:
            copy = pltpu.make_async_copy(source(item), slot(item, dp, ctx), loc.at[item])
        else:
            copy = column_copy(item, 0, lambda src, dst: pltpu.make_async_copy(src, dst, loc.at[item]))
        copy.start()
        local_copies.append(copy)
    z_copy = {}

    def z_send(item):
        for tile in range(1, ctx_count):

            def make(src, dst):
                return remote(src, dst, zs.at[item, tile], zr.at[item, tile], {"ctx": peers[tile]})

            if item < 2:
                z_copy[item, tile] = start(make(source(item), slot(item, dp, ctx)))
            else:
                z_copy[item, tile] = start(column_copy(item, tile, make))

    x_copy, y_copy, f_copy = {}, {}, {}

    def xy_send(item, tile):
        src = source(item) if tile == 0 and item < 2 else slot(item, dp, peers[tile])
        if tile:
            z_copy[item, tile].wait_recv()
        elif item >= 2:
            local_copies[item].wait()
        dst = slot(item, dp, peers[tile])
        x_copy[item, tile] = start(remote(src, dst, xs.at[item, tile], xr.at[item, tile], {"dp": dpx}))
        y_copy[item, tile] = start(remote(src, dst, ys.at[item, tile], yr.at[item, tile], {"dp": dpy}))

    def forward(item, tile):
        if (item + tile) % 2 == 0:
            x_copy[item, tile].wait_recv()
            place_at = slot(item, dpx, peers[tile])
            target = {"dp": dpy}
        else:
            y_copy[item, tile].wait_recv()
            place_at = slot(item, dpy, peers[tile])
            target = {"dp": dpx}
        f_copy[item, tile] = start(remote(place_at, place_at, fs.at[item, tile], fr.at[item, tile], target))

    def settle(item, tile):
        if (item + tile) % 2 == 0:
            y_copy[item, tile].wait_recv()
        else:
            x_copy[item, tile].wait_recv()
        f_copy[item, tile].wait_recv()

    last = ctx_count - 1
    ways = ((1, ctx < last), (-1, ctx > 0))
    relay_sent = []

    def hop(index, buf, way, distance, origin):
        step, _ = ways[way]
        piece = buf.at[origin, core]
        return remote(piece, piece, bs.at[index, way, distance], br.at[index, way, distance], {"ctx": ctx + step})

    def spread_start(index, buf):
        for way in range(2):
            copy = hop(index, buf, way, 0, ctx)

            @pl.when(ways[way][1])
            def _():
                copy.start()

            relay_sent.append((ways[way][1], copy))

    def spread_step(index, buf, distance):
        for way in range(2):
            step, open_end = ways[way]
            origin = ctx - step * distance
            here = (origin >= 0) & (origin <= last)
            safe = jnp.clip(origin, 0, last)
            piece = buf.at[safe, core]
            got = remote(piece, piece, bs.at[index, way, distance - 1], br.at[index, way, distance - 1], to_core)
            share = remote(piece, piece, us.at[index, way, distance], ur.at[index, way, distance], to_core)

            @pl.when(here)
            def _():
                got.wait_recv()
                share.start()

            relay_sent.append((here, share))
            if distance < last:
                copy = hop(index, buf, way, distance, safe)

                @pl.when(here & open_end)
                def _():
                    copy.start()

                relay_sent.append((here & open_end, copy))

    def spread_end(index, buf, distance):
        for way in range(2):
            step, _ = ways[way]
            origin = ctx - step * distance
            piece = buf.at[jnp.clip(origin, 0, last), other]
            got = remote(piece, piece, us.at[index, way, distance], ur.at[index, way, distance], to_core)

            @pl.when((origin >= 0) & (origin <= last))
            def _():
                got.wait_recv()

    z_send(0)
    z_send(1)
    xy_send(1, 0)
    for item in (2, 3):
        z_send(item)
    e_local = pltpu.make_async_copy(cot_ref, e_all.at[ctx], loc.at[5])
    e_local.start()
    kept = []

    def keep_out(src, dst):
        copy = pltpu.make_async_copy(src, dst, out_sem.at[len(kept)])
        copy.start()
        kept.append(copy)

    for tile in tiles:
        xy_send(0, tile)
    for tile in tiles:
        forward(0, tile)
    for tile in range(1, ctx_count):
        xy_send(1, tile)
    for tile in tiles:
        settle(0, tile)
    local_copies[0].wait()

    flat = small[...].reshape(dp_count * ctx_count * 8, small.shape[2])
    row_ref[0:1, :] = spread_row(flat[:, gain_cut[0] : gain_cut[1]], None, gain_cut[1] - gain_cut[0], width)
    row_ref[1:2, :] = spread_row(flat[:, gain_cut[1] : gain_cut[2]], None, gain_cut[2] - gain_cut[1], width)
    row_ref[2:3, :q_cols] = spread_row(flat[:, gain_cut[2] : gain_cut[3]], None, gain_cut[3] - gain_cut[2], q_cols)
    row_ref[2:3, q_cols:qkv_cols] = spread_row(
        flat[:, gain_cut[3] : gain_cut[4]], None, gain_cut[4] - gain_cut[3], qkv_cols - q_cols
    )

    step_rows = 32

    def norm_in(index, _):
        piece = pl.ds(index * step_rows, step_rows)
        val = tok_ref[piece, :].astype(f32)
        inv = lax.rsqrt(jnp.mean(val * val, axis=-1, keepdims=True) + norm_eps)
        a_ref[piece, :] = (val * inv * row_ref[0:1, :]).astype(bf16)
        return 0

    lax.fori_loop(0, rows // step_rows, norm_in, 0)
    e_local.wait()

    def mask_rows(index, _):
        per_seq = local // step_rows
        seq = index // per_seq
        piece = pl.ds(pl.multiple_of(lax.rem(index, per_seq) * step_rows, step_rows), step_rows)
        e_all[ctx, seq, piece, :] = (e_all[ctx, seq, piece, :].astype(f32) * live_ref[seq][:, 0:1]).astype(bf16)
        return 0

    lax.fori_loop(0, rows // step_rows, mask_rows, 0)
    for tile in tiles:
        forward(1, tile)
    for item in (2, 3, 4):
        xy_send(item, 0)
    for tile in tiles:
        if tile:
            xy_send(2, tile)
    for tile in tiles:
        settle(1, tile)
    local_copies[1].wait()
    keep_out(wattn, wattn_out)
    keep_out(a_ref, a_out)
    keep_out(row_ref, row_out)

    pending = [(forward, 2, 0), (forward, 3, 0), (forward, 4, 0)]
    pending += [(xy_send, 3, tile) for tile in tiles if tile]
    pending += [(forward, 2, tile) for tile in tiles if tile]
    pending += [(forward, 3, 1)] + [(xy_send, 4, tile) for tile in tiles if tile]
    pending += [(forward, 3, 2), (forward, 3, 3)]
    pending += [(forward, 4, tile) for tile in tiles if tile]

    def pump(count):
        for _ in range(min(count, len(pending))):
            action, item, tile = pending.pop(0)
            action(item, tile)

    own_keys = pl.ds(pl.multiple_of(ctx * local, local), local)
    order = [qkv_cols - 256] + list(range(0, q_cols, 256))
    kv_copies = []
    for low in order:
        val = jnp.dot(a_ref[...], wattn[:, low : low + 256], preferred_element_type=f32) + row_ref[2:3, low : low + 256]
        for head_low in (0, 128):
            head = val[:, head_low : head_low + 128]
            if low + head_low < qkv_cols - 128:
                head = head * cos_ref[...] + pltpu.roll(head, 64, 1) * sin_ref[...]
            head = head.astype(bf16)
            for seq in range(seqs):
                piece = head[seq * local : (seq + 1) * local]
                if low == qkv_cols - 256:
                    kv_ref[seq, head_low // 128, own_keys, :] = piece
                else:
                    q_ref[seq, (low + head_low) // 128] = piece
        if low == qkv_cols - 256:
            for tile in range(1, ctx_count):
                piece = kv_ref.at[:, :, own_keys, :]
                kv_copies.append(start(remote(piece, piece, ks.at[tile], kr.at[tile], {"ctx": peers[tile]})))
    keep_out(q_ref, q_out)
    pump(1)
    for copy in kv_copies:
        copy.wait_recv()
    z_send(4)
    pump(5)
    keep_out(kv_ref, kv_out)

    keys = kv_ref.shape[2]
    key_no = lax.broadcasted_iota(jnp.int32, (local, keys), 1)
    query_no = lax.broadcasted_iota(jnp.int32, (local, keys), 0) + ctx * local
    for seq in range(seqs):
        seen = same_document(seg_ref, seq, ctx, local) & (key_no <= query_no)
        hide = jnp.where(seen, 0.0, masked_score)

        def one_head(head, _):
            score = lax.dot_general(
                q_ref[seq, head], kv_ref[seq, 0], (((1,), (1,)), ((), ())), preferred_element_type=f32
            )
            score = jnp.where(hide < 0.0, masked_score, score * HEAD_DIM ** (-0.5))
            top = jnp.max(score, axis=-1, keepdims=True)
            weight = jnp.exp(score - top)
            total = jnp.sum(weight, axis=-1, keepdims=True)
            prob = (weight / total).astype(bf16)
            lse_ref[seq, head] = top + jnp.log(total)
            out = jnp.dot(prob, kv_ref[seq, 1], preferred_element_type=f32)
            o_ref[seq, head] = out.astype(bf16)
            return 0

        lax.fori_loop(0, q_cols // 128, one_head, 0)
        pump(2 - seq)
    keep_out(o_ref, o_out)
    keep_out(lse_ref, lse_out)

    o_rows = jnp.concatenate(
        [jnp.concatenate([o_ref[seq, head] for head in range(q_cols // 128)], 1) for seq in range(seqs)], 0
    )
    part_copies = []
    for index in range(width // 256):
        part[index] = lax.dot_general(
            o_rows,
            wattn[index * 256 : (index + 1) * 256, qkv_cols:],
            (((1,), (1,)), ((), ())),
            preferred_element_type=f32,
        )
        part_copies.append(
            start(remote(part.at[index], part_in.at[index], ps.at[index], pr.at[index], {"tp": other}))
        )
    for index, copy in enumerate(part_copies):
        copy.wait_recv()
        span = slice(index * 256, (index + 1) * 256)
        h_ref[:, span] = tok_ref[:, span].astype(f32) + (part[index] + part_in[index])

    def norm_mid(index, _):
        piece = pl.ds(index * step_rows, step_rows)
        val = h_ref[piece, :]
        inv = lax.rsqrt(jnp.mean(val * val, axis=-1, keepdims=True) + norm_eps)
        per_seq = local // step_rows
        b_all[ctx, index // per_seq, pl.ds(lax.rem(index, per_seq) * step_rows, step_rows), :] = (
            val * inv * row_ref[1:2, :]
        ).astype(bf16)
        return 0

    lax.fori_loop(0, rows // step_rows, norm_mid, 0)
    spread_start(1, b_all)
    keep_out(h_ref, h_out)
    pump(4)
    spread_step(1, b_all, 1)
    pump(2)
    spread_step(1, b_all, 2)
    spread_start(0, e_all)

    ff = wmlp.shape[2]
    full_ff = ff // 256 * 256
    nt = (((1,), (1,)), ((), ()))

    def ahead_columns(peer, low, size):
        span = pl.ds(low, size)
        gate = jnp.dot(b_all[peer].reshape(rows, width), wmlp[0, :, span], preferred_element_type=f32)
        up = jnp.dot(b_all[peer].reshape(rows, width), wmlp[1, :, span], preferred_element_type=f32)
        gu_ref[0, peer, :, span] = gate
        gu_ref[1, peer, :, span] = up
        z_ref[peer, :, span] = (gate * jax.nn.sigmoid(gate) * up).astype(bf16)

    def back_columns(tile, low, size):
        span, peer = pl.ds(low, size), peers[tile]
        grad = jnp.dot(e_all[peer].reshape(rows, width), wmlp[2, :, span], preferred_element_type=f32)
        gate, up = gu_ref[0, peer, :, span], gu_ref[1, peer, :, span]
        sig = jax.nn.sigmoid(gate)
        zgu[0, peer, :, span] = (grad * up * sig * (1.0 + gate * (1.0 - sig))).astype(bf16)
        zgu[1, peer, :, span] = (grad * gate * sig).astype(bf16)

    def over_columns(body):
        def columns(index, _):
            body(pl.multiple_of(index * 256, 256), 256)
            return 0

        lax.fori_loop(0, ff // 256, columns, 0)
        if full_ff < ff:
            body(full_ff, ff - full_ff)

    def ahead(tile):
        over_columns(lambda low, size: ahead_columns(peers[tile], low, size))

    for item in (2, 3):
        for tile in tiles:
            settle(item, tile)
    ahead(0)
    spread_step(1, b_all, ctx_count - 1)
    pump(1)
    for distance in range(1, ctx_count):
        spread_end(1, b_all, distance)
    keep_out(b_all, b_out)
    ahead(1)
    pump(1)
    ahead(2)
    spread_step(0, e_all, 1)
    pump(1)
    ahead(3)
    keep_out(z_ref, zgu_out.at[0])

    while pending:
        pump(1)
    for tile in tiles:
        settle(4, tile)

    give_copies = {}
    tokens_all = ctx_count * rows
    sums = width // 256

    def emit(item, index, val):
        val = val.reshape(ctx_count, seqs, local, 256)
        ours = jnp.where(core == 0, val[:, 0], val[:, 1])
        theirs = jnp.where(core == 0, val[:, 1], val[:, 0])
        span = pl.ds(pl.multiple_of(index * 256, 256), 256)
        pair[:, :, span] = ours
        give[item, index] = theirs.astype(bf16)

    def emit_send(item, index):
        give_copies[item, index] = start(
            remote(give.at[item, index], take.at[item, index], ts.at[item, index], tr.at[item, index], to_core)
        )

    def gather(item):
        for index in range(sums):
            give_copies[item, index].wait_recv()
            span = slice(index * 256, (index + 1) * 256)

            def add(tile, _):
                total = pair[tile, :, span] + take[item, index, tile].astype(f32)
                done[item, tile, :, span] = total.astype(bf16)
                return 0

            lax.fori_loop(0, ctx_count, add, 0)
            mine[item, :, span] = pair[ctx, :, span] + take[item, index, ctx].astype(f32)
        keep_out(done.at[item], sum_out.at[item])

    def wide_dot(left, right):
        return lax.dot_general(left, right, nt, preferred_element_type=f32)

    def out_sum(index, _):
        span = pl.ds(pl.multiple_of(index * 256, 256), 256)
        emit(1, index, wide_dot(z_ref[...].reshape(tokens_all, ff), wmlp[2, span, :]))
        return 0

    def back_sum(index, _):
        span = pl.ds(pl.multiple_of(index * 256, 256), 256)
        val = wide_dot(zgu[0].reshape(tokens_all, ff), wmlp[0, span, :])
        emit(0, index, val + wide_dot(zgu[1].reshape(tokens_all, ff), wmlp[1, span, :]))
        return 0

    lax.fori_loop(0, sums, out_sum, 0)
    for index in range(sums):
        emit_send(1, index)
    spread_step(0, e_all, 2)
    over_columns(lambda low, size: back_columns(0, low, size))
    gather(1)
    for tile in range(1, ctx_count):
        if tile == ctx_count - 1:
            spread_step(0, e_all, tile)
        spread_end(0, e_all, tile)
        over_columns(lambda low, size: back_columns(tile, low, size))
    keep_out(e_all, e_out)
    keep_out(zgu, zgu_out.at[1:3])
    lax.fori_loop(0, sums, back_sum, 0)
    for index in range(sums):
        emit_send(0, index)
    gather(0)
    keep_out(mine, own_out)
    for copy in kept:
        copy.wait()
    for copy in sent:
        copy.wait_send()
    for here, copy in relay_sent:

        @pl.when(here)
        def _():
            copy.wait_send()


def forward_call(tok, cot, attn_own, mlp_own, small_own, cos, sin, seg, live, qkv_cols, q_cols, gain_cut):
    dp_count, ctx_count = lax.axis_size("dp"), lax.axis_size("ctx")
    own = attn_own.shape[0]
    rows, width = tok.shape
    seqs, local = cot.shape[:2]
    full_rows = own * dp_count * ctx_count
    heads = q_cols // 128
    lanes = 128 * ctx_count
    ff = -(-mlp_own[0].shape[1] // lanes) * 128
    bf16, f32 = jnp.bfloat16, jnp.float32
    vmem, hbm = pl.BlockSpec(memory_space=pltpu.VMEM), pl.BlockSpec(memory_space=pl.ANY)
    group = (ctx_count, seqs, local, width)
    kept = [
        ((rows, width), f32),
        ((rows, width), bf16),
        ((seqs, heads, local, 128), bf16),
        ((seqs, 2, local * ctx_count, 128), bf16),
        ((seqs, heads, local, 128), bf16),
        ((seqs, heads, local, 1), f32),
        ((8, width), f32),
    ]
    weights = ((full_rows, attn_own.shape[1]), bf16)
    outs = [weights, (group, bf16)] + kept
    outs += [((3, ctx_count, rows, ff), bf16), ((2, ctx_count, local, width), bf16), ((2, local, width), f32)]
    outs += [(group, bf16)]
    chunks = width // 256
    scratch = [weights, ((3, full_rows, ff), bf16), (group, bf16), (group, bf16)] + kept
    scratch += [
        ((dp_count * ctx_count, 8, small_own.shape[1]), f32),
        ((chunks, rows, 256), f32),
        ((chunks, rows, 256), f32),
        ((2, ctx_count, rows, ff), f32),
        ((ctx_count, rows, ff), bf16),
        ((2, ctx_count, rows, ff), bf16),
        ((ctx_count, local, width), f32),
        ((2, chunks, ctx_count, local, 256), bf16),
        ((2, chunks, ctx_count, local, 256), bf16),
        ((2, ctx_count, local, width), bf16),
        ((2, local, width), f32),
    ]
    dma = pltpu.SemaphoreType.DMA
    return pl.pallas_call(
        functools.partial(forward_kernel, (dp_count, ctx_count, own, qkv_cols, q_cols, gain_cut)),
        out_shape=[jax.ShapeDtypeStruct(shape, kind) for shape, kind in outs],
        in_specs=[vmem] + [hbm] * 6 + [vmem] * 4,
        out_specs=[hbm] * len(outs),
        scratch_shapes=[pltpu.VMEM(*entry) for entry in scratch]
        + [dma((5, ctx_count)) for _ in range(8)]
        + [dma((ctx_count,)), dma((ctx_count,)), dma((chunks,)), dma((chunks,))]
        + [dma((2, 2, ctx_count)) for _ in range(4)]
        + [dma((2, chunks)), dma((2, chunks)), dma((8,)), dma((20,))],
        compiler_params=pltpu.CompilerParams(
            collective_id=0, has_side_effects=True, vmem_limit_bytes=65 * 1024 * 1024 - 65536
        ),
        name="forward_kernel",
    )(tok, cot, attn_own, *mlp_own, small_own, cos, sin, seg, live)


def xor_rank(rank, step, count):
    value = jnp.int32(0)
    bit = 1
    while bit < count:
        digit = lax.rem(rank // bit, 2)
        value = value + bit * (digit + (1 - 2 * digit) * ((step // bit) % 2))
        bit *= 2
    return value


def backward_kernel(
    sizes,
    sum_in,
    own_in,
    zgu_in,
    b_in,
    e_in,
    cot_hbm,
    tok_hbm,
    h_hbm,
    a_hbm,
    q_hbm,
    kv_hbm,
    o_hbm,
    lse_hbm,
    wattn_hbm,
    live_ref,
    row_ref,
    cos_ref,
    sin_ref,
    seg_ref,
    act_ref,
    dx_ref,
    zin,
    gat_ref,
    rows_ref,
    gout,
    lin,
    sum_v,
    fin,
    left_ref,
    right_ref,
    block_ref,
    keep,
    r1,
    r2,
    keep_at,
    send_at,
    r1_at,
    r2_at,
    zin_at,
    hb_ref,
    do_ref,
    prob_ref,
    ds_ref,
    dkv_ref,
    dkv_bf,
    dkv_in,
    dqkv_ref,
    part,
    part_in,
    zss,
    zrs,
    fs,
    fr,
    ld,
    kd,
    gd,
    s1,
    v1,
    s2,
    v2,
    s3,
    v3,
    ks,
    kr,
    ps,
    pr,
    gs,
    gr,
    acc_ref,
    sm_in,
    sm_sum,
    cot_ref,
    tok_ref,
    h_ref,
    a_ref,
    q_ref,
    kv_ref,
    o_ref,
    lse_ref,
    wattn,
    in_sem,
):
    dp_count, ctx_count, own, qkv_cols, q_cols = sizes
    dp, ctx, core = lax.axis_index("dp"), lax.axis_index("ctx"), lax.axis_index("tp")
    bf16, f32 = jnp.bfloat16, jnp.float32
    seqs, local, width = cot_ref.shape
    loads = []
    for src, dst in (
        (cot_hbm, cot_ref),
        (tok_hbm, tok_ref),
        (h_hbm, h_ref),
        (a_hbm, a_ref),
        (q_hbm, q_ref),
        (kv_hbm, kv_ref),
        (o_hbm, o_ref),
        (lse_hbm, lse_ref),
        (wattn_hbm, wattn),
    ):
        loads.append(pltpu.make_async_copy(src, dst, in_sem.at[len(loads)]))
    group = own * ctx_count
    ff = zgu_in.shape[3]
    heads = q_cols // 128
    other = 1 - core
    peers = [xor_rank(ctx, step, ctx_count) for step in range(ctx_count)]
    nodes = [xor_rank(dp, step, dp_count) for step in range(dp_count)]
    to_x, to_y, to_core = {"dp": nodes[1]}, {"dp": nodes[2]}, {"tp": other}
    greet([to_x, to_y, to_core] + [{"ctx": peers[step]} for step in range(1, ctx_count)])
    sent = []

    def start(copy):
        copy.start()
        sent.append(copy)
        return copy

    def rows_of(count, size, body):
        def one(index, _):
            body(pl.ds(pl.multiple_of(index * size, size), size))
            return 0

        lax.fori_loop(0, count // size, one, 0)

    last = ctx_count - 1
    ends = (ctx == 0, ctx == last)
    fin_copy, relay_sent = {}, []
    sums_of = (fin, act_ref)

    def line_step(index, turn):
        for way, step in ((0, 1), (1, -1)):
            owner = ctx + step * (ctx_count - turn)
            active = (owner >= 0) & (owner <= last)
            safe = jnp.clip(owner, 0, last)
            target = {"ctx": ctx + step}

            def message(src):
                return remote(
                    src,
                    lin.at[index, way, turn - 1],
                    zss.at[index, way, turn - 1],
                    zrs.at[index, way, turn - 1],
                    target,
                )

            fresh = message(sum_v.at[index, safe])

            @pl.when(active & ends[way])
            def _():
                fresh.start()

            relay_sent.append((active, fresh))
            if turn > 1:
                held = lin.at[index, way, turn - 2]
                got = remote(
                    held, held, zss.at[index, way, turn - 2], zrs.at[index, way, turn - 2], target
                )

                @pl.when(active & jnp.logical_not(ends[way]))
                def _():
                    got.wait_recv()

                    def add(piece):
                        lin[index, way, turn - 2, piece, :] = (
                            lin[index, way, turn - 2, piece, :].astype(f32) + sum_v[index, safe, piece, :].astype(f32)
                        ).astype(bf16)

                    rows_of(local, 32, add)
                    message(held).start()

    def collect_fin(index):
        into = sums_of[index]
        for way, step in ((0, 1), (1, -1)):
            held = lin.at[index, way, last - 1]
            got = remote(
                held, held, zss.at[index, way, last - 1], zrs.at[index, way, last - 1], {"ctx": ctx + step}
            )

            @pl.when(jnp.logical_not(ends[way]))
            def _():
                got.wait_recv()

                def add(piece):
                    into[core, piece, :] = into[core, piece, :] + lin[index, way, last - 1, piece, :].astype(f32)

                rows_of(local, 32, add)

        fin_copy[index] = remote(into.at[core], into.at[core], fs.at[index], fr.at[index], to_core)
        fin_copy[index].start()

    halves = {}
    for item in range(3):
        cut = (ff // 256 + 1) * 128
        halves[item] = ((0, cut), (cut, ff)) if item != 1 else ((cut, ff), (0, cut))
    middle = qkv_cols + (wattn.shape[1] - qkv_cols) // 2
    halves[3] = ((qkv_cols, middle), (middle, wattn.shape[1]))
    quarter = qkv_cols // 4
    halves[4] = ((0, quarter), (quarter, 2 * quarter))
    halves[5] = ((2 * quarter, 3 * quarter), (3 * quarter, qkv_cols))
    first_to, second_to = (to_y, to_x), (to_x, to_y)
    first_keys = ((2, 3), (1, 3))
    one_copy, two_copy, three_copy, keep_copy = {}, {}, {}, {}

    def cols(item, half):
        low, high = halves[item][half]
        return slice(low, high)

    def refs(item):
        if item < 3:
            return keep.at[item], r1.at[item], r2.at[item]
        return keep_at, r1_at, r2_at

    def block_of(item, key):
        return gout.at[item, key]

    def stage_one(item, half):
        span = cols(item, half)
        for slot, key in enumerate(first_keys[half]):
            src = block_of(item, key).at[:, span] if item < 3 else send_at.at[slot, :, span]
            one_copy[item, half, slot] = start(
                remote(
                    src,
                    refs(item)[1].at[slot, :, span],
                    s1.at[item, half, slot],
                    v1.at[item, half, slot],
                    first_to[half],
                )
            )

    def stage_two(item, half):
        span = cols(item, half)
        mine, first, second = refs(item)
        if item < 3:
            keep_copy[item, half].wait()
        one_copy[item, half, 1].wait_recv()

        def add(piece):
            mine[1, piece, span] = (mine[1, piece, span].astype(f32) + first[1, piece, span].astype(f32)).astype(bf16)

        rows_of(group, 96, add)
        two_copy[item, half] = start(
            remote(mine.at[1, :, span], second.at[:, span], s2.at[item, half], v2.at[item, half], second_to[half])
        )

    def stage_three(item, half):
        span = cols(item, half)
        mine, first, second = refs(item)
        if item < 3:
            keep_copy[item, 2].wait() if half == 0 else None
        one_copy[item, half, 0].wait_recv()
        two_copy[item, half].wait_recv()

        def total(piece):
            return mine[0, piece, span].astype(f32) + first[0, piece, span].astype(f32) + second[piece, span].astype(f32)

        if item >= 3:
            gat_ref[:, span] = total(pl.ds(pl.multiple_of(ctx * own, own), own))

        def add(piece):
            mine[0, piece, span] = total(piece).astype(bf16)

        rows_of(group, 96, add)
        if item < 3:
            there = zin.at[item, :, pl.ds(pl.multiple_of(ctx * ff + span.start, 128), span.stop - span.start)]
        else:
            there = zin_at.at[ctx, :, span]
        for tile in range(1, ctx_count):
            piece = pl.ds(pl.multiple_of(peers[tile] * own, own), own)
            three_copy[item, half, tile] = start(
                remote(
                    mine.at[0, piece, span],
                    there,
                    s3.at[item, half, tile],
                    v3.at[item, half, tile],
                    {"ctx": peers[tile]},
                )
            )
        if item < 3:
            piece = pl.ds(pl.multiple_of(ctx * own, own), own)
            copy = pltpu.make_async_copy(mine.at[0, piece, span], there, kd.at[item, 3 + half])
            copy.start()
            three_copy[item, half, 0] = copy

    def stage_four(item, half):
        span = cols(item, half)
        for tile in range(1, ctx_count):
            three_copy[item, half, tile].wait_recv()
        if item < 3:
            three_copy[item, half, 0].wait()
        else:
            total = gat_ref[:, span]
            for tile in range(1, ctx_count):
                total = total + zin_at[peers[tile], :, span].astype(f32)
            gat_ref[:, span] = total

    def keep_load(item):
        for half in range(2):
            span = cols(item, half)
            copy = pltpu.make_async_copy(
                block_of(item, 1 + half).at[:, span], keep.at[item, 1, :, span], kd.at[item, half]
            )
            copy.start()
            keep_copy[item, half] = copy
        copy = pltpu.make_async_copy(block_of(item, 0), keep.at[item, 0], kd.at[item, 2])
        copy.start()
        keep_copy[item, 2] = copy

    sum_copy = pltpu.make_async_copy(sum_in, sum_v, ld.at[1])
    sum_copy.start()

    def load_left(count):
        span = pl.ds(pl.multiple_of(nodes[dp_count - 1 - count % dp_count] * group, group), group)
        source = b_in if count < 2 * dp_count else e_in
        copy = pltpu.make_async_copy(source.at[:, :, :, span], left_ref.at[count % 2], gd.at[count % 2])
        copy.start()
        return copy

    def load_right(item):
        copy = pltpu.make_async_copy(zgu_in.at[(1, 2, 0)[item]], right_ref, gd.at[2])
        copy.start()
        return copy

    right_copy = load_right(0)
    left_copies = {0: load_left(0), 1: load_left(1)}
    mine_copies = [
        pltpu.make_async_copy(own_in.at[0], fin.at[core], ld.at[0]),
        pltpu.make_async_copy(own_in.at[1], act_ref.at[core], ld.at[2]),
    ]
    for copy in mine_copies:
        copy.start()
    for copy in loads:
        copy.start()
    sum_copy.wait()
    line_step(0, 1)

    out_copy = {}

    def block(count, left_copy):
        slot = count % 2
        left_copy.wait()

        def columns(low, size):
            span = pl.ds(low, size)
            val = lax.dot_general(
                left_ref[slot].reshape(-1, group),
                right_ref[:, :, span].reshape(-1, size),
                (((0,), (0,)), ((), ())),
                preferred_element_type=f32,
            )
            block_ref[slot, :, span] = val.astype(bf16)

        def one(index, _):
            columns(pl.multiple_of(index * 256, 256), 256)
            return 0

        lax.fori_loop(0, ff // 256, one, 0)
        if ff % 256:
            columns(ff // 256 * 256, ff % 256)
        item, key = count // dp_count, dp_count - 1 - count % dp_count
        out_copy[count] = pltpu.make_async_copy(block_ref.at[slot], gout.at[item, key], gd.at[3 + slot])
        out_copy[count].start()

    def hand_over(count):
        out_copy[count].wait()
        item, key = count // dp_count, dp_count - 1 - count % dp_count
        if key == 2 and item < 2:
            stage_one(item, 0)
        if key == 1 and item < 2:
            stage_one(item, 1)
        if key == 0:
            keep_load(item)

    blocks = 3 * dp_count
    for count in range(blocks):
        if count % dp_count == 0:
            right_copy.wait()
        block(count, left_copies[count])
        if count + 2 < blocks:
            left_copies[count + 2] = load_left(count + 2)
        if count % dp_count == dp_count - 1 and count + 1 < blocks:
            right_copy = load_right(count // dp_count + 1)
        if count:
            hand_over(count - 1)
        if count == dp_count - 1:
            line_step(0, 2)
        if count == 2 * dp_count:
            line_step(0, 3)
    hand_over(blocks - 1)
    for copy in mine_copies:
        copy.wait()
    line_step(1, 1)
    for half in range(2):
        stage_two(0, half)
    for half in range(2):
        stage_one(2, half)
    for copy in loads:
        copy.wait()

    pending = [(stage_two, 1, 0), (stage_two, 1, 1)]
    pending += [(stage_three, item, half) for item in (1, 2) for half in range(2)]

    def pump(count):
        for _ in range(min(count, len(pending))):
            action, item, half = pending.pop(0)
            action(item, half)

    collect_fin(0)
    fin_copy[0].wait()

    size = 32
    per_seq = local // size

    def split(index):
        return index // per_seq, pl.ds(pl.multiple_of(lax.rem(index, per_seq) * size, size), size)

    acc_ref[...] = jnp.zeros_like(acc_ref)

    def norm_mid(index, total):
        seq, piece = split(index)
        whole = pl.ds(pl.multiple_of(index * size, size), size)
        grad, val = fin[seq, piece, :], h_ref[whole, :]
        inv = lax.rsqrt(jnp.mean(val * val, axis=-1, keepdims=True) + norm_eps)
        weighted = grad * row_ref[1:2, :]
        inner = jnp.mean(weighted * val, axis=-1, keepdims=True)
        out = cot_ref[seq, piece, :].astype(f32) * live_ref[seq][:, 0:1] + (inv * weighted - val * (inv * inv * inv) * inner)
        dx_ref[seq, piece, :] = out
        hb_ref[whole, :] = out.astype(bf16)
        return total + jnp.sum(grad * val * inv, axis=0, keepdims=True)

    acc_ref[1:2, :] = lax.fori_loop(0, seqs * per_seq, norm_mid, jnp.zeros((1, width), f32))
    line_step(1, 2)

    for low in range(0, q_cols, 256):
        val = jnp.dot(hb_ref[...], wattn[:, qkv_cols + low : qkv_cols + low + 256], preferred_element_type=f32).astype(bf16)
        for head_low in (0, 128):
            for seq in range(seqs):
                do_ref[seq, (low + head_low) // 128] = val[seq * local : (seq + 1) * local, head_low : head_low + 128]

    pump(2)

    keys = kv_ref.shape[2]
    key_no = lax.broadcasted_iota(jnp.int32, (local, keys), 1)
    query_no = lax.broadcasted_iota(jnp.int32, (local, keys), 0) + ctx * local
    scale = HEAD_DIM ** (-0.5)
    kv_copies = []
    for seq in range(seqs):
        seen = same_document(seg_ref, seq, ctx, local) & (key_no <= query_no)
        hide = jnp.where(seen, 0.0, masked_score)

        def one_head(head, _):
            query, grad_out, keys_bf, values_bf = q_ref[seq, head], do_ref[seq, head], kv_ref[seq, 0], kv_ref[seq, 1]
            score = lax.dot_general(query, keys_bf, (((1,), (1,)), ((), ())), preferred_element_type=f32) * scale
            prob = jnp.exp(jnp.where(hide < 0.0, masked_score, score) - lse_ref[seq, head])
            grad_prob = lax.dot_general(grad_out, values_bf, (((1,), (1,)), ((), ())), preferred_element_type=f32)
            row_dot = jnp.sum(grad_out.astype(f32) * o_ref[seq, head].astype(f32), axis=-1, keepdims=True)
            grad_score = (prob * (grad_prob - row_dot) * scale).astype(bf16)
            prob_ref[head] = prob.astype(bf16)
            ds_ref[head] = grad_score
            grad_query = jnp.dot(grad_score, keys_bf, preferred_element_type=f32)
            turned = grad_query * cos_ref[seq * local : (seq + 1) * local, :] + pltpu.roll(
                grad_query * sin_ref[seq * local : (seq + 1) * local, :], 64, 1
            )
            span = pl.ds(pl.multiple_of(head * 128, 128), 128)
            dqkv_ref[seq * local : (seq + 1) * local, span] = turned.astype(bf16)
            acc_ref[2:3, span] = acc_ref[2:3, span] + jnp.sum(turned, axis=0, keepdims=True)
            return 0

        lax.fori_loop(0, heads, one_head, 0)
        stacked = (heads * local, 128)
        dkv_ref[seq, 0] = lax.dot_general(
            ds_ref[...].reshape(heads * local, keys),
            q_ref[seq].reshape(stacked),
            (((0,), (0,)), ((), ())),
            preferred_element_type=f32,
        )
        dkv_ref[seq, 1] = lax.dot_general(
            prob_ref[...].reshape(heads * local, keys),
            do_ref[seq].reshape(stacked),
            (((0,), (0,)), ((), ())),
            preferred_element_type=f32,
        )
        dkv_bf[seq] = dkv_ref[seq].astype(bf16)
    for tile in range(1, ctx_count):
        piece = pl.ds(pl.multiple_of(peers[tile] * local, local), local)
        kv_copies.append(
            start(remote(dkv_bf.at[:, :, piece, :], dkv_in.at[ctx], ks.at[tile], kr.at[tile], {"ctx": peers[tile]}))
        )

    def weight_blocks(items, left_ref, right, low, high):
        for key in (3, 2, 1, 0):
            left = left_ref[:, pl.ds(pl.multiple_of(nodes[key] * group, group), group)]
            val = lax.dot_general(left, right, (((0,), (0,)), ((), ())), preferred_element_type=f32).astype(bf16)
            for item in items:
                for half in range(2):
                    span = cols(item, half)
                    piece = val[:, span.start - low : span.stop - low]
                    if key in first_keys[half]:
                        send_at[first_keys[half].index(key), :, span] = piece
                    else:
                        keep_at[0 if key == 0 else 1, :, span] = piece

    o_rows = jnp.concatenate(
        [jnp.concatenate([o_ref[seq, head] for head in range(heads)], 1) for seq in range(seqs)], 0
    )
    line_step(1, 3)
    weight_blocks((3,), hb_ref, o_rows, qkv_cols, wattn.shape[1])
    for half in range(2):
        stage_three(0, half)
    for copy in kv_copies:
        copy.wait_recv()
    own_keys = pl.ds(pl.multiple_of(ctx * local, local), local)
    for seq in range(seqs):
        for part_no in range(2):
            val = dkv_ref[seq, part_no, own_keys, :]
            for tile in range(1, ctx_count):
                val = val + dkv_in[peers[tile], seq, part_no].astype(f32)
            here = slice(seq * local, (seq + 1) * local)
            if part_no == 0:
                val = val * cos_ref[here, :] + pltpu.roll(val * sin_ref[here, :], 64, 1)
            span = slice(q_cols + part_no * 128, q_cols + (part_no + 1) * 128)
            dqkv_ref[here, span] = val.astype(bf16)
            acc_ref[2:3, span] = acc_ref[2:3, span] + jnp.sum(val, axis=0, keepdims=True)
    for half in range(2):
        stage_two(2, half)
    for half in range(2):
        stage_one(3, half)
    weight_blocks((4, 5), a_ref, dqkv_ref[...], 0, qkv_cols)
    for item in (4, 5):
        for half in range(2):
            stage_one(item, half)

    part_copies = []
    for index in range(width // 256):
        part[index] = lax.dot_general(
            dqkv_ref[...],
            wattn[index * 256 : (index + 1) * 256, :qkv_cols],
            (((1,), (1,)), ((), ())),
            preferred_element_type=f32,
        )
        part_copies.append(
            start(remote(part.at[index], part_in.at[index], ps.at[index], pr.at[index], to_core))
        )
    for index, copy in enumerate(part_copies):
        copy.wait_recv()
        for seq in range(seqs):
            here = slice(seq * local, (seq + 1) * local)
            fin[seq, :, index * 256 : (index + 1) * 256] = part[index, here, :] + part_in[index, here, :]

    def norm_in(index, total):
        seq, piece = split(index)
        whole = pl.ds(pl.multiple_of(index * size, size), size)
        grad, val = fin[seq, piece, :], tok_ref[whole, :].astype(f32)
        inv = lax.rsqrt(jnp.mean(val * val, axis=-1, keepdims=True) + norm_eps)
        weighted = grad * row_ref[0:1, :]
        inner = jnp.mean(weighted * val, axis=-1, keepdims=True)
        dx_ref[seq, piece, :] = dx_ref[seq, piece, :] + (inv * weighted - val * (inv * inv * inv) * inner)
        return total + jnp.sum(grad * val * inv, axis=0, keepdims=True)

    acc_ref[0:1, :] = lax.fori_loop(0, seqs * per_seq, norm_in, jnp.zeros((1, width), f32))

    small_copies = [
        start(remote(acc_ref, sm_in.at[tile], gs.at[tile], gr.at[tile], {"ctx": peers[tile]}))
        for tile in range(1, ctx_count)
    ]
    collect_fin(1)
    fin_copy[1].wait()

    def act_rows(index, _):
        seq, piece = split(index)
        whole = pl.ds(pl.multiple_of(index * size, size), size)
        act_ref[seq, piece, :] = (h_ref[whole, :] + act_ref[seq, piece, :]) * live_ref[seq][:, 0:1]
        return 0

    lax.fori_loop(0, seqs * per_seq, act_rows, 0)
    pump(2)
    for half in range(2):
        stage_two(3, half)
    while pending:
        pump(1)
    for half in range(2):
        stage_two(4, half)
    for half in range(2):
        stage_three(3, half)
    for half in range(2):
        stage_two(5, half)
    total = acc_ref[...]
    for tile, copy in enumerate(small_copies):
        copy.wait_recv()
        total = total + sm_in[tile + 1]
    sm_sum[0] = total
    small_turns = [
        remote(sm_sum.at[turn], sm_in.at[ctx_count + turn], gs.at[ctx_count + turn], gr.at[ctx_count + turn], target)
        for turn, target in ((0, to_x), (1, to_y))
    ]
    start(small_turns[0])
    for half in range(2):
        stage_three(4, half)
    small_turns[0].wait_recv()
    sm_sum[1] = sm_sum[0] + sm_in[ctx_count]
    start(small_turns[1])
    for half in range(2):
        stage_three(5, half)
    small_turns[1].wait_recv()
    rows_ref[...] = sm_sum[1] + sm_in[ctx_count + 1]
    for item in range(6):
        for half in range(2):
            stage_four(item, half)
    for copy in sent:
        copy.wait_send()
    for here, copy in relay_sent:

        @pl.when(here)
        def _():
            copy.wait_send()


def backward_call(inputs, sizes):
    dp_count, ctx_count, own, qkv_cols, q_cols = sizes
    bf16, f32 = jnp.bfloat16, jnp.float32
    vmem, hbm = pl.BlockSpec(memory_space=pltpu.VMEM), pl.BlockSpec(memory_space=pl.ANY)
    held = inputs[5:14]
    seqs, local, width = held[0].shape
    ff = inputs[2].shape[3]
    group = own * ctx_count
    rows, keys = seqs * local, local * ctx_count
    heads = q_cols // 128
    attn_cols = held[8].shape[1]
    chunks = width // 256
    outs = [
        ((seqs, local, width), f32, vmem),
        ((seqs, local, width), f32, vmem),
        ((3, own, ctx_count * ff), bf16, hbm),
        ((own, attn_cols), f32, vmem),
        ((8, width), f32, vmem),
        ((3, dp_count, group, ff), bf16, hbm),
    ]
    scratch = [
        ((2, 2, ctx_count - 1, local, width), bf16),
        ((2, ctx_count, local, width), bf16),
        ((seqs, local, width), f32),
        ((2, ctx_count, seqs, local, group), bf16),
        ((ctx_count, rows, ff), bf16),
        ((2, group, ff), bf16),
        ((3, 2, group, ff), bf16),
        ((3, 2, group, ff), bf16),
        ((3, group, ff), bf16),
        ((2, group, attn_cols), bf16),
        ((2, group, attn_cols), bf16),
        ((2, group, attn_cols), bf16),
        ((group, attn_cols), bf16),
        ((ctx_count, own, attn_cols), bf16),
        ((rows, width), bf16),
        ((seqs, heads, local, 128), bf16),
        ((heads, local, keys), bf16),
        ((heads, local, keys), bf16),
        ((seqs, 2, keys, 128), f32),
        ((seqs, 2, keys, 128), bf16),
        ((ctx_count, seqs, 2, local, 128), bf16),
        ((rows, qkv_cols), bf16),
        ((chunks, rows, 256), f32),
        ((chunks, rows, 256), f32),
    ]
    dma = pltpu.SemaphoreType.DMA
    sems = [dma((2, 2, ctx_count)), dma((2, 2, ctx_count)), dma((2,)), dma((2,)), dma((3,)), dma((3, 5)), dma((5,))]
    sems += [
        dma(shape)
        for shape in ((6, 2, 2), (6, 2), (6, 2, ctx_count), (ctx_count,), (chunks,), (ctx_count + 2,))
        for _ in range(2)
    ]
    final = [((8, width), f32), ((ctx_count + 2, 8, width), f32), ((2, 8, width), f32)]
    final += [(array.shape, array.dtype) for array in held]
    return pl.pallas_call(
        functools.partial(backward_kernel, sizes),
        out_shape=[jax.ShapeDtypeStruct(shape, kind) for shape, kind, _ in outs],
        in_specs=[hbm] * 14 + [vmem] * (len(inputs) - 14),
        out_specs=[spec for _, _, spec in outs],
        scratch_shapes=[pltpu.VMEM(*entry) for entry in scratch]
        + sems
        + [pltpu.VMEM(*entry) for entry in final]
        + [dma((len(held),))],
        compiler_params=pltpu.CompilerParams(
            collective_id=1, has_side_effects=True, vmem_limit_bytes=65 * 1024 * 1024 - 65536
        ),
        name="backward_kernel",
    )(*inputs)


def on_device_kernels(
    tokens,
    cotangent,
    segments,
    positions,
    counts,
    attn_gain,
    q_weight,
    q_bias,
    k_weight,
    v_weight,
    kv_bias,
    o_weight,
    mlp_gain,
    gate_weight,
    up_weight,
    down_weight,
):
    dp_count, ctx_count = lax.axis_size("dp"), lax.axis_size("ctx")
    dp_rank, ctx_rank, core = lax.axis_index("dp"), lax.axis_index("ctx"), lax.axis_index("tp")
    seq_count, local_len, width = tokens.shape
    full_len = segments.shape[1]
    row_count = seq_count * local_len
    own_rows = q_weight.shape[1]
    group_rows = own_rows * ctx_count
    q_cols, k_cols, ff_cols = q_weight.shape[2], k_weight.shape[2], gate_weight.shape[2]
    kv_local = k_cols // HEAD_DIM
    group_size = q_cols // k_cols
    qkv_cols = q_cols + 2 * k_cols
    lane = 128
    ff_block = -(-ff_cols // (lane * ctx_count)) * lane
    ff_pad = ff_block * ctx_count - ff_cols
    f32, bf16 = jnp.float32, jnp.bfloat16

    parts = (attn_gain[0], mlp_gain[0], q_bias[0].reshape(-1), kv_bias[0].reshape(-1))
    cuts = [0]
    for part_vec in parts:
        cuts.append(cuts[-1] + part_vec.shape[0])
    small_own = jnp.pad(jnp.concatenate(parts).astype(f32)[None], ((0, 7), (0, 0)))
    attn_own = jnp.concatenate([q_weight[0], k_weight[0], v_weight[0], o_weight[0]], 1)
    live_seq = (jnp.arange(seq_count, dtype=jnp.int32) < counts[0]).astype(f32)
    live = jnp.broadcast_to(live_seq[:, None, None], (seq_count, 1, 128))
    cos_tab, sin_tab = rope_tables(positions.reshape(-1))
    sign = jnp.where(jnp.arange(HEAD_DIM) < HEAD_DIM // 2, -1.0, 1.0)
    (
        w_attn,
        mid_all,
        resid_mid,
        normed_in,
        query_hm,
        keyval_hm,
        attn_hm,
        log_total,
        small_rows,
        hidden_and_grads,
        part_sums,
        part_own,
        grad_all,
    ) = forward_call(
        tokens.reshape(-1, width),
        cotangent,
        attn_own,
        (gate_weight[0], up_weight[0], down_weight[0]),
        small_own,
        cos_tab,
        sin_tab * sign,
        segments,
        live,
        qkv_cols,
        q_cols,
        cuts,
    )
    activations, input_grad, grad_ff, grad_w_attn, rows_sum, _ = backward_call(
        (
            part_sums,
            part_own,
            hidden_and_grads,
            mid_all,
            grad_all,
            cotangent,
            tokens.reshape(-1, width),
            resid_mid,
            normed_in,
            query_hm,
            keyval_hm,
            attn_hm,
            log_total,
            w_attn,
            live,
            small_rows,
            cos_tab,
            sin_tab * sign,
            segments,
        ),
        (dp_count, ctx_count, own_rows, qkv_cols, q_cols),
    )
    grad_w_gate, grad_w_up, grad_w_down = (grad_ff[item, :, :ff_cols].astype(f32) for item in range(3))
    rank = dp_rank * ctx_count + ctx_rank

    def own_part(vector, size):
        return lax.dynamic_slice_in_dim(vector, rank * size, size, 0)

    bias_kv = jnp.concatenate(
        [
            rows_sum[2, q_cols : q_cols + k_cols].reshape(kv_local, -1).T,
            rows_sum[2, q_cols + k_cols : qkv_cols].reshape(kv_local, -1).T,
        ],
        0,
    ).reshape(-1)
    own = [
        own_part(rows_sum[0], own_rows)[None],
        own_part(rows_sum[1], own_rows)[None],
        own_part(rows_sum[2, :q_cols].reshape(kv_local, -1).T.reshape(-1), cuts[3] - cuts[2]),
        own_part(bias_kv, cuts[4] - cuts[3]),
    ]
    grad_w_qkv, grad_w_out = grad_w_attn[:, :qkv_cols], grad_w_attn[:, qkv_cols:]
    return (
        activations.reshape(tokens.shape),
        input_grad.reshape(tokens.shape),
        own[0],
        grad_w_qkv[None, :, :q_cols],
        own[2].reshape(q_bias.shape),
        grad_w_qkv[None, :, q_cols : q_cols + k_cols],
        grad_w_qkv[None, :, q_cols + k_cols :],
        own[3].reshape(kv_bias.shape),
        grad_w_out[None],
        own[1],
        grad_w_gate[None],
        grad_w_up[None],
        grad_w_down[None],
    )


def solution(mesh):
    in_specs = (
        P("dp", "ctx", None),
        P("dp", "ctx", None),
        P("dp", None),
        P("dp", "ctx"),
        P("dp"),
        P(None, ("dp", "ctx")),
        P(None, ("dp", "ctx"), "tp"),
        P(None, ("dp", "ctx"), "tp"),
        P(None, ("dp", "ctx"), "tp"),
        P(None, ("dp", "ctx"), "tp"),
        P(None, ("dp", "ctx"), "tp"),
        P(None, ("dp", "ctx"), "tp"),
        P(None, ("dp", "ctx")),
        P(None, ("dp", "ctx"), "tp"),
        P(None, ("dp", "ctx"), "tp"),
        P(None, ("dp", "ctx"), "tp"),
    )
    out_specs = (
        P("dp", "ctx", None),
        P("dp", "ctx", None),
        P(None, ("dp", "ctx")),
        P(None, ("dp", "ctx"), "tp"),
        P(None, ("dp", "ctx"), "tp"),
        P(None, ("dp", "ctx"), "tp"),
        P(None, ("dp", "ctx"), "tp"),
        P(None, ("dp", "ctx"), "tp"),
        P(None, ("dp", "ctx"), "tp"),
        P(None, ("dp", "ctx")),
        P(None, ("dp", "ctx"), "tp"),
        P(None, ("dp", "ctx"), "tp"),
        P(None, ("dp", "ctx"), "tp"),
    )
    kernels_fit = mesh.shape["dp"] == 4 and mesh.shape["ctx"] == 4 and mesh.shape["tp"] == KV_HEADS
    return jax.shard_map(
        on_device_kernels if kernels_fit else on_device, mesh=mesh, in_specs=in_specs, out_specs=out_specs, check_vma=False
    )
```
